8 devices in a mesh: data: 8 (over z, y, x, core).
Axes of the slice: x: 2, y: 2, z: 1, core: 2. Of those that a mesh axis runs over, the one named last changes fastest.
Arguments:
- gradient: float32 [3, 1769472], P(None, 'data')
- master: float32 [3, 1769472], P(None, 'data')
- moment_one: float32 [3, 1769472], P(None, 'data')
- moment_two: float32 [3, 1769472], P(None, 'data')
- tokens: bfloat16 [4096, 768], P('data')
- targets: bfloat16 [4096, 768], P('data')
Outputs:
- output 1: float32 [4096], P('data')
- output 2: bfloat16 [3, 1769472], replicated
- output 3: float32 [3, 1769472], P(None, 'data')
- output 4: float32 [3, 1769472], P(None, 'data')
- output 5: float32 [3, 1769472], P(None, 'data')
All inputs are finite; a program needn't handle non-finite values.
Results may differ from the reference program's by a relative error of at most 0.00174468.
Values are sent between devices in bfloat16 or wider.
A program may use at most 1 GiB of HBM per device.

```python
import math
import jax
import jax.numpy as jnp
from jax import lax

MODEL_DIM = 768
HIDDEN_DIM = 1152
LAYERS = 3
GROUP_SIZE = 8
TOKENS_DEV = 512
ADAM_STEP = 10

HALF_SIZE = MODEL_DIM * HIDDEN_DIM
LAYER_SIZE = 2 * HALF_SIZE
BATCH_ROWS = GROUP_SIZE * TOKENS_DEV
LEARN_RATE = 0.01
BETA_ONE = 0.9
BETA_TWO = 0.95
ADAM_EPS = 1e-8
WEIGHT_DECAY = 0.1
CLIP_NORM = 1.0
NORM_EPS = 1e-6


def setup_inputs(seed: int = 0) -> dict:
    root_key = jax.random.key(seed)
    key_list = jax.random.split(root_key, 7)
    state_shape = (LAYERS, LAYER_SIZE)
    unit_scale = 1.0 / math.sqrt(LAYERS * LAYER_SIZE)
    gradient = 2.0 * unit_scale * jax.random.normal(key_list[0], state_shape, jnp.float32)
    w_first = jax.random.normal(key_list[1], (LAYERS, HALF_SIZE), jnp.float32) * MODEL_DIM ** -0.5
    w_second = jax.random.normal(key_list[2], (LAYERS, HALF_SIZE), jnp.float32) * HIDDEN_DIM ** -0.5
    master = jnp.concatenate([w_first, w_second], axis=1)
    moment_one = 0.1 * unit_scale * jax.random.normal(key_list[3], state_shape, jnp.float32)
    moment_two = unit_scale * unit_scale * jax.random.uniform(key_list[4], state_shape, jnp.float32, minval=0.02, maxval=0.08)
    tokens_f32 = jax.random.normal(key_list[5], (BATCH_ROWS, MODEL_DIM), jnp.float32)
    target_noise = jax.random.normal(key_list[6], (BATCH_ROWS, MODEL_DIM), jnp.float32)
    return {"gradient": gradient, "master": master, "moment_one": moment_one, "moment_two": moment_two, "tokens": tokens_f32.astype(jnp.bfloat16), "targets": (tokens_f32 + 0.5 * target_noise).astype(jnp.bfloat16)}


def mlp_block(hidden, w_in, w_out):
    hidden_f32 = hidden.astype(jnp.float32)
    normed = (hidden_f32 * lax.rsqrt(jnp.mean(hidden_f32 * hidden_f32, axis=-1, keepdims=True) + NORM_EPS)).astype(jnp.bfloat16)
    inner = jnp.dot(normed, w_in, preferred_element_type=jnp.float32).astype(jnp.bfloat16)
    active = jax.nn.gelu(inner.astype(jnp.float32), approximate=True).astype(jnp.bfloat16)
    return (hidden_f32 + jnp.dot(active, w_out, preferred_element_type=jnp.float32)).astype(jnp.bfloat16)


def reference(gradient, master, moment_one, moment_two, tokens, targets):
    sq_sum = jnp.sum(gradient * gradient)
    clip_scale = jnp.minimum(1.0, CLIP_NORM / jnp.sqrt(sq_sum))
    clipped = gradient * clip_scale
    new_one = BETA_ONE * moment_one + (1.0 - BETA_ONE) * clipped
    new_two = BETA_TWO * moment_two + (1.0 - BETA_TWO) * clipped * clipped
    step_size = (new_one / (1.0 - BETA_ONE ** ADAM_STEP)) / (jnp.sqrt(new_two / (1.0 - BETA_TWO ** ADAM_STEP)) + ADAM_EPS)
    new_master = master - LEARN_RATE * (step_size + WEIGHT_DECAY * master)
    weights = new_master.astype(jnp.bfloat16)
    w_in_all = weights[:, :HALF_SIZE].reshape(LAYERS, MODEL_DIM, HIDDEN_DIM)
    w_out_all = weights[:, HALF_SIZE:].reshape(LAYERS, HIDDEN_DIM, MODEL_DIM)

    def layer_step(hidden, layer_pair):
        return mlp_block(hidden, layer_pair[0], layer_pair[1]), None

    def block_rows(row_pair):
        final_hidden, unused_out = lax.scan(layer_step, row_pair[0], (w_in_all, w_out_all))
        error_val = final_hidden.astype(jnp.float32) - row_pair[1].astype(jnp.float32)
        return jnp.mean(error_val * error_val, axis=-1)

    row_blocks = (tokens.reshape(GROUP_SIZE, TOKENS_DEV, MODEL_DIM), targets.reshape(GROUP_SIZE, TOKENS_DEV, MODEL_DIM))
    row_loss = lax.map(block_rows, row_blocks).reshape(BATCH_ROWS)
    return row_loss, weights, new_master, new_one, new_two
```

```python
import functools

import jax
import jax.numpy as jnp
from jax import lax
from jax.experimental import pallas as pl
from jax.experimental.pallas import tpu as pltpu
from jax.sharding import PartitionSpec as P

LEARN_RATE = 0.01
BETA_ONE = 0.9
BETA_TWO = 0.95
ADAM_EPS = 1e-8
WEIGHT_DECAY = 0.1
ADAM_STEP = 10
CLIP_NORM = 1.0
NORM_EPS = 1e-6

MESH = pl.DeviceIdType.MESH
LANES = 128
GROUP = 8
F32 = jnp.float32
BF16 = jnp.bfloat16


def gather_kernel(dims, grad_hbm, master_hbm, one_hbm, two_hbm, tok_hbm, tgt_hbm,
                  packed_ref, master_out, one_out, two_out, loss_ref,
                  w_in, w_out, grad_v, master_v, one_v, two_v, tok_v, tgt_v,
                  part_ref, wide_ref, normed_ref, active_ref, hidden_ref,
                  load_sem, part_send, part_recv, send_sem, recv_sem):
    layers, model_dim, hidden_dim, rows, chunks = dims
    in_rows = chunks * LANES // hidden_dim
    out_rows = chunks * LANES // model_dim
    half_chunks = chunks // 2

    me = lax.axis_index("data")
    core = lax.rem(me, 2)
    x_pos = lax.rem(me // 2, 2)
    y_pos = me // 4
    partner = me + 1 - 2 * core
    x_peer = me + 2 - 4 * x_pos
    y_peer = me + 4 - 8 * y_pos
    diag = x_peer + 4 - 8 * y_pos

    state = ((grad_hbm, grad_v), (master_hbm, master_v), (one_hbm, one_v), (two_hbm, two_v))

    def load(which, layer):
        src, dst = state[which]
        return pltpu.make_async_copy(src.at[:, layer, :], dst.at[layer], load_sem.at[which, layer])

    for which in range(4):
        for layer in range(layers):
            load(which, layer).start()
    tok_load = pltpu.make_async_copy(tok_hbm, tok_v, load_sem.at[4, 0])
    tgt_load = pltpu.make_async_copy(tgt_hbm, tgt_v, load_sem.at[4, 1])
    tok_load.start()
    tgt_load.start()

    barrier = pltpu.get_barrier_semaphore()
    for step in range(1, GROUP):
        pl.semaphore_signal(barrier, inc=1, device_id=(lax.rem(me + step, GROUP),), device_id_type=MESH)

    sums = tuple(jnp.zeros((8, LANES), F32) for _ in range(8))
    for layer in range(layers):
        load(0, layer).wait()

        def square(idx, carry):
            base = pl.multiple_of(idx * 64, 64)
            block = grad_v[layer, pl.ds(base, 64), :]
            return tuple(carry[k] + block[8 * k:8 * k + 8] * block[8 * k:8 * k + 8] for k in range(8))

        sums = lax.fori_loop(0, chunks // 64, square, sums)
    mine = ((sums[0] + sums[1]) + (sums[2] + sums[3])) + ((sums[4] + sums[5]) + (sums[6] + sums[7]))
    part_ref[me] = mine
    pl.semaphore_wait(barrier, GROUP - 1)

    def part_copy(step):
        return pltpu.make_async_remote_copy(
            src_ref=part_ref.at[me], dst_ref=part_ref.at[me],
            send_sem=part_send.at[step], recv_sem=part_recv.at[step],
            device_id=(lax.rem(me + step, GROUP),), device_id_type=MESH)

    def part_arrival(step):
        slot = lax.rem(me + GROUP - step, GROUP)
        return pltpu.make_async_remote_copy(
            src_ref=part_ref.at[slot], dst_ref=part_ref.at[slot],
            send_sem=part_send.at[step], recv_sem=part_recv.at[step],
            device_id=(me,), device_id_type=MESH)

    for step in range(1, GROUP):
        part_copy(step).start()
    for step in range(1, GROUP):
        part_arrival(step).wait_recv()
    total = part_ref[0]
    for slot in range(1, GROUP):
        total = total + part_ref[slot]
    total = jnp.sum(jnp.sum(total, axis=0, keepdims=True), axis=1, keepdims=True)
    clip = jnp.minimum(1.0, CLIP_NORM / jnp.sqrt(total))
    clip = jnp.broadcast_to(clip, (8, LANES))

    def piece(kind, layer, device, half):
        slot = lax.rem(device, 4)
        if kind == 0:
            return w_in.at[layer, pl.ds(pl.multiple_of(slot * in_rows + half * (in_rows // 2), 16), in_rows // 2), :]
        return w_out.at[layer, pl.ds(pl.multiple_of(slot * out_rows + half * (out_rows // 2), 16), out_rows // 2), :]

    def copy(kind, layer, device, half, index, target):
        ref = piece(kind, layer, device, half)
        return pltpu.make_async_remote_copy(
            src_ref=ref, dst_ref=ref, send_sem=send_sem.at[layer, index],
            recv_sem=recv_sem.at[layer, index], device_id=(target,), device_id_type=MESH)

    def by_kind(function):
        for y_value in range(2):
            @pl.when(y_pos == y_value)
            def _():
                function(y_value)

    one_scale = 1.0 / (1.0 - BETA_ONE ** ADAM_STEP)
    two_scale = 1.0 / (1.0 - BETA_TWO ** ADAM_STEP)

    def adam(layer, half):
        def update(idx, _):
            base = pl.multiple_of(half * half_chunks + idx * 48, 8)
            for k in range(6):
                at = pl.ds(pl.multiple_of(base + 8 * k, 8), 8)
                clipped = grad_v[layer, at, :] * clip
                new_one = BETA_ONE * one_v[layer, at, :] + (1.0 - BETA_ONE) * clipped
                new_two = BETA_TWO * two_v[layer, at, :] + (1.0 - BETA_TWO) * clipped * clipped
                step_size = (new_one * one_scale) / (jnp.sqrt(new_two * two_scale) + ADAM_EPS)
                old = master_v[layer, at, :]
                master_out[layer, at, :] = old - LEARN_RATE * (step_size + WEIGHT_DECAY * old)
                one_out[layer, at, :] = new_one
                two_out[layer, at, :] = new_two
            return 0

        lax.fori_loop(0, half_chunks // 48, update, 0)

    def round_rows(kind, layer, half):
        width = hidden_dim if kind == 0 else model_dim
        count = in_rows if kind == 0 else out_rows
        per_row = width // LANES
        dst = w_in if kind == 0 else w_out
        slot = lax.rem(me, 4)

        def body(idx, _):
            base = half * half_chunks + idx * (16 * per_row)
            row = pl.multiple_of(slot * count + half * (count // 2) + idx * 16, 16)
            for col in range(per_row):
                top = master_out[layer, pl.ds(base + col, 8, stride=per_row), :]
                low = master_out[layer, pl.ds(base + 8 * per_row + col, 8, stride=per_row), :]
                dst[layer, pl.ds(row, 16), col * LANES:(col + 1) * LANES] = jnp.concatenate([top, low], axis=0).astype(BF16)
            return 0

        lax.fori_loop(0, count // 32, body, 0)

    for layer in range(layers):
        for which in range(1, 4):
            load(which, layer).wait()
        for half in range(2):
            adam(layer, half)

            def send_own(kind):
                round_rows(kind, layer, half)
                copy(kind, layer, me, half, half, x_peer).start()
                copy(kind, layer, me, half, 2 + half, y_peer).start()
                copy(kind, layer, me, half, 6 + half, partner).start()

            by_kind(send_own)

    def pack(kind, device):
        width = hidden_dim if kind == 0 else model_dim
        count = in_rows if kind == 0 else out_rows
        per_row = width // LANES
        src = w_in if kind == 0 else w_out
        slot = lax.rem(device, 4)

        def spread(idx, _):
            row = pl.multiple_of(slot * count + idx * 16, 16)
            for layer in range(layers):
                for col in range(per_row):
                    tile = src[layer, pl.ds(row, 16), col * LANES:(col + 1) * LANES].astype(F32)
                    base = layer + 4 * (idx * (16 * per_row) + col)
                    wide_ref[pl.ds(base, 8, stride=4 * per_row), :] = tile[0:8]
                    wide_ref[pl.ds(base + 32 * per_row, 8, stride=4 * per_row), :] = tile[8:16]
            return 0

        lax.fori_loop(0, count // 16, spread, 0)

        def squeeze(idx, _):
            src_at = pl.multiple_of(idx * 128, 128)
            block = wide_ref[pl.ds(src_at, 128), :].astype(BF16).reshape(32, 4, LANES)
            packed_ref[pl.ds(device * chunks + idx * 32, 32), :, :] = block[:, :layers, :]
            return 0

        lax.fori_loop(0, 4 * chunks // 128, squeeze, 0)

    def partner_of(device):
        return device + 1 - 2 * core

    def mlp(layer):
        def block(idx, _):
            at = pl.ds(pl.multiple_of(idx * 256, 256), 256)
            hidden = hidden_ref[at, :].astype(F32)
            scale = lax.rsqrt(jnp.mean(hidden * hidden, axis=-1, keepdims=True) + NORM_EPS)
            normed_ref[...] = (hidden * scale).astype(BF16)
            for col in range(0, hidden_dim, 384):
                inner = jnp.dot(normed_ref[...], w_in[layer, :, col:col + 384], preferred_element_type=F32).astype(BF16)
                active_ref[:, col:col + 384] = jax.nn.gelu(inner.astype(F32), approximate=True).astype(BF16)
            for col in range(0, model_dim, 256):
                add = jnp.dot(active_ref[...], w_out[layer, :, col:col + 256], preferred_element_type=F32)
                hidden_ref[at, col:col + 256] = (hidden_ref[at, col:col + 256].astype(F32) + add).astype(BF16)
            return 0

        lax.fori_loop(0, rows // 256, block, 0)

    tok_load.wait()
    tgt_load.wait()
    hidden_ref[...] = tok_v[...]

    for layer in range(layers):
        def forward(kind):
            for half in range(2):
                copy(kind, layer, x_peer, half, half, me).wait_recv()
                if half == 0:
                    copy(kind, layer, x_peer, half, 4, y_peer).start()
                copy(kind, layer, x_peer, half, 8 + half, partner).start()
                copy(1 - kind, layer, y_peer, half, 2 + half, me).wait_recv()
                if half == 1:
                    copy(1 - kind, layer, y_peer, half, 5, x_peer).start()
                copy(1 - kind, layer, y_peer, half, 10 + half, partner).start()
            for half in range(2):
                copy(kind, layer, partner, half, 6 + half, me).wait_recv()

        by_kind(forward)

    def pack_near(kind):
        pack(kind, me)
        pack(kind, partner)
        pack(kind, x_peer)
        pack(1 - kind, y_peer)
        for layer in range(layers):
            for half in range(2):
                copy(kind, layer, partner_of(x_peer), half, 8 + half, me).wait_recv()
                copy(1 - kind, layer, partner_of(y_peer), half, 10 + half, me).wait_recv()
        pack(kind, partner_of(x_peer))
        pack(1 - kind, partner_of(y_peer))

    by_kind(pack_near)

    for layer in range(layers):
        def far(kind):
            for half in range(2):
                copy(1 - kind, layer, diag, half, 4 + half, me).wait_recv()
                copy(1 - kind, layer, diag, half, 12 + half, partner).start()
            for half in range(2):
                copy(1 - kind, layer, partner_of(diag), half, 12 + half, me).wait_recv()

        by_kind(far)
        mlp(layer)

    def pack_far(kind):
        pack(1 - kind, diag)
        pack(1 - kind, partner_of(diag))

    by_kind(pack_far)

    for idx in range(rows // LANES):
        at = slice(idx * LANES, (idx + 1) * LANES)
        error = hidden_ref[at, :].astype(F32) - tgt_v[at, :].astype(F32)
        error = error * error
        folded = error[:, 0:LANES]
        for col in range(LANES, model_dim, LANES):
            folded = folded + error[:, col:col + LANES]
        loss_ref[idx:idx + 1, :] = jnp.sum(folded.T, axis=0, keepdims=True) * (1.0 / model_dim)

    for step in range(1, GROUP):
        part_copy(step).wait_send()

    def drain(kind):
        for layer in range(layers):
            for half in range(2):
                copy(kind, layer, me, half, half, x_peer).wait_send()
                copy(kind, layer, me, half, 2 + half, y_peer).wait_send()
                copy(kind, layer, me, half, 6 + half, partner).wait_send()
                copy(kind, layer, x_peer, half, 8 + half, partner).wait_send()
                copy(1 - kind, layer, y_peer, half, 10 + half, partner).wait_send()
                copy(1 - kind, layer, diag, half, 12 + half, partner).wait_send()
            copy(kind, layer, x_peer, 0, 4, y_peer).wait_send()
            copy(1 - kind, layer, y_peer, 1, 5, x_peer).wait_send()

    by_kind(drain)


def write_kernel(layers, pieces, packed_ref, master_ref, one_ref, two_ref, loss_ref,
                 packed_hbm, master_hbm, one_hbm, two_hbm, loss_hbm, sem):
    copies = [pltpu.make_async_copy(loss_ref, loss_hbm, sem.at[0])]
    span = packed_ref.shape[0] // pieces
    for idx in range(pieces):
        at = pl.ds(idx * span, span)
        copies.append(pltpu.make_async_copy(packed_ref.at[at], packed_hbm.at[at], sem.at[1 + idx]))
    for which, (src, dst) in enumerate(((master_ref, master_hbm), (one_ref, one_hbm), (two_ref, two_hbm))):
        for layer in range(layers):
            copies.append(pltpu.make_async_copy(src.at[layer], dst.at[:, layer, :], sem.at[1 + pieces + which * layers + layer]))
    for item in copies:
        item.start()
    for item in copies:
        item.wait()


def solution(mesh):
    group_size = mesh.shape["data"]
    state_spec = P(None, "data")
    row_spec = P("data", None)

    def local_step(grad_shard, master_shard, one_shard, two_shard, tok_rows, tgt_rows):
        rows, model_dim = tok_rows.shape
        layers, cols = master_shard.shape
        half_size = cols * group_size // 2
        hidden_dim = half_size // model_dim
        chunks = cols // LANES
        dims = (layers, model_dim, hidden_dim, rows, chunks)
        tiled = [a.reshape(layers, chunks, LANES).transpose(1, 0, 2) for a in (grad_shard, master_shard, one_shard, two_shard)]
        state_v = pltpu.VMEM((layers, chunks, LANES), F32)
        hbm = pl.BlockSpec(memory_space=pltpu.HBM)
        vmem = pl.BlockSpec(memory_space=pltpu.VMEM)
        state_out = state_v
        packed, new_master, new_one, new_two, loss = pl.pallas_call(
            functools.partial(gather_kernel, dims),
            name="gather_step",
            out_shape=(pltpu.VMEM((chunks * group_size, layers, LANES), BF16), state_out, state_out, state_out,
                       jax.ShapeDtypeStruct((rows // LANES, LANES), F32)),
            in_specs=[hbm] * 6,
            out_specs=(vmem,) * 5,
            scratch_shapes=[
                pltpu.VMEM((layers, model_dim, hidden_dim), BF16),
                pltpu.VMEM((layers, hidden_dim, model_dim), BF16),
                state_v, state_v, state_v, state_v,
                pltpu.VMEM((rows, model_dim), BF16),
                pltpu.VMEM((rows, model_dim), BF16),
                pltpu.VMEM((group_size, 8, LANES), F32),
                pltpu.VMEM((4 * chunks, LANES), F32),
                pltpu.VMEM((256, model_dim), BF16),
                pltpu.VMEM((256, hidden_dim), BF16),
                pltpu.VMEM((rows, model_dim), BF16),
                pltpu.SemaphoreType.DMA((5, layers)),
                pltpu.SemaphoreType.DMA((group_size,)),
                pltpu.SemaphoreType.DMA((group_size,)),
                pltpu.SemaphoreType.DMA((layers, 14)),
                pltpu.SemaphoreType.DMA((layers, 14)),
            ],
            compiler_params=pltpu.CompilerParams(collective_id=0, has_side_effects=True, vmem_limit_bytes=28 << 20),
        )(*[pltpu.with_memory_space_constraint(a, pltpu.HBM) for a in (*tiled, tok_rows, tgt_rows)])
        state_tile = jax.ShapeDtypeStruct((chunks, layers, LANES), F32)
        pieces = 8
        weights, new_master, new_one, new_two, row_loss = pl.pallas_call(
            functools.partial(write_kernel, layers, pieces),
            name="write_out",
            out_shape=(jax.ShapeDtypeStruct((chunks * group_size, layers, LANES), BF16), state_tile, state_tile, state_tile,
                       jax.ShapeDtypeStruct((rows // LANES, LANES), F32)),
            in_specs=[vmem] * 5,
            out_specs=(hbm,) * 5,
            scratch_shapes=[pltpu.SemaphoreType.DMA((1 + pieces + 3 * layers,))],
            compiler_params=pltpu.CompilerParams(vmem_limit_bytes=2 << 20),
        )(packed, new_master, new_one, new_two, loss)

        def flat(a):
            return a.transpose(1, 0, 2).reshape(layers, a.shape[0] * LANES)

        return row_loss.reshape(rows), flat(weights), flat(new_master), flat(new_one), flat(new_two)

    return jax.shard_map(local_step, mesh=mesh, in_specs=(state_spec, state_spec, state_spec, state_spec, row_spec, row_spec), out_specs=(P("data"), P(), state_spec, state_spec, state_spec), check_vma=False)
```

```python
import functools

import jax
import jax.numpy as jnp
from jax import lax
from jax.experimental import pallas as pl
from jax.experimental.pallas import tpu as pltpu
from jax.sharding import PartitionSpec as P

LEARN_RATE = 0.01
BETA_ONE = 0.9
BETA_TWO = 0.95
ADAM_EPS = 1e-8
WEIGHT_DECAY = 0.1
ADAM_STEP = 10
CLIP_NORM = 1.0
NORM_EPS = 1e-6

MESH = pl.DeviceIdType.MESH
LANES = 128
GROUP = 8
F32 = jnp.float32
BF16 = jnp.bfloat16


def spread_piece(dims, kind, device, weights, wide_ref):
    layers, model_dim, hidden_dim, rows, chunks = dims
    per_row = (hidden_dim if kind == 0 else model_dim) // LANES
    count = chunks // per_row
    src = weights[kind]
    slot = lax.rem(device, 4)

    def spread(idx, _):
        row = pl.multiple_of(slot * count + idx * 16, 16)
        for layer in range(layers):
            for col in range(per_row):
                tile = src[layer, pl.ds(row, 16), col * LANES:(col + 1) * LANES].astype(F32)
                base = layer + 4 * (idx * (16 * per_row) + col)
                wide_ref[pl.ds(base, 8, stride=4 * per_row), :] = tile[0:8]
                wide_ref[pl.ds(base + 32 * per_row, 8, stride=4 * per_row), :] = tile[8:16]
        return 0

    lax.fori_loop(0, count // 16, spread, 0)


def mlp_block(dims, layer, w_in, w_out, hidden_ref, normed_ref, active_ref):
    layers, model_dim, hidden_dim, rows, chunks = dims

    def block(idx, _):
        at = pl.ds(pl.multiple_of(idx * 256, 256), 256)
        hidden = hidden_ref[at, :].astype(F32)
        scale = lax.rsqrt(jnp.mean(hidden * hidden, axis=-1, keepdims=True) + NORM_EPS)
        normed_ref[...] = (hidden * scale).astype(BF16)
        for col in range(0, hidden_dim, 384):
            inner = jnp.dot(normed_ref[...], w_in[layer, :, col:col + 384], preferred_element_type=F32).astype(BF16)
            active_ref[:, col:col + 384] = jax.nn.gelu(inner.astype(F32), approximate=True).astype(BF16)
        for col in range(0, model_dim, 256):
            add = jnp.dot(active_ref[...], w_out[layer, :, col:col + 256], preferred_element_type=F32)
            hidden_ref[at, col:col + 256] = (hidden_ref[at, col:col + 256].astype(F32) + add).astype(BF16)
        return 0

    lax.fori_loop(0, rows // 256, block, 0)


def places():
    me = lax.axis_index("data")
    core = lax.rem(me, 2)
    x_pos = lax.rem(me // 2, 2)
    y_pos = me // 4
    x_peer = me + 2 - 4 * x_pos
    y_peer = me + 4 - 8 * y_pos
    return me, core, y_pos, x_peer, y_peer, x_peer + 4 - 8 * y_pos


def gather_kernel(dims, grad_hbm, master_hbm, one_hbm, two_hbm, tok_hbm,
                  p0, p1, p2, p3, p4, p5, master_out, one_out, two_out, w_in, w_out, hidden_ref,
                  grad_v, master_v, one_v, two_v,
                  part_ref, wide_ref, normed_ref, active_ref,
                  load_sem, part_send, part_recv, send_sem, recv_sem):
    layers, model_dim, hidden_dim, rows, chunks = dims
    in_rows = chunks * LANES // hidden_dim
    out_rows = chunks * LANES // model_dim
    half_chunks = chunks // 2

    me, core, y_pos, x_peer, y_peer, diag = places()
    partner = me + 1 - 2 * core

    state = ((grad_hbm, grad_v), (master_hbm, master_v), (one_hbm, one_v), (two_hbm, two_v))

    def load(which, layer):
        src, dst = state[which]
        return pltpu.make_async_copy(src.at[:, layer, :], dst.at[layer], load_sem.at[which, layer])

    for which in range(4):
        for layer in range(layers):
            load(which, layer).start()
    tok_load = pltpu.make_async_copy(tok_hbm, hidden_ref, load_sem.at[4, 0])
    tok_load.start()

    barrier = pltpu.get_barrier_semaphore()
    for step in range(1, GROUP):
        pl.semaphore_signal(barrier, inc=1, device_id=(lax.rem(me + step, GROUP),), device_id_type=MESH)

    sums = tuple(jnp.zeros((8, LANES), F32) for _ in range(8))
    for layer in range(layers):
        load(0, layer).wait()

        def square(idx, carry):
            base = pl.multiple_of(idx * 64, 64)
            block = grad_v[layer, pl.ds(base, 64), :]
            return tuple(carry[k] + block[8 * k:8 * k + 8] * block[8 * k:8 * k + 8] for k in range(8))

        sums = lax.fori_loop(0, chunks // 64, square, sums)
    mine = ((sums[0] + sums[1]) + (sums[2] + sums[3])) + ((sums[4] + sums[5]) + (sums[6] + sums[7]))
    part_ref[me] = mine
    pl.semaphore_wait(barrier, GROUP - 1)

    def part_copy(step):
        return pltpu.make_async_remote_copy(
            src_ref=part_ref.at[me], dst_ref=part_ref.at[me],
            send_sem=part_send.at[step], recv_sem=part_recv.at[step],
            device_id=(lax.rem(me + step, GROUP),), device_id_type=MESH)

    def part_arrival(step):
        slot = lax.rem(me + GROUP - step, GROUP)
        return pltpu.make_async_remote_copy(
            src_ref=part_ref.at[slot], dst_ref=part_ref.at[slot],
            send_sem=part_send.at[step], recv_sem=part_recv.at[step],
            device_id=(me,), device_id_type=MESH)

    for step in range(1, GROUP):
        part_copy(step).start()
    for step in range(1, GROUP):
        part_arrival(step).wait_recv()
    total = part_ref[0]
    for slot in range(1, GROUP):
        total = total + part_ref[slot]
    total = jnp.sum(jnp.sum(total, axis=0, keepdims=True), axis=1, keepdims=True)
    clip = jnp.minimum(1.0, CLIP_NORM / jnp.sqrt(total))
    clip = jnp.broadcast_to(clip, (8, LANES))

    def piece(kind, layer, device, half):
        slot = lax.rem(device, 4)
        if kind == 0:
            return w_in.at[layer, pl.ds(pl.multiple_of(slot * in_rows + half * (in_rows // 2), 16), in_rows // 2), :]
        return w_out.at[layer, pl.ds(pl.multiple_of(slot * out_rows + half * (out_rows // 2), 16), out_rows // 2), :]

    def copy(kind, layer, device, half, index, target):
        ref = piece(kind, layer, device, half)
        return pltpu.make_async_remote_copy(
            src_ref=ref, dst_ref=ref, send_sem=send_sem.at[layer, index],
            recv_sem=recv_sem.at[layer, index], device_id=(target,), device_id_type=MESH)

    def by_kind(function):
        for y_value in range(2):
            @pl.when(y_pos == y_value)
            def _():
                function(y_value)

    one_scale = 1.0 / (1.0 - BETA_ONE ** ADAM_STEP)
    two_scale = 1.0 / (1.0 - BETA_TWO ** ADAM_STEP)

    def adam(layer, half):
        def update(idx, _):
            base = pl.multiple_of(half * half_chunks + idx * 48, 8)
            for k in range(6):
                at = pl.ds(pl.multiple_of(base + 8 * k, 8), 8)
                clipped = grad_v[layer, at, :] * clip
                new_one = BETA_ONE * one_v[layer, at, :] + (1.0 - BETA_ONE) * clipped
                new_two = BETA_TWO * two_v[layer, at, :] + (1.0 - BETA_TWO) * clipped * clipped
                step_size = (new_one * one_scale) / (jnp.sqrt(new_two * two_scale) + ADAM_EPS)
                old = master_v[layer, at, :]
                master_out[layer, at, :] = old - LEARN_RATE * (step_size + WEIGHT_DECAY * old)
                one_out[layer, at, :] = new_one
                two_out[layer, at, :] = new_two
            return 0

        lax.fori_loop(0, half_chunks // 48, update, 0)

    def round_rows(kind, layer, half):
        width = hidden_dim if kind == 0 else model_dim
        count = in_rows if kind == 0 else out_rows
        per_row = width // LANES
        dst = w_in if kind == 0 else w_out
        slot = lax.rem(me, 4)

        def body(idx, _):
            base = half * half_chunks + idx * (16 * per_row)
            row = pl.multiple_of(slot * count + half * (count // 2) + idx * 16, 16)
            for col in range(per_row):
                top = master_out[layer, pl.ds(base + col, 8, stride=per_row), :]
                low = master_out[layer, pl.ds(base + 8 * per_row + col, 8, stride=per_row), :]
                dst[layer, pl.ds(row, 16), col * LANES:(col + 1) * LANES] = jnp.concatenate([top, low], axis=0).astype(BF16)
            return 0

        lax.fori_loop(0, count // 32, body, 0)

    for layer in range(layers):
        for which in range(1, 4):
            load(which, layer).wait()
        for half in range(2):
            adam(layer, half)

            def send_own(kind):
                round_rows(kind, layer, half)
                copy(kind, layer, me, half, half, x_peer).start()
                copy(kind, layer, me, half, 2 + half, y_peer).start()
                copy(kind, layer, me, half, 6 + half, partner).start()

            by_kind(send_own)

    def pack(kind, device, packed_ref):
        spread_piece(dims, kind, device, (w_in, w_out), wide_ref)

        def squeeze(idx, _):
            block = wide_ref[pl.ds(pl.multiple_of(idx * 128, 128), 128), :].astype(BF16).reshape(32, 4, LANES)
            packed_ref[pl.ds(idx * 32, 32), :, :] = block[:, :layers, :]
            return 0

        lax.fori_loop(0, 4 * chunks // 128, squeeze, 0)

    def partner_of(device):
        return device + 1 - 2 * core

    tok_load.wait()

    for layer in range(layers):
        def forward(kind):
            for half in range(2):
                copy(kind, layer, x_peer, half, half, me).wait_recv()
                if half == 0:
                    copy(kind, layer, x_peer, half, 4, y_peer).start()
                copy(kind, layer, x_peer, half, 8 + half, partner).start()
                copy(1 - kind, layer, y_peer, half, 2 + half, me).wait_recv()
                if half == 1:
                    copy(1 - kind, layer, y_peer, half, 5, x_peer).start()
                copy(1 - kind, layer, y_peer, half, 10 + half, partner).start()
            for half in range(2):
                copy(kind, layer, partner, half, 6 + half, me).wait_recv()

        by_kind(forward)

    def pack_near(kind):
        pack(kind, me, p0)
        pack(kind, partner, p1)
        pack(kind, x_peer, p2)
        pack(1 - kind, y_peer, p4)
        for layer in range(layers):
            for half in range(2):
                copy(kind, layer, partner_of(x_peer), half, 8 + half, me).wait_recv()
                copy(1 - kind, layer, partner_of(y_peer), half, 10 + half, me).wait_recv()
        pack(kind, partner_of(x_peer), p3)
        pack(1 - kind, partner_of(y_peer), p5)

    by_kind(pack_near)

    for layer in range(layers):
        def far(kind):
            for half in range(2):
                copy(1 - kind, layer, diag, half, 4 + half, me).wait_recv()
                copy(1 - kind, layer, diag, half, 12 + half, partner).start()
            for half in range(2):
                copy(1 - kind, layer, partner_of(diag), half, 12 + half, me).wait_recv()

        by_kind(far)
        if layer < layers - 1:
            mlp_block(dims, layer, w_in, w_out, hidden_ref, normed_ref, active_ref)

    for step in range(1, GROUP):
        part_copy(step).wait_send()

    def drain(kind):
        for layer in range(layers):
            for half in range(2):
                copy(kind, layer, me, half, half, x_peer).wait_send()
                copy(kind, layer, me, half, 2 + half, y_peer).wait_send()
                copy(kind, layer, me, half, 6 + half, partner).wait_send()
                copy(kind, layer, x_peer, half, 8 + half, partner).wait_send()
                copy(1 - kind, layer, y_peer, half, 10 + half, partner).wait_send()
                copy(1 - kind, layer, diag, half, 12 + half, partner).wait_send()
            copy(kind, layer, x_peer, 0, 4, y_peer).wait_send()
            copy(1 - kind, layer, y_peer, 1, 5, x_peer).wait_send()

    by_kind(drain)


def finish_kernel(dims, p0, p1, p2, p3, p4, p5, master_ref, one_ref, two_ref, w_in, w_out, last_ref, tgt_ref,
                  packed_hbm, master_hbm, one_hbm, two_hbm, loss_ref,
                  far_ref, wide_ref, normed_ref, active_ref, hidden_ref, sem, far_sem):
    layers, model_dim, hidden_dim, rows, chunks = dims
    me, core, y_pos, x_peer, y_peer, diag = places()
    twin = 1 - 2 * core

    copies = []
    for idx, (ref, device) in enumerate(((p0, me), (p1, me + twin), (p2, x_peer), (p3, x_peer + twin), (p4, y_peer), (p5, y_peer + twin))):
        copies.append(pltpu.make_async_copy(ref, packed_hbm.at[pl.ds(device * chunks, chunks)], sem.at[idx]))
    for which, (src, dst) in enumerate(((master_ref, master_hbm), (one_ref, one_hbm), (two_ref, two_hbm))):
        for layer in range(layers):
            copies.append(pltpu.make_async_copy(src.at[layer], dst.at[:, layer, :], sem.at[6 + which * layers + layer]))
    for item in copies:
        item.start()

    far_copies = []
    for idx, device in enumerate((diag, diag + twin)):
        for y_value in range(2):
            @pl.when(y_pos == y_value)
            def _():
                spread_piece(dims, 1 - y_value, device, (w_in, w_out), wide_ref)

        def squeeze(at, _):
            block = wide_ref[pl.ds(pl.multiple_of(at * 128, 128), 128), :].astype(BF16).reshape(32, 4, LANES)
            far_ref[idx, pl.ds(at * 32, 32), :, :] = block[:, :layers, :]
            return 0

        lax.fori_loop(0, 4 * chunks // 128, squeeze, 0)
        far_copies.append(pltpu.make_async_copy(far_ref.at[idx], packed_hbm.at[pl.ds(device * chunks, chunks)], far_sem.at[idx]))
        far_copies[-1].start()

    hidden_ref[...] = last_ref[...]
    mlp_block(dims, layers - 1, w_in, w_out, hidden_ref, normed_ref, active_ref)

    for idx in range(rows // LANES):
        at = slice(idx * LANES, (idx + 1) * LANES)
        error = hidden_ref[at, :].astype(F32) - tgt_ref[at, :].astype(F32)
        error = error * error
        folded = error[:, 0:LANES]
        for col in range(LANES, model_dim, LANES):
            folded = folded + error[:, col:col + LANES]
        loss_ref[idx:idx + 1, :] = jnp.sum(folded.T, axis=0, keepdims=True) * (1.0 / model_dim)

    for item in copies + far_copies:
        item.wait()


def solution(mesh):
    group_size = mesh.shape["data"]
    state_spec = P(None, "data")
    row_spec = P("data", None)

    def local_step(grad_shard, master_shard, one_shard, two_shard, tok_rows, tgt_rows):
        rows, model_dim = tok_rows.shape
        layers, cols = master_shard.shape
        half_size = cols * group_size // 2
        hidden_dim = half_size // model_dim
        chunks = cols // LANES
        dims = (layers, model_dim, hidden_dim, rows, chunks)
        tiled = [a.reshape(layers, chunks, LANES).transpose(1, 0, 2) for a in (grad_shard, master_shard, one_shard, two_shard)]
        state_v = pltpu.VMEM((layers, chunks, LANES), F32)
        hbm = pl.BlockSpec(memory_space=pltpu.HBM)
        vmem = pl.BlockSpec(memory_space=pltpu.VMEM)
        state_out = state_v
        w_in_v = pltpu.VMEM((layers, model_dim, hidden_dim), BF16)
        w_out_v = pltpu.VMEM((layers, hidden_dim, model_dim), BF16)
        hidden_v = pltpu.VMEM((rows, model_dim), BF16)
        wide_v = pltpu.VMEM((4 * chunks, LANES), F32)
        normed_v = pltpu.VMEM((256, model_dim), BF16)
        active_v = pltpu.VMEM((256, hidden_dim), BF16)
        packed_v = pltpu.VMEM((chunks, layers, LANES), BF16)
        gathered = pl.pallas_call(
            functools.partial(gather_kernel, dims),
            name="gather_step",
            out_shape=(*(packed_v,) * 6, state_v, state_v, state_v, w_in_v, w_out_v, hidden_v),
            in_specs=[hbm] * 5,
            out_specs=(vmem,) * 12,
            scratch_shapes=[
                state_v, state_v, state_v, state_v,
                pltpu.VMEM((group_size, 8, LANES), F32),
                wide_v, normed_v, active_v,
                pltpu.SemaphoreType.DMA((5, layers)),
                pltpu.SemaphoreType.DMA((group_size,)),
                pltpu.SemaphoreType.DMA((group_size,)),
                pltpu.SemaphoreType.DMA((layers, 14)),
                pltpu.SemaphoreType.DMA((layers, 14)),
            ],
            compiler_params=pltpu.CompilerParams(collective_id=0, has_side_effects=True, vmem_limit_bytes=19 << 20),
        )(*[pltpu.with_memory_space_constraint(a, pltpu.HBM) for a in (*tiled, tok_rows)])
        state_tile = jax.ShapeDtypeStruct((chunks, layers, LANES), F32)
        weights, new_master, new_one, new_two, row_loss = pl.pallas_call(
            functools.partial(finish_kernel, dims),
            name="finish",
            out_shape=(jax.ShapeDtypeStruct((chunks * group_size, layers, LANES), BF16), state_tile, state_tile, state_tile,
                       jax.ShapeDtypeStruct((rows // LANES, LANES), F32)),
            in_specs=[vmem] * 13,
            out_specs=(hbm, hbm, hbm, hbm, vmem),
            scratch_shapes=[
                pltpu.VMEM((2, chunks, layers, LANES), BF16),
                wide_v, normed_v, active_v, hidden_v,
                pltpu.SemaphoreType.DMA((6 + 3 * layers,)),
                pltpu.SemaphoreType.DMA((2,)),
            ],
            compiler_params=pltpu.CompilerParams(vmem_limit_bytes=14 << 20),
        )(*gathered, tgt_rows)

        def flat(a):
            return a.transpose(1, 0, 2).reshape(layers, a.shape[0] * LANES)

        return row_loss.reshape(rows), flat(weights), flat(new_master), flat(new_one), flat(new_two)

    return jax.shard_map(local_step, mesh=mesh, in_specs=(state_spec, state_spec, state_spec, state_spec, row_spec, row_spec), out_specs=(P("data"), P(), state_spec, state_spec, state_spec), check_vma=False)
```

```python
import functools

import jax
import jax.numpy as jnp
from jax import lax
from jax.experimental import pallas as pl
from jax.experimental.pallas import tpu as pltpu
from jax.sharding import PartitionSpec as P

LEARN_RATE = 0.01
BETA_ONE = 0.9
BETA_TWO = 0.95
ADAM_EPS = 1e-8
WEIGHT_DECAY = 0.1
ADAM_STEP = 10
CLIP_NORM = 1.0
NORM_EPS = 1e-6

MESH = pl.DeviceIdType.MESH
LANES = 128
GROUP = 8
F32 = jnp.float32
BF16 = jnp.bfloat16


def spread_piece(dims, kind, device, weights, wide_ref):
    layers, model_dim, hidden_dim, rows, chunks = dims
    per_row = (hidden_dim if kind == 0 else model_dim) // LANES
    count = chunks // per_row
    src = weights[kind]
    slot = lax.rem(device, 4)

    def spread(idx, _):
        row = pl.multiple_of(slot * count + idx * 16, 16)
        for layer in range(layers):
            for col in range(per_row):
                tile = src[layer, pl.ds(row, 16), col * LANES:(col + 1) * LANES].astype(F32)
                base = layer + 4 * (idx * (16 * per_row) + col)
                wide_ref[pl.ds(base, 8, stride=4 * per_row), :] = tile[0:8]
                wide_ref[pl.ds(base + 32 * per_row, 8, stride=4 * per_row), :] = tile[8:16]
        return 0

    lax.fori_loop(0, count // 16, spread, 0)


def mlp_block(dims, layer, w_in, w_out, hidden_ref, normed_ref, active_ref):
    layers, model_dim, hidden_dim, rows, chunks = dims

    def block(idx, _):
        at = pl.ds(pl.multiple_of(idx * 256, 256), 256)
        hidden = hidden_ref[at, :].astype(F32)
        scale = lax.rsqrt(jnp.mean(hidden * hidden, axis=-1, keepdims=True) + NORM_EPS)
        normed_ref[...] = (hidden * scale).astype(BF16)
        for col in range(0, hidden_dim, 384):
            inner = jnp.dot(normed_ref[...], w_in[layer, :, col:col + 384], preferred_element_type=F32).astype(BF16)
            active_ref[:, col:col + 384] = jax.nn.gelu(inner.astype(F32), approximate=True).astype(BF16)
        for col in range(0, model_dim, 256):
            add = jnp.dot(active_ref[...], w_out[layer, :, col:col + 256], preferred_element_type=F32)
            hidden_ref[at, col:col + 256] = (hidden_ref[at, col:col + 256].astype(F32) + add).astype(BF16)
        return 0

    lax.fori_loop(0, rows // 256, block, 0)


def places():
    me = lax.axis_index("data")
    core = lax.rem(me, 2)
    x_pos = lax.rem(me // 2, 2)
    y_pos = me // 4
    x_peer = me + 2 - 4 * x_pos
    y_peer = me + 4 - 8 * y_pos
    return me, core, y_pos, x_peer, y_peer, x_peer + 4 - 8 * y_pos


def gather_kernel(dims, grad_hbm, master_hbm, one_hbm, two_hbm, tok_hbm,
                  p0, p1, p2, p3, p4, p5, master_out, one_out, two_out, w_in, w_out, hidden_ref,
                  grad_v, master_v, one_v, two_v,
                  part_ref, wide_ref, normed_ref, active_ref,
                  load_sem, part_send, part_recv, send_sem, recv_sem):
    layers, model_dim, hidden_dim, rows, chunks = dims
    in_rows = chunks * LANES // hidden_dim
    out_rows = chunks * LANES // model_dim
    half_chunks = chunks // 2

    me, core, y_pos, x_peer, y_peer, diag = places()
    partner = me + 1 - 2 * core

    state = ((grad_hbm, grad_v), (master_hbm, master_v), (one_hbm, one_v), (two_hbm, two_v))

    def load(which, layer):
        src, dst = state[which]
        return pltpu.make_async_copy(src.at[:, layer, :], dst.at[layer], load_sem.at[which, layer])

    for layer in range(layers):
        load(0, layer).start()
    tok_load = pltpu.make_async_copy(tok_hbm, hidden_ref, load_sem.at[4, 0])

    barrier = pltpu.get_barrier_semaphore()
    for step in range(1, GROUP):
        pl.semaphore_signal(barrier, inc=1, device_id=(lax.rem(me + step, GROUP),), device_id_type=MESH)

    sums = tuple(jnp.zeros((8, LANES), F32) for _ in range(8))
    for layer in range(layers):
        load(0, layer).wait()
        if layer == layers - 1:
            for item in range(layers):
                for which in range(1, 4):
                    load(which, item).start()
            tok_load.start()

        def square(idx, carry):
            base = pl.multiple_of(idx * 64, 64)
            block = grad_v[layer, pl.ds(base, 64), :]
            return tuple(carry[k] + block[8 * k:8 * k + 8] * block[8 * k:8 * k + 8] for k in range(8))

        sums = lax.fori_loop(0, chunks // 64, square, sums)
    mine = ((sums[0] + sums[1]) + (sums[2] + sums[3])) + ((sums[4] + sums[5]) + (sums[6] + sums[7]))
    part_ref[me] = mine
    pl.semaphore_wait(barrier, GROUP - 1)

    def part_copy(step):
        return pltpu.make_async_remote_copy(
            src_ref=part_ref.at[me], dst_ref=part_ref.at[me],
            send_sem=part_send.at[step], recv_sem=part_recv.at[step],
            device_id=(lax.rem(me + step, GROUP),), device_id_type=MESH)

    def part_arrival(step):
        slot = lax.rem(me + GROUP - step, GROUP)
        return pltpu.make_async_remote_copy(
            src_ref=part_ref.at[slot], dst_ref=part_ref.at[slot],
            send_sem=part_send.at[step], recv_sem=part_recv.at[step],
            device_id=(me,), device_id_type=MESH)

    for step in range(1, GROUP):
        part_copy(step).start()
    for step in range(1, GROUP):
        part_arrival(step).wait_recv()
    total = part_ref[0]
    for slot in range(1, GROUP):
        total = total + part_ref[slot]
    total = jnp.sum(jnp.sum(total, axis=0, keepdims=True), axis=1, keepdims=True)
    clip = jnp.minimum(1.0, CLIP_NORM / jnp.sqrt(total))
    clip = jnp.broadcast_to(clip, (8, LANES))

    def piece(kind, layer, device, half):
        slot = lax.rem(device, 4)
        if kind == 0:
            return w_in.at[layer, pl.ds(pl.multiple_of(slot * in_rows + half * (in_rows // 2), 16), in_rows // 2), :]
        return w_out.at[layer, pl.ds(pl.multiple_of(slot * out_rows + half * (out_rows // 2), 16), out_rows // 2), :]

    def copy(kind, layer, device, half, index, target):
        ref = piece(kind, layer, device, half)
        return pltpu.make_async_remote_copy(
            src_ref=ref, dst_ref=ref, send_sem=send_sem.at[layer, index],
            recv_sem=recv_sem.at[layer, index], device_id=(target,), device_id_type=MESH)

    def by_kind(function):
        for y_value in range(2):
            @pl.when(y_pos == y_value)
            def _():
                function(y_value)

    one_scale = 1.0 / (1.0 - BETA_ONE ** ADAM_STEP)
    two_scale = 1.0 / (1.0 - BETA_TWO ** ADAM_STEP)

    def adam(layer, half):
        def update(idx, _):
            base = pl.multiple_of(half * half_chunks + idx * 48, 8)
            for k in range(6):
                at = pl.ds(pl.multiple_of(base + 8 * k, 8), 8)
                clipped = grad_v[layer, at, :] * clip
                new_one = BETA_ONE * one_v[layer, at, :] + (1.0 - BETA_ONE) * clipped
                new_two = BETA_TWO * two_v[layer, at, :] + (1.0 - BETA_TWO) * clipped * clipped
                step_size = (new_one * one_scale) / (jnp.sqrt(new_two * two_scale) + ADAM_EPS)
                old = master_v[layer, at, :]
                master_out[layer, at, :] = old - LEARN_RATE * (step_size + WEIGHT_DECAY * old)
                one_out[layer, at, :] = new_one
                two_out[layer, at, :] = new_two
            return 0

        lax.fori_loop(0, half_chunks // 48, update, 0)

    def round_rows(kind, layer, half):
        width = hidden_dim if kind == 0 else model_dim
        count = in_rows if kind == 0 else out_rows
        per_row = width // LANES
        dst = w_in if kind == 0 else w_out
        slot = lax.rem(me, 4)

        def body(idx, _):
            base = half * half_chunks + idx * (16 * per_row)
            row = pl.multiple_of(slot * count + half * (count // 2) + idx * 16, 16)
            for col in range(per_row):
                top = master_out[layer, pl.ds(base + col, 8, stride=per_row), :]
                low = master_out[layer, pl.ds(base + 8 * per_row + col, 8, stride=per_row), :]
                dst[layer, pl.ds(row, 16), col * LANES:(col + 1) * LANES] = jnp.concatenate([top, low], axis=0).astype(BF16)
            return 0

        lax.fori_loop(0, count // 32, body, 0)

    for layer in range(layers):
        for which in range(1, 4):
            load(which, layer).wait()
        for half in range(2):
            adam(layer, half)

            def send_own(kind):
                round_rows(kind, layer, half)
                copy(kind, layer, me, half, half, x_peer).start()
                copy(kind, layer, me, half, 2 + half, y_peer).start()
                copy(kind, layer, me, half, 6 + half, partner).start()

            by_kind(send_own)

    def pack(kind, device, packed_ref):
        spread_piece(dims, kind, device, (w_in, w_out), wide_ref)

        def squeeze(idx, _):
            block = wide_ref[pl.ds(pl.multiple_of(idx * 128, 128), 128), :].astype(BF16).reshape(32, 4, LANES)
            packed_ref[pl.ds(idx * 32, 32), :, :] = block[:, :layers, :]
            return 0

        lax.fori_loop(0, 4 * chunks // 128, squeeze, 0)

    def partner_of(device):
        return device + 1 - 2 * core

    def pack_own(kind):
        pack(kind, me, p0)
        for layer in range(layers):
            for half in range(2):
                copy(kind, layer, partner, half, 6 + half, me).wait_recv()
        pack(kind, partner, p1)

    by_kind(pack_own)

    for layer in range(layers):
        def forward(kind):
            for half in range(2):
                copy(kind, layer, x_peer, half, half, me).wait_recv()
                if half == 0:
                    copy(kind, layer, x_peer, half, 4, y_peer).start()
                copy(kind, layer, x_peer, half, 8 + half, partner).start()
                copy(1 - kind, layer, y_peer, half, 2 + half, me).wait_recv()
                if half == 1:
                    copy(1 - kind, layer, y_peer, half, 5, x_peer).start()
                copy(1 - kind, layer, y_peer, half, 10 + half, partner).start()

        by_kind(forward)

    def far_arrive(kind, layer):
        for half in range(2):
            copy(1 - kind, layer, diag, half, 4 + half, me).wait_recv()
            copy(1 - kind, layer, diag, half, 12 + half, partner).start()

    def far_partner(kind, layer):
        for half in range(2):
            copy(1 - kind, layer, partner_of(diag), half, 12 + half, me).wait_recv()

    def stage_zero(kind):
        pack(kind, x_peer, p2)
        pack(1 - kind, y_peer, p4)
        far_arrive(kind, 0)
        for layer in range(layers):
            for half in range(2):
                copy(kind, layer, partner_of(x_peer), half, 8 + half, me).wait_recv()
                copy(1 - kind, layer, partner_of(y_peer), half, 10 + half, me).wait_recv()
        pack(kind, partner_of(x_peer), p3)
        far_partner(kind, 0)

    def stage_one(kind):
        far_arrive(kind, 1)
        pack(1 - kind, partner_of(y_peer), p5)
        far_partner(kind, 1)

    def stage_two(kind):
        far_arrive(kind, 2)
        far_partner(kind, 2)

    by_kind(stage_zero)
    tok_load.wait()
    mlp_block(dims, 0, w_in, w_out, hidden_ref, normed_ref, active_ref)
    by_kind(stage_one)
    mlp_block(dims, 1, w_in, w_out, hidden_ref, normed_ref, active_ref)
    by_kind(stage_two)

    for step in range(1, GROUP):
        part_copy(step).wait_send()

    def drain(kind):
        for layer in range(layers):
            for half in range(2):
                copy(kind, layer, me, half, half, x_peer).wait_send()
                copy(kind, layer, me, half, 2 + half, y_peer).wait_send()
                copy(kind, layer, me, half, 6 + half, partner).wait_send()
                copy(kind, layer, x_peer, half, 8 + half, partner).wait_send()
                copy(1 - kind, layer, y_peer, half, 10 + half, partner).wait_send()
                copy(1 - kind, layer, diag, half, 12 + half, partner).wait_send()
            copy(kind, layer, x_peer, 0, 4, y_peer).wait_send()
            copy(1 - kind, layer, y_peer, 1, 5, x_peer).wait_send()

    by_kind(drain)


def finish_kernel(dims, p0, p1, p2, p3, p4, p5, master_ref, one_ref, two_ref, w_in, w_out, last_ref, tgt_ref,
                  packed_hbm, master_hbm, one_hbm, two_hbm, loss_ref,
                  far_ref, wide_ref, normed_ref, active_ref, hidden_ref, sem, far_sem):
    layers, model_dim, hidden_dim, rows, chunks = dims
    me, core, y_pos, x_peer, y_peer, diag = places()
    twin = 1 - 2 * core

    copies = []
    for idx, (ref, device) in enumerate(((p0, me), (p1, me + twin), (p2, x_peer), (p3, x_peer + twin), (p4, y_peer), (p5, y_peer + twin))):
        copies.append(pltpu.make_async_copy(ref, packed_hbm.at[pl.ds(device * chunks, chunks)], sem.at[idx]))
    for which, (src, dst) in enumerate(((master_ref, master_hbm), (one_ref, one_hbm), (two_ref, two_hbm))):
        for layer in range(layers):
            copies.append(pltpu.make_async_copy(src.at[layer], dst.at[:, layer, :], sem.at[6 + which * layers + layer]))
    for item in copies:
        item.start()

    far_copies = []
    for idx, device in enumerate((diag, diag + twin)):
        for y_value in range(2):
            @pl.when(y_pos == y_value)
            def _():
                spread_piece(dims, 1 - y_value, device, (w_in, w_out), wide_ref)

        def squeeze(at, _):
            block = wide_ref[pl.ds(pl.multiple_of(at * 128, 128), 128), :].astype(BF16).reshape(32, 4, LANES)
            far_ref[idx, pl.ds(at * 32, 32), :, :] = block[:, :layers, :]
            return 0

        lax.fori_loop(0, 4 * chunks // 128, squeeze, 0)
        far_copies.append(pltpu.make_async_copy(far_ref.at[idx], packed_hbm.at[pl.ds(device * chunks, chunks)], far_sem.at[idx]))
        far_copies[-1].start()

    hidden_ref[...] = last_ref[...]
    mlp_block(dims, layers - 1, w_in, w_out, hidden_ref, normed_ref, active_ref)

    for idx in range(rows // LANES):
        at = slice(idx * LANES, (idx + 1) * LANES)
        error = hidden_ref[at, :].astype(F32) - tgt_ref[at, :].astype(F32)
        error = error * error
        folded = error[:, 0:LANES]
        for col in range(LANES, model_dim, LANES):
            folded = folded + error[:, col:col + LANES]
        loss_ref[idx:idx + 1, :] = jnp.sum(folded.T, axis=0, keepdims=True) * (1.0 / model_dim)

    for item in copies + far_copies:
        item.wait()


def solution(mesh):
    group_size = mesh.shape["data"]
    state_spec = P(None, "data")
    row_spec = P("data", None)

    def local_step(grad_shard, master_shard, one_shard, two_shard, tok_rows, tgt_rows):
        rows, model_dim = tok_rows.shape
        layers, cols = master_shard.shape
        half_size = cols * group_size // 2
        hidden_dim = half_size // model_dim
        chunks = cols // LANES
        dims = (layers, model_dim, hidden_dim, rows, chunks)
        tiled = [a.reshape(layers, chunks, LANES).transpose(1, 0, 2) for a in (grad_shard, master_shard, one_shard, two_shard)]
        state_v = pltpu.VMEM((layers, chunks, LANES), F32)
        hbm = pl.BlockSpec(memory_space=pltpu.HBM)
        vmem = pl.BlockSpec(memory_space=pltpu.VMEM)
        state_out = state_v
        w_in_v = pltpu.VMEM((layers, model_dim, hidden_dim), BF16)
        w_out_v = pltpu.VMEM((layers, hidden_dim, model_dim), BF16)
        hidden_v = pltpu.VMEM((rows, model_dim), BF16)
        wide_v = pltpu.VMEM((4 * chunks, LANES), F32)
        normed_v = pltpu.VMEM((256, model_dim), BF16)
        active_v = pltpu.VMEM((256, hidden_dim), BF16)
        packed_v = pltpu.VMEM((chunks, layers, LANES), BF16)
        gathered = pl.pallas_call(
            functools.partial(gather_kernel, dims),
            name="gather_step",
            out_shape=(*(packed_v,) * 6, state_v, state_v, state_v, w_in_v, w_out_v, hidden_v),
            in_specs=[hbm] * 5,
            out_specs=(vmem,) * 12,
            scratch_shapes=[
                state_v, state_v, state_v, state_v,
                pltpu.VMEM((group_size, 8, LANES), F32),
                wide_v, normed_v, active_v,
                pltpu.SemaphoreType.DMA((5, layers)),
                pltpu.SemaphoreType.DMA((group_size,)),
                pltpu.SemaphoreType.DMA((group_size,)),
                pltpu.SemaphoreType.DMA((layers, 14)),
                pltpu.SemaphoreType.DMA((layers, 14)),
            ],
            compiler_params=pltpu.CompilerParams(collective_id=0, has_side_effects=True, vmem_limit_bytes=19 << 20),
        )(*[pltpu.with_memory_space_constraint(a, pltpu.HBM) for a in (*tiled, tok_rows)])
        state_tile = jax.ShapeDtypeStruct((chunks, layers, LANES), F32)
        weights, new_master, new_one, new_two, row_loss = pl.pallas_call(
            functools.partial(finish_kernel, dims),
            name="finish",
            out_shape=(jax.ShapeDtypeStruct((chunks * group_size, layers, LANES), BF16), state_tile, state_tile, state_tile,
                       jax.ShapeDtypeStruct((rows // LANES, LANES), F32)),
            in_specs=[vmem] * 13,
            out_specs=(hbm, hbm, hbm, hbm, vmem),
            scratch_shapes=[
                pltpu.VMEM((2, chunks, layers, LANES), BF16),
                wide_v, normed_v, active_v, hidden_v,
                pltpu.SemaphoreType.DMA((6 + 3 * layers,)),
                pltpu.SemaphoreType.DMA((2,)),
            ],
            compiler_params=pltpu.CompilerParams(vmem_limit_bytes=14 << 20),
        )(*gathered, tgt_rows)

        def flat(a):
            return a.transpose(1, 0, 2).reshape(layers, a.shape[0] * LANES)

        return row_loss.reshape(rows), flat(weights), flat(new_master), flat(new_one), flat(new_two)

    return jax.shard_map(local_step, mesh=mesh, in_specs=(state_spec, state_spec, state_spec, state_spec, row_spec, row_spec), out_specs=(P("data"), P(), state_spec, state_spec, state_spec), check_vma=False)
```

```python
import functools

import jax
import jax.numpy as jnp
from jax import lax
from jax.experimental import pallas as pl
from jax.experimental.pallas import tpu as pltpu
from jax.sharding import PartitionSpec as P

LEARN_RATE = 0.01
BETA_ONE = 0.9
BETA_TWO = 0.95
ADAM_EPS = 1e-8
WEIGHT_DECAY = 0.1
ADAM_STEP = 10
CLIP_NORM = 1.0
NORM_EPS = 1e-6

MESH = pl.DeviceIdType.MESH
LANES = 128
GROUP = 8
F32 = jnp.float32
BF16 = jnp.bfloat16


def spread_piece(dims, kind, device, weights, wide_ref):
    layers, model_dim, hidden_dim, rows, chunks = dims
    per_row = (hidden_dim if kind == 0 else model_dim) // LANES
    count = chunks // per_row
    src = weights[kind]
    slot = lax.rem(device, 4)

    def spread(idx, _):
        row = pl.multiple_of(slot * count + idx * 16, 16)
        for layer in range(layers):
            for col in range(per_row):
                tile = src[layer, pl.ds(row, 16), col * LANES:(col + 1) * LANES].astype(F32)
                base = layer + 4 * (idx * (16 * per_row) + col)
                wide_ref[pl.ds(base, 8, stride=4 * per_row), :] = tile[0:8]
                wide_ref[pl.ds(base + 32 * per_row, 8, stride=4 * per_row), :] = tile[8:16]
        return 0

    lax.fori_loop(0, count // 16, spread, 0)


def mlp_block(dims, layer, w_in, w_out, hidden_ref, normed_ref, active_ref):
    layers, model_dim, hidden_dim, rows, chunks = dims

    def block(idx, _):
        at = pl.ds(pl.multiple_of(idx * 256, 256), 256)
        hidden = hidden_ref[at, :].astype(F32)
        scale = lax.rsqrt(jnp.mean(hidden * hidden, axis=-1, keepdims=True) + NORM_EPS)
        normed_ref[...] = (hidden * scale).astype(BF16)
        for col in range(0, hidden_dim, 384):
            inner = jnp.dot(normed_ref[...], w_in[layer, :, col:col + 384], preferred_element_type=F32).astype(BF16)
            active_ref[:, col:col + 384] = jax.nn.gelu(inner.astype(F32), approximate=True).astype(BF16)
        for col in range(0, model_dim, 256):
            add = jnp.dot(active_ref[...], w_out[layer, :, col:col + 256], preferred_element_type=F32)
            hidden_ref[at, col:col + 256] = (hidden_ref[at, col:col + 256].astype(F32) + add).astype(BF16)
        return 0

    lax.fori_loop(0, rows // 256, block, 0)


def places():
    me = lax.axis_index("data")
    core = lax.rem(me, 2)
    x_pos = lax.rem(me // 2, 2)
    y_pos = me // 4
    x_peer = me + 2 - 4 * x_pos
    y_peer = me + 4 - 8 * y_pos
    return me, core, y_pos, x_peer, y_peer, x_peer + 4 - 8 * y_pos


def gather_kernel(dims, grad_hbm, master_hbm, one_hbm, two_hbm, tok_hbm,
                  p0, p1, p2, p3, p4, p5, master_out, one_out, two_out, w_in, w_out, hidden_ref,
                  grad_v, master_v, one_v, two_v,
                  part_ref, wide_ref, normed_ref, active_ref,
                  load_sem, part_send, part_recv, send_sem, recv_sem):
    layers, model_dim, hidden_dim, rows, chunks = dims
    in_rows = chunks * LANES // hidden_dim
    out_rows = chunks * LANES // model_dim
    half_chunks = chunks // 2

    me, core, y_pos, x_peer, y_peer, diag = places()
    partner = me + 1 - 2 * core

    state = ((grad_hbm, grad_v), (master_hbm, master_v), (one_hbm, one_v), (two_hbm, two_v))

    def load(which, layer):
        src, dst = state[which]
        return pltpu.make_async_copy(src.at[:, layer, :], dst.at[layer], load_sem.at[which, layer])

    for layer in range(layers):
        load(0, layer).start()
    tok_load = pltpu.make_async_copy(tok_hbm, hidden_ref, load_sem.at[4, 0])

    barrier = pltpu.get_barrier_semaphore()
    for step in range(1, GROUP):
        pl.semaphore_signal(barrier, inc=1, device_id=(lax.rem(me + step, GROUP),), device_id_type=MESH)

    sums = tuple(jnp.zeros((8, LANES), F32) for _ in range(8))
    for layer in range(layers):
        load(0, layer).wait()
        if layer == layers - 1:
            for item in range(layers):
                for which in range(1, 4):
                    load(which, item).start()
            tok_load.start()

        def square(idx, carry):
            base = pl.multiple_of(idx * 64, 64)
            block = grad_v[layer, pl.ds(base, 64), :]
            return tuple(carry[k] + block[8 * k:8 * k + 8] * block[8 * k:8 * k + 8] for k in range(8))

        sums = lax.fori_loop(0, chunks // 64, square, sums)
    mine = ((sums[0] + sums[1]) + (sums[2] + sums[3])) + ((sums[4] + sums[5]) + (sums[6] + sums[7]))
    part_ref[me] = mine
    pl.semaphore_wait(barrier, GROUP - 1)

    def part_copy(step):
        return pltpu.make_async_remote_copy(
            src_ref=part_ref.at[me], dst_ref=part_ref.at[me],
            send_sem=part_send.at[step], recv_sem=part_recv.at[step],
            device_id=(lax.rem(me + step, GROUP),), device_id_type=MESH)

    def part_arrival(step):
        slot = lax.rem(me + GROUP - step, GROUP)
        return pltpu.make_async_remote_copy(
            src_ref=part_ref.at[slot], dst_ref=part_ref.at[slot],
            send_sem=part_send.at[step], recv_sem=part_recv.at[step],
            device_id=(me,), device_id_type=MESH)

    for step in range(1, GROUP):
        part_copy(step).start()
    for step in range(1, GROUP):
        part_arrival(step).wait_recv()
    total = part_ref[0]
    for slot in range(1, GROUP):
        total = total + part_ref[slot]
    total = jnp.sum(jnp.sum(total, axis=0, keepdims=True), axis=1, keepdims=True)
    clip = jnp.minimum(1.0, CLIP_NORM / jnp.sqrt(total))
    clip = jnp.broadcast_to(clip, (8, LANES))

    whole = ((0, 1),)
    thirds = tuple((part, 3) for part in range(3))
    slots = {}

    def piece(kind, layer, device, half, part):
        ref, count = ((w_in, in_rows), (w_out, out_rows))[kind]
        span = count // 2 // part[1]
        at = lax.rem(device, 4) * count + half * (count // 2) + part[0] * span
        return ref.at[layer, pl.ds(pl.multiple_of(at, 16), span), :]

    def copies(kind, layer, device, half, route, target, parts=whole):
        out = []
        for part in parts:
            ref = piece(kind, layer, device, half, part)
            index = slots.setdefault((route, layer, half, part), len(slots))
            out.append(pltpu.make_async_remote_copy(
                src_ref=ref, dst_ref=ref, send_sem=send_sem.at[index],
                recv_sem=recv_sem.at[index], device_id=(target,), device_id_type=MESH))
        return out

    def start(items):
        for item in items:
            item.start()

    def arrive(items):
        for item in items:
            item.wait_recv()

    def left(items):
        for item in items:
            item.wait_send()

    def own_parts(layer, half):
        return thirds if layer == 0 and half == 0 else whole

    def far_parts(layer):
        return thirds if layer == layers - 1 else whole

    def own_x(kind, layer, half, device, target, parts=None):
        return copies(kind, layer, device, half, "own_x", target, parts or own_parts(layer, half))

    def own_y(kind, layer, half, device, target, parts=None):
        return copies(kind, layer, device, half, "own_y", target, parts or own_parts(layer, half))

    def far(kind, layer, half, device, target, parts=None):
        return copies(kind, layer, device, half, "far", target, parts or far_parts(layer))

    def pair(kind, layer, half, device, route, parts=whole):
        return copies(kind, layer, device, half, route, partner, parts)

    def by_kind(function):
        for y_value in range(2):
            @pl.when(y_pos == y_value)
            def _():
                function(y_value)

    one_scale = 1.0 / (1.0 - BETA_ONE ** ADAM_STEP)
    two_scale = 1.0 / (1.0 - BETA_TWO ** ADAM_STEP)

    def adam(layer, half, part):
        first = half * half_chunks + part[0] * (half_chunks // part[1])

        def update(idx, _):
            base = pl.multiple_of(first + idx * 48, 8)
            for k in range(6):
                at = pl.ds(pl.multiple_of(base + 8 * k, 8), 8)
                clipped = grad_v[layer, at, :] * clip
                new_one = BETA_ONE * one_v[layer, at, :] + (1.0 - BETA_ONE) * clipped
                new_two = BETA_TWO * two_v[layer, at, :] + (1.0 - BETA_TWO) * clipped * clipped
                step_size = (new_one * one_scale) / (jnp.sqrt(new_two * two_scale) + ADAM_EPS)
                old = master_v[layer, at, :]
                master_out[layer, at, :] = old - LEARN_RATE * (step_size + WEIGHT_DECAY * old)
                one_out[layer, at, :] = new_one
                two_out[layer, at, :] = new_two
            return 0

        lax.fori_loop(0, half_chunks // part[1] // 48, update, 0)

    def round_rows(kind, layer, half, part):
        width = hidden_dim if kind == 0 else model_dim
        count = in_rows if kind == 0 else out_rows
        per_row = width // LANES
        dst = w_in if kind == 0 else w_out
        slot = lax.rem(me, 4)

        def body(idx, _):
            base = half * half_chunks + part[0] * (half_chunks // part[1]) + idx * (16 * per_row)
            row = pl.multiple_of(slot * count + half * (count // 2) + part[0] * (count // 2 // part[1]) + idx * 16, 16)
            for col in range(per_row):
                top = master_out[layer, pl.ds(base + col, 8, stride=per_row), :]
                low = master_out[layer, pl.ds(base + 8 * per_row + col, 8, stride=per_row), :]
                dst[layer, pl.ds(row, 16), col * LANES:(col + 1) * LANES] = jnp.concatenate([top, low], axis=0).astype(BF16)
            return 0

        lax.fori_loop(0, count // 32 // part[1], body, 0)

    for layer in range(layers):
        for which in range(1, 4):
            load(which, layer).wait()
        for half in range(2):
            for part in own_parts(layer, half):
                adam(layer, half, part)

                def send_own(kind):
                    round_rows(kind, layer, half, part)
                    start(own_x(kind, layer, half, me, x_peer, (part,)))
                    start(own_y(kind, layer, half, me, y_peer, (part,)))
                    start(pair(kind, layer, half, me, "pair_own", (part,)))

                by_kind(send_own)

    def pack(kind, device, packed_ref):
        spread_piece(dims, kind, device, (w_in, w_out), wide_ref)

        def squeeze(idx, _):
            block = wide_ref[pl.ds(pl.multiple_of(idx * 128, 128), 128), :].astype(BF16).reshape(32, 4, LANES)
            packed_ref[pl.ds(idx * 32, 32), :, :] = block[:, :layers, :]
            return 0

        lax.fori_loop(0, 4 * chunks // 128, squeeze, 0)

    def partner_of(device):
        return device + 1 - 2 * core

    def pack_own(kind):
        pack(kind, me, p0)
        for layer in range(layers):
            for half in range(2):
                arrive(pair(kind, layer, half, partner, "pair_own", own_parts(layer, half)))
        pack(kind, partner, p1)

    by_kind(pack_own)

    for layer in range(layers):
        def forward(kind):
            for half in range(2):
                arrive(own_x(kind, layer, half, x_peer, me))
                if half == 0:
                    start(far(kind, layer, half, x_peer, y_peer))
                start(pair(kind, layer, half, x_peer, "pair_x"))
                arrive(own_y(1 - kind, layer, half, y_peer, me))
                if half == 1:
                    start(far(1 - kind, layer, half, y_peer, x_peer))
                start(pair(1 - kind, layer, half, y_peer, "pair_y"))

        by_kind(forward)

    def far_arrive(kind, layer):
        for part in far_parts(layer):
            for half in range(2):
                arrive(far(1 - kind, layer, half, diag, me, (part,)))
                start(pair(1 - kind, layer, half, diag, "pair_far", (part,)))

    def far_partner(kind, layer):
        for half in range(2):
            arrive(pair(1 - kind, layer, half, partner_of(diag), "pair_far", far_parts(layer)))

    def stage_zero(kind):
        pack(kind, x_peer, p2)
        pack(1 - kind, y_peer, p4)
        far_arrive(kind, 0)
        for layer in range(layers):
            for half in range(2):
                arrive(pair(kind, layer, half, partner_of(x_peer), "pair_x"))
                arrive(pair(1 - kind, layer, half, partner_of(y_peer), "pair_y"))
        pack(kind, partner_of(x_peer), p3)
        far_partner(kind, 0)

    def stage_one(kind):
        far_arrive(kind, 1)
        pack(1 - kind, partner_of(y_peer), p5)
        far_partner(kind, 1)

    def stage_two(kind):
        far_arrive(kind, 2)
        far_partner(kind, 2)

    by_kind(stage_zero)
    tok_load.wait()
    mlp_block(dims, 0, w_in, w_out, hidden_ref, normed_ref, active_ref)
    by_kind(stage_one)
    mlp_block(dims, 1, w_in, w_out, hidden_ref, normed_ref, active_ref)
    by_kind(stage_two)

    for step in range(1, GROUP):
        part_copy(step).wait_send()

    def drain(kind):
        for layer in range(layers):
            for half in range(2):
                left(own_x(kind, layer, half, me, x_peer))
                left(own_y(kind, layer, half, me, y_peer))
                left(pair(kind, layer, half, me, "pair_own", own_parts(layer, half)))
                left(pair(kind, layer, half, x_peer, "pair_x"))
                left(pair(1 - kind, layer, half, y_peer, "pair_y"))
                left(pair(1 - kind, layer, half, diag, "pair_far", far_parts(layer)))
            left(far(kind, layer, 0, x_peer, y_peer))
            left(far(1 - kind, layer, 1, y_peer, x_peer))

    by_kind(drain)


def finish_kernel(dims, p0, p1, p2, p3, p4, p5, master_ref, one_ref, two_ref, w_in, w_out, last_ref, tgt_ref,
                  packed_hbm, master_hbm, one_hbm, two_hbm, loss_hbm,
                  loss_ref, far_ref, wide_ref, normed_ref, active_ref, hidden_ref, sem, far_sem):
    layers, model_dim, hidden_dim, rows, chunks = dims
    me, core, y_pos, x_peer, y_peer, diag = places()
    twin = 1 - 2 * core

    copies = []
    for idx, (ref, device) in enumerate(((p0, me), (p1, me + twin), (p2, x_peer), (p3, x_peer + twin), (p4, y_peer), (p5, y_peer + twin))):
        copies.append(pltpu.make_async_copy(ref, packed_hbm.at[pl.ds(device * chunks, chunks)], sem.at[idx]))
    for which, (src, dst) in enumerate(((master_ref, master_hbm), (one_ref, one_hbm), (two_ref, two_hbm))):
        for layer in range(layers):
            copies.append(pltpu.make_async_copy(src.at[layer], dst.at[:, layer, :], sem.at[6 + which * layers + layer]))
    for item in copies:
        item.start()

    far_copies = []
    for idx, device in enumerate((diag, diag + twin)):
        for y_value in range(2):
            @pl.when(y_pos == y_value)
            def _():
                spread_piece(dims, 1 - y_value, device, (w_in, w_out), wide_ref)

        def squeeze(at, _):
            block = wide_ref[pl.ds(pl.multiple_of(at * 128, 128), 128), :].astype(BF16).reshape(32, 4, LANES)
            far_ref[idx, pl.ds(at * 32, 32), :, :] = block[:, :layers, :]
            return 0

        lax.fori_loop(0, 4 * chunks // 128, squeeze, 0)
        far_copies.append(pltpu.make_async_copy(far_ref.at[idx], packed_hbm.at[pl.ds(device * chunks, chunks)], far_sem.at[idx]))
        far_copies[-1].start()

    hidden_ref[...] = last_ref[...]
    mlp_block(dims, layers - 1, w_in, w_out, hidden_ref, normed_ref, active_ref)

    for idx in range(rows // LANES):
        at = slice(idx * LANES, (idx + 1) * LANES)
        error = hidden_ref[at, :].astype(F32) - tgt_ref[at, :].astype(F32)
        error = error * error
        folded = error[:, 0:LANES]
        for col in range(LANES, model_dim, LANES):
            folded = folded + error[:, col:col + LANES]
        loss_ref[idx:idx + 1, :] = jnp.sum(folded.T, axis=0, keepdims=True) * (1.0 / model_dim)

    loss_copy = pltpu.make_async_copy(loss_ref, loss_hbm, far_sem.at[2])
    loss_copy.start()
    for item in copies + far_copies + [loss_copy]:
        item.wait()


def solution(mesh):
    group_size = mesh.shape["data"]
    state_spec = P(None, "data")
    row_spec = P("data", None)

    def local_step(grad_shard, master_shard, one_shard, two_shard, tok_rows, tgt_rows):
        rows, model_dim = tok_rows.shape
        layers, cols = master_shard.shape
        half_size = cols * group_size // 2
        hidden_dim = half_size // model_dim
        chunks = cols // LANES
        dims = (layers, model_dim, hidden_dim, rows, chunks)
        tiled = [a.reshape(layers, chunks, LANES).transpose(1, 0, 2) for a in (grad_shard, master_shard, one_shard, two_shard)]
        state_v = pltpu.VMEM((layers, chunks, LANES), F32)
        hbm = pl.BlockSpec(memory_space=pltpu.HBM)
        vmem = pl.BlockSpec(memory_space=pltpu.VMEM)
        state_out = state_v
        w_in_v = pltpu.VMEM((layers, model_dim, hidden_dim), BF16)
        w_out_v = pltpu.VMEM((layers, hidden_dim, model_dim), BF16)
        hidden_v = pltpu.VMEM((rows, model_dim), BF16)
        wide_v = pltpu.VMEM((4 * chunks, LANES), F32)
        normed_v = pltpu.VMEM((256, model_dim), BF16)
        active_v = pltpu.VMEM((256, hidden_dim), BF16)
        packed_v = pltpu.VMEM((chunks, layers, LANES), BF16)
        gathered = pl.pallas_call(
            functools.partial(gather_kernel, dims),
            name="gather_step",
            out_shape=(*(packed_v,) * 6, state_v, state_v, state_v, w_in_v, w_out_v, hidden_v),
            in_specs=[hbm] * 5,
            out_specs=(vmem,) * 12,
            scratch_shapes=[
                state_v, state_v, state_v, state_v,
                pltpu.VMEM((group_size, 8, LANES), F32),
                wide_v, normed_v, active_v,
                pltpu.SemaphoreType.DMA((5, layers)),
                pltpu.SemaphoreType.DMA((group_size,)),
                pltpu.SemaphoreType.DMA((group_size,)),
                pltpu.SemaphoreType.DMA((96,)),
                pltpu.SemaphoreType.DMA((96,)),
            ],
            compiler_params=pltpu.CompilerParams(collective_id=0, has_side_effects=True, vmem_limit_bytes=19 << 20),
        )(*[pltpu.with_memory_space_constraint(a, pltpu.HBM) for a in (*tiled, tok_rows)])
        state_tile = jax.ShapeDtypeStruct((chunks, layers, LANES), F32)
        weights, new_master, new_one, new_two, row_loss = pl.pallas_call(
            functools.partial(finish_kernel, dims),
            name="finish",
            out_shape=(jax.ShapeDtypeStruct((chunks * group_size, layers, LANES), BF16), state_tile, state_tile, state_tile,
                       jax.ShapeDtypeStruct((rows // LANES, LANES), F32)),
            in_specs=[vmem] * 13,
            out_specs=(hbm,) * 5,
            scratch_shapes=[
                pltpu.VMEM((rows // LANES, LANES), F32),
                pltpu.VMEM((2, chunks, layers, LANES), BF16),
                wide_v, normed_v, active_v, hidden_v,
                pltpu.SemaphoreType.DMA((6 + 3 * layers,)),
                pltpu.SemaphoreType.DMA((3,)),
            ],
            compiler_params=pltpu.CompilerParams(vmem_limit_bytes=14 << 20),
        )(*gathered, tgt_rows)

        def flat(a):
            return a.transpose(1, 0, 2).reshape(layers, a.shape[0] * LANES)

        return row_loss.reshape(rows), flat(weights), flat(new_master), flat(new_one), flat(new_two)

    return jax.shard_map(local_step, mesh=mesh, in_specs=(state_spec, state_spec, state_spec, state_spec, row_spec, row_spec), out_specs=(P("data"), P(), state_spec, state_spec, state_spec), check_vma=False)
```

```python
import functools

import jax
import jax.numpy as jnp
from jax import lax
from jax.experimental import pallas as pl
from jax.experimental.pallas import tpu as pltpu
from jax.sharding import PartitionSpec as P

LEARN_RATE = 0.01
BETA_ONE = 0.9
BETA_TWO = 0.95
ADAM_EPS = 1e-8
WEIGHT_DECAY = 0.1
ADAM_STEP = 10
CLIP_NORM = 1.0
NORM_EPS = 1e-6

MESH = pl.DeviceIdType.MESH
LANES = 128
GROUP = 8
F32 = jnp.float32
BF16 = jnp.bfloat16


def spread_piece(dims, kind, device, weights, wide_ref):
    layers, model_dim, hidden_dim, rows, chunks = dims
    per_row = (hidden_dim if kind == 0 else model_dim) // LANES
    count = chunks // per_row
    src = weights[kind]
    slot = lax.rem(device, 4)

    def spread(idx, _):
        row = pl.multiple_of(slot * count + idx * 16, 16)
        for layer in range(layers):
            for col in range(per_row):
                tile = src[layer, pl.ds(row, 16), col * LANES:(col + 1) * LANES].astype(F32)
                base = layer + 4 * (idx * (16 * per_row) + col)
                wide_ref[pl.ds(base, 8, stride=4 * per_row), :] = tile[0:8]
                wide_ref[pl.ds(base + 32 * per_row, 8, stride=4 * per_row), :] = tile[8:16]
        return 0

    lax.fori_loop(0, count // 16, spread, 0)


def mlp_block(dims, layer, w_in, w_out, hidden_ref, normed_ref, active_ref):
    layers, model_dim, hidden_dim, rows, chunks = dims

    def block(idx, _):
        at = pl.ds(pl.multiple_of(idx * 256, 256), 256)
        hidden = hidden_ref[at, :].astype(F32)
        scale = lax.rsqrt(jnp.mean(hidden * hidden, axis=-1, keepdims=True) + NORM_EPS)
        normed_ref[...] = (hidden * scale).astype(BF16)
        for col in range(0, hidden_dim, 384):
            inner = jnp.dot(normed_ref[...], w_in[layer, :, col:col + 384], preferred_element_type=F32).astype(BF16)
            active_ref[:, col:col + 384] = jax.nn.gelu(inner.astype(F32), approximate=True).astype(BF16)
        for col in range(0, model_dim, 256):
            add = jnp.dot(active_ref[...], w_out[layer, :, col:col + 256], preferred_element_type=F32)
            hidden_ref[at, col:col + 256] = (hidden_ref[at, col:col + 256].astype(F32) + add).astype(BF16)
        return 0

    lax.fori_loop(0, rows // 256, block, 0)


def places():
    me = lax.axis_index("data")
    core = lax.rem(me, 2)
    x_pos = lax.rem(me // 2, 2)
    y_pos = me // 4
    x_peer = me + 2 - 4 * x_pos
    y_peer = me + 4 - 8 * y_pos
    return me, core, y_pos, x_peer, y_peer, x_peer + 4 - 8 * y_pos


def gather_kernel(dims, grad_hbm, master_hbm, one_hbm, two_hbm, tok_hbm,
                  p0, p1, p2, p3, p4, p5, master_out, one_out, two_out, w_in, w_out, hidden_ref,
                  grad_v, master_v, one_v, two_v,
                  part_ref, wide_ref, normed_ref, active_ref,
                  load_sem, part_send, part_recv, send_sem, recv_sem):
    layers, model_dim, hidden_dim, rows, chunks = dims
    in_rows = chunks * LANES // hidden_dim
    out_rows = chunks * LANES // model_dim

    me, core, y_pos, x_peer, y_peer, diag = places()
    partner = me + 1 - 2 * core

    state = ((grad_hbm, grad_v), (master_hbm, master_v), (one_hbm, one_v), (two_hbm, two_v))

    def load(which, layer):
        src, dst = state[which]
        return pltpu.make_async_copy(src.at[:, layer, :], dst.at[layer], load_sem.at[which, layer])

    for layer in range(layers):
        load(0, layer).start()
    tok_load = pltpu.make_async_copy(tok_hbm, hidden_ref, load_sem.at[4, 0])

    barrier = pltpu.get_barrier_semaphore()
    for step in range(1, GROUP):
        pl.semaphore_signal(barrier, inc=1, device_id=(lax.rem(me + step, GROUP),), device_id_type=MESH)

    sums = tuple(jnp.zeros((8, LANES), F32) for _ in range(8))
    for layer in range(layers):
        load(0, layer).wait()
        if layer == layers - 1:
            for item in range(layers):
                for which in range(1, 4):
                    load(which, item).start()
            tok_load.start()

        def square(idx, carry):
            base = pl.multiple_of(idx * 64, 64)
            block = grad_v[layer, pl.ds(base, 64), :]
            return tuple(carry[k] + block[8 * k:8 * k + 8] * block[8 * k:8 * k + 8] for k in range(8))

        sums = lax.fori_loop(0, chunks // 64, square, sums)
    mine = ((sums[0] + sums[1]) + (sums[2] + sums[3])) + ((sums[4] + sums[5]) + (sums[6] + sums[7]))
    part_ref[me] = mine
    pl.semaphore_wait(barrier, GROUP - 1)

    def part_copy(step):
        return pltpu.make_async_remote_copy(
            src_ref=part_ref.at[me], dst_ref=part_ref.at[me],
            send_sem=part_send.at[step], recv_sem=part_recv.at[step],
            device_id=(lax.rem(me + step, GROUP),), device_id_type=MESH)

    def part_arrival(step):
        slot = lax.rem(me + GROUP - step, GROUP)
        return pltpu.make_async_remote_copy(
            src_ref=part_ref.at[slot], dst_ref=part_ref.at[slot],
            send_sem=part_send.at[step], recv_sem=part_recv.at[step],
            device_id=(me,), device_id_type=MESH)

    for step in range(1, GROUP):
        part_copy(step).start()
    for step in range(1, GROUP):
        part_arrival(step).wait_recv()
    total = part_ref[0]
    for slot in range(1, GROUP):
        total = total + part_ref[slot]
    total = jnp.sum(jnp.sum(total, axis=0, keepdims=True), axis=1, keepdims=True)
    clip = jnp.minimum(1.0, CLIP_NORM / jnp.sqrt(total))
    clip = jnp.broadcast_to(clip, (8, LANES))

    slots = {}

    def piece(kind, layer, device, part):
        ref, count = ((w_in, in_rows), (w_out, out_rows))[kind]
        span = count // part[1]
        at = lax.rem(device, 4) * count + part[0] * span
        return ref.at[layer, pl.ds(pl.multiple_of(at, 16), span), :]

    def copies(kind, layer, device, route, target, parts):
        out = []
        for part in parts:
            ref = piece(kind, layer, device, part)
            index = slots.setdefault((route, layer, part), len(slots))
            out.append(pltpu.make_async_remote_copy(
                src_ref=ref, dst_ref=ref, send_sem=send_sem.at[index],
                recv_sem=recv_sem.at[index], device_id=(target,), device_id_type=MESH))
        return out

    def start(items):
        for item in items:
            item.start()

    def arrive(items):
        for item in items:
            item.wait_recv()

    def left(items):
        for item in items:
            item.wait_send()

    def own_parts(layer):
        return ((0, 2), (1, 2))

    def own_x(kind, layer, device, target, parts=None):
        return copies(kind, layer, device, "own_x", target, parts or own_parts(layer))

    def own_y(kind, layer, device, target, parts=None):
        return copies(kind, layer, device, "own_y", target, parts or own_parts(layer))

    def far(kind, layer, half, device, target):
        return copies(kind, layer, device, "far", target, ((half, 2),))

    def pair(kind, layer, device, route, parts):
        return copies(kind, layer, device, route, partner, parts)

    HALVES = ((0, 2), (1, 2))

    def by_kind(function):
        for y_value in range(2):
            @pl.when(y_pos == y_value)
            def _():
                function(y_value)

    one_scale = 1.0 / (1.0 - BETA_ONE ** ADAM_STEP)
    two_scale = 1.0 / (1.0 - BETA_TWO ** ADAM_STEP)

    def adam(layer, part):
        first = part[0] * (chunks // part[1])

        def update(idx, _):
            base = pl.multiple_of(first + idx * 48, 8)
            for k in range(6):
                at = pl.ds(pl.multiple_of(base + 8 * k, 8), 8)
                clipped = grad_v[layer, at, :] * clip
                new_one = BETA_ONE * one_v[layer, at, :] + (1.0 - BETA_ONE) * clipped
                new_two = BETA_TWO * two_v[layer, at, :] + (1.0 - BETA_TWO) * clipped * clipped
                step_size = (new_one * one_scale) / (jnp.sqrt(new_two * two_scale) + ADAM_EPS)
                old = master_v[layer, at, :]
                master_out[layer, at, :] = old - LEARN_RATE * (step_size + WEIGHT_DECAY * old)
                one_out[layer, at, :] = new_one
                two_out[layer, at, :] = new_two
            return 0

        lax.fori_loop(0, chunks // part[1] // 48, update, 0)

    def round_rows(kind, layer, part):
        width = hidden_dim if kind == 0 else model_dim
        count = in_rows if kind == 0 else out_rows
        per_row = width // LANES
        dst = w_in if kind == 0 else w_out
        slot = lax.rem(me, 4)

        def body(idx, _):
            base = part[0] * (chunks // part[1]) + idx * (16 * per_row)
            row = pl.multiple_of(slot * count + part[0] * (count // part[1]) + idx * 16, 16)
            for col in range(per_row):
                top = master_out[layer, pl.ds(base + col, 8, stride=per_row), :]
                low = master_out[layer, pl.ds(base + 8 * per_row + col, 8, stride=per_row), :]
                dst[layer, pl.ds(row, 16), col * LANES:(col + 1) * LANES] = jnp.concatenate([top, low], axis=0).astype(BF16)
            return 0

        lax.fori_loop(0, count // 16 // part[1], body, 0)

    for layer in range(layers):
        for which in range(1, 4):
            load(which, layer).wait()
        for part in own_parts(layer):
            adam(layer, part)

            def send_own(kind):
                round_rows(kind, layer, part)
                start(own_x(kind, layer, me, x_peer, (part,)))
                start(own_y(kind, layer, me, y_peer, (part,)))
                start(pair(kind, layer, me, "pair_own", (part,)))

            by_kind(send_own)

    def pack(kind, device, packed_ref):
        spread_piece(dims, kind, device, (w_in, w_out), wide_ref)

        def squeeze(idx, _):
            at = pl.ds(pl.multiple_of(idx * 256, 256), 256)
            packed_ref[at, :] = wide_ref[at, :].astype(BF16)
            return 0

        lax.fori_loop(0, 4 * chunks // 256, squeeze, 0)

    def partner_of(device):
        return device + 1 - 2 * core

    def pack_own(kind):
        pack(kind, me, p0)
        for layer in range(layers):
            arrive(pair(kind, layer, partner, "pair_own", own_parts(layer)))
        pack(kind, partner, p1)

    by_kind(pack_own)

    for layer in range(layers):
        def forward(kind):
            for at, part in enumerate(own_parts(layer)):
                last = at == len(own_parts(layer)) - 1
                arrive(own_x(kind, layer, x_peer, me, (part,)))
                if at == 0:
                    start(far(kind, layer, 0, x_peer, y_peer))
                start(pair(kind, layer, x_peer, "pair_x", (part,)))
                arrive(own_y(1 - kind, layer, y_peer, me, (part,)))
                if last:
                    start(far(1 - kind, layer, 1, y_peer, x_peer))
                start(pair(1 - kind, layer, y_peer, "pair_y", (part,)))

        by_kind(forward)

    def far_arrive(kind, layer):
        for half in range(2):
            arrive(far(1 - kind, layer, half, diag, me))
            start(pair(1 - kind, layer, diag, "pair_far", ((half, 2),)))

    def far_partner(kind, layer):
        arrive(pair(1 - kind, layer, partner_of(diag), "pair_far", HALVES))

    def stage_zero(kind):
        pack(kind, x_peer, p2)
        pack(1 - kind, y_peer, p4)
        for layer in range(layers):
            arrive(pair(kind, layer, partner_of(x_peer), "pair_x", own_parts(layer)))
            arrive(pair(1 - kind, layer, partner_of(y_peer), "pair_y", own_parts(layer)))
        pack(kind, partner_of(x_peer), p3)
        pack(1 - kind, partner_of(y_peer), p5)
        far_arrive(kind, 0)
        far_partner(kind, 0)

    def stage_one(kind):
        far_arrive(kind, 1)
        far_partner(kind, 1)

    def stage_two(kind):
        far_arrive(kind, 2)
        far_partner(kind, 2)

    by_kind(stage_zero)
    tok_load.wait()
    mlp_block(dims, 0, w_in, w_out, hidden_ref, normed_ref, active_ref)
    by_kind(stage_one)
    mlp_block(dims, 1, w_in, w_out, hidden_ref, normed_ref, active_ref)
    by_kind(stage_two)

    for step in range(1, GROUP):
        part_copy(step).wait_send()

    def drain(kind):
        for layer in range(layers):
            left(own_x(kind, layer, me, x_peer))
            left(own_y(kind, layer, me, y_peer))
            left(pair(kind, layer, me, "pair_own", own_parts(layer)))
            left(pair(kind, layer, x_peer, "pair_x", own_parts(layer)))
            left(pair(1 - kind, layer, y_peer, "pair_y", own_parts(layer)))
            left(pair(1 - kind, layer, diag, "pair_far", HALVES))
            left(far(kind, layer, 0, x_peer, y_peer))
            left(far(1 - kind, layer, 1, y_peer, x_peer))

    by_kind(drain)


def finish_kernel(dims, p0, p1, p2, p3, p4, p5, master_ref, one_ref, two_ref, w_in, w_out, last_ref, tgt_ref,
                  packed_hbm, master_hbm, one_hbm, two_hbm, loss_hbm,
                  loss_ref, far_ref, wide_ref, normed_ref, active_ref, hidden_ref, sem, far_sem):
    layers, model_dim, hidden_dim, rows, chunks = dims
    me, core, y_pos, x_peer, y_peer, diag = places()
    twin = 1 - 2 * core

    copies = []
    for idx, (ref, device) in enumerate(((p0, me), (p1, me + twin), (p2, x_peer), (p3, x_peer + twin), (p4, y_peer), (p5, y_peer + twin))):
        copies.append(pltpu.make_async_copy(ref, packed_hbm.at[pl.ds(device * chunks, chunks)], sem.at[idx]))
    for which, (src, dst) in enumerate(((master_ref, master_hbm), (one_ref, one_hbm), (two_ref, two_hbm))):
        for layer in range(layers):
            copies.append(pltpu.make_async_copy(src.at[layer], dst.at[:, layer, :], sem.at[6 + which * layers + layer]))
    for item in copies:
        item.start()

    far_copies = []
    for idx, device in enumerate((diag, diag + twin)):
        for y_value in range(2):
            @pl.when(y_pos == y_value)
            def _():
                spread_piece(dims, 1 - y_value, device, (w_in, w_out), wide_ref)

        def squeeze(at, _):
            block = wide_ref[pl.ds(pl.multiple_of(at * 128, 128), 128), :].astype(BF16).reshape(32, 4, LANES)
            far_ref[idx, pl.ds(at * 32, 32), :, :] = block[:, :layers, :]
            return 0

        lax.fori_loop(0, 4 * chunks // 128, squeeze, 0)
        far_copies.append(pltpu.make_async_copy(far_ref.at[idx], packed_hbm.at[pl.ds(device * chunks, chunks)], far_sem.at[idx]))
        far_copies[-1].start()

    hidden_ref[...] = last_ref[...]
    mlp_block(dims, layers - 1, w_in, w_out, hidden_ref, normed_ref, active_ref)

    for idx in range(rows // LANES):
        at = slice(idx * LANES, (idx + 1) * LANES)
        error = hidden_ref[at, :].astype(F32) - tgt_ref[at, :].astype(F32)
        error = error * error
        folded = error[:, 0:LANES]
        for col in range(LANES, model_dim, LANES):
            folded = folded + error[:, col:col + LANES]
        loss_ref[idx:idx + 1, :] = jnp.sum(folded.T, axis=0, keepdims=True) * (1.0 / model_dim)

    loss_copy = pltpu.make_async_copy(loss_ref, loss_hbm, far_sem.at[2])
    loss_copy.start()
    for item in copies + far_copies + [loss_copy]:
        item.wait()


def solution(mesh):
    group_size = mesh.shape["data"]
    state_spec = P(None, "data")
    row_spec = P("data", None)

    def local_step(grad_shard, master_shard, one_shard, two_shard, tok_rows, tgt_rows):
        rows, model_dim = tok_rows.shape
        layers, cols = master_shard.shape
        half_size = cols * group_size // 2
        hidden_dim = half_size // model_dim
        chunks = cols // LANES
        dims = (layers, model_dim, hidden_dim, rows, chunks)
        tiled = [a.reshape(layers, chunks, LANES).transpose(1, 0, 2) for a in (grad_shard, master_shard, one_shard, two_shard)]
        state_v = pltpu.VMEM((layers, chunks, LANES), F32)
        hbm = pl.BlockSpec(memory_space=pltpu.HBM)
        vmem = pl.BlockSpec(memory_space=pltpu.VMEM)
        state_out = state_v
        w_in_v = pltpu.VMEM((layers, model_dim, hidden_dim), BF16)
        w_out_v = pltpu.VMEM((layers, hidden_dim, model_dim), BF16)
        hidden_v = pltpu.VMEM((rows, model_dim), BF16)
        wide_v = pltpu.VMEM((4 * chunks, LANES), F32)
        normed_v = pltpu.VMEM((256, model_dim), BF16)
        active_v = pltpu.VMEM((256, hidden_dim), BF16)
        packed_v = pltpu.VMEM((4 * chunks, LANES), BF16)
        gathered = pl.pallas_call(
            functools.partial(gather_kernel, dims),
            name="gather_step",
            out_shape=(*(packed_v,) * 6, state_v, state_v, state_v, w_in_v, w_out_v, hidden_v),
            in_specs=[hbm] * 5,
            out_specs=(vmem,) * 12,
            scratch_shapes=[
                state_v, state_v, state_v, state_v,
                pltpu.VMEM((group_size, 8, LANES), F32),
                wide_v, normed_v, active_v,
                pltpu.SemaphoreType.DMA((5, layers)),
                pltpu.SemaphoreType.DMA((group_size,)),
                pltpu.SemaphoreType.DMA((group_size,)),
                pltpu.SemaphoreType.DMA((96,)),
                pltpu.SemaphoreType.DMA((96,)),
            ],
            compiler_params=pltpu.CompilerParams(collective_id=0, has_side_effects=True, vmem_limit_bytes=19 << 20),
        )(*[pltpu.with_memory_space_constraint(a, pltpu.HBM) for a in (*tiled, tok_rows)])
        gathered = [a.reshape(chunks, 4, LANES)[:, :layers, :] for a in gathered[:6]] + list(gathered[6:])
        state_tile = jax.ShapeDtypeStruct((chunks, layers, LANES), F32)
        weights, new_master, new_one, new_two, row_loss = pl.pallas_call(
            functools.partial(finish_kernel, dims),
            name="finish",
            out_shape=(jax.ShapeDtypeStruct((chunks * group_size, layers, LANES), BF16), state_tile, state_tile, state_tile,
                       jax.ShapeDtypeStruct((rows // LANES, LANES), F32)),
            in_specs=[vmem] * 13,
            out_specs=(hbm,) * 5,
            scratch_shapes=[
                pltpu.VMEM((rows // LANES, LANES), F32),
                pltpu.VMEM((2, chunks, layers, LANES), BF16),
                wide_v, normed_v, active_v, hidden_v,
                pltpu.SemaphoreType.DMA((6 + 3 * layers,)),
                pltpu.SemaphoreType.DMA((3,)),
            ],
            compiler_params=pltpu.CompilerParams(vmem_limit_bytes=14 << 20),
        )(*gathered, tgt_rows)

        def flat(a):
            return a.transpose(1, 0, 2).reshape(layers, a.shape[0] * LANES)

        return row_loss.reshape(rows), flat(weights), flat(new_master), flat(new_one), flat(new_two)

    return jax.shard_map(local_step, mesh=mesh, in_specs=(state_spec, state_spec, state_spec, state_spec, row_spec, row_spec), out_specs=(P("data"), P(), state_spec, state_spec, state_spec), check_vma=False)
```

```python
import functools

import jax
import jax.numpy as jnp
from jax import lax
from jax.experimental import pallas as pl
from jax.experimental.pallas import tpu as pltpu
from jax.sharding import PartitionSpec as P

LEARN_RATE = 0.01
BETA_ONE = 0.9
BETA_TWO = 0.95
ADAM_EPS = 1e-8
WEIGHT_DECAY = 0.1
ADAM_STEP = 10
CLIP_NORM = 1.0
NORM_EPS = 1e-6

MESH = pl.DeviceIdType.MESH
LANES = 128
GROUP = 8
F32 = jnp.float32
BF16 = jnp.bfloat16


def spread_piece(dims, kind, device, weights, wide_ref):
    layers, model_dim, hidden_dim, rows, chunks = dims
    per_row = (hidden_dim if kind == 0 else model_dim) // LANES
    count = chunks // per_row
    src = weights[kind]
    slot = lax.rem(device, 4)

    def spread(idx, _):
        row = pl.multiple_of(slot * count + idx * 16, 16)
        for layer in range(layers):
            for col in range(per_row):
                tile = src[layer, pl.ds(row, 16), col * LANES:(col + 1) * LANES].astype(F32)
                base = layer + 4 * (idx * (16 * per_row) + col)
                wide_ref[pl.ds(base, 8, stride=4 * per_row), :] = tile[0:8]
                wide_ref[pl.ds(base + 32 * per_row, 8, stride=4 * per_row), :] = tile[8:16]
        return 0

    lax.fori_loop(0, count // 16, spread, 0)


def mlp_block(dims, layer, w_in, w_out, hidden_ref, normed_ref, active_ref):
    layers, model_dim, hidden_dim, rows, chunks = dims

    def block(idx, _):
        at = pl.ds(pl.multiple_of(idx * 256, 256), 256)
        hidden = hidden_ref[at, :].astype(F32)
        scale = lax.rsqrt(jnp.mean(hidden * hidden, axis=-1, keepdims=True) + NORM_EPS)
        normed_ref[...] = (hidden * scale).astype(BF16)
        for col in range(0, hidden_dim, 384):
            inner = jnp.dot(normed_ref[...], w_in[layer, :, col:col + 384], preferred_element_type=F32).astype(BF16)
            active_ref[:, col:col + 384] = jax.nn.gelu(inner.astype(F32), approximate=True).astype(BF16)
        for col in range(0, model_dim, 256):
            add = jnp.dot(active_ref[...], w_out[layer, :, col:col + 256], preferred_element_type=F32)
            hidden_ref[at, col:col + 256] = (hidden_ref[at, col:col + 256].astype(F32) + add).astype(BF16)
        return 0

    lax.fori_loop(0, rows // 256, block, 0)


def places():
    me = lax.axis_index("data")
    core = lax.rem(me, 2)
    x_pos = lax.rem(me // 2, 2)
    y_pos = me // 4
    x_peer = me + 2 - 4 * x_pos
    y_peer = me + 4 - 8 * y_pos
    return me, core, y_pos, x_peer, y_peer, x_peer + 4 - 8 * y_pos


def gather_kernel(dims, grad_hbm, master_hbm, one_hbm, two_hbm, tok_hbm,
                  p0, p1, p2, p3, p4, p5, master_out, one_out, two_out, w_in, w_out, hidden_ref,
                  grad_v, master_v, one_v, two_v,
                  part_ref, wide_ref, normed_ref, active_ref,
                  load_sem, part_send, part_recv, send_sem, recv_sem):
    layers, model_dim, hidden_dim, rows, chunks = dims
    in_rows = chunks * LANES // hidden_dim
    out_rows = chunks * LANES // model_dim

    me, core, y_pos, x_peer, y_peer, diag = places()
    partner = me + 1 - 2 * core

    state = ((grad_hbm, grad_v), (master_hbm, master_v), (one_hbm, one_v), (two_hbm, two_v))

    def load(which, layer):
        src, dst = state[which]
        return pltpu.make_async_copy(src.at[:, layer, :], dst.at[layer], load_sem.at[which, layer])

    for layer in range(layers):
        load(0, layer).start()
    tok_load = pltpu.make_async_copy(tok_hbm, hidden_ref, load_sem.at[4, 0])

    barrier = pltpu.get_barrier_semaphore()
    for step in range(1, GROUP):
        pl.semaphore_signal(barrier, inc=1, device_id=(lax.rem(me + step, GROUP),), device_id_type=MESH)

    sums = tuple(jnp.zeros((8, LANES), F32) for _ in range(8))
    for layer in range(layers):
        load(0, layer).wait()
        if layer == layers - 1:
            for item in range(layers):
                for which in range(1, 4):
                    load(which, item).start()
            tok_load.start()

        def square(idx, carry):
            base = pl.multiple_of(idx * 64, 64)
            block = grad_v[layer, pl.ds(base, 64), :]
            return tuple(carry[k] + block[8 * k:8 * k + 8] * block[8 * k:8 * k + 8] for k in range(8))

        sums = lax.fori_loop(0, chunks // 64, square, sums)
    mine = ((sums[0] + sums[1]) + (sums[2] + sums[3])) + ((sums[4] + sums[5]) + (sums[6] + sums[7]))
    part_ref[me] = mine
    pl.semaphore_wait(barrier, GROUP - 1)

    def part_copy(step):
        return pltpu.make_async_remote_copy(
            src_ref=part_ref.at[me], dst_ref=part_ref.at[me],
            send_sem=part_send.at[step], recv_sem=part_recv.at[step],
            device_id=(lax.rem(me + step, GROUP),), device_id_type=MESH)

    def part_arrival(step):
        slot = lax.rem(me + GROUP - step, GROUP)
        return pltpu.make_async_remote_copy(
            src_ref=part_ref.at[slot], dst_ref=part_ref.at[slot],
            send_sem=part_send.at[step], recv_sem=part_recv.at[step],
            device_id=(me,), device_id_type=MESH)

    for step in range(1, GROUP):
        part_copy(step).start()
    for step in range(1, GROUP):
        part_arrival(step).wait_recv()
    total = part_ref[0]
    for slot in range(1, GROUP):
        total = total + part_ref[slot]
    total = jnp.sum(jnp.sum(total, axis=0, keepdims=True), axis=1, keepdims=True)
    clip = jnp.minimum(1.0, CLIP_NORM / jnp.sqrt(total))
    clip = jnp.broadcast_to(clip, (8, LANES))

    slots = {}

    def piece(kind, layer, device, part):
        ref, count = ((w_in, in_rows), (w_out, out_rows))[kind]
        span = count // part[1]
        at = lax.rem(device, 4) * count + part[0] * span
        return ref.at[layer, pl.ds(pl.multiple_of(at, 16), span), :]

    def copies(kind, layer, device, route, target, parts):
        out = []
        for part in parts:
            ref = piece(kind, layer, device, part)
            index = slots.setdefault((route, layer, part), len(slots))
            out.append(pltpu.make_async_remote_copy(
                src_ref=ref, dst_ref=ref, send_sem=send_sem.at[index],
                recv_sem=recv_sem.at[index], device_id=(target,), device_id_type=MESH))
        return out

    def start(items):
        for item in items:
            item.start()

    def arrive(items):
        for item in items:
            item.wait_recv()

    def left(items):
        for item in items:
            item.wait_send()

    def own_parts(layer):
        return ((0, 6), (1, 6), (2, 6), (1, 2)) if layer == 0 else ((0, 2), (1, 2))

    def far_parts(layer, half):
        return tuple((3 * half + at, 6) for at in range(3)) if layer == layers - 1 else ((half, 2),)

    def own_x(kind, layer, device, target, parts=None):
        return copies(kind, layer, device, "own_x", target, parts or own_parts(layer))

    def own_y(kind, layer, device, target, parts=None):
        return copies(kind, layer, device, "own_y", target, parts or own_parts(layer))

    def far(kind, layer, half, device, target, parts=None):
        return copies(kind, layer, device, "far", target, parts or far_parts(layer, half))

    def pair(kind, layer, device, route, parts):
        return copies(kind, layer, device, route, partner, parts)

    def by_kind(function):
        for y_value in range(2):
            @pl.when(y_pos == y_value)
            def _():
                function(y_value)

    one_scale = 1.0 / (1.0 - BETA_ONE ** ADAM_STEP)
    two_scale = 1.0 / (1.0 - BETA_TWO ** ADAM_STEP)

    def adam(layer, part):
        first = part[0] * (chunks // part[1])

        def update(idx, _):
            base = pl.multiple_of(first + idx * 48, 8)
            for k in range(6):
                at = pl.ds(pl.multiple_of(base + 8 * k, 8), 8)
                clipped = grad_v[layer, at, :] * clip
                new_one = BETA_ONE * one_v[layer, at, :] + (1.0 - BETA_ONE) * clipped
                new_two = BETA_TWO * two_v[layer, at, :] + (1.0 - BETA_TWO) * clipped * clipped
                step_size = (new_one * one_scale) / (jnp.sqrt(new_two * two_scale) + ADAM_EPS)
                old = master_v[layer, at, :]
                master_out[layer, at, :] = old - LEARN_RATE * (step_size + WEIGHT_DECAY * old)
                one_out[layer, at, :] = new_one
                two_out[layer, at, :] = new_two
            return 0

        lax.fori_loop(0, chunks // part[1] // 48, update, 0)

    def round_rows(kind, layer, part):
        width = hidden_dim if kind == 0 else model_dim
        count = in_rows if kind == 0 else out_rows
        per_row = width // LANES
        dst = w_in if kind == 0 else w_out
        slot = lax.rem(me, 4)

        def body(idx, _):
            base = part[0] * (chunks // part[1]) + idx * (16 * per_row)
            row = pl.multiple_of(slot * count + part[0] * (count // part[1]) + idx * 16, 16)
            for col in range(per_row):
                top = master_out[layer, pl.ds(base + col, 8, stride=per_row), :]
                low = master_out[layer, pl.ds(base + 8 * per_row + col, 8, stride=per_row), :]
                dst[layer, pl.ds(row, 16), col * LANES:(col + 1) * LANES] = jnp.concatenate([top, low], axis=0).astype(BF16)
            return 0

        lax.fori_loop(0, count // 16 // part[1], body, 0)

    for layer in range(layers):
        for which in range(1, 4):
            load(which, layer).wait()
        for part in own_parts(layer):
            adam(layer, part)

            def send_own(kind):
                round_rows(kind, layer, part)
                if layer < layers - 1:
                    start(own_x(kind, layer, me, x_peer, (part,)))
                    start(own_y(kind, layer, me, y_peer, (part,)))
                start(pair(kind, layer, me, "pair_own", (part,)))

            by_kind(send_own)

    def pack(kind, device, packed_ref):
        spread_piece(dims, kind, device, (w_in, w_out), wide_ref)

        def squeeze(idx, _):
            at = pl.ds(pl.multiple_of(idx * 256, 256), 256)
            packed_ref[at, :] = wide_ref[at, :].astype(BF16)
            return 0

        lax.fori_loop(0, 4 * chunks // 256, squeeze, 0)

    def partner_of(device):
        return device + 1 - 2 * core

    def forward(kind, layer):
        x_order = own_parts(layer)
        y_order = x_order[::-1] if layer == layers - 1 else x_order
        for x_part, y_part in zip(x_order, y_order):
            arrive(own_x(kind, layer, x_peer, me, (x_part,)))
            if x_part in ((0, 2), (2, 6)):
                start(far(kind, layer, 0, x_peer, y_peer))
            start(pair(kind, layer, x_peer, "pair_x", (x_part,)))
            arrive(own_y(1 - kind, layer, y_peer, me, (y_part,)))
            if y_part == (1, 2):
                start(far(1 - kind, layer, 1, y_peer, x_peer))
            start(pair(1 - kind, layer, y_peer, "pair_y", (y_part,)))

    def far_arrive(kind, layer):
        for parts in zip(far_parts(layer, 0), far_parts(layer, 1)):
            for half in range(2):
                arrive(far(1 - kind, layer, half, diag, me, (parts[half],)))
                start(pair(1 - kind, layer, diag, "pair_far", (parts[half],)))

    def far_partner(kind, layer):
        arrive(pair(1 - kind, layer, partner_of(diag), "pair_far", far_parts(layer, 0) + far_parts(layer, 1)))

    def near_partner(kind, layer):
        arrive(pair(kind, layer, partner_of(x_peer), "pair_x", own_parts(layer)))
        arrive(pair(1 - kind, layer, partner_of(y_peer), "pair_y", own_parts(layer)))

    def stage_own(kind):
        pack(kind, me, p0)
        forward(kind, 0)
        for layer in range(layers):
            arrive(pair(kind, layer, partner, "pair_own", own_parts(layer)))
        pack(kind, partner, p1)
        forward(kind, 1)
        start(own_x(kind, layers - 1, me, x_peer))
        start(own_y(kind, layers - 1, me, y_peer)[::-1])
        near_partner(kind, 0)
        far_arrive(kind, 0)
        near_partner(kind, 1)
        far_partner(kind, 0)

    def stage_one(kind):
        far_arrive(kind, 1)
        far_partner(kind, 1)

    def stage_two(kind):
        forward(kind, 2)
        pack(kind, x_peer, p2)
        pack(1 - kind, y_peer, p4)
        near_partner(kind, 2)
        pack(kind, partner_of(x_peer), p3)
        pack(1 - kind, partner_of(y_peer), p5)
        far_arrive(kind, 2)
        far_partner(kind, 2)

    by_kind(stage_own)
    tok_load.wait()
    mlp_block(dims, 0, w_in, w_out, hidden_ref, normed_ref, active_ref)
    by_kind(stage_one)
    mlp_block(dims, 1, w_in, w_out, hidden_ref, normed_ref, active_ref)
    by_kind(stage_two)

    for step in range(1, GROUP):
        part_copy(step).wait_send()

    def drain(kind):
        for layer in range(layers):
            left(own_x(kind, layer, me, x_peer))
            left(own_y(kind, layer, me, y_peer))
            left(pair(kind, layer, me, "pair_own", own_parts(layer)))
            left(pair(kind, layer, x_peer, "pair_x", own_parts(layer)))
            left(pair(1 - kind, layer, y_peer, "pair_y", own_parts(layer)))
            left(pair(1 - kind, layer, diag, "pair_far", far_parts(layer, 0) + far_parts(layer, 1)))
            left(far(kind, layer, 0, x_peer, y_peer))
            left(far(1 - kind, layer, 1, y_peer, x_peer))

    by_kind(drain)


def finish_kernel(dims, p0, p1, p2, p3, p4, p5, master_ref, one_ref, two_ref, w_in, w_out, last_ref, tgt_ref,
                  packed_hbm, master_hbm, one_hbm, two_hbm, loss_hbm,
                  loss_ref, far_ref, wide_ref, normed_ref, active_ref, hidden_ref, sem, far_sem):
    layers, model_dim, hidden_dim, rows, chunks = dims
    me, core, y_pos, x_peer, y_peer, diag = places()
    twin = 1 - 2 * core

    copies = []
    for idx, (ref, device) in enumerate(((p0, me), (p1, me + twin), (p2, x_peer), (p3, x_peer + twin), (p4, y_peer), (p5, y_peer + twin))):
        copies.append(pltpu.make_async_copy(ref, packed_hbm.at[pl.ds(device * chunks, chunks)], sem.at[idx]))
    for which, (src, dst) in enumerate(((master_ref, master_hbm), (one_ref, one_hbm), (two_ref, two_hbm))):
        for layer in range(layers):
            copies.append(pltpu.make_async_copy(src.at[layer], dst.at[:, layer, :], sem.at[6 + which * layers + layer]))
    for item in copies:
        item.start()

    far_copies = []
    for idx, device in enumerate((diag, diag + twin)):
        for y_value in range(2):
            @pl.when(y_pos == y_value)
            def _():
                spread_piece(dims, 1 - y_value, device, (w_in, w_out), wide_ref)

        def squeeze(at, _):
            block = wide_ref[pl.ds(pl.multiple_of(at * 128, 128), 128), :].astype(BF16).reshape(32, 4, LANES)
            far_ref[idx, pl.ds(at * 32, 32), :, :] = block[:, :layers, :]
            return 0

        lax.fori_loop(0, 4 * chunks // 128, squeeze, 0)
        far_copies.append(pltpu.make_async_copy(far_ref.at[idx], packed_hbm.at[pl.ds(device * chunks, chunks)], far_sem.at[idx]))
        far_copies[-1].start()

    hidden_ref[...] = last_ref[...]
    mlp_block(dims, layers - 1, w_in, w_out, hidden_ref, normed_ref, active_ref)

    for idx in range(rows // LANES):
        at = slice(idx * LANES, (idx + 1) * LANES)
        error = hidden_ref[at, :].astype(F32) - tgt_ref[at, :].astype(F32)
        error = error * error
        folded = error[:, 0:LANES]
        for col in range(LANES, model_dim, LANES):
            folded = folded + error[:, col:col + LANES]
        loss_ref[idx:idx + 1, :] = jnp.sum(folded.T, axis=0, keepdims=True) * (1.0 / model_dim)

    loss_copy = pltpu.make_async_copy(loss_ref, loss_hbm, far_sem.at[2])
    loss_copy.start()
    for item in copies + far_copies + [loss_copy]:
        item.wait()


def solution(mesh):
    group_size = mesh.shape["data"]
    state_spec = P(None, "data")
    row_spec = P("data", None)

    def local_step(grad_shard, master_shard, one_shard, two_shard, tok_rows, tgt_rows):
        rows, model_dim = tok_rows.shape
        layers, cols = master_shard.shape
        half_size = cols * group_size // 2
        hidden_dim = half_size // model_dim
        chunks = cols // LANES
        dims = (layers, model_dim, hidden_dim, rows, chunks)
        tiled = [a.reshape(layers, chunks, LANES).transpose(1, 0, 2) for a in (grad_shard, master_shard, one_shard, two_shard)]
        state_v = pltpu.VMEM((layers, chunks, LANES), F32)
        hbm = pl.BlockSpec(memory_space=pltpu.HBM)
        vmem = pl.BlockSpec(memory_space=pltpu.VMEM)
        state_out = state_v
        w_in_v = pltpu.VMEM((layers, model_dim, hidden_dim), BF16)
        w_out_v = pltpu.VMEM((layers, hidden_dim, model_dim), BF16)
        hidden_v = pltpu.VMEM((rows, model_dim), BF16)
        wide_v = pltpu.VMEM((4 * chunks, LANES), F32)
        normed_v = pltpu.VMEM((256, model_dim), BF16)
        active_v = pltpu.VMEM((256, hidden_dim), BF16)
        packed_v = pltpu.VMEM((4 * chunks, LANES), BF16)
        gathered = pl.pallas_call(
            functools.partial(gather_kernel, dims),
            name="gather_step",
            out_shape=(*(packed_v,) * 6, state_v, state_v, state_v, w_in_v, w_out_v, hidden_v),
            in_specs=[hbm] * 5,
            out_specs=(vmem,) * 12,
            scratch_shapes=[
                state_v, state_v, state_v, state_v,
                pltpu.VMEM((group_size, 8, LANES), F32),
                wide_v, normed_v, active_v,
                pltpu.SemaphoreType.DMA((5, layers)),
                pltpu.SemaphoreType.DMA((group_size,)),
                pltpu.SemaphoreType.DMA((group_size,)),
                pltpu.SemaphoreType.DMA((96,)),
                pltpu.SemaphoreType.DMA((96,)),
            ],
            compiler_params=pltpu.CompilerParams(collective_id=0, has_side_effects=True, vmem_limit_bytes=19 << 20),
        )(*[pltpu.with_memory_space_constraint(a, pltpu.HBM) for a in (*tiled, tok_rows)])
        gathered = [a.reshape(chunks, 4, LANES)[:, :layers, :] for a in gathered[:6]] + list(gathered[6:])
        state_tile = jax.ShapeDtypeStruct((chunks, layers, LANES), F32)
        weights, new_master, new_one, new_two, row_loss = pl.pallas_call(
            functools.partial(finish_kernel, dims),
            name="finish",
            out_shape=(jax.ShapeDtypeStruct((chunks * group_size, layers, LANES), BF16), state_tile, state_tile, state_tile,
                       jax.ShapeDtypeStruct((rows // LANES, LANES), F32)),
            in_specs=[vmem] * 13,
            out_specs=(hbm,) * 5,
            scratch_shapes=[
                pltpu.VMEM((rows // LANES, LANES), F32),
                pltpu.VMEM((2, chunks, layers, LANES), BF16),
                wide_v, normed_v, active_v, hidden_v,
                pltpu.SemaphoreType.DMA((6 + 3 * layers,)),
                pltpu.SemaphoreType.DMA((3,)),
            ],
            compiler_params=pltpu.CompilerParams(vmem_limit_bytes=14 << 20),
        )(*gathered, tgt_rows)

        def flat(a):
            return a.transpose(1, 0, 2).reshape(layers, a.shape[0] * LANES)

        return row_loss.reshape(rows), flat(weights), flat(new_master), flat(new_one), flat(new_two)

    return jax.shard_map(local_step, mesh=mesh, in_specs=(state_spec, state_spec, state_spec, state_spec, row_spec, row_spec), out_specs=(P("data"), P(), state_spec, state_spec, state_spec), check_vma=False)
```

```python
import functools

import jax
import jax.numpy as jnp
from jax import lax
from jax.experimental import pallas as pl
from jax.experimental.pallas import tpu as pltpu
from jax.sharding import PartitionSpec as P

LEARN_RATE = 0.01
BETA_ONE = 0.9
BETA_TWO = 0.95
ADAM_EPS = 1e-8
WEIGHT_DECAY = 0.1
ADAM_STEP = 10
CLIP_NORM = 1.0
NORM_EPS = 1e-6

MESH = pl.DeviceIdType.MESH
LANES = 128
GROUP = 8
F32 = jnp.float32
BF16 = jnp.bfloat16


def spread_piece(dims, kind, device, weights, wide_ref):
    layers, model_dim, hidden_dim, rows, chunks = dims
    per_row = (hidden_dim if kind == 0 else model_dim) // LANES
    count = chunks // per_row
    src = weights[kind]
    slot = lax.rem(device, 4)

    def spread(idx, _):
        row = pl.multiple_of(slot * count + idx * 16, 16)
        for layer in range(layers):
            for col in range(per_row):
                tile = src[layer, pl.ds(row, 16), col * LANES:(col + 1) * LANES].astype(F32)
                base = layer + 4 * (idx * (16 * per_row) + col)
                wide_ref[pl.ds(base, 8, stride=4 * per_row), :] = tile[0:8]
                wide_ref[pl.ds(base + 32 * per_row, 8, stride=4 * per_row), :] = tile[8:16]
        return 0

    lax.fori_loop(0, count // 16, spread, 0)


def mlp_block(dims, layer, w_in, w_out, hidden_ref, normed_ref, active_ref):
    layers, model_dim, hidden_dim, rows, chunks = dims

    def block(idx, _):
        at = pl.ds(pl.multiple_of(idx * 256, 256), 256)
        hidden = hidden_ref[at, :].astype(F32)
        scale = lax.rsqrt(jnp.mean(hidden * hidden, axis=-1, keepdims=True) + NORM_EPS)
        normed_ref[...] = (hidden * scale).astype(BF16)
        for col in range(0, hidden_dim, 384):
            inner = jnp.dot(normed_ref[...], w_in[layer, :, col:col + 384], preferred_element_type=F32).astype(BF16)
            active_ref[:, col:col + 384] = jax.nn.gelu(inner.astype(F32), approximate=True).astype(BF16)
        for col in range(0, model_dim, 256):
            add = jnp.dot(active_ref[...], w_out[layer, :, col:col + 256], preferred_element_type=F32)
            hidden_ref[at, col:col + 256] = (hidden_ref[at, col:col + 256].astype(F32) + add).astype(BF16)
        return 0

    lax.fori_loop(0, rows // 256, block, 0)


def places():
    me = lax.axis_index("data")
    core = lax.rem(me, 2)
    x_pos = lax.rem(me // 2, 2)
    y_pos = me // 4
    x_peer = me + 2 - 4 * x_pos
    y_peer = me + 4 - 8 * y_pos
    return me, core, y_pos, x_peer, y_peer, x_peer + 4 - 8 * y_pos


def gather_kernel(dims, grad_hbm, master_hbm, one_hbm, two_hbm, tok_hbm,
                  p0, p1, p2, p3, p4, p5, master_out, one_out, two_out, w_in, w_out, hidden_ref,
                  grad_v, master_v, one_v, two_v,
                  part_ref, wide_ref, normed_ref, active_ref,
                  load_sem, part_send, part_recv, send_sem, recv_sem):
    layers, model_dim, hidden_dim, rows, chunks = dims
    in_rows = chunks * LANES // hidden_dim
    out_rows = chunks * LANES // model_dim

    me, core, y_pos, x_peer, y_peer, diag = places()
    partner = me + 1 - 2 * core

    state = ((grad_hbm, grad_v), (master_hbm, master_v), (one_hbm, one_v), (two_hbm, two_v))

    def load(which, layer):
        src, dst = state[which]
        return pltpu.make_async_copy(src.at[:, layer, :], dst.at[layer], load_sem.at[which, layer])

    for layer in range(layers):
        load(0, layer).start()
    tok_load = pltpu.make_async_copy(tok_hbm, hidden_ref, load_sem.at[4, 0])

    barrier = pltpu.get_barrier_semaphore()
    for step in range(1, GROUP):
        pl.semaphore_signal(barrier, inc=1, device_id=(lax.rem(me + step, GROUP),), device_id_type=MESH)

    sums = tuple(jnp.zeros((8, LANES), F32) for _ in range(8))
    for layer in range(layers):
        load(0, layer).wait()
        if layer == layers - 1:
            for which in range(1, 4):
                load(which, 0).start()

        def square(idx, carry):
            base = pl.multiple_of(idx * 64, 64)
            block = grad_v[layer, pl.ds(base, 64), :]
            return tuple(carry[k] + block[8 * k:8 * k + 8] * block[8 * k:8 * k + 8] for k in range(8))

        sums = lax.fori_loop(0, chunks // 64, square, sums)
    mine = ((sums[0] + sums[1]) + (sums[2] + sums[3])) + ((sums[4] + sums[5]) + (sums[6] + sums[7]))
    part_ref[me] = mine
    pl.semaphore_wait(barrier, GROUP - 1)

    def part_copy(step):
        return pltpu.make_async_remote_copy(
            src_ref=part_ref.at[me], dst_ref=part_ref.at[me],
            send_sem=part_send.at[step], recv_sem=part_recv.at[step],
            device_id=(lax.rem(me + step, GROUP),), device_id_type=MESH)

    def part_arrival(step):
        slot = lax.rem(me + GROUP - step, GROUP)
        return pltpu.make_async_remote_copy(
            src_ref=part_ref.at[slot], dst_ref=part_ref.at[slot],
            send_sem=part_send.at[step], recv_sem=part_recv.at[step],
            device_id=(me,), device_id_type=MESH)

    for step in range(1, GROUP):
        part_copy(step).start()
    for item in range(1, layers):
        for which in range(1, 4):
            load(which, item).start()
    tok_load.start()
    for step in range(1, GROUP):
        part_arrival(step).wait_recv()
    total = part_ref[0]
    for slot in range(1, GROUP):
        total = total + part_ref[slot]
    total = jnp.sum(jnp.sum(total, axis=0, keepdims=True), axis=1, keepdims=True)
    clip = jnp.minimum(1.0, CLIP_NORM / jnp.sqrt(total))
    clip = jnp.broadcast_to(clip, (8, LANES))

    slots = {}

    def piece(kind, layer, device, part):
        ref, count = ((w_in, in_rows), (w_out, out_rows))[kind]
        span = count // part[1]
        at = lax.rem(device, 4) * count + part[0] * span
        return ref.at[layer, pl.ds(pl.multiple_of(at, 16), span), :]

    def copies(kind, layer, device, route, target, parts):
        out = []
        for part in parts:
            ref = piece(kind, layer, device, part)
            index = slots.setdefault((route, layer, part), len(slots))
            out.append(pltpu.make_async_remote_copy(
                src_ref=ref, dst_ref=ref, send_sem=send_sem.at[index],
                recv_sem=recv_sem.at[index], device_id=(target,), device_id_type=MESH))
        return out

    def start(items):
        for item in items:
            item.start()

    def arrive(items):
        for item in items:
            item.wait_recv()

    def left(items):
        for item in items:
            item.wait_send()

    def own_parts(layer):
        return ((0, 6), (1, 6), (2, 6), (1, 2)) if layer == 0 else ((0, 2), (1, 2))

    def far_parts(layer, half):
        return tuple((3 * half + at, 6) for at in range(3)) if layer == layers - 1 else ((half, 2),)

    def own_x(kind, layer, device, target, parts=None):
        return copies(kind, layer, device, "own_x", target, parts or own_parts(layer))

    def own_y(kind, layer, device, target, parts=None):
        return copies(kind, layer, device, "own_y", target, parts or own_parts(layer))

    def far(kind, layer, half, device, target, parts=None):
        return copies(kind, layer, device, "far", target, parts or far_parts(layer, half))

    def pair(kind, layer, device, route, parts):
        return copies(kind, layer, device, route, partner, parts)

    def by_kind(function):
        for y_value in range(2):
            @pl.when(y_pos == y_value)
            def _():
                function(y_value)

    one_scale = 1.0 / (1.0 - BETA_ONE ** ADAM_STEP)
    two_scale = 1.0 / (1.0 - BETA_TWO ** ADAM_STEP)

    def adam(layer, part):
        first = part[0] * (chunks // part[1])

        def update(idx, _):
            base = pl.multiple_of(first + idx * 48, 8)
            for k in range(6):
                at = pl.ds(pl.multiple_of(base + 8 * k, 8), 8)
                clipped = grad_v[layer, at, :] * clip
                new_one = BETA_ONE * one_v[layer, at, :] + (1.0 - BETA_ONE) * clipped
                new_two = BETA_TWO * two_v[layer, at, :] + (1.0 - BETA_TWO) * clipped * clipped
                step_size = (new_one * one_scale) / (jnp.sqrt(new_two * two_scale) + ADAM_EPS)
                old = master_v[layer, at, :]
                master_out[layer, at, :] = old - LEARN_RATE * (step_size + WEIGHT_DECAY * old)
                one_out[layer, at, :] = new_one
                two_out[layer, at, :] = new_two
            return 0

        lax.fori_loop(0, chunks // part[1] // 48, update, 0)

    def round_rows(kind, layer, part):
        width = hidden_dim if kind == 0 else model_dim
        count = in_rows if kind == 0 else out_rows
        per_row = width // LANES
        dst = w_in if kind == 0 else w_out
        slot = lax.rem(me, 4)

        def body(idx, _):
            base = part[0] * (chunks // part[1]) + idx * (16 * per_row)
            row = pl.multiple_of(slot * count + part[0] * (count // part[1]) + idx * 16, 16)
            for col in range(per_row):
                top = master_out[layer, pl.ds(base + col, 8, stride=per_row), :]
                low = master_out[layer, pl.ds(base + 8 * per_row + col, 8, stride=per_row), :]
                dst[layer, pl.ds(row, 16), col * LANES:(col + 1) * LANES] = jnp.concatenate([top, low], axis=0).astype(BF16)
            return 0

        lax.fori_loop(0, count // 16 // part[1], body, 0)

    for layer in range(layers):
        for which in range(1, 4):
            load(which, layer).wait()
        for part in own_parts(layer):
            adam(layer, part)

            def send_own(kind):
                round_rows(kind, layer, part)
                if layer < layers - 1:
                    start(own_x(kind, layer, me, x_peer, (part,)))
                    start(own_y(kind, layer, me, y_peer, (part,)))
                start(pair(kind, layer, me, "pair_own", (part,)))

            by_kind(send_own)

    def pack(kind, device, packed_ref):
        spread_piece(dims, kind, device, (w_in, w_out), wide_ref)

        def squeeze(idx, _):
            at = pl.ds(pl.multiple_of(idx * 256, 256), 256)
            packed_ref[at, :] = wide_ref[at, :].astype(BF16)
            return 0

        lax.fori_loop(0, 4 * chunks // 256, squeeze, 0)

    def partner_of(device):
        return device + 1 - 2 * core

    def forward(kind, layer):
        x_order = own_parts(layer)
        y_order = x_order[::-1] if layer == layers - 1 else x_order
        for x_part, y_part in zip(x_order, y_order):
            arrive(own_x(kind, layer, x_peer, me, (x_part,)))
            if x_part in ((0, 2), (2, 6)):
                start(far(kind, layer, 0, x_peer, y_peer))
            start(pair(kind, layer, x_peer, "pair_x", (x_part,)))
            arrive(own_y(1 - kind, layer, y_peer, me, (y_part,)))
            if y_part == (1, 2):
                start(far(1 - kind, layer, 1, y_peer, x_peer))
            start(pair(1 - kind, layer, y_peer, "pair_y", (y_part,)))

    def far_arrive(kind, layer, only=None):
        for idx, parts in enumerate(zip(far_parts(layer, 0), far_parts(layer, 1))):
            if only is not None and idx != only:
                continue
            for half in range(2):
                arrive(far(1 - kind, layer, half, diag, me, (parts[half],)))
                start(pair(1 - kind, layer, diag, "pair_far", (parts[half],)))

    def far_partner(kind, layer):
        arrive(pair(1 - kind, layer, partner_of(diag), "pair_far", far_parts(layer, 0) + far_parts(layer, 1)))

    def near_partner(kind, layer):
        arrive(pair(kind, layer, partner_of(x_peer), "pair_x", own_parts(layer)))
        arrive(pair(1 - kind, layer, partner_of(y_peer), "pair_y", own_parts(layer)))

    def stage_own(kind):
        pack(kind, me, p0)
        forward(kind, 0)
        for layer in range(layers):
            arrive(pair(kind, layer, partner, "pair_own", own_parts(layer)))
        pack(kind, partner, p1)
        forward(kind, 1)
        start(own_x(kind, layers - 1, me, x_peer))
        start(own_y(kind, layers - 1, me, y_peer)[::-1])
        near_partner(kind, 0)
        far_arrive(kind, 0)
        near_partner(kind, 1)
        far_partner(kind, 0)

    def stage_one(kind):
        far_arrive(kind, 1)
        far_partner(kind, 1)

    def stage_two(kind):
        forward(kind, 2)
        pack(kind, x_peer, p2)
        pack(1 - kind, y_peer, p4)
        near_partner(kind, 2)
        far_arrive(kind, 2, 0)
        pack(kind, partner_of(x_peer), p3)
        far_arrive(kind, 2, 1)
        pack(1 - kind, partner_of(y_peer), p5)
        far_arrive(kind, 2, 2)
        far_partner(kind, 2)

    by_kind(stage_own)
    tok_load.wait()
    mlp_block(dims, 0, w_in, w_out, hidden_ref, normed_ref, active_ref)
    by_kind(stage_one)
    mlp_block(dims, 1, w_in, w_out, hidden_ref, normed_ref, active_ref)
    by_kind(stage_two)

    for step in range(1, GROUP):
        part_copy(step).wait_send()

    def drain(kind):
        for layer in range(layers):
            left(own_x(kind, layer, me, x_peer))
            left(own_y(kind, layer, me, y_peer))
            left(pair(kind, layer, me, "pair_own", own_parts(layer)))
            left(pair(kind, layer, x_peer, "pair_x", own_parts(layer)))
            left(pair(1 - kind, layer, y_peer, "pair_y", own_parts(layer)))
            left(pair(1 - kind, layer, diag, "pair_far", far_parts(layer, 0) + far_parts(layer, 1)))
            left(far(kind, layer, 0, x_peer, y_peer))
            left(far(1 - kind, layer, 1, y_peer, x_peer))

    by_kind(drain)


def finish_kernel(dims, p0, p1, p2, p3, p4, p5, master_ref, one_ref, two_ref, w_in, w_out, last_ref, tgt_ref,
                  packed_hbm, master_hbm, one_hbm, two_hbm, loss_hbm,
                  loss_ref, far_ref, wide_ref, normed_ref, active_ref, hidden_ref, sem, far_sem):
    layers, model_dim, hidden_dim, rows, chunks = dims
    me, core, y_pos, x_peer, y_peer, diag = places()
    twin = 1 - 2 * core

    copies = []
    for idx, (ref, device) in enumerate(((p0, me), (p1, me + twin), (p2, x_peer), (p3, x_peer + twin), (p4, y_peer), (p5, y_peer + twin))):
        copies.append(pltpu.make_async_copy(ref, packed_hbm.at[pl.ds(device * chunks, chunks)], sem.at[idx]))
    for which, (src, dst) in enumerate(((master_ref, master_hbm), (one_ref, one_hbm), (two_ref, two_hbm))):
        for layer in range(layers):
            copies.append(pltpu.make_async_copy(src.at[layer], dst.at[:, layer, :], sem.at[6 + which * layers + layer]))
    for item in copies:
        item.start()

    far_copies = []
    for idx, device in enumerate((diag, diag + twin)):
        for y_value in range(2):
            @pl.when(y_pos == y_value)
            def _():
                spread_piece(dims, 1 - y_value, device, (w_in, w_out), wide_ref)

        def squeeze(at, _):
            block = wide_ref[pl.ds(pl.multiple_of(at * 128, 128), 128), :].astype(BF16).reshape(32, 4, LANES)
            far_ref[idx, pl.ds(at * 32, 32), :, :] = block[:, :layers, :]
            return 0

        lax.fori_loop(0, 4 * chunks // 128, squeeze, 0)
        far_copies.append(pltpu.make_async_copy(far_ref.at[idx], packed_hbm.at[pl.ds(device * chunks, chunks)], far_sem.at[idx]))
        far_copies[-1].start()

    hidden_ref[...] = last_ref[...]
    mlp_block(dims, layers - 1, w_in, w_out, hidden_ref, normed_ref, active_ref)

    for idx in range(rows // LANES):
        at = slice(idx * LANES, (idx + 1) * LANES)
        error = hidden_ref[at, :].astype(F32) - tgt_ref[at, :].astype(F32)
        error = error * error
        folded = error[:, 0:LANES]
        for col in range(LANES, model_dim, LANES):
            folded = folded + error[:, col:col + LANES]
        loss_ref[idx:idx + 1, :] = jnp.sum(folded.T, axis=0, keepdims=True) * (1.0 / model_dim)

    loss_copy = pltpu.make_async_copy(loss_ref, loss_hbm, far_sem.at[2])
    loss_copy.start()
    for item in copies + far_copies + [loss_copy]:
        item.wait()


def solution(mesh):
    group_size = mesh.shape["data"]
    state_spec = P(None, "data")
    row_spec = P("data", None)

    def local_step(grad_shard, master_shard, one_shard, two_shard, tok_rows, tgt_rows):
        rows, model_dim = tok_rows.shape
        layers, cols = master_shard.shape
        half_size = cols * group_size // 2
        hidden_dim = half_size // model_dim
        chunks = cols // LANES
        dims = (layers, model_dim, hidden_dim, rows, chunks)
        tiled = [a.reshape(layers, chunks, LANES).transpose(1, 0, 2) for a in (grad_shard, master_shard, one_shard, two_shard)]
        state_v = pltpu.VMEM((layers, chunks, LANES), F32)
        hbm = pl.BlockSpec(memory_space=pltpu.HBM)
        vmem = pl.BlockSpec(memory_space=pltpu.VMEM)
        state_out = state_v
        w_in_v = pltpu.VMEM((layers, model_dim, hidden_dim), BF16)
        w_out_v = pltpu.VMEM((layers, hidden_dim, model_dim), BF16)
        hidden_v = pltpu.VMEM((rows, model_dim), BF16)
        wide_v = pltpu.VMEM((4 * chunks, LANES), F32)
        normed_v = pltpu.VMEM((256, model_dim), BF16)
        active_v = pltpu.VMEM((256, hidden_dim), BF16)
        packed_v = pltpu.VMEM((4 * chunks, LANES), BF16)
        gathered = pl.pallas_call(
            functools.partial(gather_kernel, dims),
            name="gather_step",
            out_shape=(*(packed_v,) * 6, state_v, state_v, state_v, w_in_v, w_out_v, hidden_v),
            in_specs=[hbm] * 5,
            out_specs=(vmem,) * 12,
            scratch_shapes=[
                state_v, state_v, state_v, state_v,
                pltpu.VMEM((group_size, 8, LANES), F32),
                wide_v, normed_v, active_v,
                pltpu.SemaphoreType.DMA((5, layers)),
                pltpu.SemaphoreType.DMA((group_size,)),
                pltpu.SemaphoreType.DMA((group_size,)),
                pltpu.SemaphoreType.DMA((96,)),
                pltpu.SemaphoreType.DMA((96,)),
            ],
            compiler_params=pltpu.CompilerParams(collective_id=0, has_side_effects=True, vmem_limit_bytes=19 << 20),
        )(*[pltpu.with_memory_space_constraint(a, pltpu.HBM) for a in (*tiled, tok_rows)])
        gathered = [a.reshape(chunks, 4, LANES)[:, :layers, :] for a in gathered[:6]] + list(gathered[6:])
        state_tile = jax.ShapeDtypeStruct((chunks, layers, LANES), F32)
        weights, new_master, new_one, new_two, row_loss = pl.pallas_call(
            functools.partial(finish_kernel, dims),
            name="finish",
            out_shape=(jax.ShapeDtypeStruct((chunks * group_size, layers, LANES), BF16), state_tile, state_tile, state_tile,
                       jax.ShapeDtypeStruct((rows // LANES, LANES), F32)),
            in_specs=[vmem] * 13,
            out_specs=(hbm,) * 5,
            scratch_shapes=[
                pltpu.VMEM((rows // LANES, LANES), F32),
                pltpu.VMEM((2, chunks, layers, LANES), BF16),
                wide_v, normed_v, active_v, hidden_v,
                pltpu.SemaphoreType.DMA((6 + 3 * layers,)),
                pltpu.SemaphoreType.DMA((3,)),
            ],
            compiler_params=pltpu.CompilerParams(vmem_limit_bytes=14 << 20),
        )(*gathered, tgt_rows)

        def flat(a):
            return a.transpose(1, 0, 2).reshape(layers, a.shape[0] * LANES)

        return row_loss.reshape(rows), flat(weights), flat(new_master), flat(new_one), flat(new_two)

    return jax.shard_map(local_step, mesh=mesh, in_specs=(state_spec, state_spec, state_spec, state_spec, row_spec, row_spec), out_specs=(P("data"), P(), state_spec, state_spec, state_spec), check_vma=False)
```

```python
import functools

import jax
import jax.numpy as jnp
from jax import lax
from jax.experimental import pallas as pl
from jax.experimental.pallas import tpu as pltpu
from jax.sharding import PartitionSpec as P

LEARN_RATE = 0.01
BETA_ONE = 0.9
BETA_TWO = 0.95
ADAM_EPS = 1e-8
WEIGHT_DECAY = 0.1
ADAM_STEP = 10
CLIP_NORM = 1.0
NORM_EPS = 1e-6

MESH = pl.DeviceIdType.MESH
LANES = 128
GROUP = 8
F32 = jnp.float32
BF16 = jnp.bfloat16


def spread_piece(dims, kind, device, weights, wide_ref):
    layers, model_dim, hidden_dim, rows, chunks = dims
    per_row = (hidden_dim if kind == 0 else model_dim) // LANES
    count = chunks // per_row
    src = weights[kind]
    slot = lax.rem(device, 4)

    def spread(idx, _):
        row = pl.multiple_of(slot * count + idx * 16, 16)
        for layer in range(layers):
            for col in range(per_row):
                tile = src[layer, pl.ds(row, 16), col * LANES:(col + 1) * LANES].astype(F32)
                base = layer + 4 * (idx * (16 * per_row) + col)
                wide_ref[pl.ds(base, 8, stride=4 * per_row), :] = tile[0:8]
                wide_ref[pl.ds(base + 32 * per_row, 8, stride=4 * per_row), :] = tile[8:16]
        return 0

    lax.fori_loop(0, count // 16, spread, 0)


def mlp_block(dims, layer, w_in, w_out, hidden_ref, normed_ref, active_ref):
    layers, model_dim, hidden_dim, rows, chunks = dims

    def block(idx, _):
        at = pl.ds(pl.multiple_of(idx * 256, 256), 256)
        hidden = hidden_ref[at, :].astype(F32)
        scale = lax.rsqrt(jnp.mean(hidden * hidden, axis=-1, keepdims=True) + NORM_EPS)
        normed_ref[...] = (hidden * scale).astype(BF16)
        for col in range(0, hidden_dim, 384):
            inner = jnp.dot(normed_ref[...], w_in[layer, :, col:col + 384], preferred_element_type=F32).astype(BF16)
            active_ref[:, col:col + 384] = jax.nn.gelu(inner.astype(F32), approximate=True).astype(BF16)
        for col in range(0, model_dim, 256):
            add = jnp.dot(active_ref[...], w_out[layer, :, col:col + 256], preferred_element_type=F32)
            hidden_ref[at, col:col + 256] = (hidden_ref[at, col:col + 256].astype(F32) + add).astype(BF16)
        return 0

    lax.fori_loop(0, rows // 256, block, 0)


def places():
    me = lax.axis_index("data")
    core = lax.rem(me, 2)
    x_pos = lax.rem(me // 2, 2)
    y_pos = me // 4
    x_peer = me + 2 - 4 * x_pos
    y_peer = me + 4 - 8 * y_pos
    return me, core, y_pos, x_peer, y_peer, x_peer + 4 - 8 * y_pos


def gather_kernel(dims, grad_hbm, master_hbm, one_hbm, two_hbm, tok_hbm,
                  p0, p1, p2, p3, p4, p5, master_out, one_out, two_out, w_in, w_out, hidden_ref,
                  grad_v, master_v, one_v, two_v,
                  part_ref, wide_ref, normed_ref, active_ref,
                  load_sem, part_send, part_recv, send_sem, recv_sem):
    layers, model_dim, hidden_dim, rows, chunks = dims
    in_rows = chunks * LANES // hidden_dim
    out_rows = chunks * LANES // model_dim

    me, core, y_pos, x_peer, y_peer, diag = places()
    partner = me + 1 - 2 * core

    state = ((grad_hbm, grad_v), (master_hbm, master_v), (one_hbm, one_v), (two_hbm, two_v))

    def load(which, layer):
        src, dst = state[which]
        return pltpu.make_async_copy(src.at[:, layer, :], dst.at[layer], load_sem.at[which, layer])

    for layer in range(layers):
        load(0, layer).start()
    tok_load = pltpu.make_async_copy(tok_hbm, hidden_ref, load_sem.at[4, 0])

    barrier = pltpu.get_barrier_semaphore()
    for step in range(1, GROUP):
        pl.semaphore_signal(barrier, inc=1, device_id=(lax.rem(me + step, GROUP),), device_id_type=MESH)

    sums = tuple(jnp.zeros((8, LANES), F32) for _ in range(8))
    for layer in range(layers):
        load(0, layer).wait()
        if layer == layers - 1:
            for which in range(1, 4):
                load(which, 0).start()

        def square(idx, carry):
            base = pl.multiple_of(idx * 64, 64)
            block = grad_v[layer, pl.ds(base, 64), :]
            return tuple(carry[k] + block[8 * k:8 * k + 8] * block[8 * k:8 * k + 8] for k in range(8))

        sums = lax.fori_loop(0, chunks // 64, square, sums)
    mine = ((sums[0] + sums[1]) + (sums[2] + sums[3])) + ((sums[4] + sums[5]) + (sums[6] + sums[7]))
    part_ref[me] = mine
    pl.semaphore_wait(barrier, GROUP - 1)

    def part_copy(step):
        return pltpu.make_async_remote_copy(
            src_ref=part_ref.at[me], dst_ref=part_ref.at[me],
            send_sem=part_send.at[step], recv_sem=part_recv.at[step],
            device_id=(lax.rem(me + step, GROUP),), device_id_type=MESH)

    def part_arrival(step):
        slot = lax.rem(me + GROUP - step, GROUP)
        return pltpu.make_async_remote_copy(
            src_ref=part_ref.at[slot], dst_ref=part_ref.at[slot],
            send_sem=part_send.at[step], recv_sem=part_recv.at[step],
            device_id=(me,), device_id_type=MESH)

    for step in range(1, GROUP):
        part_copy(step).start()
    for item in range(1, layers):
        for which in range(1, 4):
            load(which, item).start()
    tok_load.start()
    for step in range(1, GROUP):
        part_arrival(step).wait_recv()
    total = part_ref[0]
    for slot in range(1, GROUP):
        total = total + part_ref[slot]
    total = jnp.sum(jnp.sum(total, axis=0, keepdims=True), axis=1, keepdims=True)
    clip = jnp.minimum(1.0, CLIP_NORM / jnp.sqrt(total))
    clip = jnp.broadcast_to(clip, (8, LANES))

    slots = {}

    def piece(kind, layer, device, part):
        ref, count = ((w_in, in_rows), (w_out, out_rows))[kind]
        span = count // part[1]
        at = lax.rem(device, 4) * count + part[0] * span
        return ref.at[layer, pl.ds(pl.multiple_of(at, 16), span), :]

    def copies(kind, layer, device, route, target, parts):
        out = []
        for part in parts:
            ref = piece(kind, layer, device, part)
            index = slots.setdefault((route, layer, part), len(slots))
            out.append(pltpu.make_async_remote_copy(
                src_ref=ref, dst_ref=ref, send_sem=send_sem.at[index],
                recv_sem=recv_sem.at[index], device_id=(target,), device_id_type=MESH))
        return out

    def start(items):
        for item in items:
            item.start()

    def arrive(items):
        for item in items:
            item.wait_recv()

    def left(items):
        for item in items:
            item.wait_send()

    def own_parts(layer):
        return ((0, 1),) if layer == 1 else ((0, 2), (1, 2))

    def far_parts(layer, half):
        return ((half, 2),)

    def own_x(kind, layer, device, target, parts=None):
        return copies(kind, layer, device, "own_x", target, parts or own_parts(layer))

    def own_y(kind, layer, device, target, parts=None):
        return copies(kind, layer, device, "own_y", target, parts or own_parts(layer))

    def far(kind, layer, half, device, target, parts=None):
        return copies(kind, layer, device, "far", target, parts or far_parts(layer, half))

    def pair(kind, layer, device, route, parts):
        return copies(kind, layer, device, route, partner, parts)

    def by_kind(function):
        for y_value in range(2):
            @pl.when(y_pos == y_value)
            def _():
                function(y_value)

    one_scale = 1.0 / (1.0 - BETA_ONE ** ADAM_STEP)
    two_scale = 1.0 / (1.0 - BETA_TWO ** ADAM_STEP)

    def adam(layer, part):
        first = part[0] * (chunks // part[1])

        def update(idx, _):
            base = pl.multiple_of(first + idx * 48, 8)
            for k in range(6):
                at = pl.ds(pl.multiple_of(base + 8 * k, 8), 8)
                clipped = grad_v[layer, at, :] * clip
                new_one = BETA_ONE * one_v[layer, at, :] + (1.0 - BETA_ONE) * clipped
                new_two = BETA_TWO * two_v[layer, at, :] + (1.0 - BETA_TWO) * clipped * clipped
                step_size = (new_one * one_scale) / (jnp.sqrt(new_two * two_scale) + ADAM_EPS)
                old = master_v[layer, at, :]
                master_out[layer, at, :] = old - LEARN_RATE * (step_size + WEIGHT_DECAY * old)
                one_out[layer, at, :] = new_one
                two_out[layer, at, :] = new_two
            return 0

        lax.fori_loop(0, chunks // part[1] // 48, update, 0)

    def round_rows(kind, layer, part):
        width = hidden_dim if kind == 0 else model_dim
        count = in_rows if kind == 0 else out_rows
        per_row = width // LANES
        dst = w_in if kind == 0 else w_out
        slot = lax.rem(me, 4)

        def body(idx, _):
            base = part[0] * (chunks // part[1]) + idx * (16 * per_row)
            row = pl.multiple_of(slot * count + part[0] * (count // part[1]) + idx * 16, 16)
            for col in range(per_row):
                top = master_out[layer, pl.ds(base + col, 8, stride=per_row), :]
                low = master_out[layer, pl.ds(base + 8 * per_row + col, 8, stride=per_row), :]
                dst[layer, pl.ds(row, 16), col * LANES:(col + 1) * LANES] = jnp.concatenate([top, low], axis=0).astype(BF16)
            return 0

        lax.fori_loop(0, count // 16 // part[1], body, 0)

    for layer in range(layers):
        for which in range(1, 4):
            load(which, layer).wait()
        for part in own_parts(layer):
            adam(layer, part)

            def send_own(kind):
                round_rows(kind, layer, part)
                if layer < layers - 1:
                    start(own_x(kind, layer, me, x_peer, (part,)))
                    start(own_y(kind, layer, me, y_peer, (part,)))
                start(pair(kind, layer, me, "pair_own", (part,)))

            by_kind(send_own)

    def pack(kind, device, packed_ref):
        spread_piece(dims, kind, device, (w_in, w_out), wide_ref)

        def squeeze(idx, _):
            at = pl.ds(pl.multiple_of(idx * 256, 256), 256)
            packed_ref[at, :] = wide_ref[at, :].astype(BF16)
            return 0

        lax.fori_loop(0, 4 * chunks // 256, squeeze, 0)

    def partner_of(device):
        return device + 1 - 2 * core

    def forward(kind, layer):
        x_order = own_parts(layer)
        y_order = x_order[::-1] if layer == layers - 1 else x_order
        for x_part, y_part in zip(x_order, y_order):
            arrive(own_x(kind, layer, x_peer, me, (x_part,)))
            if x_part in ((0, 2), (0, 1)):
                start(far(kind, layer, 0, x_peer, y_peer))
            start(pair(kind, layer, x_peer, "pair_x", (x_part,)))
            arrive(own_y(1 - kind, layer, y_peer, me, (y_part,)))
            if y_part in ((1, 2), (0, 1)):
                start(far(1 - kind, layer, 1, y_peer, x_peer))
            start(pair(1 - kind, layer, y_peer, "pair_y", (y_part,)))

    def far_arrive(kind, layer, only=None):
        for idx, parts in enumerate(zip(far_parts(layer, 0), far_parts(layer, 1))):
            if only is not None and idx != only:
                continue
            for half in range(2):
                arrive(far(1 - kind, layer, half, diag, me, (parts[half],)))
                start(pair(1 - kind, layer, diag, "pair_far", (parts[half],)))

    def far_partner(kind, layer):
        arrive(pair(1 - kind, layer, partner_of(diag), "pair_far", far_parts(layer, 0) + far_parts(layer, 1)))

    def near_partner(kind, layer):
        arrive(pair(kind, layer, partner_of(x_peer), "pair_x", own_parts(layer)))
        arrive(pair(1 - kind, layer, partner_of(y_peer), "pair_y", own_parts(layer)))

    def stage_own(kind):
        pack(kind, me, p0)
        forward(kind, 0)
        for layer in range(layers):
            arrive(pair(kind, layer, partner, "pair_own", own_parts(layer)))
        pack(kind, partner, p1)
        forward(kind, 1)
        start(own_x(kind, layers - 1, me, x_peer))
        start(own_y(kind, layers - 1, me, y_peer)[::-1])
        near_partner(kind, 0)
        far_arrive(kind, 0)
        near_partner(kind, 1)
        far_partner(kind, 0)

    def stage_one(kind):
        far_arrive(kind, 1)
        far_partner(kind, 1)

    def stage_two(kind):
        forward(kind, 2)
        pack(kind, x_peer, p2)
        pack(1 - kind, y_peer, p4)
        near_partner(kind, 2)
        pack(kind, partner_of(x_peer), p3)
        pack(1 - kind, partner_of(y_peer), p5)
        far_arrive(kind, 2)
        far_partner(kind, 2)

    by_kind(stage_own)
    tok_load.wait()
    mlp_block(dims, 0, w_in, w_out, hidden_ref, normed_ref, active_ref)
    by_kind(stage_one)
    mlp_block(dims, 1, w_in, w_out, hidden_ref, normed_ref, active_ref)
    by_kind(stage_two)

    for step in range(1, GROUP):
        part_copy(step).wait_send()

    def drain(kind):
        for layer in range(layers):
            left(own_x(kind, layer, me, x_peer))
            left(own_y(kind, layer, me, y_peer))
            left(pair(kind, layer, me, "pair_own", own_parts(layer)))
            left(pair(kind, layer, x_peer, "pair_x", own_parts(layer)))
            left(pair(1 - kind, layer, y_peer, "pair_y", own_parts(layer)))
            left(pair(1 - kind, layer, diag, "pair_far", far_parts(layer, 0) + far_parts(layer, 1)))
            left(far(kind, layer, 0, x_peer, y_peer))
            left(far(1 - kind, layer, 1, y_peer, x_peer))

    by_kind(drain)


def finish_kernel(dims, p0, p1, p2, p3, p4, p5, master_ref, one_ref, two_ref, w_in, w_out, last_ref, tgt_ref,
                  packed_hbm, master_hbm, one_hbm, two_hbm, loss_hbm,
                  loss_ref, far_ref, wide_ref, normed_ref, active_ref, hidden_ref, sem, far_sem):
    layers, model_dim, hidden_dim, rows, chunks = dims
    me, core, y_pos, x_peer, y_peer, diag = places()
    twin = 1 - 2 * core

    copies = []
    for idx, (ref, device) in enumerate(((p0, me), (p1, me + twin), (p2, x_peer), (p3, x_peer + twin), (p4, y_peer), (p5, y_peer + twin))):
        copies.append(pltpu.make_async_copy(ref, packed_hbm.at[pl.ds(device * chunks, chunks)], sem.at[idx]))
    for which, (src, dst) in enumerate(((master_ref, master_hbm), (one_ref, one_hbm), (two_ref, two_hbm))):
        for layer in range(layers):
            copies.append(pltpu.make_async_copy(src.at[layer], dst.at[:, layer, :], sem.at[6 + which * layers + layer]))
    for item in copies:
        item.start()

    far_copies = []
    for idx, device in enumerate((diag, diag + twin)):
        for y_value in range(2):
            @pl.when(y_pos == y_value)
            def _():
                spread_piece(dims, 1 - y_value, device, (w_in, w_out), wide_ref)

        def squeeze(at, _):
            block = wide_ref[pl.ds(pl.multiple_of(at * 128, 128), 128), :].astype(BF16).reshape(32, 4, LANES)
            far_ref[idx, pl.ds(at * 32, 32), :, :] = block[:, :layers, :]
            return 0

        lax.fori_loop(0, 4 * chunks // 128, squeeze, 0)
        far_copies.append(pltpu.make_async_copy(far_ref.at[idx], packed_hbm.at[pl.ds(device * chunks, chunks)], far_sem.at[idx]))
        far_copies[-1].start()

    hidden_ref[...] = last_ref[...]
    mlp_block(dims, layers - 1, w_in, w_out, hidden_ref, normed_ref, active_ref)

    for idx in range(rows // LANES):
        at = slice(idx * LANES, (idx + 1) * LANES)
        error = hidden_ref[at, :].astype(F32) - tgt_ref[at, :].astype(F32)
        error = error * error
        folded = error[:, 0:LANES]
        for col in range(LANES, model_dim, LANES):
            folded = folded + error[:, col:col + LANES]
        loss_ref[idx:idx + 1, :] = jnp.sum(folded.T, axis=0, keepdims=True) * (1.0 / model_dim)

    loss_copy = pltpu.make_async_copy(loss_ref, loss_hbm, far_sem.at[2])
    loss_copy.start()
    for item in copies + far_copies + [loss_copy]:
        item.wait()


def solution(mesh):
    group_size = mesh.shape["data"]
    state_spec = P(None, "data")
    row_spec = P("data", None)

    def local_step(grad_shard, master_shard, one_shard, two_shard, tok_rows, tgt_rows):
        rows, model_dim = tok_rows.shape
        layers, cols = master_shard.shape
        half_size = cols * group_size // 2
        hidden_dim = half_size // model_dim
        chunks = cols // LANES
        dims = (layers, model_dim, hidden_dim, rows, chunks)
        tiled = [a.reshape(layers, chunks, LANES).transpose(1, 0, 2) for a in (grad_shard, master_shard, one_shard, two_shard)]
        state_v = pltpu.VMEM((layers, chunks, LANES), F32)
        hbm = pl.BlockSpec(memory_space=pltpu.HBM)
        vmem = pl.BlockSpec(memory_space=pltpu.VMEM)
        state_out = state_v
        w_in_v = pltpu.VMEM((layers, model_dim, hidden_dim), BF16)
        w_out_v = pltpu.VMEM((layers, hidden_dim, model_dim), BF16)
        hidden_v = pltpu.VMEM((rows, model_dim), BF16)
        wide_v = pltpu.VMEM((4 * chunks, LANES), F32)
        normed_v = pltpu.VMEM((256, model_dim), BF16)
        active_v = pltpu.VMEM((256, hidden_dim), BF16)
        packed_v = pltpu.VMEM((4 * chunks, LANES), BF16)
        gathered = pl.pallas_call(
            functools.partial(gather_kernel, dims),
            name="gather_step",
            out_shape=(*(packed_v,) * 6, state_v, state_v, state_v, w_in_v, w_out_v, hidden_v),
            in_specs=[hbm] * 5,
            out_specs=(vmem,) * 12,
            scratch_shapes=[
                state_v, state_v, state_v, state_v,
                pltpu.VMEM((group_size, 8, LANES), F32),
                wide_v, normed_v, active_v,
                pltpu.SemaphoreType.DMA((5, layers)),
                pltpu.SemaphoreType.DMA((group_size,)),
                pltpu.SemaphoreType.DMA((group_size,)),
                pltpu.SemaphoreType.DMA((96,)),
                pltpu.SemaphoreType.DMA((96,)),
            ],
            compiler_params=pltpu.CompilerParams(collective_id=0, has_side_effects=True, vmem_limit_bytes=19 << 20),
        )(*[pltpu.with_memory_space_constraint(a, pltpu.HBM) for a in (*tiled, tok_rows)])
        gathered = [a.reshape(chunks, 4, LANES)[:, :layers, :] for a in gathered[:6]] + list(gathered[6:])
        state_tile = jax.ShapeDtypeStruct((chunks, layers, LANES), F32)
        weights, new_master, new_one, new_two, row_loss = pl.pallas_call(
            functools.partial(finish_kernel, dims),
            name="finish",
            out_shape=(jax.ShapeDtypeStruct((chunks * group_size, layers, LANES), BF16), state_tile, state_tile, state_tile,
                       jax.ShapeDtypeStruct((rows // LANES, LANES), F32)),
            in_specs=[vmem] * 13,
            out_specs=(hbm,) * 5,
            scratch_shapes=[
                pltpu.VMEM((rows // LANES, LANES), F32),
                pltpu.VMEM((2, chunks, layers, LANES), BF16),
                wide_v, normed_v, active_v, hidden_v,
                pltpu.SemaphoreType.DMA((6 + 3 * layers,)),
                pltpu.SemaphoreType.DMA((3,)),
            ],
            compiler_params=pltpu.CompilerParams(vmem_limit_bytes=14 << 20),
        )(*gathered, tgt_rows)

        def flat(a):
            return a.transpose(1, 0, 2).reshape(layers, a.shape[0] * LANES)

        return row_loss.reshape(rows), flat(weights), flat(new_master), flat(new_one), flat(new_two)

    return jax.shard_map(local_step, mesh=mesh, in_specs=(state_spec, state_spec, state_spec, state_spec, row_spec, row_spec), out_specs=(P("data"), P(), state_spec, state_spec, state_spec), check_vma=False)
```

```python
import functools

import jax
import jax.numpy as jnp
from jax import lax
from jax.experimental import pallas as pl
from jax.experimental.pallas import tpu as pltpu
from jax.sharding import PartitionSpec as P

LEARN_RATE = 0.01
BETA_ONE = 0.9
BETA_TWO = 0.95
ADAM_EPS = 1e-8
WEIGHT_DECAY = 0.1
ADAM_STEP = 10
CLIP_NORM = 1.0
NORM_EPS = 1e-6

MESH = pl.DeviceIdType.MESH
LANES = 128
GROUP = 8
F32 = jnp.float32
BF16 = jnp.bfloat16


def spread_piece(dims, kind, device, weights, wide_ref):
    layers, model_dim, hidden_dim, rows, chunks = dims
    per_row = (hidden_dim if kind == 0 else model_dim) // LANES
    count = chunks // per_row
    src = weights[kind]
    slot = lax.rem(device, 4)

    def spread(idx, _):
        row = pl.multiple_of(slot * count + idx * 16, 16)
        for layer in range(layers):
            for col in range(per_row):
                tile = src[layer, pl.ds(row, 16), col * LANES:(col + 1) * LANES].astype(F32)
                base = layer + 4 * (idx * (16 * per_row) + col)
                wide_ref[pl.ds(base, 8, stride=4 * per_row), :] = tile[0:8]
                wide_ref[pl.ds(base + 32 * per_row, 8, stride=4 * per_row), :] = tile[8:16]
        return 0

    lax.fori_loop(0, count // 16, spread, 0)


def mlp_block(dims, layer, w_in, w_out, hidden_ref, normed_ref, active_ref):
    layers, model_dim, hidden_dim, rows, chunks = dims

    def block(idx, _):
        at = pl.ds(pl.multiple_of(idx * 256, 256), 256)
        hidden = hidden_ref[at, :].astype(F32)
        scale = lax.rsqrt(jnp.mean(hidden * hidden, axis=-1, keepdims=True) + NORM_EPS)
        normed_ref[...] = (hidden * scale).astype(BF16)
        for col in range(0, hidden_dim, 384):
            inner = jnp.dot(normed_ref[...], w_in[layer, :, col:col + 384], preferred_element_type=F32).astype(BF16)
            active_ref[:, col:col + 384] = jax.nn.gelu(inner.astype(F32), approximate=True).astype(BF16)
        for col in range(0, model_dim, 256):
            add = jnp.dot(active_ref[...], w_out[layer, :, col:col + 256], preferred_element_type=F32)
            hidden_ref[at, col:col + 256] = (hidden_ref[at, col:col + 256].astype(F32) + add).astype(BF16)
        return 0

    lax.fori_loop(0, rows // 256, block, 0)


def places():
    me = lax.axis_index("data")
    core = lax.rem(me, 2)
    x_pos = lax.rem(me // 2, 2)
    y_pos = me // 4
    x_peer = me + 2 - 4 * x_pos
    y_peer = me + 4 - 8 * y_pos
    return me, core, y_pos, x_peer, y_peer, x_peer + 4 - 8 * y_pos


def gather_kernel(dims, grad_hbm, master_hbm, one_hbm, two_hbm, tok_hbm,
                  p0, p1, p2, p3, p4, p5, master_out, one_out, two_out, w_in, w_out, hidden_ref,
                  grad_v, master_v, one_v, two_v,
                  part_ref, wide_ref, normed_ref, active_ref,
                  load_sem, grad_sem, part_send, part_recv, send_sem, recv_sem):
    layers, model_dim, hidden_dim, rows, chunks = dims
    in_rows = chunks * LANES // hidden_dim
    out_rows = chunks * LANES // model_dim

    me, core, y_pos, x_peer, y_peer, diag = places()
    partner = me + 1 - 2 * core

    state = ((grad_hbm, grad_v), (master_hbm, master_v), (one_hbm, one_v), (two_hbm, two_v))

    def load(which, layer):
        src, dst = state[which]
        return pltpu.make_async_copy(src.at[:, layer, :], dst.at[layer], load_sem.at[which, layer])

    span = chunks // 3

    def grad_load(layer, part):
        at = pl.ds(part * span, span)
        return pltpu.make_async_copy(grad_hbm.at[at, layer, :], grad_v.at[layer, at], grad_sem.at[layer, part])

    for layer in range(layers):
        for part in range(3):
            grad_load(layer, part).start()
    tok_load = pltpu.make_async_copy(tok_hbm, hidden_ref, load_sem.at[4, 0])

    barrier = pltpu.get_barrier_semaphore()
    for step in range(1, GROUP):
        pl.semaphore_signal(barrier, inc=1, device_id=(lax.rem(me + step, GROUP),), device_id_type=MESH)

    sums = tuple(jnp.zeros((8, LANES), F32) for _ in range(8))
    for layer in range(layers):
        for part in range(3):
            grad_load(layer, part).wait()
            if layer == layers - 1 and part == 2:
                for which in range(1, 4):
                    load(which, 0).start()

            def square(idx, carry):
                base = pl.multiple_of(part * span + idx * 64, 64)
                block = grad_v[layer, pl.ds(base, 64), :]
                return tuple(carry[k] + block[8 * k:8 * k + 8] * block[8 * k:8 * k + 8] for k in range(8))

            sums = lax.fori_loop(0, span // 64, square, sums)
    mine = ((sums[0] + sums[1]) + (sums[2] + sums[3])) + ((sums[4] + sums[5]) + (sums[6] + sums[7]))
    part_ref[me] = jnp.sum(mine, axis=0, keepdims=True)
    pl.semaphore_wait(barrier, GROUP - 1)

    def part_copy(step):
        return pltpu.make_async_remote_copy(
            src_ref=part_ref.at[me], dst_ref=part_ref.at[me],
            send_sem=part_send.at[step], recv_sem=part_recv.at[step],
            device_id=(lax.rem(me + step, GROUP),), device_id_type=MESH)

    def part_arrival(step):
        slot = lax.rem(me + GROUP - step, GROUP)
        return pltpu.make_async_remote_copy(
            src_ref=part_ref.at[slot], dst_ref=part_ref.at[slot],
            send_sem=part_send.at[step], recv_sem=part_recv.at[step],
            device_id=(me,), device_id_type=MESH)

    for step in range(1, GROUP):
        part_copy(step).start()
    for item in range(1, layers):
        for which in range(1, 4):
            load(which, item).start()
    tok_load.start()
    for step in range(1, GROUP):
        part_arrival(step).wait_recv()
    total = part_ref[0]
    for slot in range(1, GROUP):
        total = total + part_ref[slot]
    total = jnp.sum(total, axis=1, keepdims=True)
    clip = jnp.minimum(1.0, CLIP_NORM / jnp.sqrt(total))
    clip = jnp.broadcast_to(clip, (8, LANES))

    slots = {}

    def piece(kind, layer, device, part):
        ref, count = ((w_in, in_rows), (w_out, out_rows))[kind]
        span = count // part[1]
        at = lax.rem(device, 4) * count + part[0] * span
        return ref.at[layer, pl.ds(pl.multiple_of(at, 16), span), :]

    def copies(kind, layer, device, route, target, parts):
        out = []
        for part in parts:
            ref = piece(kind, layer, device, part)
            index = slots.setdefault((route, layer, part), len(slots))
            out.append(pltpu.make_async_remote_copy(
                src_ref=ref, dst_ref=ref, send_sem=send_sem.at[index],
                recv_sem=recv_sem.at[index], device_id=(target,), device_id_type=MESH))
        return out

    def start(items):
        for item in items:
            item.start()

    def arrive(items):
        for item in items:
            item.wait_recv()

    def left(items):
        for item in items:
            item.wait_send()

    def own_parts(layer):
        return ((0, 6), (1, 6), (2, 6), (1, 2)) if layer == 0 else ((0, 2), (1, 2))

    def far_parts(layer, half):
        return tuple((3 * half + at, 6) for at in range(3)) if layer == layers - 1 else ((half, 2),)

    def own_x(kind, layer, device, target, parts=None):
        return copies(kind, layer, device, "own_x", target, parts or own_parts(layer))

    def own_y(kind, layer, device, target, parts=None):
        return copies(kind, layer, device, "own_y", target, parts or own_parts(layer))

    def far(kind, layer, half, device, target, parts=None):
        return copies(kind, layer, device, "far", target, parts or far_parts(layer, half))

    def pair(kind, layer, device, route, parts):
        return copies(kind, layer, device, route, partner, parts)

    def by_kind(function):
        for y_value in range(2):
            @pl.when(y_pos == y_value)
            def _():
                function(y_value)

    one_scale = 1.0 / (1.0 - BETA_ONE ** ADAM_STEP)
    two_scale = 1.0 / (1.0 - BETA_TWO ** ADAM_STEP)

    def adam(layer, part):
        first = part[0] * (chunks // part[1])

        def update(idx, _):
            base = pl.multiple_of(first + idx * 48, 8)
            for k in range(6):
                at = pl.ds(pl.multiple_of(base + 8 * k, 8), 8)
                clipped = grad_v[layer, at, :] * clip
                new_one = BETA_ONE * one_v[layer, at, :] + (1.0 - BETA_ONE) * clipped
                new_two = BETA_TWO * two_v[layer, at, :] + (1.0 - BETA_TWO) * clipped * clipped
                step_size = (new_one * one_scale) / (jnp.sqrt(new_two * two_scale) + ADAM_EPS)
                old = master_v[layer, at, :]
                master_out[layer, at, :] = old - LEARN_RATE * (step_size + WEIGHT_DECAY * old)
                one_out[layer, at, :] = new_one
                two_out[layer, at, :] = new_two
            return 0

        lax.fori_loop(0, chunks // part[1] // 48, update, 0)

    def round_rows(kind, layer, part):
        width = hidden_dim if kind == 0 else model_dim
        count = in_rows if kind == 0 else out_rows
        per_row = width // LANES
        dst = w_in if kind == 0 else w_out
        slot = lax.rem(me, 4)

        def body(idx, _):
            base = part[0] * (chunks // part[1]) + idx * (16 * per_row)
            row = pl.multiple_of(slot * count + part[0] * (count // part[1]) + idx * 16, 16)
            for col in range(per_row):
                top = master_out[layer, pl.ds(base + col, 8, stride=per_row), :]
                low = master_out[layer, pl.ds(base + 8 * per_row + col, 8, stride=per_row), :]
                dst[layer, pl.ds(row, 16), col * LANES:(col + 1) * LANES] = jnp.concatenate([top, low], axis=0).astype(BF16)
            return 0

        lax.fori_loop(0, count // 16 // part[1], body, 0)

    for layer in range(layers):
        for which in range(1, 4):
            load(which, layer).wait()
        for part in own_parts(layer):
            adam(layer, part)

            def send_own(kind):
                round_rows(kind, layer, part)
                if layer < layers - 1:
                    start(own_x(kind, layer, me, x_peer, (part,)))
                    start(own_y(kind, layer, me, y_peer, (part,)))
                start(pair(kind, layer, me, "pair_own", (part,)))

            by_kind(send_own)

    def pack(kind, device, packed_ref):
        spread_piece(dims, kind, device, (w_in, w_out), wide_ref)

        def squeeze(idx, _):
            at = pl.ds(pl.multiple_of(idx * 256, 256), 256)
            packed_ref[at, :] = wide_ref[at, :].astype(BF16)
            return 0

        lax.fori_loop(0, 4 * chunks // 256, squeeze, 0)

    def partner_of(device):
        return device + 1 - 2 * core

    def drain(kind):
        for layer in range(layers):
            left(own_x(kind, layer, me, x_peer))
            left(own_y(kind, layer, me, y_peer))
            left(pair(kind, layer, me, "pair_own", own_parts(layer)))
            left(pair(kind, layer, x_peer, "pair_x", own_parts(layer)))
            left(pair(1 - kind, layer, y_peer, "pair_y", own_parts(layer)))
            if layer < layers - 1:
                left(pair(1 - kind, layer, diag, "pair_far", far_parts(layer, 0) + far_parts(layer, 1)))
                left(far(kind, layer, 0, x_peer, y_peer))
                left(far(1 - kind, layer, 1, y_peer, x_peer))
        for step in range(1, GROUP):
            part_copy(step).wait_send()

    def drain_last(kind):
        layer = layers - 1
        left(far(kind, layer, 0, x_peer, y_peer))
        left(far(1 - kind, layer, 1, y_peer, x_peer))
        left(pair(1 - kind, layer, diag, "pair_far", far_parts(layer, 0) + far_parts(layer, 1)))

    def forward(kind, layer):
        x_order = own_parts(layer)
        y_order = x_order[::-1] if layer == layers - 1 else x_order
        for x_part, y_part in zip(x_order, y_order):
            arrive(own_x(kind, layer, x_peer, me, (x_part,)))
            if x_part in ((0, 2), (2, 6)):
                start(far(kind, layer, 0, x_peer, y_peer))
            start(pair(kind, layer, x_peer, "pair_x", (x_part,)))
            arrive(own_y(1 - kind, layer, y_peer, me, (y_part,)))
            if y_part == (1, 2):
                start(far(1 - kind, layer, 1, y_peer, x_peer))
            start(pair(1 - kind, layer, y_peer, "pair_y", (y_part,)))

    def far_arrive(kind, layer, only=None):
        for idx, parts in enumerate(zip(far_parts(layer, 0), far_parts(layer, 1))):
            if only is not None and idx != only:
                continue
            for half in range(2):
                arrive(far(1 - kind, layer, half, diag, me, (parts[half],)))
                start(pair(1 - kind, layer, diag, "pair_far", (parts[half],)))

    def far_partner(kind, layer):
        arrive(pair(1 - kind, layer, partner_of(diag), "pair_far", far_parts(layer, 0) + far_parts(layer, 1)))

    def near_partner(kind, layer):
        arrive(pair(kind, layer, partner_of(x_peer), "pair_x", own_parts(layer)))
        arrive(pair(1 - kind, layer, partner_of(y_peer), "pair_y", own_parts(layer)))

    def stage_own(kind):
        pack(kind, me, p0)
        forward(kind, 0)
        for layer in range(layers):
            arrive(pair(kind, layer, partner, "pair_own", own_parts(layer)))
        pack(kind, partner, p1)
        forward(kind, 1)
        start(own_x(kind, layers - 1, me, x_peer))
        start(own_y(kind, layers - 1, me, y_peer)[::-1])
        near_partner(kind, 0)
        far_arrive(kind, 0)
        near_partner(kind, 1)
        far_partner(kind, 0)

    def stage_one(kind):
        far_arrive(kind, 1)
        far_partner(kind, 1)

    def stage_two(kind):
        forward(kind, 2)
        pack(kind, x_peer, p2)
        pack(1 - kind, y_peer, p4)
        near_partner(kind, 2)
        far_arrive(kind, 2, 0)
        pack(kind, partner_of(x_peer), p3)
        far_arrive(kind, 2, 1)
        pack(1 - kind, partner_of(y_peer), p5)
        drain(kind)
        far_arrive(kind, 2, 2)
        far_partner(kind, 2)
        drain_last(kind)

    by_kind(stage_own)
    tok_load.wait()
    mlp_block(dims, 0, w_in, w_out, hidden_ref, normed_ref, active_ref)
    by_kind(stage_one)
    mlp_block(dims, 1, w_in, w_out, hidden_ref, normed_ref, active_ref)
    by_kind(stage_two)


def finish_kernel(dims, p0, p1, p2, p3, p4, p5, master_ref, one_ref, two_ref, w_in, w_out, last_ref, tgt_ref,
                  packed_hbm, master_hbm, one_hbm, two_hbm, loss_hbm,
                  loss_ref, far_ref, wide_ref, normed_ref, active_ref, hidden_ref, sem, far_sem):
    layers, model_dim, hidden_dim, rows, chunks = dims
    me, core, y_pos, x_peer, y_peer, diag = places()
    twin = 1 - 2 * core

    copies = []
    for which, (src, dst) in enumerate(((master_ref, master_hbm), (one_ref, one_hbm), (two_ref, two_hbm))):
        for layer in range(layers):
            copies.append(pltpu.make_async_copy(src.at[layer], dst.at[:, layer, :], sem.at[6 + which * layers + layer]))
    for idx, (ref, device) in enumerate(((p0, me), (p1, me + twin), (p2, x_peer), (p3, x_peer + twin), (p4, y_peer), (p5, y_peer + twin))):
        copies.append(pltpu.make_async_copy(ref, packed_hbm.at[pl.ds(device * chunks, chunks)], sem.at[idx]))
    for item in copies:
        item.start()

    far_copies = []
    for idx, device in enumerate((diag, diag + twin)):
        for y_value in range(2):
            @pl.when(y_pos == y_value)
            def _():
                spread_piece(dims, 1 - y_value, device, (w_in, w_out), wide_ref)

        def squeeze(at, _):
            block = wide_ref[pl.ds(pl.multiple_of(at * 128, 128), 128), :].astype(BF16).reshape(32, 4, LANES)
            far_ref[idx, pl.ds(at * 32, 32), :, :] = block[:, :layers, :]
            return 0

        lax.fori_loop(0, 4 * chunks // 128, squeeze, 0)
        far_copies.append(pltpu.make_async_copy(far_ref.at[idx], packed_hbm.at[pl.ds(device * chunks, chunks)], far_sem.at[idx]))
        far_copies[-1].start()

    hidden_ref[...] = last_ref[...]
    mlp_block(dims, layers - 1, w_in, w_out, hidden_ref, normed_ref, active_ref)

    for idx in range(rows // LANES):
        at = slice(idx * LANES, (idx + 1) * LANES)
        error = hidden_ref[at, :].astype(F32) - tgt_ref[at, :].astype(F32)
        error = error * error
        folded = error[:, 0:LANES]
        for col in range(LANES, model_dim, LANES):
            folded = folded + error[:, col:col + LANES]
        loss_ref[idx:idx + 1, :] = jnp.sum(folded.T, axis=0, keepdims=True) * (1.0 / model_dim)

    loss_copy = pltpu.make_async_copy(loss_ref, loss_hbm, far_sem.at[2])
    loss_copy.start()
    for item in copies + far_copies + [loss_copy]:
        item.wait()


def solution(mesh):
    group_size = mesh.shape["data"]
    state_spec = P(None, "data")
    row_spec = P("data", None)

    def local_step(grad_shard, master_shard, one_shard, two_shard, tok_rows, tgt_rows):
        rows, model_dim = tok_rows.shape
        layers, cols = master_shard.shape
        half_size = cols * group_size // 2
        hidden_dim = half_size // model_dim
        chunks = cols // LANES
        dims = (layers, model_dim, hidden_dim, rows, chunks)
        tiled = [a.reshape(layers, chunks, LANES).transpose(1, 0, 2) for a in (grad_shard, master_shard, one_shard, two_shard)]
        state_v = pltpu.VMEM((layers, chunks, LANES), F32)
        hbm = pl.BlockSpec(memory_space=pltpu.HBM)
        vmem = pl.BlockSpec(memory_space=pltpu.VMEM)
        state_out = state_v
        w_in_v = pltpu.VMEM((layers, model_dim, hidden_dim), BF16)
        w_out_v = pltpu.VMEM((layers, hidden_dim, model_dim), BF16)
        hidden_v = pltpu.VMEM((rows, model_dim), BF16)
        wide_v = pltpu.VMEM((4 * chunks, LANES), F32)
        normed_v = pltpu.VMEM((256, model_dim), BF16)
        active_v = pltpu.VMEM((256, hidden_dim), BF16)
        packed_v = pltpu.VMEM((4 * chunks, LANES), BF16)
        gathered = pl.pallas_call(
            functools.partial(gather_kernel, dims),
            name="gather_step",
            out_shape=(*(packed_v,) * 6, state_v, state_v, state_v, w_in_v, w_out_v, hidden_v),
            in_specs=[hbm] * 5,
            out_specs=(vmem,) * 12,
            scratch_shapes=[
                state_v, state_v, state_v, state_v,
                pltpu.VMEM((group_size, 1, LANES), F32),
                wide_v, normed_v, active_v,
                pltpu.SemaphoreType.DMA((5, layers)),
                pltpu.SemaphoreType.DMA((layers, 3)),
                pltpu.SemaphoreType.DMA((group_size,)),
                pltpu.SemaphoreType.DMA((group_size,)),
                pltpu.SemaphoreType.DMA((96,)),
                pltpu.SemaphoreType.DMA((96,)),
            ],
            compiler_params=pltpu.CompilerParams(collective_id=0, has_side_effects=True, vmem_limit_bytes=19 << 20),
        )(*[pltpu.with_memory_space_constraint(a, pltpu.HBM) for a in (*tiled, tok_rows)])
        gathered = [a.reshape(chunks, 4, LANES)[:, :layers, :] for a in gathered[:6]] + list(gathered[6:])
        state_tile = jax.ShapeDtypeStruct((chunks, layers, LANES), F32)
        weights, new_master, new_one, new_two, row_loss = pl.pallas_call(
            functools.partial(finish_kernel, dims),
            name="finish",
            out_shape=(jax.ShapeDtypeStruct((chunks * group_size, layers, LANES), BF16), state_tile, state_tile, state_tile,
                       jax.ShapeDtypeStruct((rows // LANES, LANES), F32)),
            in_specs=[vmem] * 13,
            out_specs=(hbm,) * 5,
            scratch_shapes=[
                pltpu.VMEM((rows // LANES, LANES), F32),
                pltpu.VMEM((2, chunks, layers, LANES), BF16),
                wide_v, normed_v, active_v, hidden_v,
                pltpu.SemaphoreType.DMA((6 + 3 * layers,)),
                pltpu.SemaphoreType.DMA((3,)),
            ],
            compiler_params=pltpu.CompilerParams(vmem_limit_bytes=14 << 20),
        )(*gathered, tgt_rows)

        def flat(a):
            return a.transpose(1, 0, 2).reshape(layers, a.shape[0] * LANES)

        return row_loss.reshape(rows), flat(weights), flat(new_master), flat(new_one), flat(new_two)

    return jax.shard_map(local_step, mesh=mesh, in_specs=(state_spec, state_spec, state_spec, state_spec, row_spec, row_spec), out_specs=(P("data"), P(), state_spec, state_spec, state_spec), check_vma=False)
```

```python
import functools

import jax
import jax.numpy as jnp
from jax import lax
from jax.experimental import pallas as pl
from jax.experimental.pallas import tpu as pltpu
from jax.sharding import PartitionSpec as P

LEARN_RATE = 0.01
BETA_ONE = 0.9
BETA_TWO = 0.95
ADAM_EPS = 1e-8
WEIGHT_DECAY = 0.1
ADAM_STEP = 10
CLIP_NORM = 1.0
NORM_EPS = 1e-6

MESH = pl.DeviceIdType.MESH
LANES = 128
GROUP = 8
F32 = jnp.float32
BF16 = jnp.bfloat16


def spread_piece(dims, kind, device, weights, wide_ref):
    layers, model_dim, hidden_dim, rows, chunks = dims
    per_row = (hidden_dim if kind == 0 else model_dim) // LANES
    count = chunks // per_row
    src = weights[kind]
    slot = lax.rem(device, 4)

    def spread(idx, _):
        row = pl.multiple_of(slot * count + idx * 16, 16)
        for layer in range(layers):
            for col in range(per_row):
                tile = src[layer, pl.ds(row, 16), col * LANES:(col + 1) * LANES].astype(F32)
                base = layer + 4 * (idx * (16 * per_row) + col)
                wide_ref[pl.ds(base, 8, stride=4 * per_row), :] = tile[0:8]
                wide_ref[pl.ds(base + 32 * per_row, 8, stride=4 * per_row), :] = tile[8:16]
        return 0

    lax.fori_loop(0, count // 16, spread, 0)


def mlp_block(dims, layer, w_in, w_out, hidden_ref, normed_ref, active_ref):
    layers, model_dim, hidden_dim, rows, chunks = dims

    def block(idx, _):
        at = pl.ds(pl.multiple_of(idx * 256, 256), 256)
        hidden = hidden_ref[at, :].astype(F32)
        scale = lax.rsqrt(jnp.mean(hidden * hidden, axis=-1, keepdims=True) + NORM_EPS)
        normed_ref[...] = (hidden * scale).astype(BF16)
        for col in range(0, hidden_dim, 384):
            inner = jnp.dot(normed_ref[...], w_in[layer, :, col:col + 384], preferred_element_type=F32).astype(BF16)
            active_ref[:, col:col + 384] = jax.nn.gelu(inner.astype(F32), approximate=True).astype(BF16)
        for col in range(0, model_dim, 256):
            add = jnp.dot(active_ref[...], w_out[layer, :, col:col + 256], preferred_element_type=F32)
            hidden_ref[at, col:col + 256] = (hidden_ref[at, col:col + 256].astype(F32) + add).astype(BF16)
        return 0

    lax.fori_loop(0, rows // 256, block, 0)


def places():
    me = lax.axis_index("data")
    core = lax.rem(me, 2)
    x_pos = lax.rem(me // 2, 2)
    y_pos = me // 4
    x_peer = me + 2 - 4 * x_pos
    y_peer = me + 4 - 8 * y_pos
    return me, core, y_pos, x_peer, y_peer, x_peer + 4 - 8 * y_pos


def gather_kernel(dims, grad_hbm, master_hbm, one_hbm, two_hbm, tok_hbm,
                  p0, p1, p2, p3, p4, p5, master_out, one_out, two_out, w_in, w_out, hidden_ref,
                  grad_v, master_v, one_v, two_v,
                  part_ref, wide_ref, normed_ref, active_ref,
                  load_sem, grad_sem, part_send, part_recv, send_sem, recv_sem):
    layers, model_dim, hidden_dim, rows, chunks = dims
    in_rows = chunks * LANES // hidden_dim
    out_rows = chunks * LANES // model_dim

    me, core, y_pos, x_peer, y_peer, diag = places()
    partner = me + 1 - 2 * core

    state = ((grad_hbm, grad_v), (master_hbm, master_v), (one_hbm, one_v), (two_hbm, two_v))

    def load(which, layer):
        src, dst = state[which]
        return pltpu.make_async_copy(src.at[:, layer, :], dst.at[layer], load_sem.at[which, layer])

    loads = 9
    span = chunks // loads

    def grad_load(layer, part):
        at = pl.ds(part * span, span)
        return pltpu.make_async_copy(grad_hbm.at[at, layer, :], grad_v.at[layer, at], grad_sem.at[layer, part])

    for layer in range(layers):
        for part in range(loads):
            grad_load(layer, part).start()
    tok_load = pltpu.make_async_copy(tok_hbm, hidden_ref, load_sem.at[4, 0])

    barrier = pltpu.get_barrier_semaphore()
    for step in range(1, GROUP):
        pl.semaphore_signal(barrier, inc=1, device_id=(lax.rem(me + step, GROUP),), device_id_type=MESH)

    sums = tuple(jnp.zeros((8, LANES), F32) for _ in range(8))
    for layer in range(layers):
        for part in range(loads):
            grad_load(layer, part).wait()
            if layer == layers - 1 and part == loads - 1:
                for which in range(1, 4):
                    load(which, 0).start()

            def square(idx, carry):
                base = pl.multiple_of(part * span + idx * 64, 64)
                block = grad_v[layer, pl.ds(base, 64), :]
                return tuple(carry[k] + block[8 * k:8 * k + 8] * block[8 * k:8 * k + 8] for k in range(8))

            sums = lax.fori_loop(0, span // 64, square, sums)
    mine = ((sums[0] + sums[1]) + (sums[2] + sums[3])) + ((sums[4] + sums[5]) + (sums[6] + sums[7]))
    part_ref[me] = jnp.sum(mine, axis=0, keepdims=True)
    pl.semaphore_wait(barrier, GROUP - 1)

    def part_copy(step):
        return pltpu.make_async_remote_copy(
            src_ref=part_ref.at[me], dst_ref=part_ref.at[me],
            send_sem=part_send.at[step], recv_sem=part_recv.at[step],
            device_id=(lax.rem(me + step, GROUP),), device_id_type=MESH)

    def part_arrival(step):
        slot = lax.rem(me + GROUP - step, GROUP)
        return pltpu.make_async_remote_copy(
            src_ref=part_ref.at[slot], dst_ref=part_ref.at[slot],
            send_sem=part_send.at[step], recv_sem=part_recv.at[step],
            device_id=(me,), device_id_type=MESH)

    for step in range(1, GROUP):
        part_copy(step).start()
    for item in range(1, layers):
        for which in range(1, 4):
            load(which, item).start()
    tok_load.start()
    for step in range(1, GROUP):
        part_arrival(step).wait_recv()
    total = part_ref[0]
    for slot in range(1, GROUP):
        total = total + part_ref[slot]
    total = jnp.sum(total, axis=1, keepdims=True)
    clip = jnp.minimum(1.0, CLIP_NORM / jnp.sqrt(total))
    clip = jnp.broadcast_to(clip, (8, LANES))

    slots = {}

    def piece(kind, layer, device, part):
        ref, count = ((w_in, in_rows), (w_out, out_rows))[kind]
        span = count // part[1]
        at = lax.rem(device, 4) * count + part[0] * span
        return ref.at[layer, pl.ds(pl.multiple_of(at, 8), span), :]

    def copies(kind, layer, device, route, target, parts):
        out = []
        for part in parts:
            ref = piece(kind, layer, device, part)
            index = slots.setdefault((route, layer, part), len(slots))
            out.append(pltpu.make_async_remote_copy(
                src_ref=ref, dst_ref=ref, send_sem=send_sem.at[index],
                recv_sem=recv_sem.at[index], device_id=(target,), device_id_type=MESH))
        return out

    def start(items):
        for item in items:
            item.start()

    def arrive(items):
        for item in items:
            item.wait_recv()

    def left(items):
        for item in items:
            item.wait_send()

    def own_parts(layer):
        return ((0, 6), (1, 6), (2, 6), (1, 2)) if layer == 0 else ((0, 2), (1, 2))

    def far_parts(layer, half):
        return ((3 * half, 6), (3 * half + 1, 6), (6 * half + 4, 12), (6 * half + 5, 12)) if layer == layers - 1 else ((half, 2),)

    def own_x(kind, layer, device, target, parts=None):
        return copies(kind, layer, device, "own_x", target, parts or own_parts(layer))

    def own_y(kind, layer, device, target, parts=None):
        return copies(kind, layer, device, "own_y", target, parts or own_parts(layer))

    def far(kind, layer, half, device, target, parts=None):
        return copies(kind, layer, device, "far", target, parts or far_parts(layer, half))

    def pair(kind, layer, device, route, parts):
        return copies(kind, layer, device, route, partner, parts)

    def by_kind(function):
        for y_value in range(2):
            @pl.when(y_pos == y_value)
            def _():
                function(y_value)

    one_scale = 1.0 / (1.0 - BETA_ONE ** ADAM_STEP)
    two_scale = 1.0 / (1.0 - BETA_TWO ** ADAM_STEP)

    def adam(layer, part):
        first = part[0] * (chunks // part[1])

        def update(idx, _):
            base = pl.multiple_of(first + idx * 48, 8)
            for k in range(6):
                at = pl.ds(pl.multiple_of(base + 8 * k, 8), 8)
                clipped = grad_v[layer, at, :] * clip
                new_one = BETA_ONE * one_v[layer, at, :] + (1.0 - BETA_ONE) * clipped
                new_two = BETA_TWO * two_v[layer, at, :] + (1.0 - BETA_TWO) * clipped * clipped
                step_size = (new_one * one_scale) / (jnp.sqrt(new_two * two_scale) + ADAM_EPS)
                old = master_v[layer, at, :]
                master_out[layer, at, :] = old - LEARN_RATE * (step_size + WEIGHT_DECAY * old)
                one_out[layer, at, :] = new_one
                two_out[layer, at, :] = new_two
            return 0

        lax.fori_loop(0, chunks // part[1] // 48, update, 0)

    def round_rows(kind, layer, part):
        width = hidden_dim if kind == 0 else model_dim
        count = in_rows if kind == 0 else out_rows
        per_row = width // LANES
        dst = w_in if kind == 0 else w_out
        slot = lax.rem(me, 4)

        def body(idx, _):
            base = part[0] * (chunks // part[1]) + idx * (16 * per_row)
            row = pl.multiple_of(slot * count + part[0] * (count // part[1]) + idx * 16, 16)
            for col in range(per_row):
                top = master_out[layer, pl.ds(base + col, 8, stride=per_row), :]
                low = master_out[layer, pl.ds(base + 8 * per_row + col, 8, stride=per_row), :]
                dst[layer, pl.ds(row, 16), col * LANES:(col + 1) * LANES] = jnp.concatenate([top, low], axis=0).astype(BF16)
            return 0

        lax.fori_loop(0, count // 16 // part[1], body, 0)

    for layer in range(layers):
        for which in range(1, 4):
            load(which, layer).wait()
        for part in own_parts(layer):
            adam(layer, part)

            def send_own(kind):
                round_rows(kind, layer, part)
                if layer < layers - 1:
                    start(own_x(kind, layer, me, x_peer, (part,)))
                    start(own_y(kind, layer, me, y_peer, (part,)))
                start(pair(kind, layer, me, "pair_own", (part,)))

            by_kind(send_own)

    def pack(kind, device, packed_ref):
        spread_piece(dims, kind, device, (w_in, w_out), wide_ref)

        def squeeze(idx, _):
            at = pl.ds(pl.multiple_of(idx * 256, 256), 256)
            packed_ref[at, :] = wide_ref[at, :].astype(BF16)
            return 0

        lax.fori_loop(0, 4 * chunks // 256, squeeze, 0)

    def partner_of(device):
        return device + 1 - 2 * core

    def drain(kind):
        for layer in range(layers):
            left(own_x(kind, layer, me, x_peer))
            left(own_y(kind, layer, me, y_peer))
            left(pair(kind, layer, me, "pair_own", own_parts(layer)))
            left(pair(kind, layer, x_peer, "pair_x", own_parts(layer)))
            left(pair(1 - kind, layer, y_peer, "pair_y", own_parts(layer)))
            if layer < layers - 1:
                left(pair(1 - kind, layer, diag, "pair_far", far_parts(layer, 0) + far_parts(layer, 1)))
                left(far(kind, layer, 0, x_peer, y_peer))
                left(far(1 - kind, layer, 1, y_peer, x_peer))
        for step in range(1, GROUP):
            part_copy(step).wait_send()

    def drain_last(kind):
        layer = layers - 1
        left(far(kind, layer, 0, x_peer, y_peer))
        left(far(1 - kind, layer, 1, y_peer, x_peer))
        left(pair(1 - kind, layer, diag, "pair_far", far_parts(layer, 0) + far_parts(layer, 1)))

    def forward(kind, layer):
        x_order = own_parts(layer)
        y_order = x_order[::-1] if layer == layers - 1 else x_order
        for x_part, y_part in zip(x_order, y_order):
            arrive(own_x(kind, layer, x_peer, me, (x_part,)))
            if x_part in ((0, 2), (2, 6)):
                start(far(kind, layer, 0, x_peer, y_peer))
            start(pair(kind, layer, x_peer, "pair_x", (x_part,)))
            arrive(own_y(1 - kind, layer, y_peer, me, (y_part,)))
            if y_part == (1, 2):
                start(far(1 - kind, layer, 1, y_peer, x_peer))
            start(pair(1 - kind, layer, y_peer, "pair_y", (y_part,)))

    def far_arrive(kind, layer, only=None):
        for idx, parts in enumerate(zip(far_parts(layer, 0), far_parts(layer, 1))):
            if only is not None and idx != only:
                continue
            for half in range(2):
                arrive(far(1 - kind, layer, half, diag, me, (parts[half],)))
                start(pair(1 - kind, layer, diag, "pair_far", (parts[half],)))

    def far_partner(kind, layer):
        arrive(pair(1 - kind, layer, partner_of(diag), "pair_far", far_parts(layer, 0) + far_parts(layer, 1)))

    def near_partner(kind, layer):
        arrive(pair(kind, layer, partner_of(x_peer), "pair_x", own_parts(layer)))
        arrive(pair(1 - kind, layer, partner_of(y_peer), "pair_y", own_parts(layer)))

    def stage_own(kind):
        pack(kind, me, p0)
        forward(kind, 0)
        for layer in range(layers):
            arrive(pair(kind, layer, partner, "pair_own", own_parts(layer)))
        pack(kind, partner, p1)
        forward(kind, 1)
        start(own_x(kind, layers - 1, me, x_peer))
        start(own_y(kind, layers - 1, me, y_peer)[::-1])
        near_partner(kind, 0)
        far_arrive(kind, 0)
        near_partner(kind, 1)
        far_partner(kind, 0)

    def stage_one(kind):
        far_arrive(kind, 1)
        far_partner(kind, 1)

    def stage_two(kind):
        forward(kind, 2)
        pack(kind, x_peer, p2)
        pack(1 - kind, y_peer, p4)
        near_partner(kind, 2)
        far_arrive(kind, 2, 0)
        pack(kind, partner_of(x_peer), p3)
        far_arrive(kind, 2, 1)
        pack(1 - kind, partner_of(y_peer), p5)
        drain(kind)
        far_arrive(kind, 2, 2)
        far_arrive(kind, 2, 3)
        far_partner(kind, 2)
        drain_last(kind)

    by_kind(stage_own)
    tok_load.wait()
    mlp_block(dims, 0, w_in, w_out, hidden_ref, normed_ref, active_ref)
    by_kind(stage_one)
    mlp_block(dims, 1, w_in, w_out, hidden_ref, normed_ref, active_ref)
    by_kind(stage_two)


def finish_kernel(dims, p0, p1, p2, p3, p4, p5, master_ref, one_ref, two_ref, w_in, w_out, last_ref, tgt_ref,
                  packed_hbm, master_hbm, one_hbm, two_hbm, loss_hbm,
                  loss_ref, far_ref, wide_ref, normed_ref, active_ref, hidden_ref, sem, far_sem):
    layers, model_dim, hidden_dim, rows, chunks = dims
    me, core, y_pos, x_peer, y_peer, diag = places()
    twin = 1 - 2 * core

    copies = []
    for which, (src, dst) in enumerate(((master_ref, master_hbm), (one_ref, one_hbm), (two_ref, two_hbm))):
        for layer in range(layers):
            copies.append(pltpu.make_async_copy(src.at[layer], dst.at[:, layer, :], sem.at[6 + which * layers + layer]))
    for idx, (ref, device) in enumerate(((p0, me), (p1, me + twin), (p2, x_peer), (p3, x_peer + twin), (p4, y_peer), (p5, y_peer + twin))):
        copies.append(pltpu.make_async_copy(ref, packed_hbm.at[pl.ds(device * chunks, chunks)], sem.at[idx]))
    for item in copies:
        item.start()

    far_copies = []
    for idx, device in enumerate((diag, diag + twin)):
        for y_value in range(2):
            @pl.when(y_pos == y_value)
            def _():
                spread_piece(dims, 1 - y_value, device, (w_in, w_out), wide_ref)

        def squeeze(at, _):
            block = wide_ref[pl.ds(pl.multiple_of(at * 128, 128), 128), :].astype(BF16).reshape(32, 4, LANES)
            far_ref[idx, pl.ds(at * 32, 32), :, :] = block[:, :layers, :]
            return 0

        lax.fori_loop(0, 4 * chunks // 128, squeeze, 0)
        far_copies.append(pltpu.make_async_copy(far_ref.at[idx], packed_hbm.at[pl.ds(device * chunks, chunks)], far_sem.at[idx]))
        far_copies[-1].start()

    hidden_ref[...] = last_ref[...]
    mlp_block(dims, layers - 1, w_in, w_out, hidden_ref, normed_ref, active_ref)

    for idx in range(rows // LANES):
        at = slice(idx * LANES, (idx + 1) * LANES)
        error = hidden_ref[at, :].astype(F32) - tgt_ref[at, :].astype(F32)
        error = error * error
        folded = error[:, 0:LANES]
        for col in range(LANES, model_dim, LANES):
            folded = folded + error[:, col:col + LANES]
        loss_ref[idx:idx + 1, :] = jnp.sum(folded.T, axis=0, keepdims=True) * (1.0 / model_dim)

    loss_copy = pltpu.make_async_copy(loss_ref, loss_hbm, far_sem.at[2])
    loss_copy.start()
    for item in copies + far_copies + [loss_copy]:
        item.wait()


def solution(mesh):
    group_size = mesh.shape["data"]
    state_spec = P(None, "data")
    row_spec = P("data", None)

    def local_step(grad_shard, master_shard, one_shard, two_shard, tok_rows, tgt_rows):
        rows, model_dim = tok_rows.shape
        layers, cols = master_shard.shape
        half_size = cols * group_size // 2
        hidden_dim = half_size // model_dim
        chunks = cols // LANES
        dims = (layers, model_dim, hidden_dim, rows, chunks)
        tiled = [a.reshape(layers, chunks, LANES).transpose(1, 0, 2) for a in (grad_shard, master_shard, one_shard, two_shard)]
        state_v = pltpu.VMEM((layers, chunks, LANES), F32)
        hbm = pl.BlockSpec(memory_space=pltpu.HBM)
        vmem = pl.BlockSpec(memory_space=pltpu.VMEM)
        state_out = state_v
        w_in_v = pltpu.VMEM((layers, model_dim, hidden_dim), BF16)
        w_out_v = pltpu.VMEM((layers, hidden_dim, model_dim), BF16)
        hidden_v = pltpu.VMEM((rows, model_dim), BF16)
        wide_v = pltpu.VMEM((4 * chunks, LANES), F32)
        normed_v = pltpu.VMEM((256, model_dim), BF16)
        active_v = pltpu.VMEM((256, hidden_dim), BF16)
        packed_v = pltpu.VMEM((4 * chunks, LANES), BF16)
        gathered = pl.pallas_call(
            functools.partial(gather_kernel, dims),
            name="gather_step",
            out_shape=(*(packed_v,) * 6, state_v, state_v, state_v, w_in_v, w_out_v, hidden_v),
            in_specs=[hbm] * 5,
            out_specs=(vmem,) * 12,
            scratch_shapes=[
                state_v, state_v, state_v, state_v,
                pltpu.VMEM((group_size, 1, LANES), F32),
                wide_v, normed_v, active_v,
                pltpu.SemaphoreType.DMA((5, layers)),
                pltpu.SemaphoreType.DMA((layers, 9)),
                pltpu.SemaphoreType.DMA((group_size,)),
                pltpu.SemaphoreType.DMA((group_size,)),
                pltpu.SemaphoreType.DMA((96,)),
                pltpu.SemaphoreType.DMA((96,)),
            ],
            compiler_params=pltpu.CompilerParams(collective_id=0, has_side_effects=True, vmem_limit_bytes=19 << 20),
        )(*[pltpu.with_memory_space_constraint(a, pltpu.HBM) for a in (*tiled, tok_rows)])
        gathered = [a.reshape(chunks, 4, LANES)[:, :layers, :] for a in gathered[:6]] + list(gathered[6:])
        state_tile = jax.ShapeDtypeStruct((chunks, layers, LANES), F32)
        weights, new_master, new_one, new_two, row_loss = pl.pallas_call(
            functools.partial(finish_kernel, dims),
            name="finish",
            out_shape=(jax.ShapeDtypeStruct((chunks * group_size, layers, LANES), BF16), state_tile, state_tile, state_tile,
                       jax.ShapeDtypeStruct((rows // LANES, LANES), F32)),
            in_specs=[vmem] * 13,
            out_specs=(hbm,) * 5,
            scratch_shapes=[
                pltpu.VMEM((rows // LANES, LANES), F32),
                pltpu.VMEM((2, chunks, layers, LANES), BF16),
                wide_v, normed_v, active_v, hidden_v,
                pltpu.SemaphoreType.DMA((6 + 3 * layers,)),
                pltpu.SemaphoreType.DMA((3,)),
            ],
            compiler_params=pltpu.CompilerParams(vmem_limit_bytes=14 << 20),
        )(*gathered, tgt_rows)

        def flat(a):
            return a.transpose(1, 0, 2).reshape(layers, a.shape[0] * LANES)

        return row_loss.reshape(rows), flat(weights), flat(new_master), flat(new_one), flat(new_two)

    return jax.shard_map(local_step, mesh=mesh, in_specs=(state_spec, state_spec, state_spec, state_spec, row_spec, row_spec), out_specs=(P("data"), P(), state_spec, state_spec, state_spec), check_vma=False)
```

```python
import functools

import jax
import jax.numpy as jnp
from jax import lax
from jax.experimental import pallas as pl
from jax.experimental.pallas import tpu as pltpu
from jax.sharding import PartitionSpec as P

LEARN_RATE = 0.01
BETA_ONE = 0.9
BETA_TWO = 0.95
ADAM_EPS = 1e-8
WEIGHT_DECAY = 0.1
ADAM_STEP = 10
CLIP_NORM = 1.0
NORM_EPS = 1e-6

MESH = pl.DeviceIdType.MESH
LANES = 128
GROUP = 8
F32 = jnp.float32
BF16 = jnp.bfloat16


def spread_piece(dims, kind, device, weights, wide_ref):
    layers, model_dim, hidden_dim, rows, chunks = dims
    per_row = (hidden_dim if kind == 0 else model_dim) // LANES
    count = chunks // per_row
    src = weights[kind]
    slot = lax.rem(device, 4)

    def spread(idx, _):
        row = pl.multiple_of(slot * count + idx * 16, 16)
        for layer in range(layers):
            for col in range(per_row):
                tile = src[layer, pl.ds(row, 16), col * LANES:(col + 1) * LANES].astype(F32)
                base = layer + 4 * (idx * (16 * per_row) + col)
                wide_ref[pl.ds(base, 8, stride=4 * per_row), :] = tile[0:8]
                wide_ref[pl.ds(base + 32 * per_row, 8, stride=4 * per_row), :] = tile[8:16]
        return 0

    lax.fori_loop(0, count // 16, spread, 0)


def mlp_block(dims, layer, w_in, w_out, hidden_ref, normed_ref, active_ref):
    layers, model_dim, hidden_dim, rows, chunks = dims

    def block(idx, _):
        at = pl.ds(pl.multiple_of(idx * 256, 256), 256)
        hidden = hidden_ref[at, :].astype(F32)
        scale = lax.rsqrt(jnp.mean(hidden * hidden, axis=-1, keepdims=True) + NORM_EPS)
        normed_ref[...] = (hidden * scale).astype(BF16)
        for col in range(0, hidden_dim, 384):
            inner = jnp.dot(normed_ref[...], w_in[layer, :, col:col + 384], preferred_element_type=F32).astype(BF16)
            active_ref[:, col:col + 384] = jax.nn.gelu(inner.astype(F32), approximate=True).astype(BF16)
        for col in range(0, model_dim, 256):
            add = jnp.dot(active_ref[...], w_out[layer, :, col:col + 256], preferred_element_type=F32)
            hidden_ref[at, col:col + 256] = (hidden_ref[at, col:col + 256].astype(F32) + add).astype(BF16)
        return 0

    lax.fori_loop(0, rows // 256, block, 0)


def places():
    me = lax.axis_index("data")
    core = lax.rem(me, 2)
    x_pos = lax.rem(me // 2, 2)
    y_pos = me // 4
    x_peer = me + 2 - 4 * x_pos
    y_peer = me + 4 - 8 * y_pos
    return me, core, y_pos, x_peer, y_peer, x_peer + 4 - 8 * y_pos


def gather_kernel(dims, grad_hbm, master_hbm, one_hbm, two_hbm, tok_hbm,
                  p0, p1, p2, p3, p4, p5, master_out, one_out, two_out, w_in, w_out, hidden_ref,
                  grad_v, master_v, one_v, two_v,
                  part_ref, wide_ref, normed_ref, active_ref,
                  load_sem, grad_sem, part_send, part_recv, send_sem, recv_sem):
    layers, model_dim, hidden_dim, rows, chunks = dims
    in_rows = chunks * LANES // hidden_dim
    out_rows = chunks * LANES // model_dim

    me, core, y_pos, x_peer, y_peer, diag = places()
    partner = me + 1 - 2 * core

    state = ((grad_hbm, grad_v), (master_hbm, master_v), (one_hbm, one_v), (two_hbm, two_v))

    def load(which, layer):
        src, dst = state[which]
        return pltpu.make_async_copy(src.at[:, layer, :], dst.at[layer], load_sem.at[which, layer])

    span = chunks // 3

    def grad_load(layer, part):
        at = pl.ds(part * span, span)
        return pltpu.make_async_copy(grad_hbm.at[at, layer, :], grad_v.at[layer, at], grad_sem.at[layer, part])

    for layer in range(layers):
        for part in range(3):
            grad_load(layer, part).start()
    tok_load = pltpu.make_async_copy(tok_hbm, hidden_ref, load_sem.at[4, 0])

    barrier = pltpu.get_barrier_semaphore()
    for step in range(1, GROUP):
        pl.semaphore_signal(barrier, inc=1, device_id=(lax.rem(me + step, GROUP),), device_id_type=MESH)

    sums = tuple(jnp.zeros((8, LANES), F32) for _ in range(8))
    for layer in range(layers):
        for part in range(3):
            grad_load(layer, part).wait()
            if layer == layers - 1 and part == 2:
                for which in range(1, 4):
                    load(which, 0).start()

            def square(idx, carry):
                base = pl.multiple_of(part * span + idx * 64, 64)
                block = grad_v[layer, pl.ds(base, 64), :]
                return tuple(carry[k] + block[8 * k:8 * k + 8] * block[8 * k:8 * k + 8] for k in range(8))

            sums = lax.fori_loop(0, span // 64, square, sums)
    mine = ((sums[0] + sums[1]) + (sums[2] + sums[3])) + ((sums[4] + sums[5]) + (sums[6] + sums[7]))
    part_ref[me] = jnp.sum(mine, axis=0, keepdims=True)
    pl.semaphore_wait(barrier, GROUP - 1)

    def part_copy(step):
        return pltpu.make_async_remote_copy(
            src_ref=part_ref.at[me], dst_ref=part_ref.at[me],
            send_sem=part_send.at[step], recv_sem=part_recv.at[step],
            device_id=(lax.rem(me + step, GROUP),), device_id_type=MESH)

    def part_arrival(step):
        slot = lax.rem(me + GROUP - step, GROUP)
        return pltpu.make_async_remote_copy(
            src_ref=part_ref.at[slot], dst_ref=part_ref.at[slot],
            send_sem=part_send.at[step], recv_sem=part_recv.at[step],
            device_id=(me,), device_id_type=MESH)

    for step in range(1, GROUP):
        part_copy(step).start()
    for item in range(1, layers):
        for which in range(1, 4):
            load(which, item).start()
    tok_load.start()
    for step in range(1, GROUP):
        part_arrival(step).wait_recv()
    total = part_ref[0]
    for slot in range(1, GROUP):
        total = total + part_ref[slot]
    total = jnp.sum(total, axis=1, keepdims=True)
    clip = jnp.minimum(1.0, CLIP_NORM / jnp.sqrt(total))
    clip = jnp.broadcast_to(clip, (8, LANES))

    slots = {}

    def piece(kind, layer, device, part):
        ref, count = ((w_in, in_rows), (w_out, out_rows))[kind]
        span = count // part[1]
        at = lax.rem(device, 4) * count + part[0] * span
        return ref.at[layer, pl.ds(pl.multiple_of(at, 16), span), :]

    def copies(kind, layer, device, route, target, parts):
        out = []
        for part in parts:
            ref = piece(kind, layer, device, part)
            index = slots.setdefault((route, layer, part), len(slots))
            out.append(pltpu.make_async_remote_copy(
                src_ref=ref, dst_ref=ref, send_sem=send_sem.at[index],
                recv_sem=recv_sem.at[index], device_id=(target,), device_id_type=MESH))
        return out

    def start(items):
        for item in items:
            item.start()

    def arrive(items):
        for item in items:
            item.wait_recv()

    def left(items):
        for item in items:
            item.wait_send()

    def own_parts(layer):
        return ((0, 6), (1, 6), (2, 6), (1, 2)) if layer == 0 else ((0, 2), (1, 2))

    def far_parts(layer, half):
        return tuple((3 * half + at, 6) for at in range(3)) if layer == layers - 1 else ((half, 2),)

    def own_x(kind, layer, device, target, parts=None):
        return copies(kind, layer, device, "own_x", target, parts or own_parts(layer))

    def own_y(kind, layer, device, target, parts=None):
        return copies(kind, layer, device, "own_y", target, parts or own_parts(layer))

    def far(kind, layer, half, device, target, parts=None):
        return copies(kind, layer, device, "far", target, parts or far_parts(layer, half))

    def pair(kind, layer, device, route, parts):
        return copies(kind, layer, device, route, partner, parts)

    def by_kind(function):
        for y_value in range(2):
            @pl.when(y_pos == y_value)
            def _():
                function(y_value)

    one_scale = 1.0 / (1.0 - BETA_ONE ** ADAM_STEP)
    two_scale = 1.0 / (1.0 - BETA_TWO ** ADAM_STEP)

    def adam(layer, part):
        first = part[0] * (chunks // part[1])

        def update(idx, _):
            base = pl.multiple_of(first + idx * 48, 8)
            for k in range(6):
                at = pl.ds(pl.multiple_of(base + 8 * k, 8), 8)
                clipped = grad_v[layer, at, :] * clip
                new_one = BETA_ONE * one_v[layer, at, :] + (1.0 - BETA_ONE) * clipped
                new_two = BETA_TWO * two_v[layer, at, :] + (1.0 - BETA_TWO) * clipped * clipped
                step_size = (new_one * one_scale) / (jnp.sqrt(new_two * two_scale) + ADAM_EPS)
                old = master_v[layer, at, :]
                master_out[layer, at, :] = old - LEARN_RATE * (step_size + WEIGHT_DECAY * old)
                one_out[layer, at, :] = new_one
                two_out[layer, at, :] = new_two
            return 0

        lax.fori_loop(0, chunks // part[1] // 48, update, 0)

    def round_rows(kind, layer, part):
        width = hidden_dim if kind == 0 else model_dim
        count = in_rows if kind == 0 else out_rows
        per_row = width // LANES
        dst = w_in if kind == 0 else w_out
        slot = lax.rem(me, 4)

        def body(idx, _):
            base = part[0] * (chunks // part[1]) + idx * (16 * per_row)
            row = pl.multiple_of(slot * count + part[0] * (count // part[1]) + idx * 16, 16)
            for col in range(per_row):
                top = master_out[layer, pl.ds(base + col, 8, stride=per_row), :]
                low = master_out[layer, pl.ds(base + 8 * per_row + col, 8, stride=per_row), :]
                dst[layer, pl.ds(row, 16), col * LANES:(col + 1) * LANES] = jnp.concatenate([top, low], axis=0).astype(BF16)
            return 0

        lax.fori_loop(0, count // 16 // part[1], body, 0)

    for layer in range(layers):
        for which in range(1, 4):
            load(which, layer).wait()
        for part in own_parts(layer):
            adam(layer, part)

            def send_own(kind):
                round_rows(kind, layer, part)
                if layer < layers - 1:
                    start(own_x(kind, layer, me, x_peer, (part,)))
                    start(own_y(kind, layer, me, y_peer, (part,)))
                start(pair(kind, layer, me, "pair_own", (part,)))

            by_kind(send_own)

    def pack(kind, device, packed_ref):
        spread_piece(dims, kind, device, (w_in, w_out), wide_ref)

        def squeeze(idx, _):
            at = pl.ds(pl.multiple_of(idx * 256, 256), 256)
            packed_ref[at, :] = wide_ref[at, :].astype(BF16)
            return 0

        lax.fori_loop(0, 4 * chunks // 256, squeeze, 0)

    def partner_of(device):
        return device + 1 - 2 * core

    def drain(kind):
        for layer in range(layers):
            left(own_x(kind, layer, me, x_peer))
            left(own_y(kind, layer, me, y_peer))
            left(pair(kind, layer, me, "pair_own", own_parts(layer)))
            left(pair(kind, layer, x_peer, "pair_x", own_parts(layer)))
            left(pair(1 - kind, layer, y_peer, "pair_y", own_parts(layer)))
            if layer < layers - 1:
                left(pair(1 - kind, layer, diag, "pair_far", far_parts(layer, 0) + far_parts(layer, 1)))
                left(far(kind, layer, 0, x_peer, y_peer))
                left(far(1 - kind, layer, 1, y_peer, x_peer))
        for step in range(1, GROUP):
            part_copy(step).wait_send()

    def drain_last(kind):
        layer = layers - 1
        left(far(kind, layer, 0, x_peer, y_peer))
        left(far(1 - kind, layer, 1, y_peer, x_peer))
        left(pair(1 - kind, layer, diag, "pair_far", far_parts(layer, 0) + far_parts(layer, 1)))

    def forward(kind, layer):
        x_order = own_parts(layer)
        y_order = x_order[::-1] if layer == layers - 1 else x_order
        for x_part, y_part in zip(x_order, y_order):
            arrive(own_x(kind, layer, x_peer, me, (x_part,)))
            if x_part in ((0, 2), (2, 6)):
                start(far(kind, layer, 0, x_peer, y_peer))
            start(pair(kind, layer, x_peer, "pair_x", (x_part,)))
            arrive(own_y(1 - kind, layer, y_peer, me, (y_part,)))
            if y_part == (1, 2):
                start(far(1 - kind, layer, 1, y_peer, x_peer))
            start(pair(1 - kind, layer, y_peer, "pair_y", (y_part,)))

    def far_arrive(kind, layer, only=None):
        for idx, parts in enumerate(zip(far_parts(layer, 0), far_parts(layer, 1))):
            if only is not None and idx != only:
                continue
            for half in range(2):
                arrive(far(1 - kind, layer, half, diag, me, (parts[half],)))
                start(pair(1 - kind, layer, diag, "pair_far", (parts[half],)))

    def far_partner(kind, layer):
        arrive(pair(1 - kind, layer, partner_of(diag), "pair_far", far_parts(layer, 0) + far_parts(layer, 1)))

    def near_partner(kind, layer):
        arrive(pair(kind, layer, partner_of(x_peer), "pair_x", own_parts(layer)))
        arrive(pair(1 - kind, layer, partner_of(y_peer), "pair_y", own_parts(layer)))

    def stage_own(kind):
        pack(kind, me, p0)
        forward(kind, 0)
        for layer in range(layers):
            arrive(pair(kind, layer, partner, "pair_own", own_parts(layer)))
        pack(kind, partner, p1)
        forward(kind, 1)
        start(own_x(kind, layers - 1, me, x_peer))
        start(own_y(kind, layers - 1, me, y_peer)[::-1])
        near_partner(kind, 0)
        far_arrive(kind, 0)
        near_partner(kind, 1)
        far_partner(kind, 0)

    def stage_one(kind):
        far_arrive(kind, 1)
        far_partner(kind, 1)

    def stage_two(kind):
        forward(kind, 2)
        pack(kind, x_peer, p2)
        pack(1 - kind, y_peer, p4)
        near_partner(kind, 2)
        far_arrive(kind, 2, 0)
        pack(kind, partner_of(x_peer), p3)
        far_arrive(kind, 2, 1)
        pack(1 - kind, partner_of(y_peer), p5)
        drain(kind)
        far_arrive(kind, 2, 2)
        far_partner(kind, 2)
        drain_last(kind)

    by_kind(stage_own)
    tok_load.wait()
    mlp_block(dims, 0, w_in, w_out, hidden_ref, normed_ref, active_ref)
    by_kind(stage_one)
    mlp_block(dims, 1, w_in, w_out, hidden_ref, normed_ref, active_ref)
    by_kind(stage_two)


def finish_kernel(dims, p0, p1, p2, p3, p4, p5, master_ref, one_ref, two_ref, w_in, w_out, last_ref, tgt_ref,
                  packed_hbm, master_hbm, one_hbm, two_hbm, loss_hbm,
                  loss_ref, far_ref, wide_ref, normed_ref, active_ref, hidden_ref, sem, far_sem):
    layers, model_dim, hidden_dim, rows, chunks = dims
    me, core, y_pos, x_peer, y_peer, diag = places()
    twin = 1 - 2 * core

    copies = []
    span = chunks // 3
    for which, (src, dst) in enumerate(((master_ref, master_hbm), (one_ref, one_hbm), (two_ref, two_hbm))):
        for layer in range(layers):
            for part in range(3):
                at = pl.ds(part * span, span)
                copies.append(pltpu.make_async_copy(src.at[layer, at], dst.at[at, layer, :], sem.at[len(copies)]))
    for idx, (ref, device) in enumerate(((p0, me), (p1, me + twin), (p2, x_peer), (p3, x_peer + twin), (p4, y_peer), (p5, y_peer + twin))):
        for part in range(3):
            copies.append(pltpu.make_async_copy(ref.at[pl.ds(part * span, span)], packed_hbm.at[pl.ds(device * chunks + part * span, span)], sem.at[len(copies)]))
    for item in copies:
        item.start()

    far_copies = []
    for idx, device in enumerate((diag, diag + twin)):
        for y_value in range(2):
            @pl.when(y_pos == y_value)
            def _():
                spread_piece(dims, 1 - y_value, device, (w_in, w_out), wide_ref)

        def squeeze(at, _):
            block = wide_ref[pl.ds(pl.multiple_of(at * 128, 128), 128), :].astype(BF16).reshape(32, 4, LANES)
            far_ref[idx, pl.ds(at * 32, 32), :, :] = block[:, :layers, :]
            return 0

        lax.fori_loop(0, 4 * chunks // 128, squeeze, 0)
        for part in range(3):
            far_copies.append(pltpu.make_async_copy(far_ref.at[idx, pl.ds(part * span, span)], packed_hbm.at[pl.ds(device * chunks + part * span, span)], far_sem.at[3 * idx + part]))
            far_copies[-1].start()

    hidden_ref[...] = last_ref[...]
    mlp_block(dims, layers - 1, w_in, w_out, hidden_ref, normed_ref, active_ref)

    for idx in range(rows // LANES):
        at = slice(idx * LANES, (idx + 1) * LANES)
        error = hidden_ref[at, :].astype(F32) - tgt_ref[at, :].astype(F32)
        error = error * error
        folded = error[:, 0:LANES]
        for col in range(LANES, model_dim, LANES):
            folded = folded + error[:, col:col + LANES]
        loss_ref[idx:idx + 1, :] = jnp.sum(folded.T, axis=0, keepdims=True) * (1.0 / model_dim)

    loss_copy = pltpu.make_async_copy(loss_ref, loss_hbm, far_sem.at[6])
    loss_copy.start()
    for item in copies + far_copies + [loss_copy]:
        item.wait()


def solution(mesh):
    group_size = mesh.shape["data"]
    state_spec = P(None, "data")
    row_spec = P("data", None)

    def local_step(grad_shard, master_shard, one_shard, two_shard, tok_rows, tgt_rows):
        rows, model_dim = tok_rows.shape
        layers, cols = master_shard.shape
        half_size = cols * group_size // 2
        hidden_dim = half_size // model_dim
        chunks = cols // LANES
        dims = (layers, model_dim, hidden_dim, rows, chunks)
        tiled = [a.reshape(layers, chunks, LANES).transpose(1, 0, 2) for a in (grad_shard, master_shard, one_shard, two_shard)]
        state_v = pltpu.VMEM((layers, chunks, LANES), F32)
        hbm = pl.BlockSpec(memory_space=pltpu.HBM)
        vmem = pl.BlockSpec(memory_space=pltpu.VMEM)
        state_out = state_v
        w_in_v = pltpu.VMEM((layers, model_dim, hidden_dim), BF16)
        w_out_v = pltpu.VMEM((layers, hidden_dim, model_dim), BF16)
        hidden_v = pltpu.VMEM((rows, model_dim), BF16)
        wide_v = pltpu.VMEM((4 * chunks, LANES), F32)
        normed_v = pltpu.VMEM((256, model_dim), BF16)
        active_v = pltpu.VMEM((256, hidden_dim), BF16)
        packed_v = pltpu.VMEM((4 * chunks, LANES), BF16)
        gathered = pl.pallas_call(
            functools.partial(gather_kernel, dims),
            name="gather_step",
            out_shape=(*(packed_v,) * 6, state_v, state_v, state_v, w_in_v, w_out_v, hidden_v),
            in_specs=[hbm] * 5,
            out_specs=(vmem,) * 12,
            scratch_shapes=[
                state_v, state_v, state_v, state_v,
                pltpu.VMEM((group_size, 1, LANES), F32),
                wide_v, normed_v, active_v,
                pltpu.SemaphoreType.DMA((5, layers)),
                pltpu.SemaphoreType.DMA((layers, 3)),
                pltpu.SemaphoreType.DMA((group_size,)),
                pltpu.SemaphoreType.DMA((group_size,)),
                pltpu.SemaphoreType.DMA((96,)),
                pltpu.SemaphoreType.DMA((96,)),
            ],
            compiler_params=pltpu.CompilerParams(collective_id=0, has_side_effects=True, vmem_limit_bytes=19 << 20),
        )(*[pltpu.with_memory_space_constraint(a, pltpu.HBM) for a in (*tiled, tok_rows)])
        gathered = [a.reshape(chunks, 4, LANES)[:, :layers, :] for a in gathered[:6]] + list(gathered[6:])
        state_tile = jax.ShapeDtypeStruct((chunks, layers, LANES), F32)
        weights, new_master, new_one, new_two, row_loss = pl.pallas_call(
            functools.partial(finish_kernel, dims),
            name="finish",
            out_shape=(jax.ShapeDtypeStruct((chunks * group_size, layers, LANES), BF16), state_tile, state_tile, state_tile,
                       jax.ShapeDtypeStruct((rows // LANES, LANES), F32)),
            in_specs=[vmem] * 13,
            out_specs=(hbm,) * 5,
            scratch_shapes=[
                pltpu.VMEM((rows // LANES, LANES), F32),
                pltpu.VMEM((2, chunks, layers, LANES), BF16),
                wide_v, normed_v, active_v, hidden_v,
                pltpu.SemaphoreType.DMA((18 + 9 * layers,)),
                pltpu.SemaphoreType.DMA((7,)),
            ],
            compiler_params=pltpu.CompilerParams(vmem_limit_bytes=14 << 20),
        )(*gathered, tgt_rows)

        def flat(a):
            return a.transpose(1, 0, 2).reshape(layers, a.shape[0] * LANES)

        return row_loss.reshape(rows), flat(weights), flat(new_master), flat(new_one), flat(new_two)

    return jax.shard_map(local_step, mesh=mesh, in_specs=(state_spec, state_spec, state_spec, state_spec, row_spec, row_spec), out_specs=(P("data"), P(), state_spec, state_spec, state_spec), check_vma=False)
```

```python
import functools

import jax
import jax.numpy as jnp
from jax import lax
from jax.experimental import pallas as pl
from jax.experimental.pallas import tpu as pltpu
from jax.sharding import PartitionSpec as P

LEARN_RATE = 0.01
BETA_ONE = 0.9
BETA_TWO = 0.95
ADAM_EPS = 1e-8
WEIGHT_DECAY = 0.1
ADAM_STEP = 10
CLIP_NORM = 1.0
NORM_EPS = 1e-6

MESH = pl.DeviceIdType.MESH
LANES = 128
GROUP = 8
F32 = jnp.float32
BF16 = jnp.bfloat16


def spread_piece(dims, kind, device, weights, wide_ref):
    layers, model_dim, hidden_dim, rows, chunks = dims
    per_row = (hidden_dim if kind == 0 else model_dim) // LANES
    count = chunks // per_row
    src = weights[kind]
    slot = lax.rem(device, 4)

    def spread(idx, _):
        row = pl.multiple_of(slot * count + idx * 16, 16)
        for layer in range(layers):
            for col in range(per_row):
                tile = src[layer, pl.ds(row, 16), col * LANES:(col + 1) * LANES].astype(F32)
                base = layer + 4 * (idx * (16 * per_row) + col)
                wide_ref[pl.ds(base, 8, stride=4 * per_row), :] = tile[0:8]
                wide_ref[pl.ds(base + 32 * per_row, 8, stride=4 * per_row), :] = tile[8:16]
        return 0

    lax.fori_loop(0, count // 16, spread, 0)


def mlp_block(dims, layer, w_in, w_out, hidden_ref, normed_ref, active_ref):
    layers, model_dim, hidden_dim, rows, chunks = dims

    def block(idx, _):
        at = pl.ds(pl.multiple_of(idx * 256, 256), 256)
        hidden = hidden_ref[at, :].astype(F32)
        scale = lax.rsqrt(jnp.mean(hidden * hidden, axis=-1, keepdims=True) + NORM_EPS)
        normed_ref[...] = (hidden * scale).astype(BF16)
        for col in range(0, hidden_dim, 384):
            inner = jnp.dot(normed_ref[...], w_in[layer, :, col:col + 384], preferred_element_type=F32).astype(BF16)
            active_ref[:, col:col + 384] = jax.nn.gelu(inner.astype(F32), approximate=True).astype(BF16)
        for col in range(0, model_dim, 256):
            add = jnp.dot(active_ref[...], w_out[layer, :, col:col + 256], preferred_element_type=F32)
            hidden_ref[at, col:col + 256] = (hidden_ref[at, col:col + 256].astype(F32) + add).astype(BF16)
        return 0

    lax.fori_loop(0, rows // 256, block, 0)


def places():
    me = lax.axis_index("data")
    core = lax.rem(me, 2)
    x_pos = lax.rem(me // 2, 2)
    y_pos = me // 4
    x_peer = me + 2 - 4 * x_pos
    y_peer = me + 4 - 8 * y_pos
    return me, core, y_pos, x_peer, y_peer, x_peer + 4 - 8 * y_pos


def gather_kernel(dims, grad_hbm, master_hbm, one_hbm, two_hbm, tok_hbm,
                  p0, p1, p2, p3, p4, p5, master_out, one_out, two_out, w_in, w_out, hidden_ref,
                  grad_v, master_v, one_v, two_v,
                  part_ref, wide_ref, normed_ref, active_ref,
                  load_sem, grad_sem, part_send, part_recv, send_sem, recv_sem):
    layers, model_dim, hidden_dim, rows, chunks = dims
    in_rows = chunks * LANES // hidden_dim
    out_rows = chunks * LANES // model_dim

    me, core, y_pos, x_peer, y_peer, diag = places()
    partner = me + 1 - 2 * core

    state = ((grad_hbm, grad_v), (master_hbm, master_v), (one_hbm, one_v), (two_hbm, two_v))

    def load(which, layer):
        src, dst = state[which]
        return pltpu.make_async_copy(src.at[:, layer, :], dst.at[layer], load_sem.at[which, layer])

    span = chunks // 3

    def grad_load(layer, part):
        at = pl.ds(part * span, span)
        return pltpu.make_async_copy(grad_hbm.at[at, layer, :], grad_v.at[layer, at], grad_sem.at[layer, part])

    for layer in range(layers):
        for part in range(3):
            grad_load(layer, part).start()
    tok_load = pltpu.make_async_copy(tok_hbm, hidden_ref, load_sem.at[4, 0])

    barrier = pltpu.get_barrier_semaphore()
    for step in range(1, GROUP):
        pl.semaphore_signal(barrier, inc=1, device_id=(lax.rem(me + step, GROUP),), device_id_type=MESH)

    sums = tuple(jnp.zeros((8, LANES), F32) for _ in range(8))
    for layer in range(layers):
        for part in range(3):
            grad_load(layer, part).wait()
            if layer == layers - 1 and part == 2:
                for which in range(1, 4):
                    load(which, 0).start()

            def square(idx, carry):
                base = pl.multiple_of(part * span + idx * 64, 64)
                block = grad_v[layer, pl.ds(base, 64), :]
                return tuple(carry[k] + block[8 * k:8 * k + 8] * block[8 * k:8 * k + 8] for k in range(8))

            sums = lax.fori_loop(0, span // 64, square, sums)
    mine = ((sums[0] + sums[1]) + (sums[2] + sums[3])) + ((sums[4] + sums[5]) + (sums[6] + sums[7]))
    part_ref[me] = jnp.sum(mine, axis=0, keepdims=True)
    pl.semaphore_wait(barrier, GROUP - 1)

    def part_copy(step):
        return pltpu.make_async_remote_copy(
            src_ref=part_ref.at[me], dst_ref=part_ref.at[me],
            send_sem=part_send.at[step], recv_sem=part_recv.at[step],
            device_id=(lax.rem(me + step, GROUP),), device_id_type=MESH)

    def part_arrival(step):
        slot = lax.rem(me + GROUP - step, GROUP)
        return pltpu.make_async_remote_copy(
            src_ref=part_ref.at[slot], dst_ref=part_ref.at[slot],
            send_sem=part_send.at[step], recv_sem=part_recv.at[step],
            device_id=(me,), device_id_type=MESH)

    for step in range(1, GROUP):
        part_copy(step).start()
    for item in range(1, layers):
        for which in range(1, 4):
            load(which, item).start()
    tok_load.start()
    for step in range(1, GROUP):
        part_arrival(step).wait_recv()
    total = part_ref[0]
    for slot in range(1, GROUP):
        total = total + part_ref[slot]
    total = jnp.sum(total, axis=1, keepdims=True)
    clip = jnp.minimum(1.0, CLIP_NORM / jnp.sqrt(total))
    clip = jnp.broadcast_to(clip, (8, LANES))

    slots = {}

    def piece(kind, layer, device, part):
        ref, count = ((w_in, in_rows), (w_out, out_rows))[kind]
        span = count // part[1]
        at = lax.rem(device, 4) * count + part[0] * span
        return ref.at[layer, pl.ds(pl.multiple_of(at, 16), span), :]

    def copies(kind, layer, device, route, target, parts):
        out = []
        for part in parts:
            ref = piece(kind, layer, device, part)
            index = slots.setdefault((route, layer, part), len(slots))
            out.append(pltpu.make_async_remote_copy(
                src_ref=ref, dst_ref=ref, send_sem=send_sem.at[index],
                recv_sem=recv_sem.at[index], device_id=(target,), device_id_type=MESH))
        return out

    def start(items):
        for item in items:
            item.start()

    def arrive(items):
        for item in items:
            item.wait_recv()

    def left(items):
        for item in items:
            item.wait_send()

    def own_parts(layer):
        return ((0, 6), (1, 6), (2, 6), (1, 2)) if layer == 0 else ((0, 2), (1, 2))

    def far_parts(layer, half):
        return tuple((3 * half + at, 6) for at in range(3)) if layer == layers - 1 else ((half, 2),)

    def own_x(kind, layer, device, target, parts=None):
        return copies(kind, layer, device, "own_x", target, parts or own_parts(layer))

    def own_y(kind, layer, device, target, parts=None):
        return copies(kind, layer, device, "own_y", target, parts or own_parts(layer))

    def far(kind, layer, half, device, target, parts=None):
        return copies(kind, layer, device, "far", target, parts or far_parts(layer, half))

    def pair(kind, layer, device, route, parts):
        return copies(kind, layer, device, route, partner, parts)

    def by_kind(function):
        for y_value in range(2):
            @pl.when(y_pos == y_value)
            def _():
                function(y_value)

    one_scale = 1.0 / (1.0 - BETA_ONE ** ADAM_STEP)
    two_scale = 1.0 / (1.0 - BETA_TWO ** ADAM_STEP)

    def adam(layer, part):
        first = part[0] * (chunks // part[1])

        def update(idx, _):
            base = pl.multiple_of(first + idx * 48, 8)
            for k in range(6):
                at = pl.ds(pl.multiple_of(base + 8 * k, 8), 8)
                clipped = grad_v[layer, at, :] * clip
                new_one = BETA_ONE * one_v[layer, at, :] + (1.0 - BETA_ONE) * clipped
                new_two = BETA_TWO * two_v[layer, at, :] + (1.0 - BETA_TWO) * clipped * clipped
                step_size = (new_one * one_scale) / (jnp.sqrt(new_two * two_scale) + ADAM_EPS)
                old = master_v[layer, at, :]
                master_out[layer, at, :] = old - LEARN_RATE * (step_size + WEIGHT_DECAY * old)
                one_out[layer, at, :] = new_one
                two_out[layer, at, :] = new_two
            return 0

        lax.fori_loop(0, chunks // part[1] // 48, update, 0)

    def round_rows(kind, layer, part):
        width = hidden_dim if kind == 0 else model_dim
        count = in_rows if kind == 0 else out_rows
        per_row = width // LANES
        dst = w_in if kind == 0 else w_out
        slot = lax.rem(me, 4)

        def body(idx, _):
            base = part[0] * (chunks // part[1]) + idx * (16 * per_row)
            row = pl.multiple_of(slot * count + part[0] * (count // part[1]) + idx * 16, 16)
            for col in range(per_row):
                top = master_out[layer, pl.ds(base + col, 8, stride=per_row), :]
                low = master_out[layer, pl.ds(base + 8 * per_row + col, 8, stride=per_row), :]
                dst[layer, pl.ds(row, 16), col * LANES:(col + 1) * LANES] = jnp.concatenate([top, low], axis=0).astype(BF16)
            return 0

        lax.fori_loop(0, count // 16 // part[1], body, 0)

    for layer in range(layers):
        for which in range(1, 4):
            load(which, layer).wait()
        for part in own_parts(layer):
            adam(layer, part)

            def send_own(kind):
                round_rows(kind, layer, part)
                if layer < layers - 1:
                    start(own_x(kind, layer, me, x_peer, (part,)))
                    start(own_y(kind, layer, me, y_peer, (part,)))
                start(pair(kind, layer, me, "pair_own", (part,)))

            by_kind(send_own)

    def pack(kind, device, packed_ref):
        spread_piece(dims, kind, device, (w_in, w_out), wide_ref)

        def squeeze(idx, _):
            at = pl.ds(pl.multiple_of(idx * 256, 256), 256)
            packed_ref[at, :] = wide_ref[at, :].astype(BF16)
            return 0

        lax.fori_loop(0, 4 * chunks // 256, squeeze, 0)

    def partner_of(device):
        return device + 1 - 2 * core

    def drain(kind):
        for layer in range(layers):
            left(own_x(kind, layer, me, x_peer))
            left(own_y(kind, layer, me, y_peer))
            left(pair(kind, layer, me, "pair_own", own_parts(layer)))
            left(pair(kind, layer, x_peer, "pair_x", own_parts(layer)))
            left(pair(1 - kind, layer, y_peer, "pair_y", own_parts(layer)))
            if layer < layers - 1:
                left(pair(1 - kind, layer, diag, "pair_far", far_parts(layer, 0) + far_parts(layer, 1)))
                left(far(kind, layer, 0, x_peer, y_peer))
                left(far(1 - kind, layer, 1, y_peer, x_peer))
        for step in range(1, GROUP):
            part_copy(step).wait_send()

    def last_parts(half):
        return far_parts(layers - 1, half)[-1:]

    def start_far(kind, layer, half, device, target):
        if layer < layers - 1:
            start(far(kind, layer, half, device, target))
            return
        start(far(kind, layer, half, device, target, far_parts(layer, half)[:-1]))

        @pl.when(core == 1)
        def _():
            start(far(kind, layer, half, device, target, last_parts(half)))

    def extra(kind, half, device, route, target):
        return copies(kind, layers - 1, device, route, target, last_parts(half))

    def forward(kind, layer):
        x_order = own_parts(layer)
        y_order = x_order[::-1] if layer == layers - 1 else x_order
        for x_part, y_part in zip(x_order, y_order):
            arrive(own_x(kind, layer, x_peer, me, (x_part,)))
            if x_part in ((0, 2), (2, 6)):
                start_far(kind, layer, 0, x_peer, y_peer)
            start(pair(kind, layer, x_peer, "pair_x", (x_part,)))
            arrive(own_y(1 - kind, layer, y_peer, me, (y_part,)))
            if y_part == (1, 2):
                start_far(1 - kind, layer, 1, y_peer, x_peer)
            start(pair(1 - kind, layer, y_peer, "pair_y", (y_part,)))

    def far_arrive(kind, layer, only=None):
        for idx, parts in enumerate(zip(far_parts(layer, 0), far_parts(layer, 1))):
            if only is not None and idx != only:
                continue
            for half in range(2):
                arrive(far(1 - kind, layer, half, diag, me, (parts[half],)))
                start(pair(1 - kind, layer, diag, "pair_far", (parts[half],)))

    def far_partner(kind, layer):
        arrive(pair(1 - kind, layer, partner_of(diag), "pair_far", far_parts(layer, 0) + far_parts(layer, 1)))

    def near_partner(kind, layer, x_parts=None, y_parts=None):
        arrive(pair(kind, layer, partner_of(x_peer), "pair_x", x_parts or own_parts(layer)))
        arrive(pair(1 - kind, layer, partner_of(y_peer), "pair_y", y_parts or own_parts(layer)))

    def stage_own(kind):
        pack(kind, me, p0)
        forward(kind, 0)
        for layer in range(layers):
            arrive(pair(kind, layer, partner, "pair_own", own_parts(layer)))
        pack(kind, partner, p1)
        forward(kind, 1)
        start(own_x(kind, layers - 1, me, x_peer))
        start(own_y(kind, layers - 1, me, y_peer)[::-1])
        near_partner(kind, 0)
        far_arrive(kind, 0)
        near_partner(kind, 1)
        far_partner(kind, 0)

    def stage_one(kind):
        far_arrive(kind, 1)
        far_partner(kind, 1)

    def stage_two(kind):
        last = layers - 1
        early = far_parts(last, 0)[:-1] + far_parts(last, 1)[:-1]
        late = last_parts(0) + last_parts(1)
        forward(kind, last)
        near_partner(kind, last, ((0, 2),), ((1, 2),))

        @pl.when(core == 1)
        def _():
            start(extra(kind, 0, partner_of(x_peer), "extra", y_peer))
            start(extra(1 - kind, 1, partner_of(y_peer), "extra", x_peer))

        pack(kind, x_peer, p2)
        pack(1 - kind, y_peer, p4)
        near_partner(kind, last, ((1, 2),), ((0, 2),))
        far_arrive(kind, last, 0)
        pack(kind, partner_of(x_peer), p3)
        far_arrive(kind, last, 1)
        pack(1 - kind, partner_of(y_peer), p5)
        drain(kind)
        arrive(pair(1 - kind, last, partner_of(diag), "pair_far", early))

        @pl.when(core == 1)
        def _():
            far_arrive(kind, last, 2)
            for half in range(2):
                arrive(extra(1 - kind, half, partner_of(diag), "extra", me))
                start(extra(1 - kind, half, partner_of(diag), "pair_extra", partner))
            left(pair(1 - kind, last, diag, "pair_far", late))
            left(far(kind, last, 0, x_peer, y_peer, last_parts(0)))
            left(far(1 - kind, last, 1, y_peer, x_peer, last_parts(1)))
            left(extra(kind, 0, partner_of(x_peer), "extra", y_peer))
            left(extra(1 - kind, 1, partner_of(y_peer), "extra", x_peer))
            for half in range(2):
                left(extra(1 - kind, half, partner_of(diag), "pair_extra", partner))

        @pl.when(core == 0)
        def _():
            arrive(pair(1 - kind, last, partner_of(diag), "pair_far", late))
            for half in range(2):
                arrive(extra(1 - kind, half, diag, "pair_extra", me))

        left(pair(1 - kind, last, diag, "pair_far", early))
        left(far(kind, last, 0, x_peer, y_peer, far_parts(last, 0)[:-1]))
        left(far(1 - kind, last, 1, y_peer, x_peer, far_parts(last, 1)[:-1]))

    by_kind(stage_own)
    tok_load.wait()
    mlp_block(dims, 0, w_in, w_out, hidden_ref, normed_ref, active_ref)
    by_kind(stage_one)
    mlp_block(dims, 1, w_in, w_out, hidden_ref, normed_ref, active_ref)
    by_kind(stage_two)


def finish_kernel(dims, p0, p1, p2, p3, p4, p5, master_ref, one_ref, two_ref, w_in, w_out, last_ref, tgt_ref,
                  packed_hbm, master_hbm, one_hbm, two_hbm, loss_hbm,
                  loss_ref, far_ref, wide_ref, normed_ref, active_ref, hidden_ref, sem, far_sem):
    layers, model_dim, hidden_dim, rows, chunks = dims
    me, core, y_pos, x_peer, y_peer, diag = places()
    twin = 1 - 2 * core

    copies = []
    for which, (src, dst) in enumerate(((master_ref, master_hbm), (one_ref, one_hbm), (two_ref, two_hbm))):
        for layer in range(layers):
            copies.append(pltpu.make_async_copy(src.at[layer], dst.at[:, layer, :], sem.at[6 + which * layers + layer]))
    for idx, (ref, device) in enumerate(((p0, me), (p1, me + twin), (p2, x_peer), (p3, x_peer + twin), (p4, y_peer), (p5, y_peer + twin))):
        copies.append(pltpu.make_async_copy(ref, packed_hbm.at[pl.ds(device * chunks, chunks)], sem.at[idx]))
    for item in copies:
        item.start()

    far_copies = []
    for idx, device in enumerate((diag, diag + twin)):
        for y_value in range(2):
            @pl.when(y_pos == y_value)
            def _():
                spread_piece(dims, 1 - y_value, device, (w_in, w_out), wide_ref)

        def squeeze(at, _):
            block = wide_ref[pl.ds(pl.multiple_of(at * 128, 128), 128), :].astype(BF16).reshape(32, 4, LANES)
            far_ref[idx, pl.ds(at * 32, 32), :, :] = block[:, :layers, :]
            return 0

        lax.fori_loop(0, 4 * chunks // 128, squeeze, 0)
        far_copies.append(pltpu.make_async_copy(far_ref.at[idx], packed_hbm.at[pl.ds(device * chunks, chunks)], far_sem.at[idx]))
        far_copies[-1].start()

    hidden_ref[...] = last_ref[...]
    mlp_block(dims, layers - 1, w_in, w_out, hidden_ref, normed_ref, active_ref)

    for idx in range(rows // LANES):
        at = slice(idx * LANES, (idx + 1) * LANES)
        error = hidden_ref[at, :].astype(F32) - tgt_ref[at, :].astype(F32)
        error = error * error
        folded = error[:, 0:LANES]
        for col in range(LANES, model_dim, LANES):
            folded = folded + error[:, col:col + LANES]
        loss_ref[idx:idx + 1, :] = jnp.sum(folded.T, axis=0, keepdims=True) * (1.0 / model_dim)

    loss_copy = pltpu.make_async_copy(loss_ref, loss_hbm, far_sem.at[2])
    loss_copy.start()
    for item in copies + far_copies + [loss_copy]:
        item.wait()


def solution(mesh):
    group_size = mesh.shape["data"]
    state_spec = P(None, "data")
    row_spec = P("data", None)

    def local_step(grad_shard, master_shard, one_shard, two_shard, tok_rows, tgt_rows):
        rows, model_dim = tok_rows.shape
        layers, cols = master_shard.shape
        half_size = cols * group_size // 2
        hidden_dim = half_size // model_dim
        chunks = cols // LANES
        dims = (layers, model_dim, hidden_dim, rows, chunks)
        tiled = [a.reshape(layers, chunks, LANES).transpose(1, 0, 2) for a in (grad_shard, master_shard, one_shard, two_shard)]
        state_v = pltpu.VMEM((layers, chunks, LANES), F32)
        hbm = pl.BlockSpec(memory_space=pltpu.HBM)
        vmem = pl.BlockSpec(memory_space=pltpu.VMEM)
        state_out = state_v
        w_in_v = pltpu.VMEM((layers, model_dim, hidden_dim), BF16)
        w_out_v = pltpu.VMEM((layers, hidden_dim, model_dim), BF16)
        hidden_v = pltpu.VMEM((rows, model_dim), BF16)
        wide_v = pltpu.VMEM((4 * chunks, LANES), F32)
        normed_v = pltpu.VMEM((256, model_dim), BF16)
        active_v = pltpu.VMEM((256, hidden_dim), BF16)
        packed_v = pltpu.VMEM((4 * chunks, LANES), BF16)
        gathered = pl.pallas_call(
            functools.partial(gather_kernel, dims),
            name="gather_step",
            out_shape=(*(packed_v,) * 6, state_v, state_v, state_v, w_in_v, w_out_v, hidden_v),
            in_specs=[hbm] * 5,
            out_specs=(vmem,) * 12,
            scratch_shapes=[
                state_v, state_v, state_v, state_v,
                pltpu.VMEM((group_size, 1, LANES), F32),
                wide_v, normed_v, active_v,
                pltpu.SemaphoreType.DMA((5, layers)),
                pltpu.SemaphoreType.DMA((layers, 3)),
                pltpu.SemaphoreType.DMA((group_size,)),
                pltpu.SemaphoreType.DMA((group_size,)),
                pltpu.SemaphoreType.DMA((96,)),
                pltpu.SemaphoreType.DMA((96,)),
            ],
            compiler_params=pltpu.CompilerParams(collective_id=0, has_side_effects=True, vmem_limit_bytes=19 << 20),
        )(*[pltpu.with_memory_space_constraint(a, pltpu.HBM) for a in (*tiled, tok_rows)])
        gathered = [a.reshape(chunks, 4, LANES)[:, :layers, :] for a in gathered[:6]] + list(gathered[6:])
        state_tile = jax.ShapeDtypeStruct((chunks, layers, LANES), F32)
        weights, new_master, new_one, new_two, row_loss = pl.pallas_call(
            functools.partial(finish_kernel, dims),
            name="finish",
            out_shape=(jax.ShapeDtypeStruct((chunks * group_size, layers, LANES), BF16), state_tile, state_tile, state_tile,
                       jax.ShapeDtypeStruct((rows // LANES, LANES), F32)),
            in_specs=[vmem] * 13,
            out_specs=(hbm,) * 5,
            scratch_shapes=[
                pltpu.VMEM((rows // LANES, LANES), F32),
                pltpu.VMEM((2, chunks, layers, LANES), BF16),
                wide_v, normed_v, active_v, hidden_v,
                pltpu.SemaphoreType.DMA((6 + 3 * layers,)),
                pltpu.SemaphoreType.DMA((3,)),
            ],
            compiler_params=pltpu.CompilerParams(vmem_limit_bytes=14 << 20),
        )(*gathered, tgt_rows)

        def flat(a):
            return a.transpose(1, 0, 2).reshape(layers, a.shape[0] * LANES)

        return row_loss.reshape(rows), flat(weights), flat(new_master), flat(new_one), flat(new_two)

    return jax.shard_map(local_step, mesh=mesh, in_specs=(state_spec, state_spec, state_spec, state_spec, row_spec, row_spec), out_specs=(P("data"), P(), state_spec, state_spec, state_spec), check_vma=False)
```

```python
import functools

import jax
import jax.numpy as jnp
from jax import lax
from jax.experimental import pallas as pl
from jax.experimental.pallas import tpu as pltpu
from jax.sharding import PartitionSpec as P

LEARN_RATE = 0.01
BETA_ONE = 0.9
BETA_TWO = 0.95
ADAM_EPS = 1e-8
WEIGHT_DECAY = 0.1
ADAM_STEP = 10
CLIP_NORM = 1.0
NORM_EPS = 1e-6

MESH = pl.DeviceIdType.MESH
LANES = 128
GROUP = 8
F32 = jnp.float32
BF16 = jnp.bfloat16


def spread_piece(dims, kind, device, weights, wide_ref):
    layers, model_dim, hidden_dim, rows, chunks = dims
    per_row = (hidden_dim if kind == 0 else model_dim) // LANES
    count = chunks // per_row
    src = weights[kind]
    slot = lax.rem(device, 4)

    def spread(idx, _):
        row = pl.multiple_of(slot * count + idx * 16, 16)
        for layer in range(layers):
            for col in range(per_row):
                tile = src[layer, pl.ds(row, 16), col * LANES:(col + 1) * LANES].astype(F32)
                base = layer + 4 * (idx * (16 * per_row) + col)
                wide_ref[pl.ds(base, 8, stride=4 * per_row), :] = tile[0:8]
                wide_ref[pl.ds(base + 32 * per_row, 8, stride=4 * per_row), :] = tile[8:16]
        return 0

    lax.fori_loop(0, count // 16, spread, 0)


def mlp_block(dims, layer, w_in, w_out, hidden_ref, normed_ref, active_ref):
    layers, model_dim, hidden_dim, rows, chunks = dims

    def block(idx, _):
        at = pl.ds(pl.multiple_of(idx * 256, 256), 256)
        hidden = hidden_ref[at, :].astype(F32)
        scale = lax.rsqrt(jnp.mean(hidden * hidden, axis=-1, keepdims=True) + NORM_EPS)
        normed_ref[...] = (hidden * scale).astype(BF16)
        for col in range(0, hidden_dim, 384):
            inner = jnp.dot(normed_ref[...], w_in[layer, :, col:col + 384], preferred_element_type=F32).astype(BF16)
            active_ref[:, col:col + 384] = jax.nn.gelu(inner.astype(F32), approximate=True).astype(BF16)
        for col in range(0, model_dim, 256):
            add = jnp.dot(active_ref[...], w_out[layer, :, col:col + 256], preferred_element_type=F32)
            hidden_ref[at, col:col + 256] = (hidden_ref[at, col:col + 256].astype(F32) + add).astype(BF16)
        return 0

    lax.fori_loop(0, rows // 256, block, 0)


def places():
    me = lax.axis_index("data")
    core = lax.rem(me, 2)
    x_pos = lax.rem(me // 2, 2)
    y_pos = me // 4
    x_peer = me + 2 - 4 * x_pos
    y_peer = me + 4 - 8 * y_pos
    return me, core, y_pos, x_peer, y_peer, x_peer + 4 - 8 * y_pos


def gather_kernel(dims, grad_hbm, master_hbm, one_hbm, two_hbm, tok_hbm,
                  p0, p1, p2, p3, p4, p5, master_out, one_out, two_out, w_in, w_out, hidden_ref,
                  grad_v, master_v, one_v, two_v,
                  part_ref, wide_ref, normed_ref, active_ref,
                  load_sem, grad_sem, part_send, part_recv, send_sem, recv_sem):
    layers, model_dim, hidden_dim, rows, chunks = dims
    in_rows = chunks * LANES // hidden_dim
    out_rows = chunks * LANES // model_dim

    me, core, y_pos, x_peer, y_peer, diag = places()
    partner = me + 1 - 2 * core

    state = ((grad_hbm, grad_v), (master_hbm, master_v), (one_hbm, one_v), (two_hbm, two_v))

    def load(which, layer):
        src, dst = state[which]
        return pltpu.make_async_copy(src.at[:, layer, :], dst.at[layer], load_sem.at[which, layer])

    span = chunks // 3

    def grad_load(layer, part):
        at = pl.ds(part * span, span)
        return pltpu.make_async_copy(grad_hbm.at[at, layer, :], grad_v.at[layer, at], grad_sem.at[layer, part])

    for layer in range(layers):
        for part in range(3):
            grad_load(layer, part).start()
    tok_load = pltpu.make_async_copy(tok_hbm, hidden_ref, load_sem.at[4, 0])

    barrier = pltpu.get_barrier_semaphore()
    for step in range(1, GROUP):
        pl.semaphore_signal(barrier, inc=1, device_id=(lax.rem(me + step, GROUP),), device_id_type=MESH)

    sums = tuple(jnp.zeros((8, LANES), F32) for _ in range(8))
    for layer in range(layers):
        for part in range(3):
            grad_load(layer, part).wait()
            if layer == layers - 1 and part == 2:
                for which in range(1, 4):
                    load(which, 0).start()

            def square(idx, carry):
                base = pl.multiple_of(part * span + idx * 64, 64)
                block = grad_v[layer, pl.ds(base, 64), :]
                return tuple(carry[k] + block[8 * k:8 * k + 8] * block[8 * k:8 * k + 8] for k in range(8))

            sums = lax.fori_loop(0, span // 64, square, sums)
    mine = ((sums[0] + sums[1]) + (sums[2] + sums[3])) + ((sums[4] + sums[5]) + (sums[6] + sums[7]))
    part_ref[me] = jnp.sum(mine, axis=0, keepdims=True)
    pl.semaphore_wait(barrier, GROUP - 1)

    def part_copy(step):
        return pltpu.make_async_remote_copy(
            src_ref=part_ref.at[me], dst_ref=part_ref.at[me],
            send_sem=part_send.at[step], recv_sem=part_recv.at[step],
            device_id=(lax.rem(me + step, GROUP),), device_id_type=MESH)

    def part_arrival(step):
        slot = lax.rem(me + GROUP - step, GROUP)
        return pltpu.make_async_remote_copy(
            src_ref=part_ref.at[slot], dst_ref=part_ref.at[slot],
            send_sem=part_send.at[step], recv_sem=part_recv.at[step],
            device_id=(me,), device_id_type=MESH)

    for step in range(1, GROUP):
        part_copy(step).start()
    for item in range(1, layers):
        for which in range(1, 4):
            load(which, item).start()
    tok_load.start()
    for step in range(1, GROUP):
        part_arrival(step).wait_recv()
    total = part_ref[0]
    for slot in range(1, GROUP):
        total = total + part_ref[slot]
    total = jnp.sum(total, axis=1, keepdims=True)
    clip = jnp.minimum(1.0, CLIP_NORM / jnp.sqrt(total))
    clip = jnp.broadcast_to(clip, (8, LANES))

    slots = {}

    def piece(kind, layer, device, part):
        ref, count = ((w_in, in_rows), (w_out, out_rows))[kind]
        span = count // part[1]
        at = lax.rem(device, 4) * count + part[0] * span
        return ref.at[layer, pl.ds(pl.multiple_of(at, 16), span), :]

    def copies(kind, layer, device, route, target, parts):
        out = []
        for part in parts:
            ref = piece(kind, layer, device, part)
            index = slots.setdefault((route, layer, part), len(slots))
            out.append(pltpu.make_async_remote_copy(
                src_ref=ref, dst_ref=ref, send_sem=send_sem.at[index],
                recv_sem=recv_sem.at[index], device_id=(target,), device_id_type=MESH))
        return out

    def start(items):
        for item in items:
            item.start()

    def arrive(items):
        for item in items:
            item.wait_recv()

    def left(items):
        for item in items:
            item.wait_send()

    def own_parts(layer):
        return ((0, 6), (1, 6), (2, 6), (1, 2)) if layer == 0 else ((0, 2), (1, 2))

    def far_parts(layer, half):
        return tuple((3 * half + at, 6) for at in range(3)) if layer == layers - 1 else ((half, 2),)

    def own_x(kind, layer, device, target, parts=None):
        return copies(kind, layer, device, "own_x", target, parts or own_parts(layer))

    def own_y(kind, layer, device, target, parts=None):
        return copies(kind, layer, device, "own_y", target, parts or own_parts(layer))

    def far(kind, layer, half, device, target, parts=None):
        return copies(kind, layer, device, "far", target, parts or far_parts(layer, half))

    def pair(kind, layer, device, route, parts):
        return copies(kind, layer, device, route, partner, parts)

    def by_kind(function):
        for y_value in range(2):
            @pl.when(y_pos == y_value)
            def _():
                function(y_value)

    one_scale = 1.0 / (1.0 - BETA_ONE ** ADAM_STEP)
    two_scale = 1.0 / (1.0 - BETA_TWO ** ADAM_STEP)

    def adam(layer, part):
        first = part[0] * (chunks // part[1])

        def update(idx, _):
            base = pl.multiple_of(first + idx * 48, 8)
            for k in range(6):
                at = pl.ds(pl.multiple_of(base + 8 * k, 8), 8)
                clipped = grad_v[layer, at, :] * clip
                new_one = BETA_ONE * one_v[layer, at, :] + (1.0 - BETA_ONE) * clipped
                new_two = BETA_TWO * two_v[layer, at, :] + (1.0 - BETA_TWO) * clipped * clipped
                step_size = (new_one * one_scale) / (jnp.sqrt(new_two * two_scale) + ADAM_EPS)
                old = master_v[layer, at, :]
                master_out[layer, at, :] = old - LEARN_RATE * (step_size + WEIGHT_DECAY * old)
                one_out[layer, at, :] = new_one
                two_out[layer, at, :] = new_two
            return 0

        lax.fori_loop(0, chunks // part[1] // 48, update, 0)

    def round_rows(kind, layer, part):
        width = hidden_dim if kind == 0 else model_dim
        count = in_rows if kind == 0 else out_rows
        per_row = width // LANES
        dst = w_in if kind == 0 else w_out
        slot = lax.rem(me, 4)

        def body(idx, _):
            base = part[0] * (chunks // part[1]) + idx * (16 * per_row)
            row = pl.multiple_of(slot * count + part[0] * (count // part[1]) + idx * 16, 16)
            for col in range(per_row):
                top = master_out[layer, pl.ds(base + col, 8, stride=per_row), :]
                low = master_out[layer, pl.ds(base + 8 * per_row + col, 8, stride=per_row), :]
                dst[layer, pl.ds(row, 16), col * LANES:(col + 1) * LANES] = jnp.concatenate([top, low], axis=0).astype(BF16)
            return 0

        lax.fori_loop(0, count // 16 // part[1], body, 0)

    for layer in range(layers):
        for which in range(1, 4):
            load(which, layer).wait()
        for part in own_parts(layer):
            adam(layer, part)

            def send_own(kind):
                round_rows(kind, layer, part)
                if layer < layers - 1:
                    start(own_x(kind, layer, me, x_peer, (part,)))
                    start(own_y(kind, layer, me, y_peer, (part,)))
                start(pair(kind, layer, me, "pair_own", (part,)))

            by_kind(send_own)

    def pack(kind, device, packed_ref):
        spread_piece(dims, kind, device, (w_in, w_out), wide_ref)

        def squeeze(idx, _):
            at = pl.ds(pl.multiple_of(idx * 256, 256), 256)
            packed_ref[at, :] = wide_ref[at, :].astype(BF16)
            return 0

        lax.fori_loop(0, 4 * chunks // 256, squeeze, 0)

    def partner_of(device):
        return device + 1 - 2 * core

    def drain(kind):
        for layer in range(layers):
            left(own_x(kind, layer, me, x_peer))
            left(own_y(kind, layer, me, y_peer))
            left(pair(kind, layer, me, "pair_own", own_parts(layer)))
            left(pair(kind, layer, x_peer, "pair_x", own_parts(layer)))
            left(pair(1 - kind, layer, y_peer, "pair_y", own_parts(layer)))
            if layer < layers - 1:
                left(pair(1 - kind, layer, diag, "pair_far", far_parts(layer, 0) + far_parts(layer, 1)))
                left(far(kind, layer, 0, x_peer, y_peer))
                left(far(1 - kind, layer, 1, y_peer, x_peer))
        for step in range(1, GROUP):
            part_copy(step).wait_send()

    def last_parts(half):
        return far_parts(layers - 1, half)[-1:]

    def start_far(kind, layer, half, device, target):
        if layer < layers - 1:
            start(far(kind, layer, half, device, target))
            return
        start(far(kind, layer, half, device, target, far_parts(layer, half)[:-1]))

        @pl.when(core == 0)
        def _():
            start(far(kind, layer, half, device, target, last_parts(half)))

    def extra(kind, half, device, route, target):
        return copies(kind, layers - 1, device, route, target, last_parts(half))

    def forward(kind, layer):
        x_order = own_parts(layer)
        y_order = x_order[::-1] if layer == layers - 1 else x_order
        for x_part, y_part in zip(x_order, y_order):
            arrive(own_x(kind, layer, x_peer, me, (x_part,)))
            if x_part in ((0, 2), (2, 6)):
                start_far(kind, layer, 0, x_peer, y_peer)
            start(pair(kind, layer, x_peer, "pair_x", (x_part,)))
            arrive(own_y(1 - kind, layer, y_peer, me, (y_part,)))
            if y_part == (1, 2):
                start_far(1 - kind, layer, 1, y_peer, x_peer)
            start(pair(1 - kind, layer, y_peer, "pair_y", (y_part,)))

    def far_arrive(kind, layer, only=None):
        for idx, parts in enumerate(zip(far_parts(layer, 0), far_parts(layer, 1))):
            if only is not None and idx != only:
                continue
            for half in range(2):
                arrive(far(1 - kind, layer, half, diag, me, (parts[half],)))
                start(pair(1 - kind, layer, diag, "pair_far", (parts[half],)))

    def far_partner(kind, layer):
        arrive(pair(1 - kind, layer, partner_of(diag), "pair_far", far_parts(layer, 0) + far_parts(layer, 1)))

    def near_partner(kind, layer, x_parts=None, y_parts=None):
        arrive(pair(kind, layer, partner_of(x_peer), "pair_x", x_parts or own_parts(layer)))
        arrive(pair(1 - kind, layer, partner_of(y_peer), "pair_y", y_parts or own_parts(layer)))

    def stage_own(kind):
        pack(kind, me, p0)
        forward(kind, 0)
        for layer in range(layers):
            arrive(pair(kind, layer, partner, "pair_own", own_parts(layer)))
        pack(kind, partner, p1)
        forward(kind, 1)
        start(own_x(kind, layers - 1, me, x_peer))
        start(own_y(kind, layers - 1, me, y_peer)[::-1])
        near_partner(kind, 0)
        far_arrive(kind, 0)
        near_partner(kind, 1)
        far_partner(kind, 0)

    def stage_one(kind):
        far_arrive(kind, 1)
        far_partner(kind, 1)

    def stage_two(kind):
        last = layers - 1
        early = far_parts(last, 0)[:-1] + far_parts(last, 1)[:-1]
        late = last_parts(0) + last_parts(1)
        forward(kind, last)
        near_partner(kind, last, ((0, 2),), ((1, 2),))

        @pl.when(core == 0)
        def _():
            start(extra(kind, 0, partner_of(x_peer), "extra", y_peer))
            start(extra(1 - kind, 1, partner_of(y_peer), "extra", x_peer))

        pack(kind, x_peer, p2)
        pack(1 - kind, y_peer, p4)
        near_partner(kind, last, ((1, 2),), ((0, 2),))
        far_arrive(kind, last, 0)
        pack(kind, partner_of(x_peer), p3)
        far_arrive(kind, last, 1)
        pack(1 - kind, partner_of(y_peer), p5)
        drain(kind)
        arrive(pair(1 - kind, last, partner_of(diag), "pair_far", early))

        @pl.when(core == 0)
        def _():
            far_arrive(kind, last, 2)
            for half in range(2):
                arrive(extra(1 - kind, half, partner_of(diag), "extra", me))
                start(extra(1 - kind, half, partner_of(diag), "pair_extra", partner))
            left(pair(1 - kind, last, diag, "pair_far", late))
            left(far(kind, last, 0, x_peer, y_peer, last_parts(0)))
            left(far(1 - kind, last, 1, y_peer, x_peer, last_parts(1)))
            left(extra(kind, 0, partner_of(x_peer), "extra", y_peer))
            left(extra(1 - kind, 1, partner_of(y_peer), "extra", x_peer))
            for half in range(2):
                left(extra(1 - kind, half, partner_of(diag), "pair_extra", partner))

        @pl.when(core == 1)
        def _():
            arrive(pair(1 - kind, last, partner_of(diag), "pair_far", late))
            for half in range(2):
                arrive(extra(1 - kind, half, diag, "pair_extra", me))

        left(pair(1 - kind, last, diag, "pair_far", early))
        left(far(kind, last, 0, x_peer, y_peer, far_parts(last, 0)[:-1]))
        left(far(1 - kind, last, 1, y_peer, x_peer, far_parts(last, 1)[:-1]))

    by_kind(stage_own)
    tok_load.wait()
    mlp_block(dims, 0, w_in, w_out, hidden_ref, normed_ref, active_ref)
    by_kind(stage_one)
    mlp_block(dims, 1, w_in, w_out, hidden_ref, normed_ref, active_ref)
    by_kind(stage_two)


def finish_kernel(dims, p0, p1, p2, p3, p4, p5, master_ref, one_ref, two_ref, w_in, w_out, last_ref, tgt_ref,
                  packed_hbm, master_hbm, one_hbm, two_hbm, loss_hbm,
                  loss_ref, far_ref, wide_ref, normed_ref, active_ref, hidden_ref, sem, far_sem):
    layers, model_dim, hidden_dim, rows, chunks = dims
    me, core, y_pos, x_peer, y_peer, diag = places()
    twin = 1 - 2 * core

    copies = []
    for which, (src, dst) in enumerate(((master_ref, master_hbm), (one_ref, one_hbm), (two_ref, two_hbm))):
        for layer in range(layers):
            copies.append(pltpu.make_async_copy(src.at[layer], dst.at[:, layer, :], sem.at[6 + which * layers + layer]))
    for idx, (ref, device) in enumerate(((p0, me), (p1, me + twin), (p2, x_peer), (p3, x_peer + twin), (p4, y_peer), (p5, y_peer + twin))):
        copies.append(pltpu.make_async_copy(ref, packed_hbm.at[pl.ds(device * chunks, chunks)], sem.at[idx]))
    for item in copies:
        item.start()

    far_copies = []
    for idx, device in enumerate((diag, diag + twin)):
        for y_value in range(2):
            @pl.when(y_pos == y_value)
            def _():
                spread_piece(dims, 1 - y_value, device, (w_in, w_out), wide_ref)

        def squeeze(at, _):
            block = wide_ref[pl.ds(pl.multiple_of(at * 128, 128), 128), :].astype(BF16).reshape(32, 4, LANES)
            far_ref[idx, pl.ds(at * 32, 32), :, :] = block[:, :layers, :]
            return 0

        lax.fori_loop(0, 4 * chunks // 128, squeeze, 0)
        far_copies.append(pltpu.make_async_copy(far_ref.at[idx], packed_hbm.at[pl.ds(device * chunks, chunks)], far_sem.at[idx]))
        far_copies[-1].start()

    hidden_ref[...] = last_ref[...]
    mlp_block(dims, layers - 1, w_in, w_out, hidden_ref, normed_ref, active_ref)

    for idx in range(rows // LANES):
        at = slice(idx * LANES, (idx + 1) * LANES)
        error = hidden_ref[at, :].astype(F32) - tgt_ref[at, :].astype(F32)
        error = error * error
        folded = error[:, 0:LANES]
        for col in range(LANES, model_dim, LANES):
            folded = folded + error[:, col:col + LANES]
        loss_ref[idx:idx + 1, :] = jnp.sum(folded.T, axis=0, keepdims=True) * (1.0 / model_dim)

    loss_copy = pltpu.make_async_copy(loss_ref, loss_hbm, far_sem.at[2])
    loss_copy.start()
    for item in copies + far_copies + [loss_copy]:
        item.wait()


def solution(mesh):
    group_size = mesh.shape["data"]
    state_spec = P(None, "data")
    row_spec = P("data", None)

    def local_step(grad_shard, master_shard, one_shard, two_shard, tok_rows, tgt_rows):
        rows, model_dim = tok_rows.shape
        layers, cols = master_shard.shape
        half_size = cols * group_size // 2
        hidden_dim = half_size // model_dim
        chunks = cols // LANES
        dims = (layers, model_dim, hidden_dim, rows, chunks)
        tiled = [a.reshape(layers, chunks, LANES).transpose(1, 0, 2) for a in (grad_shard, master_shard, one_shard, two_shard)]
        state_v = pltpu.VMEM((layers, chunks, LANES), F32)
        hbm = pl.BlockSpec(memory_space=pltpu.HBM)
        vmem = pl.BlockSpec(memory_space=pltpu.VMEM)
        state_out = state_v
        w_in_v = pltpu.VMEM((layers, model_dim, hidden_dim), BF16)
        w_out_v = pltpu.VMEM((layers, hidden_dim, model_dim), BF16)
        hidden_v = pltpu.VMEM((rows, model_dim), BF16)
        wide_v = pltpu.VMEM((4 * chunks, LANES), F32)
        normed_v = pltpu.VMEM((256, model_dim), BF16)
        active_v = pltpu.VMEM((256, hidden_dim), BF16)
        packed_v = pltpu.VMEM((4 * chunks, LANES), BF16)
        gathered = pl.pallas_call(
            functools.partial(gather_kernel, dims),
            name="gather_step",
            out_shape=(*(packed_v,) * 6, state_v, state_v, state_v, w_in_v, w_out_v, hidden_v),
            in_specs=[hbm] * 5,
            out_specs=(vmem,) * 12,
            scratch_shapes=[
                state_v, state_v, state_v, state_v,
                pltpu.VMEM((group_size, 1, LANES), F32),
                wide_v, normed_v, active_v,
                pltpu.SemaphoreType.DMA((5, layers)),
                pltpu.SemaphoreType.DMA((layers, 3)),
                pltpu.SemaphoreType.DMA((group_size,)),
                pltpu.SemaphoreType.DMA((group_size,)),
                pltpu.SemaphoreType.DMA((96,)),
                pltpu.SemaphoreType.DMA((96,)),
            ],
            compiler_params=pltpu.CompilerParams(collective_id=0, has_side_effects=True, vmem_limit_bytes=19 << 20),
        )(*[pltpu.with_memory_space_constraint(a, pltpu.HBM) for a in (*tiled, tok_rows)])
        gathered = [a.reshape(chunks, 4, LANES)[:, :layers, :] for a in gathered[:6]] + list(gathered[6:])
        state_tile = jax.ShapeDtypeStruct((chunks, layers, LANES), F32)
        weights, new_master, new_one, new_two, row_loss = pl.pallas_call(
            functools.partial(finish_kernel, dims),
            name="finish",
            out_shape=(jax.ShapeDtypeStruct((chunks * group_size, layers, LANES), BF16), state_tile, state_tile, state_tile,
                       jax.ShapeDtypeStruct((rows // LANES, LANES), F32)),
            in_specs=[vmem] * 13,
            out_specs=(hbm,) * 5,
            scratch_shapes=[
                pltpu.VMEM((rows // LANES, LANES), F32),
                pltpu.VMEM((2, chunks, layers, LANES), BF16),
                wide_v, normed_v, active_v, hidden_v,
                pltpu.SemaphoreType.DMA((6 + 3 * layers,)),
                pltpu.SemaphoreType.DMA((3,)),
            ],
            compiler_params=pltpu.CompilerParams(vmem_limit_bytes=14 << 20),
        )(*gathered, tgt_rows)

        def flat(a):
            return a.transpose(1, 0, 2).reshape(layers, a.shape[0] * LANES)

        return row_loss.reshape(rows), flat(weights), flat(new_master), flat(new_one), flat(new_two)

    return jax.shard_map(local_step, mesh=mesh, in_specs=(state_spec, state_spec, state_spec, state_spec, row_spec, row_spec), out_specs=(P("data"), P(), state_spec, state_spec, state_spec), check_vma=False)
```

```python
import functools

import jax
import jax.numpy as jnp
from jax import lax
from jax.experimental import pallas as pl
from jax.experimental.pallas import tpu as pltpu
from jax.sharding import PartitionSpec as P

LEARN_RATE = 0.01
BETA_ONE = 0.9
BETA_TWO = 0.95
ADAM_EPS = 1e-8
WEIGHT_DECAY = 0.1
ADAM_STEP = 10
CLIP_NORM = 1.0
NORM_EPS = 1e-6

MESH = pl.DeviceIdType.MESH
LANES = 128
GROUP = 8
F32 = jnp.float32
BF16 = jnp.bfloat16


def spread_piece(dims, kind, device, weights, wide_ref):
    layers, model_dim, hidden_dim, rows, chunks = dims
    per_row = (hidden_dim if kind == 0 else model_dim) // LANES
    count = chunks // per_row
    src = weights[kind]
    slot = lax.rem(device, 4)

    def spread(idx, _):
        row = pl.multiple_of(slot * count + idx * 16, 16)
        for layer in range(layers):
            for col in range(per_row):
                tile = src[layer, pl.ds(row, 16), col * LANES:(col + 1) * LANES].astype(F32)
                base = layer + 4 * (idx * (16 * per_row) + col)
                wide_ref[pl.ds(base, 8, stride=4 * per_row), :] = tile[0:8]
                wide_ref[pl.ds(base + 32 * per_row, 8, stride=4 * per_row), :] = tile[8:16]
        return 0

    lax.fori_loop(0, count // 16, spread, 0)


def mlp_block(dims, layer, w_in, w_out, hidden_ref, normed_ref, active_ref):
    layers, model_dim, hidden_dim, rows, chunks = dims

    def block(idx, _):
        at = pl.ds(pl.multiple_of(idx * 256, 256), 256)
        hidden = hidden_ref[at, :].astype(F32)
        scale = lax.rsqrt(jnp.mean(hidden * hidden, axis=-1, keepdims=True) + NORM_EPS)
        normed_ref[...] = (hidden * scale).astype(BF16)
        for col in range(0, hidden_dim, 384):
            inner = jnp.dot(normed_ref[...], w_in[layer, :, col:col + 384], preferred_element_type=F32).astype(BF16)
            active_ref[:, col:col + 384] = jax.nn.gelu(inner.astype(F32), approximate=True).astype(BF16)
        for col in range(0, model_dim, 256):
            add = jnp.dot(active_ref[...], w_out[layer, :, col:col + 256], preferred_element_type=F32)
            hidden_ref[at, col:col + 256] = (hidden_ref[at, col:col + 256].astype(F32) + add).astype(BF16)
        return 0

    lax.fori_loop(0, rows // 256, block, 0)


def places():
    me = lax.axis_index("data")
    core = lax.rem(me, 2)
    x_pos = lax.rem(me // 2, 2)
    y_pos = me // 4
    x_peer = me + 2 - 4 * x_pos
    y_peer = me + 4 - 8 * y_pos
    return me, core, y_pos, x_peer, y_peer, x_peer + 4 - 8 * y_pos


def gather_kernel(dims, grad_hbm, master_hbm, one_hbm, two_hbm, tok_hbm,
                  p0, p1, p2, p3, p4, p5, master_out, one_out, two_out, w_in, w_out, hidden_ref,
                  grad_v, master_v, one_v, two_v,
                  part_ref, wide_ref, normed_ref, active_ref,
                  load_sem, grad_sem, part_send, part_recv, send_sem, recv_sem):
    layers, model_dim, hidden_dim, rows, chunks = dims
    in_rows = chunks * LANES // hidden_dim
    out_rows = chunks * LANES // model_dim

    me, core, y_pos, x_peer, y_peer, diag = places()
    partner = me + 1 - 2 * core

    state = ((grad_hbm, grad_v), (master_hbm, master_v), (one_hbm, one_v), (two_hbm, two_v))

    def load(which, layer):
        src, dst = state[which]
        return pltpu.make_async_copy(src.at[:, layer, :], dst.at[layer], load_sem.at[which, layer])

    span = chunks // 3

    def grad_load(layer, part):
        at = pl.ds(part * span, span)
        return pltpu.make_async_copy(grad_hbm.at[at, layer, :], grad_v.at[layer, at], grad_sem.at[layer, part])

    for layer in range(layers):
        for part in range(3):
            grad_load(layer, part).start()
    tok_load = pltpu.make_async_copy(tok_hbm, hidden_ref, load_sem.at[4, 0])

    barrier = pltpu.get_barrier_semaphore()
    for step in range(1, GROUP):
        pl.semaphore_signal(barrier, inc=1, device_id=(lax.rem(me + step, GROUP),), device_id_type=MESH)

    sums = tuple(jnp.zeros((8, LANES), F32) for _ in range(8))
    for layer in range(layers):
        for part in range(3):
            grad_load(layer, part).wait()
            if layer == layers - 1 and part == 2:
                for which in range(1, 4):
                    load(which, 0).start()

            def square(idx, carry):
                base = pl.multiple_of(part * span + idx * 64, 64)
                block = grad_v[layer, pl.ds(base, 64), :]
                return tuple(carry[k] + block[8 * k:8 * k + 8] * block[8 * k:8 * k + 8] for k in range(8))

            sums = lax.fori_loop(0, span // 64, square, sums)
    mine = ((sums[0] + sums[1]) + (sums[2] + sums[3])) + ((sums[4] + sums[5]) + (sums[6] + sums[7]))
    part_ref[me] = jnp.sum(mine, axis=0, keepdims=True)
    pl.semaphore_wait(barrier, GROUP - 1)

    def part_copy(step):
        return pltpu.make_async_remote_copy(
            src_ref=part_ref.at[me], dst_ref=part_ref.at[me],
            send_sem=part_send.at[step], recv_sem=part_recv.at[step],
            device_id=(lax.rem(me + step, GROUP),), device_id_type=MESH)

    def part_arrival(step):
        slot = lax.rem(me + GROUP - step, GROUP)
        return pltpu.make_async_remote_copy(
            src_ref=part_ref.at[slot], dst_ref=part_ref.at[slot],
            send_sem=part_send.at[step], recv_sem=part_recv.at[step],
            device_id=(me,), device_id_type=MESH)

    for step in range(1, GROUP):
        part_copy(step).start()
    for item in range(1, layers):
        for which in range(1, 4):
            load(which, item).start()
    tok_load.start()
    for step in range(1, GROUP):
        part_arrival(step).wait_recv()
    total = part_ref[0]
    for slot in range(1, GROUP):
        total = total + part_ref[slot]
    total = jnp.sum(total, axis=1, keepdims=True)
    clip = jnp.minimum(1.0, CLIP_NORM / jnp.sqrt(total))
    clip = jnp.broadcast_to(clip, (8, LANES))

    slots = {}

    def piece(kind, layer, device, part):
        ref, count = ((w_in, in_rows), (w_out, out_rows))[kind]
        span = count // part[1]
        at = lax.rem(device, 4) * count + part[0] * span
        return ref.at[layer, pl.ds(pl.multiple_of(at, 8), span), :]

    def copies(kind, layer, device, route, target, parts):
        out = []
        for part in parts:
            ref = piece(kind, layer, device, part)
            index = slots.setdefault((route, layer, part), len(slots))
            out.append(pltpu.make_async_remote_copy(
                src_ref=ref, dst_ref=ref, send_sem=send_sem.at[index],
                recv_sem=recv_sem.at[index], device_id=(target,), device_id_type=MESH))
        return out

    def start(items):
        for item in items:
            item.start()

    def arrive(items):
        for item in items:
            item.wait_recv()

    def left(items):
        for item in items:
            item.wait_send()

    def own_parts(layer):
        return ((0, 6), (1, 6), (2, 6), (1, 2)) if layer == 0 else ((0, 2), (1, 2))

    def far_parts(layer, half):
        return ((3 * half, 6), (3 * half + 1, 6), (6 * half + 4, 12), (6 * half + 5, 12)) if layer == layers - 1 else ((half, 2),)

    def own_x(kind, layer, device, target, parts=None):
        return copies(kind, layer, device, "own_x", target, parts or own_parts(layer))

    def own_y(kind, layer, device, target, parts=None):
        return copies(kind, layer, device, "own_y", target, parts or own_parts(layer))

    def far(kind, layer, half, device, target, parts=None):
        return copies(kind, layer, device, "far", target, parts or far_parts(layer, half))

    def pair(kind, layer, device, route, parts):
        return copies(kind, layer, device, route, partner, parts)

    def by_kind(function):
        for y_value in range(2):
            @pl.when(y_pos == y_value)
            def _():
                function(y_value)

    one_scale = 1.0 / (1.0 - BETA_ONE ** ADAM_STEP)
    two_scale = 1.0 / (1.0 - BETA_TWO ** ADAM_STEP)

    def adam(layer, part):
        first = part[0] * (chunks // part[1])

        def update(idx, _):
            base = pl.multiple_of(first + idx * 48, 8)
            for k in range(6):
                at = pl.ds(pl.multiple_of(base + 8 * k, 8), 8)
                clipped = grad_v[layer, at, :] * clip
                new_one = BETA_ONE * one_v[layer, at, :] + (1.0 - BETA_ONE) * clipped
                new_two = BETA_TWO * two_v[layer, at, :] + (1.0 - BETA_TWO) * clipped * clipped
                step_size = (new_one * one_scale) / (jnp.sqrt(new_two * two_scale) + ADAM_EPS)
                old = master_v[layer, at, :]
                master_out[layer, at, :] = old - LEARN_RATE * (step_size + WEIGHT_DECAY * old)
                one_out[layer, at, :] = new_one
                two_out[layer, at, :] = new_two
            return 0

        lax.fori_loop(0, chunks // part[1] // 48, update, 0)

    def round_rows(kind, layer, part):
        width = hidden_dim if kind == 0 else model_dim
        count = in_rows if kind == 0 else out_rows
        per_row = width // LANES
        dst = w_in if kind == 0 else w_out
        slot = lax.rem(me, 4)

        def body(idx, _):
            base = part[0] * (chunks // part[1]) + idx * (16 * per_row)
            row = pl.multiple_of(slot * count + part[0] * (count // part[1]) + idx * 16, 16)
            for col in range(per_row):
                top = master_out[layer, pl.ds(base + col, 8, stride=per_row), :]
                low = master_out[layer, pl.ds(base + 8 * per_row + col, 8, stride=per_row), :]
                dst[layer, pl.ds(row, 16), col * LANES:(col + 1) * LANES] = jnp.concatenate([top, low], axis=0).astype(BF16)
            return 0

        lax.fori_loop(0, count // 16 // part[1], body, 0)

    for layer in range(layers):
        for which in range(1, 4):
            load(which, layer).wait()
        for part in own_parts(layer):
            adam(layer, part)

            def send_own(kind):
                round_rows(kind, layer, part)
                if layer < layers - 1:
                    start(own_x(kind, layer, me, x_peer, (part,)))
                    start(own_y(kind, layer, me, y_peer, (part,)))
                start(pair(kind, layer, me, "pair_own", (part,)))

            by_kind(send_own)

    def pack(kind, device, packed_ref):
        spread_piece(dims, kind, device, (w_in, w_out), wide_ref)

        def squeeze(idx, _):
            at = pl.ds(pl.multiple_of(idx * 256, 256), 256)
            packed_ref[at, :] = wide_ref[at, :].astype(BF16)
            return 0

        lax.fori_loop(0, 4 * chunks // 256, squeeze, 0)

    def partner_of(device):
        return device + 1 - 2 * core

    def drain(kind):
        for layer in range(layers):
            left(own_x(kind, layer, me, x_peer))
            left(own_y(kind, layer, me, y_peer))
            left(pair(kind, layer, me, "pair_own", own_parts(layer)))
            left(pair(kind, layer, x_peer, "pair_x", own_parts(layer)))
            left(pair(1 - kind, layer, y_peer, "pair_y", own_parts(layer)))
            if layer < layers - 1:
                left(pair(1 - kind, layer, diag, "pair_far", far_parts(layer, 0) + far_parts(layer, 1)))
                left(far(kind, layer, 0, x_peer, y_peer))
                left(far(1 - kind, layer, 1, y_peer, x_peer))
        for step in range(1, GROUP):
            part_copy(step).wait_send()

    def last_parts(half):
        return far_parts(layers - 1, half)[-1:]

    def start_far(kind, layer, half, device, target):
        if layer < layers - 1:
            start(far(kind, layer, half, device, target))
            return
        start(far(kind, layer, half, device, target, far_parts(layer, half)[:-1]))

        @pl.when(core == 0)
        def _():
            start(far(kind, layer, half, device, target, last_parts(half)))

    def extra(kind, half, device, route, target):
        return copies(kind, layers - 1, device, route, target, last_parts(half))

    def forward(kind, layer):
        x_order = own_parts(layer)
        y_order = x_order[::-1] if layer == layers - 1 else x_order
        for x_part, y_part in zip(x_order, y_order):
            arrive(own_x(kind, layer, x_peer, me, (x_part,)))
            if x_part in ((0, 2), (2, 6)):
                start_far(kind, layer, 0, x_peer, y_peer)
            start(pair(kind, layer, x_peer, "pair_x", (x_part,)))
            arrive(own_y(1 - kind, layer, y_peer, me, (y_part,)))
            if y_part == (1, 2):
                start_far(1 - kind, layer, 1, y_peer, x_peer)
            start(pair(1 - kind, layer, y_peer, "pair_y", (y_part,)))

    def far_arrive(kind, layer, only=None):
        for idx, parts in enumerate(zip(far_parts(layer, 0), far_parts(layer, 1))):
            if only is not None and idx != only:
                continue
            for half in range(2):
                arrive(far(1 - kind, layer, half, diag, me, (parts[half],)))
                start(pair(1 - kind, layer, diag, "pair_far", (parts[half],)))

    def far_partner(kind, layer):
        arrive(pair(1 - kind, layer, partner_of(diag), "pair_far", far_parts(layer, 0) + far_parts(layer, 1)))

    def near_partner(kind, layer, x_parts=None, y_parts=None):
        arrive(pair(kind, layer, partner_of(x_peer), "pair_x", x_parts or own_parts(layer)))
        arrive(pair(1 - kind, layer, partner_of(y_peer), "pair_y", y_parts or own_parts(layer)))

    def stage_own(kind):
        pack(kind, me, p0)
        forward(kind, 0)
        for layer in range(layers):
            arrive(pair(kind, layer, partner, "pair_own", own_parts(layer)))
        pack(kind, partner, p1)
        forward(kind, 1)
        start(own_x(kind, layers - 1, me, x_peer))
        start(own_y(kind, layers - 1, me, y_peer)[::-1])
        near_partner(kind, 0)
        far_arrive(kind, 0)
        near_partner(kind, 1)
        far_partner(kind, 0)

    def stage_one(kind):
        far_arrive(kind, 1)
        far_partner(kind, 1)

    def stage_two(kind):
        last = layers - 1
        early = far_parts(last, 0)[:-1] + far_parts(last, 1)[:-1]
        late = last_parts(0) + last_parts(1)
        forward(kind, last)
        near_partner(kind, last, ((0, 2),), ((1, 2),))

        @pl.when(core == 0)
        def _():
            start(extra(kind, 0, partner_of(x_peer), "extra", y_peer))
            start(extra(1 - kind, 1, partner_of(y_peer), "extra", x_peer))

        pack(kind, x_peer, p2)
        pack(1 - kind, y_peer, p4)
        near_partner(kind, last, ((1, 2),), ((0, 2),))
        far_arrive(kind, last, 0)
        pack(kind, partner_of(x_peer), p3)
        far_arrive(kind, last, 1)
        pack(1 - kind, partner_of(y_peer), p5)
        drain(kind)
        far_arrive(kind, last, 2)
        arrive(pair(1 - kind, last, partner_of(diag), "pair_far", early))

        @pl.when(core == 0)
        def _():
            far_arrive(kind, last, 3)
            for half in range(2):
                arrive(extra(1 - kind, half, partner_of(diag), "extra", me))
                start(extra(1 - kind, half, partner_of(diag), "pair_extra", partner))
            left(pair(1 - kind, last, diag, "pair_far", late))
            left(far(kind, last, 0, x_peer, y_peer, last_parts(0)))
            left(far(1 - kind, last, 1, y_peer, x_peer, last_parts(1)))
            left(extra(kind, 0, partner_of(x_peer), "extra", y_peer))
            left(extra(1 - kind, 1, partner_of(y_peer), "extra", x_peer))
            for half in range(2):
                left(extra(1 - kind, half, partner_of(diag), "pair_extra", partner))

        @pl.when(core == 1)
        def _():
            arrive(pair(1 - kind, last, partner_of(diag), "pair_far", late))
            for half in range(2):
                arrive(extra(1 - kind, half, diag, "pair_extra", me))

        left(pair(1 - kind, last, diag, "pair_far", early))
        left(far(kind, last, 0, x_peer, y_peer, far_parts(last, 0)[:-1]))
        left(far(1 - kind, last, 1, y_peer, x_peer, far_parts(last, 1)[:-1]))

    by_kind(stage_own)
    tok_load.wait()
    mlp_block(dims, 0, w_in, w_out, hidden_ref, normed_ref, active_ref)
    by_kind(stage_one)
    mlp_block(dims, 1, w_in, w_out, hidden_ref, normed_ref, active_ref)
    by_kind(stage_two)


def finish_kernel(dims, p0, p1, p2, p3, p4, p5, master_ref, one_ref, two_ref, w_in, w_out, last_ref, tgt_ref,
                  packed_hbm, master_hbm, one_hbm, two_hbm, loss_hbm,
                  loss_ref, far_ref, wide_ref, normed_ref, active_ref, hidden_ref, sem, far_sem):
    layers, model_dim, hidden_dim, rows, chunks = dims
    me, core, y_pos, x_peer, y_peer, diag = places()
    twin = 1 - 2 * core

    copies = []
    for which, (src, dst) in enumerate(((master_ref, master_hbm), (one_ref, one_hbm), (two_ref, two_hbm))):
        for layer in range(layers):
            copies.append(pltpu.make_async_copy(src.at[layer], dst.at[:, layer, :], sem.at[6 + which * layers + layer]))
    for idx, (ref, device) in enumerate(((p0, me), (p1, me + twin), (p2, x_peer), (p3, x_peer + twin), (p4, y_peer), (p5, y_peer + twin))):
        copies.append(pltpu.make_async_copy(ref, packed_hbm.at[pl.ds(device * chunks, chunks)], sem.at[idx]))
    for item in copies:
        item.start()

    far_copies = []
    for idx, device in enumerate((diag, diag + twin)):
        for y_value in range(2):
            @pl.when(y_pos == y_value)
            def _():
                spread_piece(dims, 1 - y_value, device, (w_in, w_out), wide_ref)

        def squeeze(at, _):
            block = wide_ref[pl.ds(pl.multiple_of(at * 128, 128), 128), :].astype(BF16).reshape(32, 4, LANES)
            far_ref[idx, pl.ds(at * 32, 32), :, :] = block[:, :layers, :]
            return 0

        lax.fori_loop(0, 4 * chunks // 128, squeeze, 0)
        far_copies.append(pltpu.make_async_copy(far_ref.at[idx], packed_hbm.at[pl.ds(device * chunks, chunks)], far_sem.at[idx]))
        far_copies[-1].start()

    hidden_ref[...] = last_ref[...]
    mlp_block(dims, layers - 1, w_in, w_out, hidden_ref, normed_ref, active_ref)

    for idx in range(rows // LANES):
        at = slice(idx * LANES, (idx + 1) * LANES)
        error = hidden_ref[at, :].astype(F32) - tgt_ref[at, :].astype(F32)
        error = error * error
        folded = error[:, 0:LANES]
        for col in range(LANES, model_dim, LANES):
            folded = folded + error[:, col:col + LANES]
        loss_ref[idx:idx + 1, :] = jnp.sum(folded.T, axis=0, keepdims=True) * (1.0 / model_dim)

    loss_copy = pltpu.make_async_copy(loss_ref, loss_hbm, far_sem.at[2])
    loss_copy.start()
    for item in copies + far_copies + [loss_copy]:
        item.wait()


def solution(mesh):
    group_size = mesh.shape["data"]
    state_spec = P(None, "data")
    row_spec = P("data", None)

    def local_step(grad_shard, master_shard, one_shard, two_shard, tok_rows, tgt_rows):
        rows, model_dim = tok_rows.shape
        layers, cols = master_shard.shape
        half_size = cols * group_size // 2
        hidden_dim = half_size // model_dim
        chunks = cols // LANES
        dims = (layers, model_dim, hidden_dim, rows, chunks)
        tiled = [a.reshape(layers, chunks, LANES).transpose(1, 0, 2) for a in (grad_shard, master_shard, one_shard, two_shard)]
        state_v = pltpu.VMEM((layers, chunks, LANES), F32)
        hbm = pl.BlockSpec(memory_space=pltpu.HBM)
        vmem = pl.BlockSpec(memory_space=pltpu.VMEM)
        state_out = state_v
        w_in_v = pltpu.VMEM((layers, model_dim, hidden_dim), BF16)
        w_out_v = pltpu.VMEM((layers, hidden_dim, model_dim), BF16)
        hidden_v = pltpu.VMEM((rows, model_dim), BF16)
        wide_v = pltpu.VMEM((4 * chunks, LANES), F32)
        normed_v = pltpu.VMEM((256, model_dim), BF16)
        active_v = pltpu.VMEM((256, hidden_dim), BF16)
        packed_v = pltpu.VMEM((4 * chunks, LANES), BF16)
        gathered = pl.pallas_call(
            functools.partial(gather_kernel, dims),
            name="gather_step",
            out_shape=(*(packed_v,) * 6, state_v, state_v, state_v, w_in_v, w_out_v, hidden_v),
            in_specs=[hbm] * 5,
            out_specs=(vmem,) * 12,
            scratch_shapes=[
                state_v, state_v, state_v, state_v,
                pltpu.VMEM((group_size, 1, LANES), F32),
                wide_v, normed_v, active_v,
                pltpu.SemaphoreType.DMA((5, layers)),
                pltpu.SemaphoreType.DMA((layers, 3)),
                pltpu.SemaphoreType.DMA((group_size,)),
                pltpu.SemaphoreType.DMA((group_size,)),
                pltpu.SemaphoreType.DMA((96,)),
                pltpu.SemaphoreType.DMA((96,)),
            ],
            compiler_params=pltpu.CompilerParams(collective_id=0, has_side_effects=True, vmem_limit_bytes=19 << 20),
        )(*[pltpu.with_memory_space_constraint(a, pltpu.HBM) for a in (*tiled, tok_rows)])
        gathered = [a.reshape(chunks, 4, LANES)[:, :layers, :] for a in gathered[:6]] + list(gathered[6:])
        state_tile = jax.ShapeDtypeStruct((chunks, layers, LANES), F32)
        weights, new_master, new_one, new_two, row_loss = pl.pallas_call(
            functools.partial(finish_kernel, dims),
            name="finish",
            out_shape=(jax.ShapeDtypeStruct((chunks * group_size, layers, LANES), BF16), state_tile, state_tile, state_tile,
                       jax.ShapeDtypeStruct((rows // LANES, LANES), F32)),
            in_specs=[vmem] * 13,
            out_specs=(hbm,) * 5,
            scratch_shapes=[
                pltpu.VMEM((rows // LANES, LANES), F32),
                pltpu.VMEM((2, chunks, layers, LANES), BF16),
                wide_v, normed_v, active_v, hidden_v,
                pltpu.SemaphoreType.DMA((6 + 3 * layers,)),
                pltpu.SemaphoreType.DMA((3,)),
            ],
            compiler_params=pltpu.CompilerParams(vmem_limit_bytes=14 << 20),
        )(*gathered, tgt_rows)

        def flat(a):
            return a.transpose(1, 0, 2).reshape(layers, a.shape[0] * LANES)

        return row_loss.reshape(rows), flat(weights), flat(new_master), flat(new_one), flat(new_two)

    return jax.shard_map(local_step, mesh=mesh, in_specs=(state_spec, state_spec, state_spec, state_spec, row_spec, row_spec), out_specs=(P("data"), P(), state_spec, state_spec, state_spec), check_vma=False)
```

```python
import functools

import jax
import jax.numpy as jnp
from jax import lax
from jax.experimental import pallas as pl
from jax.experimental.pallas import tpu as pltpu
from jax.sharding import PartitionSpec as P

LEARN_RATE = 0.01
BETA_ONE = 0.9
BETA_TWO = 0.95
ADAM_EPS = 1e-8
WEIGHT_DECAY = 0.1
ADAM_STEP = 10
CLIP_NORM = 1.0
NORM_EPS = 1e-6

MESH = pl.DeviceIdType.MESH
LANES = 128
GROUP = 8
F32 = jnp.float32
BF16 = jnp.bfloat16


def spread_piece(dims, kind, device, weights, wide_ref):
    layers, model_dim, hidden_dim, rows, chunks = dims
    per_row = (hidden_dim if kind == 0 else model_dim) // LANES
    count = chunks // per_row
    src = weights[kind]
    slot = lax.rem(device, 4)

    def spread(idx, _):
        row = pl.multiple_of(slot * count + idx * 16, 16)
        for layer in range(layers):
            for col in range(per_row):
                tile = src[layer, pl.ds(row, 16), col * LANES:(col + 1) * LANES].astype(F32)
                base = layer + 4 * (idx * (16 * per_row) + col)
                wide_ref[pl.ds(base, 8, stride=4 * per_row), :] = tile[0:8]
                wide_ref[pl.ds(base + 32 * per_row, 8, stride=4 * per_row), :] = tile[8:16]
        return 0

    lax.fori_loop(0, count // 16, spread, 0)


def mlp_block(dims, layer, w_in, w_out, hidden_ref, normed_ref, active_ref):
    layers, model_dim, hidden_dim, rows, chunks = dims

    def block(idx, _):
        at = pl.ds(pl.multiple_of(idx * 256, 256), 256)
        hidden = hidden_ref[at, :].astype(F32)
        scale = lax.rsqrt(jnp.mean(hidden * hidden, axis=-1, keepdims=True) + NORM_EPS)
        normed_ref[...] = (hidden * scale).astype(BF16)
        for col in range(0, hidden_dim, 384):
            inner = jnp.dot(normed_ref[...], w_in[layer, :, col:col + 384], preferred_element_type=F32).astype(BF16)
            active_ref[:, col:col + 384] = jax.nn.gelu(inner.astype(F32), approximate=True).astype(BF16)
        for col in range(0, model_dim, 256):
            add = jnp.dot(active_ref[...], w_out[layer, :, col:col + 256], preferred_element_type=F32)
            hidden_ref[at, col:col + 256] = (hidden_ref[at, col:col + 256].astype(F32) + add).astype(BF16)
        return 0

    lax.fori_loop(0, rows // 256, block, 0)


def places():
    me = lax.axis_index("data")
    core = lax.rem(me, 2)
    x_pos = lax.rem(me // 2, 2)
    y_pos = me // 4
    x_peer = me + 2 - 4 * x_pos
    y_peer = me + 4 - 8 * y_pos
    return me, core, y_pos, x_peer, y_peer, x_peer + 4 - 8 * y_pos


def gather_kernel(dims, grad_hbm, master_hbm, one_hbm, two_hbm, tok_hbm,
                  p0, p1, p2, p4, master_out, one_out, two_out, w_in, w_out, hidden_ref,
                  grad_v, master_v, one_v, two_v,
                  part_ref, wide_ref, normed_ref, active_ref,
                  load_sem, grad_sem, part_send, part_recv, send_sem, recv_sem):
    layers, model_dim, hidden_dim, rows, chunks = dims
    in_rows = chunks * LANES // hidden_dim
    out_rows = chunks * LANES // model_dim

    me, core, y_pos, x_peer, y_peer, diag = places()
    partner = me + 1 - 2 * core

    state = ((grad_hbm, grad_v), (master_hbm, master_v), (one_hbm, one_v), (two_hbm, two_v))

    def load(which, layer):
        src, dst = state[which]
        return pltpu.make_async_copy(src.at[:, layer, :], dst.at[layer], load_sem.at[which, layer])

    span = chunks // 3

    def grad_load(layer, part):
        at = pl.ds(part * span, span)
        return pltpu.make_async_copy(grad_hbm.at[at, layer, :], grad_v.at[layer, at], grad_sem.at[layer, part])

    for layer in range(layers):
        for part in range(3):
            grad_load(layer, part).start()
    tok_load = pltpu.make_async_copy(tok_hbm, hidden_ref, load_sem.at[4, 0])

    barrier = pltpu.get_barrier_semaphore()
    for step in range(1, GROUP):
        pl.semaphore_signal(barrier, inc=1, device_id=(lax.rem(me + step, GROUP),), device_id_type=MESH)

    sums = tuple(jnp.zeros((8, LANES), F32) for _ in range(8))
    for layer in range(layers):
        for part in range(3):
            grad_load(layer, part).wait()
            if layer == layers - 1 and part == 2:
                for which in range(1, 4):
                    load(which, 0).start()

            def square(idx, carry):
                base = pl.multiple_of(part * span + idx * 64, 64)
                block = grad_v[layer, pl.ds(base, 64), :]
                return tuple(carry[k] + block[8 * k:8 * k + 8] * block[8 * k:8 * k + 8] for k in range(8))

            sums = lax.fori_loop(0, span // 64, square, sums)
    mine = ((sums[0] + sums[1]) + (sums[2] + sums[3])) + ((sums[4] + sums[5]) + (sums[6] + sums[7]))
    part_ref[me] = jnp.sum(mine, axis=0, keepdims=True)
    pl.semaphore_wait(barrier, GROUP - 1)

    def part_copy(step):
        return pltpu.make_async_remote_copy(
            src_ref=part_ref.at[me], dst_ref=part_ref.at[me],
            send_sem=part_send.at[step], recv_sem=part_recv.at[step],
            device_id=(lax.rem(me + step, GROUP),), device_id_type=MESH)

    def part_arrival(step):
        slot = lax.rem(me + GROUP - step, GROUP)
        return pltpu.make_async_remote_copy(
            src_ref=part_ref.at[slot], dst_ref=part_ref.at[slot],
            send_sem=part_send.at[step], recv_sem=part_recv.at[step],
            device_id=(me,), device_id_type=MESH)

    for step in range(1, GROUP):
        part_copy(step).start()
    for item in range(1, layers):
        for which in range(1, 4):
            load(which, item).start()
    tok_load.start()
    for step in range(1, GROUP):
        part_arrival(step).wait_recv()
    total = part_ref[0]
    for slot in range(1, GROUP):
        total = total + part_ref[slot]
    total = jnp.sum(total, axis=1, keepdims=True)
    clip = jnp.minimum(1.0, CLIP_NORM / jnp.sqrt(total))
    clip = jnp.broadcast_to(clip, (8, LANES))

    slots = {}

    def piece(kind, layer, device, part):
        ref, count = ((w_in, in_rows), (w_out, out_rows))[kind]
        span = count // part[1]
        at = lax.rem(device, 4) * count + part[0] * span
        return ref.at[layer, pl.ds(pl.multiple_of(at, 16), span), :]

    def copies(kind, layer, device, route, target, parts):
        out = []
        for part in parts:
            ref = piece(kind, layer, device, part)
            index = slots.setdefault((route, layer, part), len(slots))
            out.append(pltpu.make_async_remote_copy(
                src_ref=ref, dst_ref=ref, send_sem=send_sem.at[index],
                recv_sem=recv_sem.at[index], device_id=(target,), device_id_type=MESH))
        return out

    def start(items):
        for item in items:
            item.start()

    def arrive(items):
        for item in items:
            item.wait_recv()

    def left(items):
        for item in items:
            item.wait_send()

    def own_parts(layer):
        return ((0, 6), (1, 6), (2, 6), (1, 2)) if layer == 0 else ((0, 2), (1, 2))

    def far_parts(layer, half):
        return tuple((3 * half + at, 6) for at in range(3)) if layer == layers - 1 else ((half, 2),)

    def own_x(kind, layer, device, target, parts=None):
        return copies(kind, layer, device, "own_x", target, parts or own_parts(layer))

    def own_y(kind, layer, device, target, parts=None):
        return copies(kind, layer, device, "own_y", target, parts or own_parts(layer))

    def far(kind, layer, half, device, target, parts=None):
        return copies(kind, layer, device, "far", target, parts or far_parts(layer, half))

    def pair(kind, layer, device, route, parts):
        return copies(kind, layer, device, route, partner, parts)

    def by_kind(function):
        for y_value in range(2):
            @pl.when(y_pos == y_value)
            def _():
                function(y_value)

    one_scale = 1.0 / (1.0 - BETA_ONE ** ADAM_STEP)
    two_scale = 1.0 / (1.0 - BETA_TWO ** ADAM_STEP)

    def adam(layer, part):
        first = part[0] * (chunks // part[1])

        def update(idx, _):
            base = pl.multiple_of(first + idx * 48, 8)
            for k in range(6):
                at = pl.ds(pl.multiple_of(base + 8 * k, 8), 8)
                clipped = grad_v[layer, at, :] * clip
                new_one = BETA_ONE * one_v[layer, at, :] + (1.0 - BETA_ONE) * clipped
                new_two = BETA_TWO * two_v[layer, at, :] + (1.0 - BETA_TWO) * clipped * clipped
                step_size = (new_one * one_scale) / (jnp.sqrt(new_two * two_scale) + ADAM_EPS)
                old = master_v[layer, at, :]
                master_out[layer, at, :] = old - LEARN_RATE * (step_size + WEIGHT_DECAY * old)
                one_out[layer, at, :] = new_one
                two_out[layer, at, :] = new_two
            return 0

        lax.fori_loop(0, chunks // part[1] // 48, update, 0)

    def round_rows(kind, layer, part):
        width = hidden_dim if kind == 0 else model_dim
        count = in_rows if kind == 0 else out_rows
        per_row = width // LANES
        dst = w_in if kind == 0 else w_out
        slot = lax.rem(me, 4)

        def body(idx, _):
            base = part[0] * (chunks // part[1]) + idx * (16 * per_row)
            row = pl.multiple_of(slot * count + part[0] * (count // part[1]) + idx * 16, 16)
            for col in range(per_row):
                top = master_out[layer, pl.ds(base + col, 8, stride=per_row), :]
                low = master_out[layer, pl.ds(base + 8 * per_row + col, 8, stride=per_row), :]
                dst[layer, pl.ds(row, 16), col * LANES:(col + 1) * LANES] = jnp.concatenate([top, low], axis=0).astype(BF16)
            return 0

        lax.fori_loop(0, count // 16 // part[1], body, 0)

    for layer in range(layers):
        for which in range(1, 4):
            load(which, layer).wait()
        for part in own_parts(layer):
            adam(layer, part)

            def send_own(kind):
                round_rows(kind, layer, part)
                if layer < layers - 1:
                    start(own_x(kind, layer, me, x_peer, (part,)))
                    start(own_y(kind, layer, me, y_peer, (part,)))
                start(pair(kind, layer, me, "pair_own", (part,)))

            by_kind(send_own)

    def pack(kind, device, packed_ref):
        spread_piece(dims, kind, device, (w_in, w_out), wide_ref)

        def squeeze(idx, _):
            at = pl.ds(pl.multiple_of(idx * 256, 256), 256)
            packed_ref[at, :] = wide_ref[at, :].astype(BF16)
            return 0

        lax.fori_loop(0, 4 * chunks // 256, squeeze, 0)

    def partner_of(device):
        return device + 1 - 2 * core

    def drain(kind):
        for layer in range(layers):
            left(own_x(kind, layer, me, x_peer))
            left(own_y(kind, layer, me, y_peer))
            left(pair(kind, layer, me, "pair_own", own_parts(layer)))
            left(pair(kind, layer, x_peer, "pair_x", own_parts(layer)))
            left(pair(1 - kind, layer, y_peer, "pair_y", own_parts(layer)))
            if layer < layers - 1:
                left(pair(1 - kind, layer, diag, "pair_far", far_parts(layer, 0) + far_parts(layer, 1)))
                left(far(kind, layer, 0, x_peer, y_peer))
                left(far(1 - kind, layer, 1, y_peer, x_peer))
        for step in range(1, GROUP):
            part_copy(step).wait_send()

    def drain_last(kind):
        layer = layers - 1
        left(far(kind, layer, 0, x_peer, y_peer))
        left(far(1 - kind, layer, 1, y_peer, x_peer))
        left(pair(1 - kind, layer, diag, "pair_far", far_parts(layer, 0) + far_parts(layer, 1)))

    def forward(kind, layer):
        x_order = own_parts(layer)
        y_order = x_order[::-1] if layer == layers - 1 else x_order
        for x_part, y_part in zip(x_order, y_order):
            arrive(own_x(kind, layer, x_peer, me, (x_part,)))
            if x_part in ((0, 2), (2, 6)):
                start(far(kind, layer, 0, x_peer, y_peer))
            start(pair(kind, layer, x_peer, "pair_x", (x_part,)))
            arrive(own_y(1 - kind, layer, y_peer, me, (y_part,)))
            if y_part == (1, 2):
                start(far(1 - kind, layer, 1, y_peer, x_peer))
            start(pair(1 - kind, layer, y_peer, "pair_y", (y_part,)))

    def far_arrive(kind, layer, only=None):
        for idx, parts in enumerate(zip(far_parts(layer, 0), far_parts(layer, 1))):
            if only is not None and idx != only:
                continue
            for half in range(2):
                arrive(far(1 - kind, layer, half, diag, me, (parts[half],)))
                start(pair(1 - kind, layer, diag, "pair_far", (parts[half],)))

    def far_partner(kind, layer):
        arrive(pair(1 - kind, layer, partner_of(diag), "pair_far", far_parts(layer, 0) + far_parts(layer, 1)))

    def near_partner(kind, layer):
        arrive(pair(kind, layer, partner_of(x_peer), "pair_x", own_parts(layer)))
        arrive(pair(1 - kind, layer, partner_of(y_peer), "pair_y", own_parts(layer)))

    def stage_own(kind):
        pack(kind, me, p0)
        forward(kind, 0)
        for layer in range(layers):
            arrive(pair(kind, layer, partner, "pair_own", own_parts(layer)))
        pack(kind, partner, p1)
        forward(kind, 1)
        start(own_x(kind, layers - 1, me, x_peer))
        start(own_y(kind, layers - 1, me, y_peer)[::-1])
        near_partner(kind, 0)
        far_arrive(kind, 0)
        near_partner(kind, 1)
        far_partner(kind, 0)

    def stage_one(kind):
        far_arrive(kind, 1)
        far_partner(kind, 1)

    def stage_two(kind):
        forward(kind, 2)
        pack(kind, x_peer, p2)
        pack(1 - kind, y_peer, p4)
        near_partner(kind, 2)
        far_arrive(kind, 2, 0)
        far_arrive(kind, 2, 1)
        drain(kind)
        far_arrive(kind, 2, 2)
        far_partner(kind, 2)
        drain_last(kind)

    by_kind(stage_own)
    tok_load.wait()
    mlp_block(dims, 0, w_in, w_out, hidden_ref, normed_ref, active_ref)
    by_kind(stage_one)
    mlp_block(dims, 1, w_in, w_out, hidden_ref, normed_ref, active_ref)
    by_kind(stage_two)


def finish_kernel(dims, p0, p1, p2, p4, master_ref, one_ref, two_ref, w_in, w_out, last_ref, tgt_ref,
                  packed_hbm, master_hbm, one_hbm, two_hbm, loss_hbm,
                  loss_ref, far_ref, wide_ref, normed_ref, active_ref, hidden_ref, sem, far_sem):
    layers, model_dim, hidden_dim, rows, chunks = dims
    me, core, y_pos, x_peer, y_peer, diag = places()
    twin = 1 - 2 * core

    copies = []
    for which, (src, dst) in enumerate(((master_ref, master_hbm), (one_ref, one_hbm), (two_ref, two_hbm))):
        for layer in range(layers):
            copies.append(pltpu.make_async_copy(src.at[layer], dst.at[:, layer, :], sem.at[6 + which * layers + layer]))
    for idx, (ref, device) in enumerate(((p0, me), (p1, me + twin), (p2, x_peer), (p4, y_peer))):
        copies.append(pltpu.make_async_copy(ref, packed_hbm.at[pl.ds(device * chunks, chunks)], sem.at[idx]))
    for item in copies:
        item.start()

    far_copies = []
    for idx, (device, flip) in enumerate(((x_peer + twin, 0), (y_peer + twin, 1), (diag, 1), (diag + twin, 1))):
        for y_value in range(2):
            @pl.when(y_pos == y_value)
            def _():
                spread_piece(dims, (y_value + flip) % 2, device, (w_in, w_out), wide_ref)

        def squeeze(at, _):
            block = wide_ref[pl.ds(pl.multiple_of(at * 128, 128), 128), :].astype(BF16).reshape(32, 4, LANES)
            far_ref[idx, pl.ds(at * 32, 32), :, :] = block[:, :layers, :]
            return 0

        lax.fori_loop(0, 4 * chunks // 128, squeeze, 0)
        far_copies.append(pltpu.make_async_copy(far_ref.at[idx], packed_hbm.at[pl.ds(device * chunks, chunks)], far_sem.at[idx]))
        far_copies[-1].start()

    hidden_ref[...] = last_ref[...]
    mlp_block(dims, layers - 1, w_in, w_out, hidden_ref, normed_ref, active_ref)

    for idx in range(rows // LANES):
        at = slice(idx * LANES, (idx + 1) * LANES)
        error = hidden_ref[at, :].astype(F32) - tgt_ref[at, :].astype(F32)
        error = error * error
        folded = error[:, 0:LANES]
        for col in range(LANES, model_dim, LANES):
            folded = folded + error[:, col:col + LANES]
        loss_ref[idx:idx + 1, :] = jnp.sum(folded.T, axis=0, keepdims=True) * (1.0 / model_dim)

    loss_copy = pltpu.make_async_copy(loss_ref, loss_hbm, far_sem.at[4])
    loss_copy.start()
    for item in copies + far_copies + [loss_copy]:
        item.wait()


def solution(mesh):
    group_size = mesh.shape["data"]
    state_spec = P(None, "data")
    row_spec = P("data", None)

    def local_step(grad_shard, master_shard, one_shard, two_shard, tok_rows, tgt_rows):
        rows, model_dim = tok_rows.shape
        layers, cols = master_shard.shape
        half_size = cols * group_size // 2
        hidden_dim = half_size // model_dim
        chunks = cols // LANES
        dims = (layers, model_dim, hidden_dim, rows, chunks)
        tiled = [a.reshape(layers, chunks, LANES).transpose(1, 0, 2) for a in (grad_shard, master_shard, one_shard, two_shard)]
        state_v = pltpu.VMEM((layers, chunks, LANES), F32)
        hbm = pl.BlockSpec(memory_space=pltpu.HBM)
        vmem = pl.BlockSpec(memory_space=pltpu.VMEM)
        state_out = state_v
        w_in_v = pltpu.VMEM((layers, model_dim, hidden_dim), BF16)
        w_out_v = pltpu.VMEM((layers, hidden_dim, model_dim), BF16)
        hidden_v = pltpu.VMEM((rows, model_dim), BF16)
        wide_v = pltpu.VMEM((4 * chunks, LANES), F32)
        normed_v = pltpu.VMEM((256, model_dim), BF16)
        active_v = pltpu.VMEM((256, hidden_dim), BF16)
        packed_v = pltpu.VMEM((4 * chunks, LANES), BF16)
        gathered = pl.pallas_call(
            functools.partial(gather_kernel, dims),
            name="gather_step",
            out_shape=(*(packed_v,) * 4, state_v, state_v, state_v, w_in_v, w_out_v, hidden_v),
            in_specs=[hbm] * 5,
            out_specs=(vmem,) * 10,
            scratch_shapes=[
                state_v, state_v, state_v, state_v,
                pltpu.VMEM((group_size, 1, LANES), F32),
                wide_v, normed_v, active_v,
                pltpu.SemaphoreType.DMA((5, layers)),
                pltpu.SemaphoreType.DMA((layers, 3)),
                pltpu.SemaphoreType.DMA((group_size,)),
                pltpu.SemaphoreType.DMA((group_size,)),
                pltpu.SemaphoreType.DMA((96,)),
                pltpu.SemaphoreType.DMA((96,)),
            ],
            compiler_params=pltpu.CompilerParams(collective_id=0, has_side_effects=True, vmem_limit_bytes=19 << 20),
        )(*[pltpu.with_memory_space_constraint(a, pltpu.HBM) for a in (*tiled, tok_rows)])
        gathered = [a.reshape(chunks, 4, LANES)[:, :layers, :] for a in gathered[:4]] + list(gathered[4:])
        state_tile = jax.ShapeDtypeStruct((chunks, layers, LANES), F32)
        weights, new_master, new_one, new_two, row_loss = pl.pallas_call(
            functools.partial(finish_kernel, dims),
            name="finish",
            out_shape=(jax.ShapeDtypeStruct((chunks * group_size, layers, LANES), BF16), state_tile, state_tile, state_tile,
                       jax.ShapeDtypeStruct((rows // LANES, LANES), F32)),
            in_specs=[vmem] * 11,
            out_specs=(hbm,) * 5,
            scratch_shapes=[
                pltpu.VMEM((rows // LANES, LANES), F32),
                pltpu.VMEM((4, chunks, layers, LANES), BF16),
                wide_v, normed_v, active_v, hidden_v,
                pltpu.SemaphoreType.DMA((6 + 3 * layers,)),
                pltpu.SemaphoreType.DMA((5,)),
            ],
            compiler_params=pltpu.CompilerParams(vmem_limit_bytes=18 << 20),
        )(*gathered, tgt_rows)

        def flat(a):
            return a.transpose(1, 0, 2).reshape(layers, a.shape[0] * LANES)

        return row_loss.reshape(rows), flat(weights), flat(new_master), flat(new_one), flat(new_two)

    return jax.shard_map(local_step, mesh=mesh, in_specs=(state_spec, state_spec, state_spec, state_spec, row_spec, row_spec), out_specs=(P("data"), P(), state_spec, state_spec, state_spec), check_vma=False)
```

```python
import functools

import jax
import jax.numpy as jnp
from jax import lax
from jax.experimental import pallas as pl
from jax.experimental.pallas import tpu as pltpu
from jax.sharding import PartitionSpec as P

LEARN_RATE = 0.01
BETA_ONE = 0.9
BETA_TWO = 0.95
ADAM_EPS = 1e-8
WEIGHT_DECAY = 0.1
ADAM_STEP = 10
CLIP_NORM = 1.0
NORM_EPS = 1e-6

MESH = pl.DeviceIdType.MESH
LANES = 128
GROUP = 8
F32 = jnp.float32
BF16 = jnp.bfloat16


def spread_piece(dims, kind, device, weights, wide_ref):
    layers, model_dim, hidden_dim, rows, chunks = dims
    per_row = (hidden_dim if kind == 0 else model_dim) // LANES
    count = chunks // per_row
    src = weights[kind]
    slot = lax.rem(device, 4)

    def spread(idx, _):
        row = pl.multiple_of(slot * count + idx * 16, 16)
        for layer in range(layers):
            for col in range(per_row):
                tile = src[layer, pl.ds(row, 16), col * LANES:(col + 1) * LANES].astype(F32)
                base = layer + 4 * (idx * (16 * per_row) + col)
                wide_ref[pl.ds(base, 8, stride=4 * per_row), :] = tile[0:8]
                wide_ref[pl.ds(base + 32 * per_row, 8, stride=4 * per_row), :] = tile[8:16]
        return 0

    lax.fori_loop(0, count // 16, spread, 0)


def mlp_block(dims, layer, w_in, w_out, hidden_ref, normed_ref, active_ref):
    layers, model_dim, hidden_dim, rows, chunks = dims

    def block(idx, _):
        at = pl.ds(pl.multiple_of(idx * 256, 256), 256)
        hidden = hidden_ref[at, :].astype(F32)
        scale = lax.rsqrt(jnp.mean(hidden * hidden, axis=-1, keepdims=True) + NORM_EPS)
        normed_ref[...] = (hidden * scale).astype(BF16)
        for col in range(0, hidden_dim, 384):
            inner = jnp.dot(normed_ref[...], w_in[layer, :, col:col + 384], preferred_element_type=F32).astype(BF16)
            active_ref[:, col:col + 384] = jax.nn.gelu(inner.astype(F32), approximate=True).astype(BF16)
        for col in range(0, model_dim, 256):
            add = jnp.dot(active_ref[...], w_out[layer, :, col:col + 256], preferred_element_type=F32)
            hidden_ref[at, col:col + 256] = (hidden_ref[at, col:col + 256].astype(F32) + add).astype(BF16)
        return 0

    lax.fori_loop(0, rows // 256, block, 0)


def places():
    me = lax.axis_index("data")
    core = lax.rem(me, 2)
    x_pos = lax.rem(me // 2, 2)
    y_pos = me // 4
    x_peer = me + 2 - 4 * x_pos
    y_peer = me + 4 - 8 * y_pos
    return me, core, y_pos, x_peer, y_peer, x_peer + 4 - 8 * y_pos


def gather_kernel(dims, grad_hbm, master_hbm, one_hbm, two_hbm, tok_hbm,
                  p0, p1, p2, p3, p4, p5, master_out, one_out, two_out, w_in, w_out, hidden_ref,
                  grad_v, master_v, one_v, two_v,
                  part_ref, wide_ref, normed_ref, active_ref,
                  load_sem, grad_sem, part_send, part_recv, send_sem, recv_sem):
    layers, model_dim, hidden_dim, rows, chunks = dims
    in_rows = chunks * LANES // hidden_dim
    out_rows = chunks * LANES // model_dim

    me, core, y_pos, x_peer, y_peer, diag = places()
    partner = me + 1 - 2 * core

    state = ((grad_hbm, grad_v), (master_hbm, master_v), (one_hbm, one_v), (two_hbm, two_v))

    def load(which, layer):
        src, dst = state[which]
        return pltpu.make_async_copy(src.at[:, layer, :], dst.at[layer], load_sem.at[which, layer])

    span = chunks // 3

    def grad_load(layer, part):
        at = pl.ds(part * span, span)
        return pltpu.make_async_copy(grad_hbm.at[at, layer, :], grad_v.at[layer, at], grad_sem.at[layer, part])

    for layer in range(layers):
        for part in range(3):
            grad_load(layer, part).start()
    tok_load = pltpu.make_async_copy(tok_hbm, hidden_ref, load_sem.at[4, 0])

    barrier = pltpu.get_barrier_semaphore()
    for step in range(1, GROUP):
        pl.semaphore_signal(barrier, inc=1, device_id=(lax.rem(me + step, GROUP),), device_id_type=MESH)

    sums = tuple(jnp.zeros((8, LANES), F32) for _ in range(8))
    for layer in range(layers):
        for part in range(3):
            grad_load(layer, part).wait()
            if layer == layers - 1 and part == 2:
                for which in range(1, 4):
                    load(which, 0).start()

            def square(idx, carry):
                base = pl.multiple_of(part * span + idx * 64, 64)
                block = grad_v[layer, pl.ds(base, 64), :]
                return tuple(carry[k] + block[8 * k:8 * k + 8] * block[8 * k:8 * k + 8] for k in range(8))

            sums = lax.fori_loop(0, span // 64, square, sums)
    mine = ((sums[0] + sums[1]) + (sums[2] + sums[3])) + ((sums[4] + sums[5]) + (sums[6] + sums[7]))
    part_ref[me] = jnp.sum(mine, axis=0, keepdims=True)
    pl.semaphore_wait(barrier, GROUP - 1)

    def part_copy(step):
        return pltpu.make_async_remote_copy(
            src_ref=part_ref.at[me], dst_ref=part_ref.at[me],
            send_sem=part_send.at[step], recv_sem=part_recv.at[step],
            device_id=(lax.rem(me + step, GROUP),), device_id_type=MESH)

    def part_arrival(step):
        slot = lax.rem(me + GROUP - step, GROUP)
        return pltpu.make_async_remote_copy(
            src_ref=part_ref.at[slot], dst_ref=part_ref.at[slot],
            send_sem=part_send.at[step], recv_sem=part_recv.at[step],
            device_id=(me,), device_id_type=MESH)

    for step in range(1, GROUP):
        part_copy(step).start()
    for item in range(1, layers):
        for which in range(1, 4):
            load(which, item).start()
    tok_load.start()
    for step in range(1, GROUP):
        part_arrival(step).wait_recv()
    total = part_ref[0]
    for slot in range(1, GROUP):
        total = total + part_ref[slot]
    total = jnp.sum(total, axis=1, keepdims=True)
    clip = jnp.minimum(1.0, CLIP_NORM / jnp.sqrt(total))
    clip = jnp.broadcast_to(clip, (8, LANES))

    slots = {}

    def piece(kind, layer, device, part):
        ref, count = ((w_in, in_rows), (w_out, out_rows))[kind]
        span = count // part[1]
        at = lax.rem(device, 4) * count + part[0] * span
        return ref.at[layer, pl.ds(pl.multiple_of(at, 16), span), :]

    def copies(kind, layer, device, route, target, parts):
        out = []
        for part in parts:
            ref = piece(kind, layer, device, part)
            index = slots.setdefault((route, layer, part), len(slots))
            out.append(pltpu.make_async_remote_copy(
                src_ref=ref, dst_ref=ref, send_sem=send_sem.at[index],
                recv_sem=recv_sem.at[index], device_id=(target,), device_id_type=MESH))
        return out

    def start(items):
        for item in items:
            item.start()

    def arrive(items):
        for item in items:
            item.wait_recv()

    def left(items):
        for item in items:
            item.wait_send()

    def own_parts(layer):
        return ((0, 6), (1, 6), (2, 6), (1, 2)) if layer == 0 else ((0, 2), (1, 2))

    def far_parts(layer, half):
        return tuple((3 * half + at, 6) for at in range(3)) if layer == layers - 1 else ((half, 2),)

    def own_x(kind, layer, device, target, parts=None):
        return copies(kind, layer, device, "own_x", target, parts or own_parts(layer))

    def own_y(kind, layer, device, target, parts=None):
        return copies(kind, layer, device, "own_y", target, parts or own_parts(layer))

    def far(kind, layer, half, device, target, parts=None):
        return copies(kind, layer, device, "far", target, parts or far_parts(layer, half))

    def pair(kind, layer, device, route, parts):
        return copies(kind, layer, device, route, partner, parts)

    def by_kind(function):
        for y_value in range(2):
            @pl.when(y_pos == y_value)
            def _():
                function(y_value)

    one_scale = 1.0 / (1.0 - BETA_ONE ** ADAM_STEP)
    two_scale = 1.0 / (1.0 - BETA_TWO ** ADAM_STEP)

    def adam(layer, part):
        first = part[0] * (chunks // part[1])

        def update(idx, _):
            base = pl.multiple_of(first + idx * 48, 8)
            for k in range(6):
                at = pl.ds(pl.multiple_of(base + 8 * k, 8), 8)
                clipped = grad_v[layer, at, :] * clip
                new_one = BETA_ONE * one_v[layer, at, :] + (1.0 - BETA_ONE) * clipped
                new_two = BETA_TWO * two_v[layer, at, :] + (1.0 - BETA_TWO) * clipped * clipped
                step_size = (new_one * one_scale) / (jnp.sqrt(new_two * two_scale) + ADAM_EPS)
                old = master_v[layer, at, :]
                master_out[layer, at, :] = old - LEARN_RATE * (step_size + WEIGHT_DECAY * old)
                one_out[layer, at, :] = new_one
                two_out[layer, at, :] = new_two
            return 0

        lax.fori_loop(0, chunks // part[1] // 48, update, 0)

    def round_rows(kind, layer, part):
        width = hidden_dim if kind == 0 else model_dim
        count = in_rows if kind == 0 else out_rows
        per_row = width // LANES
        dst = w_in if kind == 0 else w_out
        slot = lax.rem(me, 4)

        def body(idx, _):
            base = part[0] * (chunks // part[1]) + idx * (16 * per_row)
            row = pl.multiple_of(slot * count + part[0] * (count // part[1]) + idx * 16, 16)
            for col in range(per_row):
                top = master_out[layer, pl.ds(base + col, 8, stride=per_row), :]
                low = master_out[layer, pl.ds(base + 8 * per_row + col, 8, stride=per_row), :]
                dst[layer, pl.ds(row, 16), col * LANES:(col + 1) * LANES] = jnp.concatenate([top, low], axis=0).astype(BF16)
            return 0

        lax.fori_loop(0, count // 16 // part[1], body, 0)

    for layer in range(layers):
        for which in range(1, 4):
            load(which, layer).wait()
        for part in own_parts(layer):
            adam(layer, part)

            def send_own(kind):
                round_rows(kind, layer, part)
                if layer < layers - 1:
                    start(own_x(kind, layer, me, x_peer, (part,)))
                    start(own_y(kind, layer, me, y_peer, (part,)))
                start(pair(kind, layer, me, "pair_own", (part,)))

            by_kind(send_own)

    def pack(kind, device, packed_ref):
        spread_piece(dims, kind, device, (w_in, w_out), wide_ref)

        def squeeze(idx, _):
            at = pl.ds(pl.multiple_of(idx * 256, 256), 256)
            packed_ref[at, :] = wide_ref[at, :].astype(BF16)
            return 0

        lax.fori_loop(0, 4 * chunks // 256, squeeze, 0)

    def partner_of(device):
        return device + 1 - 2 * core

    def drain(kind):
        for layer in range(layers):
            left(own_x(kind, layer, me, x_peer))
            left(own_y(kind, layer, me, y_peer))
            left(pair(kind, layer, me, "pair_own", own_parts(layer)))
            left(pair(kind, layer, x_peer, "pair_x", own_parts(layer)))
            left(pair(1 - kind, layer, y_peer, "pair_y", own_parts(layer)))
            if layer < layers - 1:
                left(pair(1 - kind, layer, diag, "pair_far", far_parts(layer, 0) + far_parts(layer, 1)))
                left(far(kind, layer, 0, x_peer, y_peer))
                left(far(1 - kind, layer, 1, y_peer, x_peer))
        for step in range(1, GROUP):
            part_copy(step).wait_send()

    def drain_last(kind):
        layer = layers - 1
        left(far(kind, layer, 0, x_peer, y_peer, far_parts(layer, 0)[:-1]))
        left(far(1 - kind, layer, 1, y_peer, x_peer, far_parts(layer, 1)[:-1]))

        @pl.when(chip != 0)
        def _():
            left(far(kind, layer, 0, x_peer, y_peer, far_parts(layer, 0)[-1:]))
            left(far(1 - kind, layer, 1, y_peer, x_peer, far_parts(layer, 1)[-1:]))

        @pl.when(chip == last_chip)
        def _():
            left(moved(kind, 0))
            left(moved(kind, 1))

        left(pair(1 - kind, layer, diag, "pair_far", far_parts(layer, 0) + far_parts(layer, 1)))

    chip = me // 2
    last_chip = GROUP // 2 - 1

    def start_far(kind, layer, half, device, target):
        if layer < layers - 1:
            start(far(kind, layer, half, device, target))
            return
        start(far(kind, layer, half, device, target, far_parts(layer, half)[:-1]))

        @pl.when(chip != 0)
        def _():
            start(far(kind, layer, half, device, target, far_parts(layer, half)[-1:]))

    def moved(kind, half):
        source = (y_peer, x_peer)[half]
        target = (x_peer, y_peer)[half]
        return far((1 - kind, kind)[half], layers - 1, half, source, target, far_parts(layers - 1, half)[-1:])

    def forward(kind, layer):
        x_order = own_parts(layer)
        y_order = x_order[::-1] if layer == layers - 1 else x_order
        for x_part, y_part in zip(x_order, y_order):
            arrive(own_x(kind, layer, x_peer, me, (x_part,)))
            if x_part in ((0, 2), (2, 6)):
                start_far(kind, layer, 0, x_peer, y_peer)
            start(pair(kind, layer, x_peer, "pair_x", (x_part,)))
            arrive(own_y(1 - kind, layer, y_peer, me, (y_part,)))
            if y_part == (1, 2):
                start_far(1 - kind, layer, 1, y_peer, x_peer)
            start(pair(1 - kind, layer, y_peer, "pair_y", (y_part,)))

    def far_arrive(kind, layer, only=None):
        for idx, parts in enumerate(zip(far_parts(layer, 0), far_parts(layer, 1))):
            if only is not None and idx != only:
                continue
            for half in range(2):
                arrive(far(1 - kind, layer, half, diag, me, (parts[half],)))
                start(pair(1 - kind, layer, diag, "pair_far", (parts[half],)))

    def far_partner(kind, layer):
        arrive(pair(1 - kind, layer, partner_of(diag), "pair_far", far_parts(layer, 0) + far_parts(layer, 1)))

    def near_partner(kind, layer):
        arrive(pair(kind, layer, partner_of(x_peer), "pair_x", own_parts(layer)))
        arrive(pair(1 - kind, layer, partner_of(y_peer), "pair_y", own_parts(layer)))

    def stage_own(kind):
        pack(kind, me, p0)
        forward(kind, 0)
        for layer in range(layers):
            arrive(pair(kind, layer, partner, "pair_own", own_parts(layer)))
        pack(kind, partner, p1)
        forward(kind, 1)
        start(own_x(kind, layers - 1, me, x_peer))
        start(own_y(kind, layers - 1, me, y_peer)[::-1])
        near_partner(kind, 0)
        far_arrive(kind, 0)
        near_partner(kind, 1)
        far_partner(kind, 0)

    def stage_one(kind):
        far_arrive(kind, 1)
        far_partner(kind, 1)

    def stage_two(kind):
        forward(kind, 2)

        @pl.when(chip == last_chip)
        def _():
            start(moved(kind, 0))
            start(moved(kind, 1))

        pack(kind, x_peer, p2)
        pack(1 - kind, y_peer, p4)
        near_partner(kind, 2)
        far_arrive(kind, 2, 0)
        pack(kind, partner_of(x_peer), p3)
        far_arrive(kind, 2, 1)
        pack(1 - kind, partner_of(y_peer), p5)
        drain(kind)
        far_arrive(kind, 2, 2)
        far_partner(kind, 2)
        drain_last(kind)

    by_kind(stage_own)
    tok_load.wait()
    mlp_block(dims, 0, w_in, w_out, hidden_ref, normed_ref, active_ref)
    by_kind(stage_one)
    mlp_block(dims, 1, w_in, w_out, hidden_ref, normed_ref, active_ref)
    by_kind(stage_two)


def finish_kernel(dims, p0, p1, p2, p3, p4, p5, master_ref, one_ref, two_ref, w_in, w_out, last_ref, tgt_ref,
                  packed_hbm, master_hbm, one_hbm, two_hbm, loss_hbm,
                  loss_ref, far_ref, wide_ref, normed_ref, active_ref, hidden_ref, sem, far_sem):
    layers, model_dim, hidden_dim, rows, chunks = dims
    me, core, y_pos, x_peer, y_peer, diag = places()
    twin = 1 - 2 * core

    copies = []
    for which, (src, dst) in enumerate(((master_ref, master_hbm), (one_ref, one_hbm), (two_ref, two_hbm))):
        for layer in range(layers):
            copies.append(pltpu.make_async_copy(src.at[layer], dst.at[:, layer, :], sem.at[6 + which * layers + layer]))
    for idx, (ref, device) in enumerate(((p0, me), (p1, me + twin), (p2, x_peer), (p3, x_peer + twin), (p4, y_peer), (p5, y_peer + twin))):
        copies.append(pltpu.make_async_copy(ref, packed_hbm.at[pl.ds(device * chunks, chunks)], sem.at[idx]))
    for item in copies:
        item.start()

    far_copies = []
    for idx, device in enumerate((diag, diag + twin)):
        for y_value in range(2):
            @pl.when(y_pos == y_value)
            def _():
                spread_piece(dims, 1 - y_value, device, (w_in, w_out), wide_ref)

        def squeeze(at, _):
            block = wide_ref[pl.ds(pl.multiple_of(at * 128, 128), 128), :].astype(BF16).reshape(32, 4, LANES)
            far_ref[idx, pl.ds(at * 32, 32), :, :] = block[:, :layers, :]
            return 0

        lax.fori_loop(0, 4 * chunks // 128, squeeze, 0)
        far_copies.append(pltpu.make_async_copy(far_ref.at[idx], packed_hbm.at[pl.ds(device * chunks, chunks)], far_sem.at[idx]))
        far_copies[-1].start()

    hidden_ref[...] = last_ref[...]
    mlp_block(dims, layers - 1, w_in, w_out, hidden_ref, normed_ref, active_ref)

    for idx in range(rows // LANES):
        at = slice(idx * LANES, (idx + 1) * LANES)
        error = hidden_ref[at, :].astype(F32) - tgt_ref[at, :].astype(F32)
        error = error * error
        folded = error[:, 0:LANES]
        for col in range(LANES, model_dim, LANES):
            folded = folded + error[:, col:col + LANES]
        loss_ref[idx:idx + 1, :] = jnp.sum(folded.T, axis=0, keepdims=True) * (1.0 / model_dim)

    loss_copy = pltpu.make_async_copy(loss_ref, loss_hbm, far_sem.at[2])
    loss_copy.start()
    for item in copies + far_copies + [loss_copy]:
        item.wait()


def solution(mesh):
    group_size = mesh.shape["data"]
    state_spec = P(None, "data")
    row_spec = P("data", None)

    def local_step(grad_shard, master_shard, one_shard, two_shard, tok_rows, tgt_rows):
        rows, model_dim = tok_rows.shape
        layers, cols = master_shard.shape
        half_size = cols * group_size // 2
        hidden_dim = half_size // model_dim
        chunks = cols // LANES
        dims = (layers, model_dim, hidden_dim, rows, chunks)
        tiled = [a.reshape(layers, chunks, LANES).transpose(1, 0, 2) for a in (grad_shard, master_shard, one_shard, two_shard)]
        state_v = pltpu.VMEM((layers, chunks, LANES), F32)
        hbm = pl.BlockSpec(memory_space=pltpu.HBM)
        vmem = pl.BlockSpec(memory_space=pltpu.VMEM)
        state_out = state_v
        w_in_v = pltpu.VMEM((layers, model_dim, hidden_dim), BF16)
        w_out_v = pltpu.VMEM((layers, hidden_dim, model_dim), BF16)
        hidden_v = pltpu.VMEM((rows, model_dim), BF16)
        wide_v = pltpu.VMEM((4 * chunks, LANES), F32)
        normed_v = pltpu.VMEM((256, model_dim), BF16)
        active_v = pltpu.VMEM((256, hidden_dim), BF16)
        packed_v = pltpu.VMEM((4 * chunks, LANES), BF16)
        gathered = pl.pallas_call(
            functools.partial(gather_kernel, dims),
            name="gather_step",
            out_shape=(*(packed_v,) * 6, state_v, state_v, state_v, w_in_v, w_out_v, hidden_v),
            in_specs=[hbm] * 5,
            out_specs=(vmem,) * 12,
            scratch_shapes=[
                state_v, state_v, state_v, state_v,
                pltpu.VMEM((group_size, 1, LANES), F32),
                wide_v, normed_v, active_v,
                pltpu.SemaphoreType.DMA((5, layers)),
                pltpu.SemaphoreType.DMA((layers, 3)),
                pltpu.SemaphoreType.DMA((group_size,)),
                pltpu.SemaphoreType.DMA((group_size,)),
                pltpu.SemaphoreType.DMA((96,)),
                pltpu.SemaphoreType.DMA((96,)),
            ],
            compiler_params=pltpu.CompilerParams(collective_id=0, has_side_effects=True, vmem_limit_bytes=19 << 20),
        )(*[pltpu.with_memory_space_constraint(a, pltpu.HBM) for a in (*tiled, tok_rows)])
        gathered = [a.reshape(chunks, 4, LANES)[:, :layers, :] for a in gathered[:6]] + list(gathered[6:])
        state_tile = jax.ShapeDtypeStruct((chunks, layers, LANES), F32)
        weights, new_master, new_one, new_two, row_loss = pl.pallas_call(
            functools.partial(finish_kernel, dims),
            name="finish",
            out_shape=(jax.ShapeDtypeStruct((chunks * group_size, layers, LANES), BF16), state_tile, state_tile, state_tile,
                       jax.ShapeDtypeStruct((rows // LANES, LANES), F32)),
            in_specs=[vmem] * 13,
            out_specs=(hbm,) * 5,
            scratch_shapes=[
                pltpu.VMEM((rows // LANES, LANES), F32),
                pltpu.VMEM((2, chunks, layers, LANES), BF16),
                wide_v, normed_v, active_v, hidden_v,
                pltpu.SemaphoreType.DMA((6 + 3 * layers,)),
                pltpu.SemaphoreType.DMA((3,)),
            ],
            compiler_params=pltpu.CompilerParams(vmem_limit_bytes=14 << 20),
        )(*gathered, tgt_rows)

        def flat(a):
            return a.transpose(1, 0, 2).reshape(layers, a.shape[0] * LANES)

        return row_loss.reshape(rows), flat(weights), flat(new_master), flat(new_one), flat(new_two)

    return jax.shard_map(local_step, mesh=mesh, in_specs=(state_spec, state_spec, state_spec, state_spec, row_spec, row_spec), out_specs=(P("data"), P(), state_spec, state_spec, state_spec), check_vma=False)
```

```python
import functools

import jax
import jax.numpy as jnp
from jax import lax
from jax.experimental import pallas as pl
from jax.experimental.pallas import tpu as pltpu
from jax.sharding import PartitionSpec as P

LEARN_RATE = 0.01
BETA_ONE = 0.9
BETA_TWO = 0.95
ADAM_EPS = 1e-8
WEIGHT_DECAY = 0.1
ADAM_STEP = 10
CLIP_NORM = 1.0
NORM_EPS = 1e-6

MESH = pl.DeviceIdType.MESH
LANES = 128
GROUP = 8
F32 = jnp.float32
BF16 = jnp.bfloat16


def spread_piece(dims, kind, device, weights, wide_ref):
    layers, model_dim, hidden_dim, rows, chunks = dims
    per_row = (hidden_dim if kind == 0 else model_dim) // LANES
    count = chunks // per_row
    src = weights[kind]
    slot = lax.rem(device, 4)

    def spread(idx, _):
        row = pl.multiple_of(slot * count + idx * 16, 16)
        for layer in range(layers):
            for col in range(per_row):
                tile = src[layer, pl.ds(row, 16), col * LANES:(col + 1) * LANES].astype(F32)
                base = layer + 4 * (idx * (16 * per_row) + col)
                wide_ref[pl.ds(base, 8, stride=4 * per_row), :] = tile[0:8]
                wide_ref[pl.ds(base + 32 * per_row, 8, stride=4 * per_row), :] = tile[8:16]
        return 0

    lax.fori_loop(0, count // 16, spread, 0)


def mlp_block(dims, layer, w_in, w_out, hidden_ref, normed_ref, active_ref):
    layers, model_dim, hidden_dim, rows, chunks = dims

    def block(idx, _):
        at = pl.ds(pl.multiple_of(idx * 256, 256), 256)
        hidden = hidden_ref[at, :].astype(F32)
        scale = lax.rsqrt(jnp.mean(hidden * hidden, axis=-1, keepdims=True) + NORM_EPS)
        normed_ref[...] = (hidden * scale).astype(BF16)
        for col in range(0, hidden_dim, 384):
            inner = jnp.dot(normed_ref[...], w_in[layer, :, col:col + 384], preferred_element_type=F32).astype(BF16)
            active_ref[:, col:col + 384] = jax.nn.gelu(inner.astype(F32), approximate=True).astype(BF16)
        for col in range(0, model_dim, 256):
            add = jnp.dot(active_ref[...], w_out[layer, :, col:col + 256], preferred_element_type=F32)
            hidden_ref[at, col:col + 256] = (hidden_ref[at, col:col + 256].astype(F32) + add).astype(BF16)
        return 0

    lax.fori_loop(0, rows // 256, block, 0)


def places():
    me = lax.axis_index("data")
    core = lax.rem(me, 2)
    x_pos = lax.rem(me // 2, 2)
    y_pos = me // 4
    x_peer = me + 2 - 4 * x_pos
    y_peer = me + 4 - 8 * y_pos
    return me, core, y_pos, x_peer, y_peer, x_peer + 4 - 8 * y_pos


def gather_kernel(dims, grad_hbm, master_hbm, one_hbm, two_hbm, tok_hbm,
                  p0, p1, p2, p3, p4, p5, master_out, one_out, two_out, w_in, w_out, hidden_ref,
                  grad_t, grad_v, master_v, one_v, two_v,
                  part_ref, wide_ref, normed_ref, active_ref,
                  load_sem, grad_sem, part_send, part_recv, send_sem, recv_sem):
    layers, model_dim, hidden_dim, rows, chunks = dims
    in_rows = chunks * LANES // hidden_dim
    out_rows = chunks * LANES // model_dim

    me, core, y_pos, x_peer, y_peer, diag = places()
    partner = me + 1 - 2 * core

    state = ((grad_hbm, grad_v), (master_hbm, master_v), (one_hbm, one_v), (two_hbm, two_v))

    def load(which, layer):
        src, dst = state[which]
        return pltpu.make_async_copy(src.at[:, layer, :], dst.at[layer], load_sem.at[which, layer])

    span = chunks // 3

    loads = 9
    span = chunks // loads

    def grad_load(part):
        at = pl.ds(part * span, span)
        return pltpu.make_async_copy(grad_hbm.at[at], grad_t.at[at], grad_sem.at[part])

    for part in range(loads):
        grad_load(part).start()
    tok_load = pltpu.make_async_copy(tok_hbm, hidden_ref, load_sem.at[4, 0])

    barrier = pltpu.get_barrier_semaphore()
    for step in range(1, GROUP):
        pl.semaphore_signal(barrier, inc=1, device_id=(lax.rem(me + step, GROUP),), device_id_type=MESH)

    sums = tuple(jnp.zeros((layers, LANES), F32) for _ in range(8))
    for part in range(loads):
        grad_load(part).wait()
        if part == loads - 1:
            for which in range(4):
                load(which, 0).start()

        def square(idx, carry):
            block = grad_t[pl.ds(part * span + idx * 16, 16), :, :]
            for k in range(16):
                carry = carry[:k % 8] + (carry[k % 8] + block[k] * block[k],) + carry[k % 8 + 1:]
            return carry

        sums = lax.fori_loop(0, span // 16, square, sums)
    mine = ((sums[0] + sums[1]) + (sums[2] + sums[3])) + ((sums[4] + sums[5]) + (sums[6] + sums[7]))
    part_ref[me] = jnp.sum(mine, axis=0, keepdims=True)
    pl.semaphore_wait(barrier, GROUP - 1)

    def part_copy(step):
        return pltpu.make_async_remote_copy(
            src_ref=part_ref.at[me], dst_ref=part_ref.at[me],
            send_sem=part_send.at[step], recv_sem=part_recv.at[step],
            device_id=(lax.rem(me + step, GROUP),), device_id_type=MESH)

    def part_arrival(step):
        slot = lax.rem(me + GROUP - step, GROUP)
        return pltpu.make_async_remote_copy(
            src_ref=part_ref.at[slot], dst_ref=part_ref.at[slot],
            send_sem=part_send.at[step], recv_sem=part_recv.at[step],
            device_id=(me,), device_id_type=MESH)

    for step in range(1, GROUP):
        part_copy(step).start()
    for item in range(1, layers):
        for which in range(4):
            load(which, item).start()
    tok_load.start()
    for step in range(1, GROUP):
        part_arrival(step).wait_recv()
    total = part_ref[0]
    for slot in range(1, GROUP):
        total = total + part_ref[slot]
    total = jnp.sum(total, axis=1, keepdims=True)
    clip = jnp.minimum(1.0, CLIP_NORM / jnp.sqrt(total))
    clip = jnp.broadcast_to(clip, (8, LANES))

    slots = {}

    def piece(kind, layer, device, part):
        ref, count = ((w_in, in_rows), (w_out, out_rows))[kind]
        span = count // part[1]
        at = lax.rem(device, 4) * count + part[0] * span
        return ref.at[layer, pl.ds(pl.multiple_of(at, 16), span), :]

    def copies(kind, layer, device, route, target, parts):
        out = []
        for part in parts:
            ref = piece(kind, layer, device, part)
            index = slots.setdefault((route, layer, part), len(slots))
            out.append(pltpu.make_async_remote_copy(
                src_ref=ref, dst_ref=ref, send_sem=send_sem.at[index],
                recv_sem=recv_sem.at[index], device_id=(target,), device_id_type=MESH))
        return out

    def start(items):
        for item in items:
            item.start()

    def arrive(items):
        for item in items:
            item.wait_recv()

    def left(items):
        for item in items:
            item.wait_send()

    def own_parts(layer):
        return ((0, 6), (1, 6), (2, 6), (1, 2)) if layer == 0 else ((0, 2), (1, 2))

    def far_parts(layer, half):
        return tuple((3 * half + at, 6) for at in range(3)) if layer == layers - 1 else ((half, 2),)

    def own_x(kind, layer, device, target, parts=None):
        return copies(kind, layer, device, "own_x", target, parts or own_parts(layer))

    def own_y(kind, layer, device, target, parts=None):
        return copies(kind, layer, device, "own_y", target, parts or own_parts(layer))

    def far(kind, layer, half, device, target, parts=None):
        return copies(kind, layer, device, "far", target, parts or far_parts(layer, half))

    def pair(kind, layer, device, route, parts):
        return copies(kind, layer, device, route, partner, parts)

    def by_kind(function):
        for y_value in range(2):
            @pl.when(y_pos == y_value)
            def _():
                function(y_value)

    one_scale = 1.0 / (1.0 - BETA_ONE ** ADAM_STEP)
    two_scale = 1.0 / (1.0 - BETA_TWO ** ADAM_STEP)

    def adam(layer, part):
        first = part[0] * (chunks // part[1])

        def update(idx, _):
            base = pl.multiple_of(first + idx * 48, 8)
            for k in range(6):
                at = pl.ds(pl.multiple_of(base + 8 * k, 8), 8)
                clipped = grad_v[layer, at, :] * clip
                new_one = BETA_ONE * one_v[layer, at, :] + (1.0 - BETA_ONE) * clipped
                new_two = BETA_TWO * two_v[layer, at, :] + (1.0 - BETA_TWO) * clipped * clipped
                step_size = (new_one * one_scale) / (jnp.sqrt(new_two * two_scale) + ADAM_EPS)
                old = master_v[layer, at, :]
                master_out[layer, at, :] = old - LEARN_RATE * (step_size + WEIGHT_DECAY * old)
                one_out[layer, at, :] = new_one
                two_out[layer, at, :] = new_two
            return 0

        lax.fori_loop(0, chunks // part[1] // 48, update, 0)

    def round_rows(kind, layer, part):
        width = hidden_dim if kind == 0 else model_dim
        count = in_rows if kind == 0 else out_rows
        per_row = width // LANES
        dst = w_in if kind == 0 else w_out
        slot = lax.rem(me, 4)

        def body(idx, _):
            base = part[0] * (chunks // part[1]) + idx * (16 * per_row)
            row = pl.multiple_of(slot * count + part[0] * (count // part[1]) + idx * 16, 16)
            for col in range(per_row):
                top = master_out[layer, pl.ds(base + col, 8, stride=per_row), :]
                low = master_out[layer, pl.ds(base + 8 * per_row + col, 8, stride=per_row), :]
                dst[layer, pl.ds(row, 16), col * LANES:(col + 1) * LANES] = jnp.concatenate([top, low], axis=0).astype(BF16)
            return 0

        lax.fori_loop(0, count // 16 // part[1], body, 0)

    for layer in range(layers):
        for which in range(4):
            load(which, layer).wait()
        for part in own_parts(layer):
            adam(layer, part)

            def send_own(kind):
                round_rows(kind, layer, part)
                if layer < layers - 1:
                    start(own_x(kind, layer, me, x_peer, (part,)))
                    start(own_y(kind, layer, me, y_peer, (part,)))
                start(pair(kind, layer, me, "pair_own", (part,)))

            by_kind(send_own)

    def pack(kind, device, packed_ref):
        spread_piece(dims, kind, device, (w_in, w_out), wide_ref)

        def squeeze(idx, _):
            at = pl.ds(pl.multiple_of(idx * 256, 256), 256)
            packed_ref[at, :] = wide_ref[at, :].astype(BF16)
            return 0

        lax.fori_loop(0, 4 * chunks // 256, squeeze, 0)

    def partner_of(device):
        return device + 1 - 2 * core

    def drain(kind):
        for layer in range(layers):
            left(own_x(kind, layer, me, x_peer))
            left(own_y(kind, layer, me, y_peer))
            left(pair(kind, layer, me, "pair_own", own_parts(layer)))
            left(pair(kind, layer, x_peer, "pair_x", own_parts(layer)))
            left(pair(1 - kind, layer, y_peer, "pair_y", own_parts(layer)))
            if layer < layers - 1:
                left(pair(1 - kind, layer, diag, "pair_far", far_parts(layer, 0) + far_parts(layer, 1)))
                left(far(kind, layer, 0, x_peer, y_peer))
                left(far(1 - kind, layer, 1, y_peer, x_peer))
        for step in range(1, GROUP):
            part_copy(step).wait_send()

    def drain_last(kind):
        layer = layers - 1
        left(far(kind, layer, 0, x_peer, y_peer))
        left(far(1 - kind, layer, 1, y_peer, x_peer))
        left(pair(1 - kind, layer, diag, "pair_far", far_parts(layer, 0) + far_parts(layer, 1)))

    def forward(kind, layer):
        x_order = own_parts(layer)
        y_order = x_order[::-1] if layer == layers - 1 else x_order
        for x_part, y_part in zip(x_order, y_order):
            arrive(own_x(kind, layer, x_peer, me, (x_part,)))
            if x_part in ((0, 2), (2, 6)):
                start(far(kind, layer, 0, x_peer, y_peer))
            start(pair(kind, layer, x_peer, "pair_x", (x_part,)))
            arrive(own_y(1 - kind, layer, y_peer, me, (y_part,)))
            if y_part == (1, 2):
                start(far(1 - kind, layer, 1, y_peer, x_peer))
            start(pair(1 - kind, layer, y_peer, "pair_y", (y_part,)))

    def far_arrive(kind, layer, only=None):
        for idx, parts in enumerate(zip(far_parts(layer, 0), far_parts(layer, 1))):
            if only is not None and idx != only:
                continue
            for half in range(2):
                arrive(far(1 - kind, layer, half, diag, me, (parts[half],)))
                start(pair(1 - kind, layer, diag, "pair_far", (parts[half],)))

    def far_partner(kind, layer):
        arrive(pair(1 - kind, layer, partner_of(diag), "pair_far", far_parts(layer, 0) + far_parts(layer, 1)))

    def near_partner(kind, layer):
        arrive(pair(kind, layer, partner_of(x_peer), "pair_x", own_parts(layer)))
        arrive(pair(1 - kind, layer, partner_of(y_peer), "pair_y", own_parts(layer)))

    def stage_own(kind):
        pack(kind, me, p0)
        forward(kind, 0)
        for layer in range(layers):
            arrive(pair(kind, layer, partner, "pair_own", own_parts(layer)))
        pack(kind, partner, p1)
        forward(kind, 1)
        start(own_x(kind, layers - 1, me, x_peer))
        start(own_y(kind, layers - 1, me, y_peer)[::-1])
        near_partner(kind, 0)
        far_arrive(kind, 0)
        near_partner(kind, 1)
        far_partner(kind, 0)

    def stage_one(kind):
        far_arrive(kind, 1)
        far_partner(kind, 1)

    def stage_two(kind):
        forward(kind, 2)
        pack(kind, x_peer, p2)
        pack(1 - kind, y_peer, p4)
        near_partner(kind, 2)
        far_arrive(kind, 2, 0)
        pack(kind, partner_of(x_peer), p3)
        far_arrive(kind, 2, 1)
        pack(1 - kind, partner_of(y_peer), p5)
        drain(kind)
        far_arrive(kind, 2, 2)
        far_partner(kind, 2)
        drain_last(kind)

    by_kind(stage_own)
    tok_load.wait()
    mlp_block(dims, 0, w_in, w_out, hidden_ref, normed_ref, active_ref)
    by_kind(stage_one)
    mlp_block(dims, 1, w_in, w_out, hidden_ref, normed_ref, active_ref)
    by_kind(stage_two)


def finish_kernel(dims, p0, p1, p2, p3, p4, p5, master_ref, one_ref, two_ref, w_in, w_out, last_ref, tgt_ref,
                  packed_hbm, master_hbm, one_hbm, two_hbm, loss_hbm,
                  loss_ref, far_ref, wide_ref, normed_ref, active_ref, hidden_ref, sem, far_sem):
    layers, model_dim, hidden_dim, rows, chunks = dims
    me, core, y_pos, x_peer, y_peer, diag = places()
    twin = 1 - 2 * core

    copies = []
    for which, (src, dst) in enumerate(((master_ref, master_hbm), (one_ref, one_hbm), (two_ref, two_hbm))):
        for layer in range(layers):
            copies.append(pltpu.make_async_copy(src.at[layer], dst.at[:, layer, :], sem.at[6 + which * layers + layer]))
    for idx, (ref, device) in enumerate(((p0, me), (p1, me + twin), (p2, x_peer), (p3, x_peer + twin), (p4, y_peer), (p5, y_peer + twin))):
        copies.append(pltpu.make_async_copy(ref, packed_hbm.at[pl.ds(device * chunks, chunks)], sem.at[idx]))
    for item in copies:
        item.start()

    far_copies = []
    for idx, device in enumerate((diag, diag + twin)):
        for y_value in range(2):
            @pl.when(y_pos == y_value)
            def _():
                spread_piece(dims, 1 - y_value, device, (w_in, w_out), wide_ref)

        def squeeze(at, _):
            block = wide_ref[pl.ds(pl.multiple_of(at * 128, 128), 128), :].astype(BF16).reshape(32, 4, LANES)
            far_ref[idx, pl.ds(at * 32, 32), :, :] = block[:, :layers, :]
            return 0

        lax.fori_loop(0, 4 * chunks // 128, squeeze, 0)
        far_copies.append(pltpu.make_async_copy(far_ref.at[idx], packed_hbm.at[pl.ds(device * chunks, chunks)], far_sem.at[idx]))
        far_copies[-1].start()

    hidden_ref[...] = last_ref[...]
    mlp_block(dims, layers - 1, w_in, w_out, hidden_ref, normed_ref, active_ref)

    for idx in range(rows // LANES):
        at = slice(idx * LANES, (idx + 1) * LANES)
        error = hidden_ref[at, :].astype(F32) - tgt_ref[at, :].astype(F32)
        error = error * error
        folded = error[:, 0:LANES]
        for col in range(LANES, model_dim, LANES):
            folded = folded + error[:, col:col + LANES]
        loss_ref[idx:idx + 1, :] = jnp.sum(folded.T, axis=0, keepdims=True) * (1.0 / model_dim)

    loss_copy = pltpu.make_async_copy(loss_ref, loss_hbm, far_sem.at[2])
    loss_copy.start()
    for item in copies + far_copies + [loss_copy]:
        item.wait()


def solution(mesh):
    group_size = mesh.shape["data"]
    state_spec = P(None, "data")
    row_spec = P("data", None)

    def local_step(grad_shard, master_shard, one_shard, two_shard, tok_rows, tgt_rows):
        rows, model_dim = tok_rows.shape
        layers, cols = master_shard.shape
        half_size = cols * group_size // 2
        hidden_dim = half_size // model_dim
        chunks = cols // LANES
        dims = (layers, model_dim, hidden_dim, rows, chunks)
        tiled = [a.reshape(layers, chunks, LANES).transpose(1, 0, 2) for a in (grad_shard, master_shard, one_shard, two_shard)]
        state_v = pltpu.VMEM((layers, chunks, LANES), F32)
        hbm = pl.BlockSpec(memory_space=pltpu.HBM)
        vmem = pl.BlockSpec(memory_space=pltpu.VMEM)
        state_out = state_v
        w_in_v = pltpu.VMEM((layers, model_dim, hidden_dim), BF16)
        w_out_v = pltpu.VMEM((layers, hidden_dim, model_dim), BF16)
        hidden_v = pltpu.VMEM((rows, model_dim), BF16)
        wide_v = pltpu.VMEM((4 * chunks, LANES), F32)
        normed_v = pltpu.VMEM((256, model_dim), BF16)
        active_v = pltpu.VMEM((256, hidden_dim), BF16)
        packed_v = pltpu.VMEM((4 * chunks, LANES), BF16)
        gathered = pl.pallas_call(
            functools.partial(gather_kernel, dims),
            name="gather_step",
            out_shape=(*(packed_v,) * 6, state_v, state_v, state_v, w_in_v, w_out_v, hidden_v),
            in_specs=[hbm] * 5,
            out_specs=(vmem,) * 12,
            scratch_shapes=[
                pltpu.VMEM((chunks, layers, LANES), F32),
                state_v, state_v, state_v, state_v,
                pltpu.VMEM((group_size, 1, LANES), F32),
                wide_v, normed_v, active_v,
                pltpu.SemaphoreType.DMA((5, layers)),
                pltpu.SemaphoreType.DMA((9,)),
                pltpu.SemaphoreType.DMA((group_size,)),
                pltpu.SemaphoreType.DMA((group_size,)),
                pltpu.SemaphoreType.DMA((96,)),
                pltpu.SemaphoreType.DMA((96,)),
            ],
            compiler_params=pltpu.CompilerParams(collective_id=0, has_side_effects=True, vmem_limit_bytes=23 << 20),
        )(*[pltpu.with_memory_space_constraint(a, pltpu.HBM) for a in (*tiled, tok_rows)])
        gathered = [a.reshape(chunks, 4, LANES)[:, :layers, :] for a in gathered[:6]] + list(gathered[6:])
        state_tile = jax.ShapeDtypeStruct((chunks, layers, LANES), F32)
        weights, new_master, new_one, new_two, row_loss = pl.pallas_call(
            functools.partial(finish_kernel, dims),
            name="finish",
            out_shape=(jax.ShapeDtypeStruct((chunks * group_size, layers, LANES), BF16), state_tile, state_tile, state_tile,
                       jax.ShapeDtypeStruct((rows // LANES, LANES), F32)),
            in_specs=[vmem] * 13,
            out_specs=(hbm,) * 5,
            scratch_shapes=[
                pltpu.VMEM((rows // LANES, LANES), F32),
                pltpu.VMEM((2, chunks, layers, LANES), BF16),
                wide_v, normed_v, active_v, hidden_v,
                pltpu.SemaphoreType.DMA((6 + 3 * layers,)),
                pltpu.SemaphoreType.DMA((3,)),
            ],
            compiler_params=pltpu.CompilerParams(vmem_limit_bytes=14 << 20),
        )(*gathered, tgt_rows)

        def flat(a):
            return a.transpose(1, 0, 2).reshape(layers, a.shape[0] * LANES)

        return row_loss.reshape(rows), flat(weights), flat(new_master), flat(new_one), flat(new_two)

    return jax.shard_map(local_step, mesh=mesh, in_specs=(state_spec, state_spec, state_spec, state_spec, row_spec, row_spec), out_specs=(P("data"), P(), state_spec, state_spec, state_spec), check_vma=False)
```

```python
import functools

import jax
import jax.numpy as jnp
from jax import lax
from jax.experimental import pallas as pl
from jax.experimental.pallas import tpu as pltpu
from jax.sharding import PartitionSpec as P

LEARN_RATE = 0.01
BETA_ONE = 0.9
BETA_TWO = 0.95
ADAM_EPS = 1e-8
WEIGHT_DECAY = 0.1
ADAM_STEP = 10
CLIP_NORM = 1.0
NORM_EPS = 1e-6

MESH = pl.DeviceIdType.MESH
LANES = 128
GROUP = 8
F32 = jnp.float32
BF16 = jnp.bfloat16


def spread_piece(dims, kind, device, weights, wide_ref):
    layers, model_dim, hidden_dim, rows, chunks = dims
    per_row = (hidden_dim if kind == 0 else model_dim) // LANES
    count = chunks // per_row
    src = weights[kind]
    slot = lax.rem(device, 4)

    def spread(idx, _):
        row = pl.multiple_of(slot * count + idx * 16, 16)
        for layer in range(layers):
            for col in range(per_row):
                tile = src[layer, pl.ds(row, 16), col * LANES:(col + 1) * LANES].astype(F32)
                base = layer + 4 * (idx * (16 * per_row) + col)
                wide_ref[pl.ds(base, 8, stride=4 * per_row), :] = tile[0:8]
                wide_ref[pl.ds(base + 32 * per_row, 8, stride=4 * per_row), :] = tile[8:16]
        return 0

    lax.fori_loop(0, count // 16, spread, 0)


def mlp_block(dims, layer, w_in, w_out, hidden_ref, normed_ref, active_ref):
    layers, model_dim, hidden_dim, rows, chunks = dims

    def block(idx, _):
        at = pl.ds(pl.multiple_of(idx * 256, 256), 256)
        hidden = hidden_ref[at, :].astype(F32)
        scale = lax.rsqrt(jnp.mean(hidden * hidden, axis=-1, keepdims=True) + NORM_EPS)
        normed_ref[...] = (hidden * scale).astype(BF16)
        for col in range(0, hidden_dim, 384):
            inner = jnp.dot(normed_ref[...], w_in[layer, :, col:col + 384], preferred_element_type=F32).astype(BF16)
            active_ref[:, col:col + 384] = jax.nn.gelu(inner.astype(F32), approximate=True).astype(BF16)
        for col in range(0, model_dim, 256):
            add = jnp.dot(active_ref[...], w_out[layer, :, col:col + 256], preferred_element_type=F32)
            hidden_ref[at, col:col + 256] = (hidden_ref[at, col:col + 256].astype(F32) + add).astype(BF16)
        return 0

    lax.fori_loop(0, rows // 256, block, 0)


def places():
    me = lax.axis_index("data")
    core = lax.rem(me, 2)
    x_pos = lax.rem(me // 2, 2)
    y_pos = me // 4
    x_peer = me + 2 - 4 * x_pos
    y_peer = me + 4 - 8 * y_pos
    return me, core, y_pos, x_peer, y_peer, x_peer + 4 - 8 * y_pos


def gather_kernel(dims, grad_hbm, master_hbm, one_hbm, two_hbm, tok_hbm,
                  p0, p1, p2, p3, p4, p5, master_out, one_out, two_out, w_in, w_out, hidden_ref,
                  grad_v, master_v, one_v, two_v,
                  part_ref, wide_ref, normed_ref, active_ref,
                  load_sem, grad_sem, part_send, part_recv, send_sem, recv_sem):
    layers, model_dim, hidden_dim, rows, chunks = dims
    in_rows = chunks * LANES // hidden_dim
    out_rows = chunks * LANES // model_dim

    me, core, y_pos, x_peer, y_peer, diag = places()
    partner = me + 1 - 2 * core

    state = ((grad_hbm, grad_v), (master_hbm, master_v), (one_hbm, one_v), (two_hbm, two_v))

    def load(which, layer):
        src, dst = state[which]
        return pltpu.make_async_copy(src.at[:, layer, :], dst.at[layer], load_sem.at[which, layer])

    span = chunks // 3

    def grad_load(layer, part):
        at = pl.ds(part * span, span)
        return pltpu.make_async_copy(grad_hbm.at[at, layer, :], grad_v.at[layer, at], grad_sem.at[layer, part])

    for layer in range(layers):
        for part in range(3):
            grad_load(layer, part).start()
    tok_load = pltpu.make_async_copy(tok_hbm, hidden_ref, load_sem.at[4, 0])

    barrier = pltpu.get_barrier_semaphore()
    for step in range(1, GROUP):
        pl.semaphore_signal(barrier, inc=1, device_id=(lax.rem(me + step, GROUP),), device_id_type=MESH)

    sums = tuple(jnp.zeros((8, LANES), F32) for _ in range(8))
    for layer in range(layers):
        for part in range(3):
            grad_load(layer, part).wait()
            if layer == layers - 1 and part == 2:
                for which in range(1, 4):
                    load(which, 0).start()

            def square(idx, carry):
                base = pl.multiple_of(part * span + idx * 64, 64)
                block = grad_v[layer, pl.ds(base, 64), :]
                return tuple(carry[k] + block[8 * k:8 * k + 8] * block[8 * k:8 * k + 8] for k in range(8))

            sums = lax.fori_loop(0, span // 64, square, sums)
    mine = ((sums[0] + sums[1]) + (sums[2] + sums[3])) + ((sums[4] + sums[5]) + (sums[6] + sums[7]))
    part_ref[me] = jnp.sum(mine, axis=0, keepdims=True)
    pl.semaphore_wait(barrier, GROUP - 1)

    def part_copy(step):
        return pltpu.make_async_remote_copy(
            src_ref=part_ref.at[me], dst_ref=part_ref.at[me],
            send_sem=part_send.at[step], recv_sem=part_recv.at[step],
            device_id=(lax.rem(me + step, GROUP),), device_id_type=MESH)

    def part_arrival(step):
        slot = lax.rem(me + GROUP - step, GROUP)
        return pltpu.make_async_remote_copy(
            src_ref=part_ref.at[slot], dst_ref=part_ref.at[slot],
            send_sem=part_send.at[step], recv_sem=part_recv.at[step],
            device_id=(me,), device_id_type=MESH)

    for step in range(1, GROUP):
        part_copy(step).start()
    for item in range(1, layers):
        for which in range(1, 4):
            load(which, item).start()
    tok_load.start()
    for step in range(1, GROUP):
        part_arrival(step).wait_recv()
    total = part_ref[0]
    for slot in range(1, GROUP):
        total = total + part_ref[slot]
    total = jnp.sum(total, axis=1, keepdims=True)
    clip = jnp.minimum(1.0, CLIP_NORM / jnp.sqrt(total))
    clip = jnp.broadcast_to(clip, (8, LANES))

    slots = {}

    def piece(kind, layer, device, part):
        ref, count = ((w_in, in_rows), (w_out, out_rows))[kind]
        span = count // part[1]
        at = lax.rem(device, 4) * count + part[0] * span
        return ref.at[layer, pl.ds(pl.multiple_of(at, 8), span), :]

    def copies(kind, layer, device, route, target, parts):
        out = []
        for part in parts:
            ref = piece(kind, layer, device, part)
            index = slots.setdefault((route, layer, part), len(slots))
            out.append(pltpu.make_async_remote_copy(
                src_ref=ref, dst_ref=ref, send_sem=send_sem.at[index],
                recv_sem=recv_sem.at[index], device_id=(target,), device_id_type=MESH))
        return out

    def start(items):
        for item in items:
            item.start()

    def arrive(items):
        for item in items:
            item.wait_recv()

    def left(items):
        for item in items:
            item.wait_send()

    def own_parts(layer):
        return ((0, 6), (1, 6), (2, 6), (1, 2)) if layer == 0 else ((0, 2), (1, 2))

    def far_parts(layer, half):
        return ((3 * half, 6), (3 * half + 1, 6), (6 * half + 4, 12), (6 * half + 5, 12)) if layer == layers - 1 else ((half, 2),)

    def own_x(kind, layer, device, target, parts=None):
        return copies(kind, layer, device, "own_x", target, parts or own_parts(layer))

    def own_y(kind, layer, device, target, parts=None):
        return copies(kind, layer, device, "own_y", target, parts or own_parts(layer))

    def far(kind, layer, half, device, target, parts=None):
        return copies(kind, layer, device, "far", target, parts or far_parts(layer, half))

    def pair(kind, layer, device, route, parts):
        return copies(kind, layer, device, route, partner, parts)

    def by_kind(function):
        for y_value in range(2):
            @pl.when(y_pos == y_value)
            def _():
                function(y_value)

    one_scale = 1.0 / (1.0 - BETA_ONE ** ADAM_STEP)
    two_scale = 1.0 / (1.0 - BETA_TWO ** ADAM_STEP)

    def adam(layer, part):
        first = part[0] * (chunks // part[1])

        def update(idx, _):
            base = pl.multiple_of(first + idx * 48, 8)
            for k in range(6):
                at = pl.ds(pl.multiple_of(base + 8 * k, 8), 8)
                clipped = grad_v[layer, at, :] * clip
                new_one = BETA_ONE * one_v[layer, at, :] + (1.0 - BETA_ONE) * clipped
                new_two = BETA_TWO * two_v[layer, at, :] + (1.0 - BETA_TWO) * clipped * clipped
                step_size = (new_one * one_scale) / (jnp.sqrt(new_two * two_scale) + ADAM_EPS)
                old = master_v[layer, at, :]
                master_out[layer, at, :] = old - LEARN_RATE * (step_size + WEIGHT_DECAY * old)
                one_out[layer, at, :] = new_one
                two_out[layer, at, :] = new_two
            return 0

        lax.fori_loop(0, chunks // part[1] // 48, update, 0)

    def round_rows(kind, layer, part):
        width = hidden_dim if kind == 0 else model_dim
        count = in_rows if kind == 0 else out_rows
        per_row = width // LANES
        dst = w_in if kind == 0 else w_out
        slot = lax.rem(me, 4)

        def body(idx, _):
            base = part[0] * (chunks // part[1]) + idx * (16 * per_row)
            row = pl.multiple_of(slot * count + part[0] * (count // part[1]) + idx * 16, 16)
            for col in range(per_row):
                top = master_out[layer, pl.ds(base + col, 8, stride=per_row), :]
                low = master_out[layer, pl.ds(base + 8 * per_row + col, 8, stride=per_row), :]
                dst[layer, pl.ds(row, 16), col * LANES:(col + 1) * LANES] = jnp.concatenate([top, low], axis=0).astype(BF16)
            return 0

        lax.fori_loop(0, count // 16 // part[1], body, 0)

    for layer in range(layers):
        for which in range(1, 4):
            load(which, layer).wait()
        for part in own_parts(layer):
            adam(layer, part)

            def send_own(kind):
                round_rows(kind, layer, part)
                if layer < layers - 1:
                    start(own_x(kind, layer, me, x_peer, (part,)))
                    start(own_y(kind, layer, me, y_peer, (part,)))
                start(pair(kind, layer, me, "pair_own", (part,)))

            by_kind(send_own)

    def pack(kind, device, packed_ref):
        spread_piece(dims, kind, device, (w_in, w_out), wide_ref)

        def squeeze(idx, _):
            at = pl.ds(pl.multiple_of(idx * 256, 256), 256)
            packed_ref[at, :] = wide_ref[at, :].astype(BF16)
            return 0

        lax.fori_loop(0, 4 * chunks // 256, squeeze, 0)

    def partner_of(device):
        return device + 1 - 2 * core

    def drain(kind):
        for layer in range(layers):
            left(own_x(kind, layer, me, x_peer))
            left(own_y(kind, layer, me, y_peer))
            left(pair(kind, layer, me, "pair_own", own_parts(layer)))
            left(pair(kind, layer, x_peer, "pair_x", own_parts(layer)))
            left(pair(1 - kind, layer, y_peer, "pair_y", own_parts(layer)))
            if layer < layers - 1:
                left(pair(1 - kind, layer, diag, "pair_far", far_parts(layer, 0) + far_parts(layer, 1)))
                left(far(kind, layer, 0, x_peer, y_peer))
                left(far(1 - kind, layer, 1, y_peer, x_peer))
        for step in range(1, GROUP):
            part_copy(step).wait_send()

    def drain_last(kind):
        layer = layers - 1
        left(far(kind, layer, 0, x_peer, y_peer))
        left(far(1 - kind, layer, 1, y_peer, x_peer))
        left(pair(1 - kind, layer, diag, "pair_far", far_parts(layer, 0) + far_parts(layer, 1)))

    def forward(kind, layer):
        x_order = own_parts(layer)
        y_order = x_order[::-1] if layer == layers - 1 else x_order
        for x_part, y_part in zip(x_order, y_order):
            arrive(own_x(kind, layer, x_peer, me, (x_part,)))
            if x_part in ((0, 2), (2, 6)):
                start(far(kind, layer, 0, x_peer, y_peer))
            start(pair(kind, layer, x_peer, "pair_x", (x_part,)))
            arrive(own_y(1 - kind, layer, y_peer, me, (y_part,)))
            if y_part == (1, 2):
                start(far(1 - kind, layer, 1, y_peer, x_peer))
            start(pair(1 - kind, layer, y_peer, "pair_y", (y_part,)))

    def far_arrive(kind, layer, only=None):
        for idx, parts in enumerate(zip(far_parts(layer, 0), far_parts(layer, 1))):
            if only is not None and idx != only:
                continue
            for half in range(2):
                arrive(far(1 - kind, layer, half, diag, me, (parts[half],)))
                start(pair(1 - kind, layer, diag, "pair_far", (parts[half],)))

    def far_partner(kind, layer):
        arrive(pair(1 - kind, layer, partner_of(diag), "pair_far", far_parts(layer, 0) + far_parts(layer, 1)))

    def near_partner(kind, layer):
        arrive(pair(kind, layer, partner_of(x_peer), "pair_x", own_parts(layer)))
        arrive(pair(1 - kind, layer, partner_of(y_peer), "pair_y", own_parts(layer)))

    def stage_own(kind):
        pack(kind, me, p0)
        forward(kind, 0)
        for layer in range(layers):
            arrive(pair(kind, layer, partner, "pair_own", own_parts(layer)))
        pack(kind, partner, p1)
        forward(kind, 1)
        start(own_x(kind, layers - 1, me, x_peer))
        start(own_y(kind, layers - 1, me, y_peer)[::-1])
        near_partner(kind, 0)
        far_arrive(kind, 0)
        near_partner(kind, 1)
        far_partner(kind, 0)

    def stage_one(kind):
        far_arrive(kind, 1)
        far_partner(kind, 1)

    def stage_two(kind):
        forward(kind, 2)
        pack(kind, x_peer, p2)
        pack(1 - kind, y_peer, p4)
        near_partner(kind, 2)
        far_arrive(kind, 2, 0)
        pack(kind, partner_of(x_peer), p3)
        far_arrive(kind, 2, 1)
        pack(1 - kind, partner_of(y_peer), p5)
        drain(kind)
        far_arrive(kind, 2, 2)
        far_arrive(kind, 2, 3)
        far_partner(kind, 2)
        drain_last(kind)

    by_kind(stage_own)
    tok_load.wait()
    mlp_block(dims, 0, w_in, w_out, hidden_ref, normed_ref, active_ref)
    by_kind(stage_one)
    mlp_block(dims, 1, w_in, w_out, hidden_ref, normed_ref, active_ref)
    by_kind(stage_two)


def finish_kernel(dims, p0, p1, p2, p3, p4, p5, master_ref, one_ref, two_ref, w_in, w_out, last_ref, tgt_ref,
                  packed_hbm, master_hbm, one_hbm, two_hbm, loss_hbm,
                  loss_ref, far_ref, wide_ref, normed_ref, active_ref, hidden_ref, sem, far_sem):
    layers, model_dim, hidden_dim, rows, chunks = dims
    me, core, y_pos, x_peer, y_peer, diag = places()
    twin = 1 - 2 * core

    copies = []
    for which, (src, dst) in enumerate(((master_ref, master_hbm), (one_ref, one_hbm), (two_ref, two_hbm))):
        for layer in range(layers):
            copies.append(pltpu.make_async_copy(src.at[layer], dst.at[:, layer, :], sem.at[6 + which * layers + layer]))
    for idx, (ref, device) in enumerate(((p0, me), (p1, me + twin), (p2, x_peer), (p3, x_peer + twin), (p4, y_peer), (p5, y_peer + twin))):
        copies.append(pltpu.make_async_copy(ref, packed_hbm.at[pl.ds(device * chunks, chunks)], sem.at[idx]))
    for item in copies:
        item.start()

    far_copies = []
    for idx, device in enumerate((diag, diag + twin)):
        for y_value in range(2):
            @pl.when(y_pos == y_value)
            def _():
                spread_piece(dims, 1 - y_value, device, (w_in, w_out), wide_ref)

        def squeeze(at, _):
            block = wide_ref[pl.ds(pl.multiple_of(at * 128, 128), 128), :].astype(BF16).reshape(32, 4, LANES)
            far_ref[idx, pl.ds(at * 32, 32), :, :] = block[:, :layers, :]
            return 0

        lax.fori_loop(0, 4 * chunks // 128, squeeze, 0)
        far_copies.append(pltpu.make_async_copy(far_ref.at[idx], packed_hbm.at[pl.ds(device * chunks, chunks)], far_sem.at[idx]))
        far_copies[-1].start()

    hidden_ref[...] = last_ref[...]
    mlp_block(dims, layers - 1, w_in, w_out, hidden_ref, normed_ref, active_ref)

    for idx in range(rows // LANES):
        at = slice(idx * LANES, (idx + 1) * LANES)
        error = hidden_ref[at, :].astype(F32) - tgt_ref[at, :].astype(F32)
        error = error * error
        folded = error[:, 0:LANES]
        for col in range(LANES, model_dim, LANES):
            folded = folded + error[:, col:col + LANES]
        loss_ref[idx:idx + 1, :] = jnp.sum(folded.T, axis=0, keepdims=True) * (1.0 / model_dim)

    loss_copy = pltpu.make_async_copy(loss_ref, loss_hbm, far_sem.at[2])
    loss_copy.start()
    for item in copies + far_copies + [loss_copy]:
        item.wait()


def solution(mesh):
    group_size = mesh.shape["data"]
    state_spec = P(None, "data")
    row_spec = P("data", None)

    def local_step(grad_shard, master_shard, one_shard, two_shard, tok_rows, tgt_rows):
        rows, model_dim = tok_rows.shape
        layers, cols = master_shard.shape
        half_size = cols * group_size // 2
        hidden_dim = half_size // model_dim
        chunks = cols // LANES
        dims = (layers, model_dim, hidden_dim, rows, chunks)
        tiled = [a.reshape(layers, chunks, LANES).transpose(1, 0, 2) for a in (grad_shard, master_shard, one_shard, two_shard)]
        state_v = pltpu.VMEM((layers, chunks, LANES), F32)
        hbm = pl.BlockSpec(memory_space=pltpu.HBM)
        vmem = pl.BlockSpec(memory_space=pltpu.VMEM)
        state_out = state_v
        w_in_v = pltpu.VMEM((layers, model_dim, hidden_dim), BF16)
        w_out_v = pltpu.VMEM((layers, hidden_dim, model_dim), BF16)
        hidden_v = pltpu.VMEM((rows, model_dim), BF16)
        wide_v = pltpu.VMEM((4 * chunks, LANES), F32)
        normed_v = pltpu.VMEM((256, model_dim), BF16)
        active_v = pltpu.VMEM((256, hidden_dim), BF16)
        packed_v = pltpu.VMEM((4 * chunks, LANES), BF16)
        gathered = pl.pallas_call(
            functools.partial(gather_kernel, dims),
            name="gather_step",
            out_shape=(*(packed_v,) * 6, state_v, state_v, state_v, w_in_v, w_out_v, hidden_v),
            in_specs=[hbm] * 5,
            out_specs=(vmem,) * 12,
            scratch_shapes=[
                state_v, state_v, state_v, state_v,
                pltpu.VMEM((group_size, 1, LANES), F32),
                wide_v, normed_v, active_v,
                pltpu.SemaphoreType.DMA((5, layers)),
                pltpu.SemaphoreType.DMA((layers, 3)),
                pltpu.SemaphoreType.DMA((group_size,)),
                pltpu.SemaphoreType.DMA((group_size,)),
                pltpu.SemaphoreType.DMA((96,)),
                pltpu.SemaphoreType.DMA((96,)),
            ],
            compiler_params=pltpu.CompilerParams(collective_id=0, has_side_effects=True, vmem_limit_bytes=19 << 20),
        )(*[pltpu.with_memory_space_constraint(a, pltpu.HBM) for a in (*tiled, tok_rows)])
        gathered = [a.reshape(chunks, 4, LANES)[:, :layers, :] for a in gathered[:6]] + list(gathered[6:])
        state_tile = jax.ShapeDtypeStruct((chunks, layers, LANES), F32)
        weights, new_master, new_one, new_two, row_loss = pl.pallas_call(
            functools.partial(finish_kernel, dims),
            name="finish",
            out_shape=(jax.ShapeDtypeStruct((chunks * group_size, layers, LANES), BF16), state_tile, state_tile, state_tile,
                       jax.ShapeDtypeStruct((rows // LANES, LANES), F32)),
            in_specs=[vmem] * 13,
            out_specs=(hbm,) * 5,
            scratch_shapes=[
                pltpu.VMEM((rows // LANES, LANES), F32),
                pltpu.VMEM((2, chunks, layers, LANES), BF16),
                wide_v, normed_v, active_v, hidden_v,
                pltpu.SemaphoreType.DMA((6 + 3 * layers,)),
                pltpu.SemaphoreType.DMA((3,)),
            ],
            compiler_params=pltpu.CompilerParams(vmem_limit_bytes=14 << 20),
        )(*gathered, tgt_rows)

        def flat(a):
            return a.transpose(1, 0, 2).reshape(layers, a.shape[0] * LANES)

        return row_loss.reshape(rows), flat(weights), flat(new_master), flat(new_one), flat(new_two)

    return jax.shard_map(local_step, mesh=mesh, in_specs=(state_spec, state_spec, state_spec, state_spec, row_spec, row_spec), out_specs=(P("data"), P(), state_spec, state_spec, state_spec), check_vma=False)
```

```python
import functools

import jax
import jax.numpy as jnp
from jax import lax
from jax.experimental import pallas as pl
from jax.experimental.pallas import tpu as pltpu
from jax.sharding import PartitionSpec as P

LEARN_RATE = 0.01
BETA_ONE = 0.9
BETA_TWO = 0.95
ADAM_EPS = 1e-8
WEIGHT_DECAY = 0.1
ADAM_STEP = 10
CLIP_NORM = 1.0
NORM_EPS = 1e-6

MESH = pl.DeviceIdType.MESH
LANES = 128
GROUP = 8
F32 = jnp.float32
BF16 = jnp.bfloat16


def spread_piece(dims, kind, device, weights, wide_ref):
    layers, model_dim, hidden_dim, rows, chunks = dims
    per_row = (hidden_dim if kind == 0 else model_dim) // LANES
    count = chunks // per_row
    src = weights[kind]
    slot = lax.rem(device, 4)

    def spread(idx, _):
        row = pl.multiple_of(slot * count + idx * 16, 16)
        for layer in range(layers):
            for col in range(per_row):
                tile = src[layer, pl.ds(row, 16), col * LANES:(col + 1) * LANES].astype(F32)
                base = layer + 4 * (idx * (16 * per_row) + col)
                wide_ref[pl.ds(base, 8, stride=4 * per_row), :] = tile[0:8]
                wide_ref[pl.ds(base + 32 * per_row, 8, stride=4 * per_row), :] = tile[8:16]
        return 0

    lax.fori_loop(0, count // 16, spread, 0)


def mlp_block(dims, layer, w_in, w_out, hidden_ref, normed_ref, active_ref):
    layers, model_dim, hidden_dim, rows, chunks = dims

    def block(idx, _):
        at = pl.ds(pl.multiple_of(idx * 256, 256), 256)
        hidden = hidden_ref[at, :].astype(F32)
        scale = lax.rsqrt(jnp.mean(hidden * hidden, axis=-1, keepdims=True) + NORM_EPS)
        normed_ref[...] = (hidden * scale).astype(BF16)
        for col in range(0, hidden_dim, 384):
            inner = jnp.dot(normed_ref[...], w_in[layer, :, col:col + 384], preferred_element_type=F32).astype(BF16)
            active_ref[:, col:col + 384] = jax.nn.gelu(inner.astype(F32), approximate=True).astype(BF16)
        for col in range(0, model_dim, 256):
            add = jnp.dot(active_ref[...], w_out[layer, :, col:col + 256], preferred_element_type=F32)
            hidden_ref[at, col:col + 256] = (hidden_ref[at, col:col + 256].astype(F32) + add).astype(BF16)
        return 0

    lax.fori_loop(0, rows // 256, block, 0)


def places():
    me = lax.axis_index("data")
    core = lax.rem(me, 2)
    x_pos = lax.rem(me // 2, 2)
    y_pos = me // 4
    x_peer = me + 2 - 4 * x_pos
    y_peer = me + 4 - 8 * y_pos
    return me, core, y_pos, x_peer, y_peer, x_peer + 4 - 8 * y_pos


def gather_kernel(dims, grad_hbm, master_hbm, one_hbm, two_hbm, tok_hbm,
                  p0, p1, p2, p3, p4, p5, master_out, one_out, two_out, w_in, w_out, hidden_ref,
                  grad_v, master_v, one_v, two_v,
                  part_ref, wide_ref, normed_ref, active_ref,
                  load_sem, grad_sem, part_send, part_recv, send_sem, recv_sem):
    layers, model_dim, hidden_dim, rows, chunks = dims
    in_rows = chunks * LANES // hidden_dim
    out_rows = chunks * LANES // model_dim

    me, core, y_pos, x_peer, y_peer, diag = places()
    partner = me + 1 - 2 * core

    state = ((grad_hbm, grad_v), (master_hbm, master_v), (one_hbm, one_v), (two_hbm, two_v))

    def load(which, layer):
        src, dst = state[which]
        return pltpu.make_async_copy(src.at[:, layer, :], dst.at[layer], load_sem.at[which, layer])

    span = chunks // 3

    def grad_load(layer, part):
        at = pl.ds(part * span, span)
        return pltpu.make_async_copy(grad_hbm.at[at, layer, :], grad_v.at[layer, at], grad_sem.at[layer, part])

    for layer in range(layers):
        for part in range(3):
            grad_load(layer, part).start()
    tok_load = pltpu.make_async_copy(tok_hbm, hidden_ref, load_sem.at[4, 0])

    barrier = pltpu.get_barrier_semaphore()
    for step in range(1, GROUP):
        pl.semaphore_signal(barrier, inc=1, device_id=(lax.rem(me + step, GROUP),), device_id_type=MESH)

    sums = tuple(jnp.zeros((8, LANES), F32) for _ in range(8))
    for layer in range(layers):
        for part in range(3):
            grad_load(layer, part).wait()
            if layer == layers - 1 and part == 2:
                for which in range(1, 4):
                    load(which, 0).start()

            def square(idx, carry):
                base = pl.multiple_of(part * span + idx * 64, 64)
                block = grad_v[layer, pl.ds(base, 64), :]
                return tuple(carry[k] + block[8 * k:8 * k + 8] * block[8 * k:8 * k + 8] for k in range(8))

            sums = lax.fori_loop(0, span // 64, square, sums)
    mine = ((sums[0] + sums[1]) + (sums[2] + sums[3])) + ((sums[4] + sums[5]) + (sums[6] + sums[7]))
    part_ref[me] = jnp.sum(mine, axis=0, keepdims=True)
    pl.semaphore_wait(barrier, GROUP - 1)

    def part_copy(step):
        return pltpu.make_async_remote_copy(
            src_ref=part_ref.at[me], dst_ref=part_ref.at[me],
            send_sem=part_send.at[step], recv_sem=part_recv.at[step],
            device_id=(lax.rem(me + step, GROUP),), device_id_type=MESH)

    def part_arrival(step):
        slot = lax.rem(me + GROUP - step, GROUP)
        return pltpu.make_async_remote_copy(
            src_ref=part_ref.at[slot], dst_ref=part_ref.at[slot],
            send_sem=part_send.at[step], recv_sem=part_recv.at[step],
            device_id=(me,), device_id_type=MESH)

    for step in range(1, GROUP):
        part_copy(step).start()
    for item in range(1, layers):
        for which in range(1, 4):
            load(which, item).start()
    tok_load.start()
    for step in range(1, GROUP):
        part_arrival(step).wait_recv()
    total = part_ref[0]
    for slot in range(1, GROUP):
        total = total + part_ref[slot]
    total = jnp.sum(total, axis=1, keepdims=True)
    clip = jnp.minimum(1.0, CLIP_NORM / jnp.sqrt(total))
    clip = jnp.broadcast_to(clip, (8, LANES))

    slots = {}

    def piece(kind, layer, device, part):
        ref, count = ((w_in, in_rows), (w_out, out_rows))[kind]
        span = count // part[1]
        at = lax.rem(device, 4) * count + part[0] * span
        return ref.at[layer, pl.ds(pl.multiple_of(at, 8), span), :]

    def copies(kind, layer, device, route, target, parts):
        out = []
        for part in parts:
            ref = piece(kind, layer, device, part)
            index = slots.setdefault((route, layer, part), len(slots))
            out.append(pltpu.make_async_remote_copy(
                src_ref=ref, dst_ref=ref, send_sem=send_sem.at[index],
                recv_sem=recv_sem.at[index], device_id=(target,), device_id_type=MESH))
        return out

    def start(items):
        for item in items:
            item.start()

    def arrive(items):
        for item in items:
            item.wait_recv()

    def left(items):
        for item in items:
            item.wait_send()

    def own_parts(layer):
        return ((0, 12), (1, 12), (1, 6), (2, 6), (1, 2)) if layer == 0 else ((0, 2), (1, 2))

    def far_parts(layer, half):
        return tuple((3 * half + at, 6) for at in range(3)) if layer == layers - 1 else ((half, 2),)

    def own_x(kind, layer, device, target, parts=None):
        return copies(kind, layer, device, "own_x", target, parts or own_parts(layer))

    def own_y(kind, layer, device, target, parts=None):
        return copies(kind, layer, device, "own_y", target, parts or own_parts(layer))

    def far(kind, layer, half, device, target, parts=None):
        return copies(kind, layer, device, "far", target, parts or far_parts(layer, half))

    def pair(kind, layer, device, route, parts):
        return copies(kind, layer, device, route, partner, parts)

    def by_kind(function):
        for y_value in range(2):
            @pl.when(y_pos == y_value)
            def _():
                function(y_value)

    one_scale = 1.0 / (1.0 - BETA_ONE ** ADAM_STEP)
    two_scale = 1.0 / (1.0 - BETA_TWO ** ADAM_STEP)

    def adam(layer, part):
        first = part[0] * (chunks // part[1])

        def update(idx, _):
            base = pl.multiple_of(first + idx * 48, 8)
            for k in range(6):
                at = pl.ds(pl.multiple_of(base + 8 * k, 8), 8)
                clipped = grad_v[layer, at, :] * clip
                new_one = BETA_ONE * one_v[layer, at, :] + (1.0 - BETA_ONE) * clipped
                new_two = BETA_TWO * two_v[layer, at, :] + (1.0 - BETA_TWO) * clipped * clipped
                step_size = (new_one * one_scale) / (jnp.sqrt(new_two * two_scale) + ADAM_EPS)
                old = master_v[layer, at, :]
                master_out[layer, at, :] = old - LEARN_RATE * (step_size + WEIGHT_DECAY * old)
                one_out[layer, at, :] = new_one
                two_out[layer, at, :] = new_two
            return 0

        lax.fori_loop(0, chunks // part[1] // 48, update, 0)

    def round_rows(kind, layer, part):
        width = hidden_dim if kind == 0 else model_dim
        count = in_rows if kind == 0 else out_rows
        per_row = width // LANES
        dst = w_in if kind == 0 else w_out
        slot = lax.rem(me, 4)

        step = 16 if count // part[1] % 16 == 0 else 8

        def body(idx, _):
            base = part[0] * (chunks // part[1]) + idx * (step * per_row)
            row = pl.multiple_of(slot * count + part[0] * (count // part[1]) + idx * step, 8)
            for col in range(per_row):
                block = master_out[layer, pl.ds(base + col, 8, stride=per_row), :]
                if step == 16:
                    low = master_out[layer, pl.ds(base + 8 * per_row + col, 8, stride=per_row), :]
                    block = jnp.concatenate([block, low], axis=0)
                dst[layer, pl.ds(row, step), col * LANES:(col + 1) * LANES] = block.astype(BF16)
            return 0

        lax.fori_loop(0, count // step // part[1], body, 0)

    for layer in range(layers):
        for which in range(1, 4):
            load(which, layer).wait()
        for part in own_parts(layer):
            adam(layer, part)

            def send_own(kind):
                round_rows(kind, layer, part)
                if layer < layers - 1:
                    start(own_x(kind, layer, me, x_peer, (part,)))
                    start(own_y(kind, layer, me, y_peer, (part,)))
                start(pair(kind, layer, me, "pair_own", (part,)))

            by_kind(send_own)

    def pack(kind, device, packed_ref):
        spread_piece(dims, kind, device, (w_in, w_out), wide_ref)

        def squeeze(idx, _):
            at = pl.ds(pl.multiple_of(idx * 256, 256), 256)
            packed_ref[at, :] = wide_ref[at, :].astype(BF16)
            return 0

        lax.fori_loop(0, 4 * chunks // 256, squeeze, 0)

    def partner_of(device):
        return device + 1 - 2 * core

    def drain(kind):
        for layer in range(layers):
            left(own_x(kind, layer, me, x_peer))
            left(own_y(kind, layer, me, y_peer))
            left(pair(kind, layer, me, "pair_own", own_parts(layer)))
            left(pair(kind, layer, x_peer, "pair_x", own_parts(layer)))
            left(pair(1 - kind, layer, y_peer, "pair_y", own_parts(layer)))
            if layer < layers - 1:
                left(pair(1 - kind, layer, diag, "pair_far", far_parts(layer, 0) + far_parts(layer, 1)))
                left(far(kind, layer, 0, x_peer, y_peer))
                left(far(1 - kind, layer, 1, y_peer, x_peer))
        for step in range(1, GROUP):
            part_copy(step).wait_send()

    def last_parts(half):
        return far_parts(layers - 1, half)[-1:]

    def start_far(kind, layer, half, device, target):
        if layer < layers - 1:
            start(far(kind, layer, half, device, target))
            return
        start(far(kind, layer, half, device, target, far_parts(layer, half)[:-1]))

        @pl.when(core == 0)
        def _():
            start(far(kind, layer, half, device, target, last_parts(half)))

    def extra(kind, half, device, route, target):
        return copies(kind, layers - 1, device, route, target, last_parts(half))

    def forward(kind, layer):
        x_order = own_parts(layer)
        y_order = x_order[::-1] if layer == layers - 1 else x_order
        for x_part, y_part in zip(x_order, y_order):
            arrive(own_x(kind, layer, x_peer, me, (x_part,)))
            if x_part in ((0, 2), (2, 6)):
                start_far(kind, layer, 0, x_peer, y_peer)
            start(pair(kind, layer, x_peer, "pair_x", (x_part,)))
            arrive(own_y(1 - kind, layer, y_peer, me, (y_part,)))
            if y_part == (1, 2):
                start_far(1 - kind, layer, 1, y_peer, x_peer)
            start(pair(1 - kind, layer, y_peer, "pair_y", (y_part,)))

    def far_arrive(kind, layer, only=None):
        for idx, parts in enumerate(zip(far_parts(layer, 0), far_parts(layer, 1))):
            if only is not None and idx != only:
                continue
            for half in range(2):
                arrive(far(1 - kind, layer, half, diag, me, (parts[half],)))
                start(pair(1 - kind, layer, diag, "pair_far", (parts[half],)))

    def far_partner(kind, layer):
        arrive(pair(1 - kind, layer, partner_of(diag), "pair_far", far_parts(layer, 0) + far_parts(layer, 1)))

    def near_partner(kind, layer, x_parts=None, y_parts=None):
        arrive(pair(kind, layer, partner_of(x_peer), "pair_x", x_parts or own_parts(layer)))
        arrive(pair(1 - kind, layer, partner_of(y_peer), "pair_y", y_parts or own_parts(layer)))

    def stage_own(kind):
        pack(kind, me, p0)
        forward(kind, 0)
        for layer in range(layers):
            arrive(pair(kind, layer, partner, "pair_own", own_parts(layer)))
        pack(kind, partner, p1)
        forward(kind, 1)
        start(own_x(kind, layers - 1, me, x_peer))
        start(own_y(kind, layers - 1, me, y_peer)[::-1])
        near_partner(kind, 0)
        far_arrive(kind, 0)
        near_partner(kind, 1)
        far_partner(kind, 0)

    def stage_one(kind):
        far_arrive(kind, 1)
        far_partner(kind, 1)

    def stage_two(kind):
        last = layers - 1
        early = far_parts(last, 0)[:-1] + far_parts(last, 1)[:-1]
        late = last_parts(0) + last_parts(1)
        forward(kind, last)
        near_partner(kind, last, ((0, 2),), ((1, 2),))

        @pl.when(core == 0)
        def _():
            start(extra(kind, 0, partner_of(x_peer), "extra", y_peer))
            start(extra(1 - kind, 1, partner_of(y_peer), "extra", x_peer))

        pack(kind, x_peer, p2)
        pack(1 - kind, y_peer, p4)
        near_partner(kind, last, ((1, 2),), ((0, 2),))
        far_arrive(kind, last, 0)
        pack(kind, partner_of(x_peer), p3)
        far_arrive(kind, last, 1)
        pack(1 - kind, partner_of(y_peer), p5)
        drain(kind)
        arrive(pair(1 - kind, last, partner_of(diag), "pair_far", early))

        @pl.when(core == 0)
        def _():
            far_arrive(kind, last, 2)
            for half in range(2):
                arrive(extra(1 - kind, half, partner_of(diag), "extra", me))
                start(extra(1 - kind, half, partner_of(diag), "pair_extra", partner))
            left(pair(1 - kind, last, diag, "pair_far", late))
            left(far(kind, last, 0, x_peer, y_peer, last_parts(0)))
            left(far(1 - kind, last, 1, y_peer, x_peer, last_parts(1)))
            left(extra(kind, 0, partner_of(x_peer), "extra", y_peer))
            left(extra(1 - kind, 1, partner_of(y_peer), "extra", x_peer))
            for half in range(2):
                left(extra(1 - kind, half, partner_of(diag), "pair_extra", partner))

        @pl.when(core == 1)
        def _():
            arrive(pair(1 - kind, last, partner_of(diag), "pair_far", late))
            for half in range(2):
                arrive(extra(1 - kind, half, diag, "pair_extra", me))

        left(pair(1 - kind, last, diag, "pair_far", early))
        left(far(kind, last, 0, x_peer, y_peer, far_parts(last, 0)[:-1]))
        left(far(1 - kind, last, 1, y_peer, x_peer, far_parts(last, 1)[:-1]))

    by_kind(stage_own)
    tok_load.wait()
    mlp_block(dims, 0, w_in, w_out, hidden_ref, normed_ref, active_ref)
    by_kind(stage_one)
    mlp_block(dims, 1, w_in, w_out, hidden_ref, normed_ref, active_ref)
    by_kind(stage_two)


def finish_kernel(dims, p0, p1, p2, p3, p4, p5, master_ref, one_ref, two_ref, w_in, w_out, last_ref, tgt_ref,
                  packed_hbm, master_hbm, one_hbm, two_hbm, loss_hbm,
                  loss_ref, far_ref, wide_ref, normed_ref, active_ref, hidden_ref, sem, far_sem):
    layers, model_dim, hidden_dim, rows, chunks = dims
    me, core, y_pos, x_peer, y_peer, diag = places()
    twin = 1 - 2 * core

    copies = []
    for which, (src, dst) in enumerate(((master_ref, master_hbm), (one_ref, one_hbm), (two_ref, two_hbm))):
        for layer in range(layers):
            copies.append(pltpu.make_async_copy(src.at[layer], dst.at[:, layer, :], sem.at[6 + which * layers + layer]))
    for idx, (ref, device) in enumerate(((p0, me), (p1, me + twin), (p2, x_peer), (p3, x_peer + twin), (p4, y_peer), (p5, y_peer + twin))):
        copies.append(pltpu.make_async_copy(ref, packed_hbm.at[pl.ds(device * chunks, chunks)], sem.at[idx]))
    for item in copies:
        item.start()

    far_copies = []
    for idx, device in enumerate((diag, diag + twin)):
        for y_value in range(2):
            @pl.when(y_pos == y_value)
            def _():
                spread_piece(dims, 1 - y_value, device, (w_in, w_out), wide_ref)

        def squeeze(at, _):
            block = wide_ref[pl.ds(pl.multiple_of(at * 128, 128), 128), :].astype(BF16).reshape(32, 4, LANES)
            far_ref[idx, pl.ds(at * 32, 32), :, :] = block[:, :layers, :]
            return 0

        lax.fori_loop(0, 4 * chunks // 128, squeeze, 0)
        far_copies.append(pltpu.make_async_copy(far_ref.at[idx], packed_hbm.at[pl.ds(device * chunks, chunks)], far_sem.at[idx]))
        far_copies[-1].start()

    hidden_ref[...] = last_ref[...]
    mlp_block(dims, layers - 1, w_in, w_out, hidden_ref, normed_ref, active_ref)

    for idx in range(rows // LANES):
        at = slice(idx * LANES, (idx + 1) * LANES)
        error = hidden_ref[at, :].astype(F32) - tgt_ref[at, :].astype(F32)
        error = error * error
        folded = error[:, 0:LANES]
        for col in range(LANES, model_dim, LANES):
            folded = folded + error[:, col:col + LANES]
        loss_ref[idx:idx + 1, :] = jnp.sum(folded.T, axis=0, keepdims=True) * (1.0 / model_dim)

    loss_copy = pltpu.make_async_copy(loss_ref, loss_hbm, far_sem.at[2])
    loss_copy.start()
    for item in copies + far_copies + [loss_copy]:
        item.wait()


def solution(mesh):
    group_size = mesh.shape["data"]
    state_spec = P(None, "data")
    row_spec = P("data", None)

    def local_step(grad_shard, master_shard, one_shard, two_shard, tok_rows, tgt_rows):
        rows, model_dim = tok_rows.shape
        layers, cols = master_shard.shape
        half_size = cols * group_size // 2
        hidden_dim = half_size // model_dim
        chunks = cols // LANES
        dims = (layers, model_dim, hidden_dim, rows, chunks)
        tiled = [a.reshape(layers, chunks, LANES).transpose(1, 0, 2) for a in (grad_shard, master_shard, one_shard, two_shard)]
        state_v = pltpu.VMEM((layers, chunks, LANES), F32)
        hbm = pl.BlockSpec(memory_space=pltpu.HBM)
        vmem = pl.BlockSpec(memory_space=pltpu.VMEM)
        state_out = state_v
        w_in_v = pltpu.VMEM((layers, model_dim, hidden_dim), BF16)
        w_out_v = pltpu.VMEM((layers, hidden_dim, model_dim), BF16)
        hidden_v = pltpu.VMEM((rows, model_dim), BF16)
        wide_v = pltpu.VMEM((4 * chunks, LANES), F32)
        normed_v = pltpu.VMEM((256, model_dim), BF16)
        active_v = pltpu.VMEM((256, hidden_dim), BF16)
        packed_v = pltpu.VMEM((4 * chunks, LANES), BF16)
        gathered = pl.pallas_call(
            functools.partial(gather_kernel, dims),
            name="gather_step",
            out_shape=(*(packed_v,) * 6, state_v, state_v, state_v, w_in_v, w_out_v, hidden_v),
            in_specs=[hbm] * 5,
            out_specs=(vmem,) * 12,
            scratch_shapes=[
                state_v, state_v, state_v, state_v,
                pltpu.VMEM((group_size, 1, LANES), F32),
                wide_v, normed_v, active_v,
                pltpu.SemaphoreType.DMA((5, layers)),
                pltpu.SemaphoreType.DMA((layers, 3)),
                pltpu.SemaphoreType.DMA((group_size,)),
                pltpu.SemaphoreType.DMA((group_size,)),
                pltpu.SemaphoreType.DMA((96,)),
                pltpu.SemaphoreType.DMA((96,)),
            ],
            compiler_params=pltpu.CompilerParams(collective_id=0, has_side_effects=True, vmem_limit_bytes=19 << 20),
        )(*[pltpu.with_memory_space_constraint(a, pltpu.HBM) for a in (*tiled, tok_rows)])
        gathered = [a.reshape(chunks, 4, LANES)[:, :layers, :] for a in gathered[:6]] + list(gathered[6:])
        state_tile = jax.ShapeDtypeStruct((chunks, layers, LANES), F32)
        weights, new_master, new_one, new_two, row_loss = pl.pallas_call(
            functools.partial(finish_kernel, dims),
            name="finish",
            out_shape=(jax.ShapeDtypeStruct((chunks * group_size, layers, LANES), BF16), state_tile, state_tile, state_tile,
                       jax.ShapeDtypeStruct((rows // LANES, LANES), F32)),
            in_specs=[vmem] * 13,
            out_specs=(hbm,) * 5,
            scratch_shapes=[
                pltpu.VMEM((rows // LANES, LANES), F32),
                pltpu.VMEM((2, chunks, layers, LANES), BF16),
                wide_v, normed_v, active_v, hidden_v,
                pltpu.SemaphoreType.DMA((6 + 3 * layers,)),
                pltpu.SemaphoreType.DMA((3,)),
            ],
            compiler_params=pltpu.CompilerParams(vmem_limit_bytes=14 << 20),
        )(*gathered, tgt_rows)

        def flat(a):
            return a.transpose(1, 0, 2).reshape(layers, a.shape[0] * LANES)

        return row_loss.reshape(rows), flat(weights), flat(new_master), flat(new_one), flat(new_two)

    return jax.shard_map(local_step, mesh=mesh, in_specs=(state_spec, state_spec, state_spec, state_spec, row_spec, row_spec), out_specs=(P("data"), P(), state_spec, state_spec, state_spec), check_vma=False)
```

```python
import functools

import jax
import jax.numpy as jnp
from jax import lax
from jax.experimental import pallas as pl
from jax.experimental.pallas import tpu as pltpu
from jax.sharding import PartitionSpec as P

LEARN_RATE = 0.01
BETA_ONE = 0.9
BETA_TWO = 0.95
ADAM_EPS = 1e-8
WEIGHT_DECAY = 0.1
ADAM_STEP = 10
CLIP_NORM = 1.0
NORM_EPS = 1e-6

MESH = pl.DeviceIdType.MESH
LANES = 128
GROUP = 8
F32 = jnp.float32
BF16 = jnp.bfloat16


def spread_piece(dims, kind, device, weights, wide_ref):
    layers, model_dim, hidden_dim, rows, chunks = dims
    per_row = (hidden_dim if kind == 0 else model_dim) // LANES
    count = chunks // per_row
    src = weights[kind]
    slot = lax.rem(device, 4)

    def spread(idx, _):
        row = pl.multiple_of(slot * count + idx * 16, 16)
        for layer in range(layers):
            for col in range(per_row):
                tile = src[layer, pl.ds(row, 16), col * LANES:(col + 1) * LANES].astype(F32)
                base = layer + 4 * (idx * (16 * per_row) + col)
                wide_ref[pl.ds(base, 8, stride=4 * per_row), :] = tile[0:8]
                wide_ref[pl.ds(base + 32 * per_row, 8, stride=4 * per_row), :] = tile[8:16]
        return 0

    lax.fori_loop(0, count // 16, spread, 0)


def mlp_block(dims, layer, w_in, w_out, source_ref, hidden_ref, normed_ref, active_ref):
    layers, model_dim, hidden_dim, rows, chunks = dims

    def block(idx, _):
        at = pl.ds(pl.multiple_of(idx * 256, 256), 256)
        hidden = source_ref[at, :].astype(F32)
        scale = lax.rsqrt(jnp.mean(hidden * hidden, axis=-1, keepdims=True) + NORM_EPS)
        normed_ref[...] = (hidden * scale).astype(BF16)
        for col in range(0, hidden_dim, 384):
            inner = jnp.dot(normed_ref[...], w_in[layer, :, col:col + 384], preferred_element_type=F32).astype(BF16)
            active_ref[:, col:col + 384] = jax.nn.gelu(inner.astype(F32), approximate=True).astype(BF16)
        for col in range(0, model_dim, 256):
            add = jnp.dot(active_ref[...], w_out[layer, :, col:col + 256], preferred_element_type=F32)
            hidden_ref[at, col:col + 256] = (source_ref[at, col:col + 256].astype(F32) + add).astype(BF16)
        return 0

    lax.fori_loop(0, rows // 256, block, 0)


def places():
    me = lax.axis_index("data")
    core = lax.rem(me, 2)
    x_pos = lax.rem(me // 2, 2)
    y_pos = me // 4
    x_peer = me + 2 - 4 * x_pos
    y_peer = me + 4 - 8 * y_pos
    return me, core, y_pos, x_peer, y_peer, x_peer + 4 - 8 * y_pos


def gather_kernel(dims, grad_hbm, master_hbm, one_hbm, two_hbm, tok_hbm,
                  p0, p1, p2, p3, p4, p5, master_out, one_out, two_out, w_in, w_out, hidden_ref,
                  grad_v, master_v, one_v, two_v,
                  part_ref, wide_ref, normed_ref, active_ref,
                  load_sem, grad_sem, part_send, part_recv, send_sem, recv_sem):
    layers, model_dim, hidden_dim, rows, chunks = dims
    in_rows = chunks * LANES // hidden_dim
    out_rows = chunks * LANES // model_dim

    me, core, y_pos, x_peer, y_peer, diag = places()
    partner = me + 1 - 2 * core

    state = ((grad_hbm, grad_v), (master_hbm, master_v), (one_hbm, one_v), (two_hbm, two_v))

    def load(which, layer):
        src, dst = state[which]
        return pltpu.make_async_copy(src.at[:, layer, :], dst.at[layer], load_sem.at[which, layer])

    span = chunks // 3

    def grad_load(layer, part):
        at = pl.ds(part * span, span)
        return pltpu.make_async_copy(grad_hbm.at[at, layer, :], grad_v.at[layer, at], grad_sem.at[layer, part])

    for layer in range(layers):
        for part in range(3):
            grad_load(layer, part).start()
    tok_load = pltpu.make_async_copy(tok_hbm, hidden_ref, load_sem.at[4, 0])

    barrier = pltpu.get_barrier_semaphore()
    for step in range(1, GROUP):
        pl.semaphore_signal(barrier, inc=1, device_id=(lax.rem(me + step, GROUP),), device_id_type=MESH)

    sums = tuple(jnp.zeros((8, LANES), F32) for _ in range(8))
    for layer in range(layers):
        for part in range(3):
            grad_load(layer, part).wait()
            if layer == layers - 1 and part == 2:
                for which in range(1, 4):
                    load(which, 0).start()

            def square(idx, carry):
                base = pl.multiple_of(part * span + idx * 64, 64)
                block = grad_v[layer, pl.ds(base, 64), :]
                return tuple(carry[k] + block[8 * k:8 * k + 8] * block[8 * k:8 * k + 8] for k in range(8))

            sums = lax.fori_loop(0, span // 64, square, sums)
    mine = ((sums[0] + sums[1]) + (sums[2] + sums[3])) + ((sums[4] + sums[5]) + (sums[6] + sums[7]))
    part_ref[me] = jnp.sum(mine, axis=0, keepdims=True)
    pl.semaphore_wait(barrier, GROUP - 1)

    def part_copy(step):
        return pltpu.make_async_remote_copy(
            src_ref=part_ref.at[me], dst_ref=part_ref.at[me],
            send_sem=part_send.at[step], recv_sem=part_recv.at[step],
            device_id=(lax.rem(me + step, GROUP),), device_id_type=MESH)

    def part_arrival(step):
        slot = lax.rem(me + GROUP - step, GROUP)
        return pltpu.make_async_remote_copy(
            src_ref=part_ref.at[slot], dst_ref=part_ref.at[slot],
            send_sem=part_send.at[step], recv_sem=part_recv.at[step],
            device_id=(me,), device_id_type=MESH)

    for step in range(1, GROUP):
        part_copy(step).start()
    for item in range(1, layers):
        for which in range(1, 4):
            load(which, item).start()
    tok_load.start()
    for which in range(1, 4):
        load(which, 0).wait()
    for step in range(1, GROUP):
        part_arrival(step).wait_recv()
    total = part_ref[0]
    for slot in range(1, GROUP):
        total = total + part_ref[slot]
    total = jnp.sum(total, axis=1, keepdims=True)
    clip = jnp.minimum(1.0, CLIP_NORM * lax.rsqrt(total))
    clip = jnp.broadcast_to(clip, (8, LANES))

    slots = {}

    def piece(kind, layer, device, part):
        ref, count = ((w_in, in_rows), (w_out, out_rows))[kind]
        span = count // part[1]
        at = lax.rem(device, 4) * count + part[0] * span
        return ref.at[layer, pl.ds(pl.multiple_of(at, 8), span), :]

    def copies(kind, layer, device, route, target, parts):
        out = []
        for part in parts:
            ref = piece(kind, layer, device, part)
            index = slots.setdefault((route, layer, part), len(slots))
            out.append(pltpu.make_async_remote_copy(
                src_ref=ref, dst_ref=ref, send_sem=send_sem.at[index],
                recv_sem=recv_sem.at[index], device_id=(target,), device_id_type=MESH))
        return out

    def start(items):
        for item in items:
            item.start()

    def arrive(items):
        for item in items:
            item.wait_recv()

    def left(items):
        for item in items:
            item.wait_send()

    def own_parts(layer):
        return ((0, 12), (1, 12), (1, 6), (2, 6), (1, 2)) if layer == 0 else ((0, 2), (1, 2))

    def far_parts(layer, half):
        return tuple((3 * half + at, 6) for at in range(3)) if layer == layers - 1 else ((half, 2),)

    def own_x(kind, layer, device, target, parts=None):
        return copies(kind, layer, device, "own_x", target, parts or own_parts(layer))

    def own_y(kind, layer, device, target, parts=None):
        return copies(kind, layer, device, "own_y", target, parts or own_parts(layer))

    def far(kind, layer, half, device, target, parts=None):
        return copies(kind, layer, device, "far", target, parts or far_parts(layer, half))

    def pair(kind, layer, device, route, parts):
        return copies(kind, layer, device, route, partner, parts)

    def by_kind(function):
        for y_value in range(2):
            @pl.when(y_pos == y_value)
            def _():
                function(y_value)

    one_scale = 1.0 / (1.0 - BETA_ONE ** ADAM_STEP)
    two_scale = 1.0 / (1.0 - BETA_TWO ** ADAM_STEP)

    def adam(layer, part):
        first = part[0] * (chunks // part[1])

        def update(idx, _):
            base = pl.multiple_of(first + idx * 48, 8)
            for k in range(6):
                at = pl.ds(pl.multiple_of(base + 8 * k, 8), 8)
                clipped = grad_v[layer, at, :] * clip
                new_one = BETA_ONE * one_v[layer, at, :] + (1.0 - BETA_ONE) * clipped
                new_two = BETA_TWO * two_v[layer, at, :] + (1.0 - BETA_TWO) * clipped * clipped
                step_size = (new_one * one_scale) / (jnp.sqrt(new_two * two_scale) + ADAM_EPS)
                old = master_v[layer, at, :]
                master_out[layer, at, :] = old - LEARN_RATE * (step_size + WEIGHT_DECAY * old)
                one_out[layer, at, :] = new_one
                two_out[layer, at, :] = new_two
            return 0

        lax.fori_loop(0, chunks // part[1] // 48, update, 0)

    def round_rows(kind, layer, part):
        width = hidden_dim if kind == 0 else model_dim
        count = in_rows if kind == 0 else out_rows
        per_row = width // LANES
        dst = w_in if kind == 0 else w_out
        slot = lax.rem(me, 4)

        step = 16 if count // part[1] % 16 == 0 else 8

        def body(idx, _):
            base = part[0] * (chunks // part[1]) + idx * (step * per_row)
            row = pl.multiple_of(slot * count + part[0] * (count // part[1]) + idx * step, 8)
            for col in range(per_row):
                block = master_out[layer, pl.ds(base + col, 8, stride=per_row), :]
                if step == 16:
                    low = master_out[layer, pl.ds(base + 8 * per_row + col, 8, stride=per_row), :]
                    block = jnp.concatenate([block, low], axis=0)
                dst[layer, pl.ds(row, step), col * LANES:(col + 1) * LANES] = block.astype(BF16)
            return 0

        lax.fori_loop(0, count // step // part[1], body, 0)

    for layer in range(layers):
        for which in range(1, 4) if layer else ():
            load(which, layer).wait()
        for part in own_parts(layer):
            adam(layer, part)

            def send_own(kind):
                round_rows(kind, layer, part)
                if layer < layers - 1:
                    start(own_x(kind, layer, me, x_peer, (part,)))
                    start(own_y(kind, layer, me, y_peer, (part,)))
                start(pair(kind, layer, me, "pair_own", (part,)))

            by_kind(send_own)

    def pack(kind, device, packed_ref):
        spread_piece(dims, kind, device, (w_in, w_out), wide_ref)

        def squeeze(idx, _):
            at = pl.ds(pl.multiple_of(idx * 256, 256), 256)
            packed_ref[at, :] = wide_ref[at, :].astype(BF16)
            return 0

        lax.fori_loop(0, 4 * chunks // 256, squeeze, 0)

    def partner_of(device):
        return device + 1 - 2 * core

    def drain(kind):
        for layer in range(layers):
            left(own_x(kind, layer, me, x_peer))
            left(own_y(kind, layer, me, y_peer))
            left(pair(kind, layer, me, "pair_own", own_parts(layer)))
            left(pair(kind, layer, x_peer, "pair_x", own_parts(layer)))
            left(pair(1 - kind, layer, y_peer, "pair_y", own_parts(layer)))
            if layer < layers - 1:
                left(pair(1 - kind, layer, diag, "pair_far", far_parts(layer, 0) + far_parts(layer, 1)))
                left(far(kind, layer, 0, x_peer, y_peer))
                left(far(1 - kind, layer, 1, y_peer, x_peer))
        for step in range(1, GROUP):
            part_copy(step).wait_send()

    def last_parts(half):
        return far_parts(layers - 1, half)[-1:]

    def start_far(kind, layer, half, device, target):
        if layer < layers - 1:
            start(far(kind, layer, half, device, target))
            return
        start(far(kind, layer, half, device, target, far_parts(layer, half)[:-1]))

        @pl.when(core == 0)
        def _():
            start(far(kind, layer, half, device, target, last_parts(half)))

    def extra(kind, half, device, route, target):
        return copies(kind, layers - 1, device, route, target, last_parts(half))

    def forward(kind, layer):
        x_order = own_parts(layer)
        y_order = x_order[::-1] if layer == layers - 1 else x_order
        for x_part, y_part in zip(x_order, y_order):
            arrive(own_x(kind, layer, x_peer, me, (x_part,)))
            if x_part in ((0, 2), (2, 6)):
                start_far(kind, layer, 0, x_peer, y_peer)
            start(pair(kind, layer, x_peer, "pair_x", (x_part,)))
            arrive(own_y(1 - kind, layer, y_peer, me, (y_part,)))
            if y_part == (1, 2):
                start_far(1 - kind, layer, 1, y_peer, x_peer)
            start(pair(1 - kind, layer, y_peer, "pair_y", (y_part,)))

    def far_arrive(kind, layer, only=None):
        for idx, parts in enumerate(zip(far_parts(layer, 0), far_parts(layer, 1))):
            if only is not None and idx != only:
                continue
            for half in range(2):
                arrive(far(1 - kind, layer, half, diag, me, (parts[half],)))
                start(pair(1 - kind, layer, diag, "pair_far", (parts[half],)))

    def far_partner(kind, layer):
        arrive(pair(1 - kind, layer, partner_of(diag), "pair_far", far_parts(layer, 0) + far_parts(layer, 1)))

    def near_partner(kind, layer, x_parts=None, y_parts=None):
        arrive(pair(kind, layer, partner_of(x_peer), "pair_x", x_parts or own_parts(layer)))
        arrive(pair(1 - kind, layer, partner_of(y_peer), "pair_y", y_parts or own_parts(layer)))

    def stage_own(kind):
        pack(kind, me, p0)
        forward(kind, 0)
        for layer in range(layers):
            arrive(pair(kind, layer, partner, "pair_own", own_parts(layer)))
        pack(kind, partner, p1)
        forward(kind, 1)
        start(own_x(kind, layers - 1, me, x_peer))
        start(own_y(kind, layers - 1, me, y_peer)[::-1])
        near_partner(kind, 0)
        far_arrive(kind, 0)
        near_partner(kind, 1)
        far_partner(kind, 0)

    def stage_one(kind):
        far_arrive(kind, 1)
        far_partner(kind, 1)

    def stage_two(kind):
        last = layers - 1
        early = far_parts(last, 0)[:-1] + far_parts(last, 1)[:-1]
        late = last_parts(0) + last_parts(1)
        forward(kind, last)
        near_partner(kind, last, ((0, 2),), ((1, 2),))

        @pl.when(core == 0)
        def _():
            start(extra(kind, 0, partner_of(x_peer), "extra", y_peer))
            start(extra(1 - kind, 1, partner_of(y_peer), "extra", x_peer))

        pack(kind, x_peer, p2)
        pack(1 - kind, y_peer, p4)
        near_partner(kind, last, ((1, 2),), ((0, 2),))
        far_arrive(kind, last, 0)
        pack(kind, partner_of(x_peer), p3)
        far_arrive(kind, last, 1)
        pack(1 - kind, partner_of(y_peer), p5)
        drain(kind)
        arrive(pair(1 - kind, last, partner_of(diag), "pair_far", early))

        @pl.when(core == 0)
        def _():
            far_arrive(kind, last, 2)
            for half in range(2):
                arrive(extra(1 - kind, half, partner_of(diag), "extra", me))
                start(extra(1 - kind, half, partner_of(diag), "pair_extra", partner))
            left(pair(1 - kind, last, diag, "pair_far", late))
            left(far(kind, last, 0, x_peer, y_peer, last_parts(0)))
            left(far(1 - kind, last, 1, y_peer, x_peer, last_parts(1)))
            left(extra(kind, 0, partner_of(x_peer), "extra", y_peer))
            left(extra(1 - kind, 1, partner_of(y_peer), "extra", x_peer))
            for half in range(2):
                left(extra(1 - kind, half, partner_of(diag), "pair_extra", partner))

        @pl.when(core == 1)
        def _():
            arrive(pair(1 - kind, last, partner_of(diag), "pair_far", late))
            for half in range(2):
                arrive(extra(1 - kind, half, diag, "pair_extra", me))

        left(pair(1 - kind, last, diag, "pair_far", early))
        left(far(kind, last, 0, x_peer, y_peer, far_parts(last, 0)[:-1]))
        left(far(1 - kind, last, 1, y_peer, x_peer, far_parts(last, 1)[:-1]))

    by_kind(stage_own)
    tok_load.wait()
    mlp_block(dims, 0, w_in, w_out, hidden_ref, hidden_ref, normed_ref, active_ref)
    by_kind(stage_one)
    mlp_block(dims, 1, w_in, w_out, hidden_ref, hidden_ref, normed_ref, active_ref)
    by_kind(stage_two)


def finish_kernel(dims, p0, p1, p2, p3, p4, p5, master_ref, one_ref, two_ref, w_in, w_out, last_ref, tgt_ref,
                  packed_hbm, master_hbm, one_hbm, two_hbm, loss_hbm,
                  loss_ref, far_ref, wide_ref, normed_ref, active_ref, hidden_ref, sem, far_sem):
    layers, model_dim, hidden_dim, rows, chunks = dims
    me, core, y_pos, x_peer, y_peer, diag = places()
    twin = 1 - 2 * core

    copies = []
    for which, (src, dst) in enumerate(((master_ref, master_hbm), (one_ref, one_hbm), (two_ref, two_hbm))):
        for layer in range(layers):
            copies.append(pltpu.make_async_copy(src.at[layer], dst.at[:, layer, :], sem.at[6 + which * layers + layer]))
    for idx, (ref, device) in enumerate(((p0, me), (p1, me + twin), (p2, x_peer), (p3, x_peer + twin), (p4, y_peer), (p5, y_peer + twin))):
        copies.append(pltpu.make_async_copy(ref, packed_hbm.at[pl.ds(device * chunks, chunks)], sem.at[idx]))
    for item in copies:
        item.start()

    far_copies = []
    for idx, device in enumerate((diag, diag + twin)):
        for y_value in range(2):
            @pl.when(y_pos == y_value)
            def _():
                spread_piece(dims, 1 - y_value, device, (w_in, w_out), wide_ref)

        def squeeze(at, _):
            block = wide_ref[pl.ds(pl.multiple_of(at * 128, 128), 128), :].astype(BF16).reshape(32, 4, LANES)
            far_ref[idx, pl.ds(at * 32, 32), :, :] = block[:, :layers, :]
            return 0

        lax.fori_loop(0, 4 * chunks // 128, squeeze, 0)
        far_copies.append(pltpu.make_async_copy(far_ref.at[idx], packed_hbm.at[pl.ds(device * chunks, chunks)], far_sem.at[idx]))
        far_copies[-1].start()

    mlp_block(dims, layers - 1, w_in, w_out, last_ref, hidden_ref, normed_ref, active_ref)

    for idx in range(rows // LANES):
        at = slice(idx * LANES, (idx + 1) * LANES)
        error = hidden_ref[at, :].astype(F32) - tgt_ref[at, :].astype(F32)
        error = error * error
        folded = error[:, 0:LANES]
        for col in range(LANES, model_dim, LANES):
            folded = folded + error[:, col:col + LANES]
        loss_ref[idx:idx + 1, :] = jnp.sum(folded.T, axis=0, keepdims=True) * (1.0 / model_dim)

    loss_copy = pltpu.make_async_copy(loss_ref, loss_hbm, far_sem.at[2])
    loss_copy.start()
    for item in copies + far_copies + [loss_copy]:
        item.wait()


def solution(mesh):
    group_size = mesh.shape["data"]
    state_spec = P(None, "data")
    row_spec = P("data", None)

    def local_step(grad_shard, master_shard, one_shard, two_shard, tok_rows, tgt_rows):
        rows, model_dim = tok_rows.shape
        layers, cols = master_shard.shape
        half_size = cols * group_size // 2
        hidden_dim = half_size // model_dim
        chunks = cols // LANES
        dims = (layers, model_dim, hidden_dim, rows, chunks)
        tiled = [a.reshape(layers, chunks, LANES).transpose(1, 0, 2) for a in (grad_shard, master_shard, one_shard, two_shard)]
        state_v = pltpu.VMEM((layers, chunks, LANES), F32)
        hbm = pl.BlockSpec(memory_space=pltpu.HBM)
        vmem = pl.BlockSpec(memory_space=pltpu.VMEM)
        state_out = state_v
        w_in_v = pltpu.VMEM((layers, model_dim, hidden_dim), BF16)
        w_out_v = pltpu.VMEM((layers, hidden_dim, model_dim), BF16)
        hidden_v = pltpu.VMEM((rows, model_dim), BF16)
        wide_v = pltpu.VMEM((4 * chunks, LANES), F32)
        normed_v = pltpu.VMEM((256, model_dim), BF16)
        active_v = pltpu.VMEM((256, hidden_dim), BF16)
        packed_v = pltpu.VMEM((4 * chunks, LANES), BF16)
        gathered = pl.pallas_call(
            functools.partial(gather_kernel, dims),
            name="gather_step",
            out_shape=(*(packed_v,) * 6, state_v, state_v, state_v, w_in_v, w_out_v, hidden_v),
            in_specs=[hbm] * 5,
            out_specs=(vmem,) * 12,
            scratch_shapes=[
                state_v, state_v, state_v, state_v,
                pltpu.VMEM((group_size, 1, LANES), F32),
                wide_v, normed_v, active_v,
                pltpu.SemaphoreType.DMA((5, layers)),
                pltpu.SemaphoreType.DMA((layers, 3)),
                pltpu.SemaphoreType.DMA((group_size,)),
                pltpu.SemaphoreType.DMA((group_size,)),
                pltpu.SemaphoreType.DMA((96,)),
                pltpu.SemaphoreType.DMA((96,)),
            ],
            compiler_params=pltpu.CompilerParams(collective_id=0, has_side_effects=True, vmem_limit_bytes=19 << 20),
        )(*[pltpu.with_memory_space_constraint(a, pltpu.HBM) for a in (*tiled, tok_rows)])
        gathered = [a.reshape(chunks, 4, LANES)[:, :layers, :] for a in gathered[:6]] + list(gathered[6:])
        state_tile = jax.ShapeDtypeStruct((chunks, layers, LANES), F32)
        weights, new_master, new_one, new_two, row_loss = pl.pallas_call(
            functools.partial(finish_kernel, dims),
            name="finish",
            out_shape=(jax.ShapeDtypeStruct((chunks * group_size, layers, LANES), BF16), state_tile, state_tile, state_tile,
                       jax.ShapeDtypeStruct((rows // LANES, LANES), F32)),
            in_specs=[vmem] * 13,
            out_specs=(hbm,) * 5,
            scratch_shapes=[
                pltpu.VMEM((rows // LANES, LANES), F32),
                pltpu.VMEM((2, chunks, layers, LANES), BF16),
                wide_v, normed_v, active_v, hidden_v,
                pltpu.SemaphoreType.DMA((6 + 3 * layers,)),
                pltpu.SemaphoreType.DMA((3,)),
            ],
            compiler_params=pltpu.CompilerParams(vmem_limit_bytes=14 << 20),
        )(*gathered, tgt_rows)

        def flat(a):
            return a.transpose(1, 0, 2).reshape(layers, a.shape[0] * LANES)

        return row_loss.reshape(rows), flat(weights), flat(new_master), flat(new_one), flat(new_two)

    return jax.shard_map(local_step, mesh=mesh, in_specs=(state_spec, state_spec, state_spec, state_spec, row_spec, row_spec), out_specs=(P("data"), P(), state_spec, state_spec, state_spec), check_vma=False)
```

```python
import functools

import jax
import jax.numpy as jnp
from jax import lax
from jax.experimental import pallas as pl
from jax.experimental.pallas import tpu as pltpu
from jax.sharding import PartitionSpec as P

LEARN_RATE = 0.01
BETA_ONE = 0.9
BETA_TWO = 0.95
ADAM_EPS = 1e-8
WEIGHT_DECAY = 0.1
ADAM_STEP = 10
CLIP_NORM = 1.0
NORM_EPS = 1e-6

MESH = pl.DeviceIdType.MESH
LANES = 128
GROUP = 8
F32 = jnp.float32
BF16 = jnp.bfloat16


def spread_piece(dims, kind, device, weights, wide_ref):
    layers, model_dim, hidden_dim, rows, chunks = dims
    per_row = (hidden_dim if kind == 0 else model_dim) // LANES
    count = chunks // per_row
    src = weights[kind]
    slot = lax.rem(device, 4)

    def spread(idx, _):
        row = pl.multiple_of(slot * count + idx * 16, 16)
        for layer in range(layers):
            for col in range(per_row):
                tile = src[layer, pl.ds(row, 16), col * LANES:(col + 1) * LANES].astype(F32)
                base = layer + 4 * (idx * (16 * per_row) + col)
                wide_ref[pl.ds(base, 8, stride=4 * per_row), :] = tile[0:8]
                wide_ref[pl.ds(base + 32 * per_row, 8, stride=4 * per_row), :] = tile[8:16]
        return 0

    lax.fori_loop(0, count // 16, spread, 0)


def mlp_block(dims, layer, w_in, w_out, source_ref, hidden_ref, normed_ref, active_ref):
    layers, model_dim, hidden_dim, rows, chunks = dims

    def block(idx, _):
        at = pl.ds(pl.multiple_of(idx * 256, 256), 256)
        hidden = source_ref[at, :].astype(F32)
        scale = lax.rsqrt(jnp.mean(hidden * hidden, axis=-1, keepdims=True) + NORM_EPS)
        normed_ref[...] = (hidden * scale).astype(BF16)
        for col in range(0, hidden_dim, 384):
            inner = jnp.dot(normed_ref[...], w_in[layer, :, col:col + 384], preferred_element_type=F32).astype(BF16)
            active_ref[:, col:col + 384] = jax.nn.gelu(inner.astype(F32), approximate=True).astype(BF16)
        for col in range(0, model_dim, 256):
            add = jnp.dot(active_ref[...], w_out[layer, :, col:col + 256], preferred_element_type=F32)
            hidden_ref[at, col:col + 256] = (source_ref[at, col:col + 256].astype(F32) + add).astype(BF16)
        return 0

    lax.fori_loop(0, rows // 256, block, 0)


def places():
    me = lax.axis_index("data")
    core = lax.rem(me, 2)
    x_pos = lax.rem(me // 2, 2)
    y_pos = me // 4
    x_peer = me + 2 - 4 * x_pos
    y_peer = me + 4 - 8 * y_pos
    return me, core, y_pos, x_peer, y_peer, x_peer + 4 - 8 * y_pos


def gather_kernel(dims, grad_hbm, master_hbm, one_hbm, two_hbm, tok_hbm,
                  p0, p1, p2, p3, p4, p5, master_out, one_out, two_out, w_in, w_out, hidden_ref,
                  grad_v, master_v, one_v, two_v,
                  part_ref, wide_ref, normed_ref, active_ref,
                  load_sem, grad_sem, part_send, part_recv, send_sem, recv_sem):
    layers, model_dim, hidden_dim, rows, chunks = dims
    in_rows = chunks * LANES // hidden_dim
    out_rows = chunks * LANES // model_dim

    me, core, y_pos, x_peer, y_peer, diag = places()
    partner = me + 1 - 2 * core

    state = ((grad_hbm, grad_v), (master_hbm, master_v), (one_hbm, one_v), (two_hbm, two_v))

    def load(which, layer):
        src, dst = state[which]
        return pltpu.make_async_copy(src.at[:, layer, :], dst.at[layer], load_sem.at[which, layer])

    loads = 1
    span = chunks // loads

    def grad_load(layer, part):
        at = pl.ds(part * span, span)
        return pltpu.make_async_copy(grad_hbm.at[at, layer, :], grad_v.at[layer, at], grad_sem.at[layer, part])

    for layer in range(layers):
        for part in range(loads):
            grad_load(layer, part).start()
    tok_load = pltpu.make_async_copy(tok_hbm, hidden_ref, load_sem.at[4, 0])

    barrier = pltpu.get_barrier_semaphore()
    for step in range(1, GROUP):
        pl.semaphore_signal(barrier, inc=1, device_id=(lax.rem(me + step, GROUP),), device_id_type=MESH)

    sums = tuple(jnp.zeros((8, LANES), F32) for _ in range(8))
    for layer in range(layers):
        for part in range(loads):
            grad_load(layer, part).wait()
            if layer == layers - 1 and part == loads - 1:
                for which in range(1, 4):
                    load(which, 0).start()

            def square(idx, carry):
                base = pl.multiple_of(part * span + idx * 64, 64)
                block = grad_v[layer, pl.ds(base, 64), :]
                return tuple(carry[k] + block[8 * k:8 * k + 8] * block[8 * k:8 * k + 8] for k in range(8))

            sums = lax.fori_loop(0, span // 64, square, sums)
    mine = ((sums[0] + sums[1]) + (sums[2] + sums[3])) + ((sums[4] + sums[5]) + (sums[6] + sums[7]))
    part_ref[me] = jnp.sum(mine, axis=0, keepdims=True)
    pl.semaphore_wait(barrier, GROUP - 1)

    def part_copy(step):
        return pltpu.make_async_remote_copy(
            src_ref=part_ref.at[me], dst_ref=part_ref.at[me],
            send_sem=part_send.at[step], recv_sem=part_recv.at[step],
            device_id=(lax.rem(me + step, GROUP),), device_id_type=MESH)

    def part_arrival(step):
        slot = lax.rem(me + GROUP - step, GROUP)
        return pltpu.make_async_remote_copy(
            src_ref=part_ref.at[slot], dst_ref=part_ref.at[slot],
            send_sem=part_send.at[step], recv_sem=part_recv.at[step],
            device_id=(me,), device_id_type=MESH)

    for step in range(1, GROUP):
        part_copy(step).start()
    for item in range(1, layers):
        for which in range(1, 4):
            load(which, item).start()
    tok_load.start()
    for which in range(1, 4):
        load(which, 0).wait()
    for step in range(1, GROUP):
        part_arrival(step).wait_recv()
    total = part_ref[0]
    for slot in range(1, GROUP):
        total = total + part_ref[slot]
    total = jnp.sum(total, axis=1, keepdims=True)
    clip = jnp.minimum(1.0, CLIP_NORM / jnp.sqrt(total))
    clip = jnp.broadcast_to(clip, (8, LANES))

    slots = {}

    def piece(kind, layer, device, part):
        ref, count = ((w_in, in_rows), (w_out, out_rows))[kind]
        span = count // part[1]
        at = lax.rem(device, 4) * count + part[0] * span
        return ref.at[layer, pl.ds(pl.multiple_of(at, 8), span), :]

    def copies(kind, layer, device, route, target, parts):
        out = []
        for part in parts:
            ref = piece(kind, layer, device, part)
            index = slots.setdefault((route, layer, part), len(slots))
            out.append(pltpu.make_async_remote_copy(
                src_ref=ref, dst_ref=ref, send_sem=send_sem.at[index],
                recv_sem=recv_sem.at[index], device_id=(target,), device_id_type=MESH))
        return out

    def start(items):
        for item in items:
            item.start()

    def arrive(items):
        for item in items:
            item.wait_recv()

    def left(items):
        for item in items:
            item.wait_send()

    def own_parts(layer):
        return ((0, 12), (1, 12), (1, 6), (2, 6), (1, 2)) if layer == 0 else ((0, 2), (1, 2))

    def far_parts(layer, half):
        return tuple((3 * half + at, 6) for at in range(3)) if layer == layers - 1 else ((half, 2),)

    def own_x(kind, layer, device, target, parts=None):
        return copies(kind, layer, device, "own_x", target, parts or own_parts(layer))

    def own_y(kind, layer, device, target, parts=None):
        return copies(kind, layer, device, "own_y", target, parts or own_parts(layer))

    def far(kind, layer, half, device, target, parts=None):
        return copies(kind, layer, device, "far", target, parts or far_parts(layer, half))

    def pair(kind, layer, device, route, parts):
        return copies(kind, layer, device, route, partner, parts)

    def by_kind(function):
        for y_value in range(2):
            @pl.when(y_pos == y_value)
            def _():
                function(y_value)

    one_scale = 1.0 / (1.0 - BETA_ONE ** ADAM_STEP)
    two_scale = 1.0 / (1.0 - BETA_TWO ** ADAM_STEP)

    def adam(layer, part):
        first = part[0] * (chunks // part[1])

        def update(idx, _):
            base = pl.multiple_of(first + idx * 48, 8)
            for k in range(6):
                at = pl.ds(pl.multiple_of(base + 8 * k, 8), 8)
                clipped = grad_v[layer, at, :] * clip
                new_one = BETA_ONE * one_v[layer, at, :] + (1.0 - BETA_ONE) * clipped
                new_two = BETA_TWO * two_v[layer, at, :] + (1.0 - BETA_TWO) * clipped * clipped
                step_size = (new_one * one_scale) / (jnp.sqrt(new_two * two_scale) + ADAM_EPS)
                old = master_v[layer, at, :]
                master_out[layer, at, :] = old - LEARN_RATE * (step_size + WEIGHT_DECAY * old)
                one_out[layer, at, :] = new_one
                two_out[layer, at, :] = new_two
            return 0

        lax.fori_loop(0, chunks // part[1] // 48, update, 0)

    def round_rows(kind, layer, part):
        width = hidden_dim if kind == 0 else model_dim
        count = in_rows if kind == 0 else out_rows
        per_row = width // LANES
        dst = w_in if kind == 0 else w_out
        slot = lax.rem(me, 4)

        step = 16 if count // part[1] % 16 == 0 else 8

        def body(idx, _):
            base = part[0] * (chunks // part[1]) + idx * (step * per_row)
            row = pl.multiple_of(slot * count + part[0] * (count // part[1]) + idx * step, 8)
            for col in range(per_row):
                block = master_out[layer, pl.ds(base + col, 8, stride=per_row), :]
                if step == 16:
                    low = master_out[layer, pl.ds(base + 8 * per_row + col, 8, stride=per_row), :]
                    block = jnp.concatenate([block, low], axis=0)
                dst[layer, pl.ds(row, step), col * LANES:(col + 1) * LANES] = block.astype(BF16)
            return 0

        lax.fori_loop(0, count // step // part[1], body, 0)

    for layer in range(layers):
        for which in range(1, 4) if layer else ():
            load(which, layer).wait()
        for part in own_parts(layer):
            adam(layer, part)

            def send_own(kind):
                round_rows(kind, layer, part)
                if layer < layers - 1:
                    start(own_x(kind, layer, me, x_peer, (part,)))
                    start(own_y(kind, layer, me, y_peer, (part,)))
                start(pair(kind, layer, me, "pair_own", (part,)))

            by_kind(send_own)

    def pack(kind, device, packed_ref):
        spread_piece(dims, kind, device, (w_in, w_out), wide_ref)

        def squeeze(idx, _):
            at = pl.ds(pl.multiple_of(idx * 256, 256), 256)
            packed_ref[at, :] = wide_ref[at, :].astype(BF16)
            return 0

        lax.fori_loop(0, 4 * chunks // 256, squeeze, 0)

    def partner_of(device):
        return device + 1 - 2 * core

    def drain(kind):
        for layer in range(layers):
            left(own_x(kind, layer, me, x_peer))
            left(own_y(kind, layer, me, y_peer))
            left(pair(kind, layer, me, "pair_own", own_parts(layer)))
            left(pair(kind, layer, x_peer, "pair_x", own_parts(layer)))
            left(pair(1 - kind, layer, y_peer, "pair_y", own_parts(layer)))
            if layer < layers - 1:
                left(pair(1 - kind, layer, diag, "pair_far", far_parts(layer, 0) + far_parts(layer, 1)))
                left(far(kind, layer, 0, x_peer, y_peer))
                left(far(1 - kind, layer, 1, y_peer, x_peer))
        for step in range(1, GROUP):
            part_copy(step).wait_send()

    def last_parts(half):
        return far_parts(layers - 1, half)[-1:]

    def start_far(kind, layer, half, device, target):
        if layer < layers - 1:
            start(far(kind, layer, half, device, target))
            return
        start(far(kind, layer, half, device, target, far_parts(layer, half)[:-1]))

        @pl.when(core == 0)
        def _():
            start(far(kind, layer, half, device, target, last_parts(half)))

    def extra(kind, half, device, route, target):
        return copies(kind, layers - 1, device, route, target, last_parts(half))

    def forward(kind, layer):
        x_order = own_parts(layer)
        y_order = x_order[::-1] if layer == layers - 1 else x_order
        for x_part, y_part in zip(x_order, y_order):
            arrive(own_x(kind, layer, x_peer, me, (x_part,)))
            if x_part in ((0, 2), (2, 6)):
                start_far(kind, layer, 0, x_peer, y_peer)
            start(pair(kind, layer, x_peer, "pair_x", (x_part,)))
            arrive(own_y(1 - kind, layer, y_peer, me, (y_part,)))
            if y_part == (1, 2):
                start_far(1 - kind, layer, 1, y_peer, x_peer)
            start(pair(1 - kind, layer, y_peer, "pair_y", (y_part,)))

    def far_arrive(kind, layer, only=None):
        for idx, parts in enumerate(zip(far_parts(layer, 0), far_parts(layer, 1))):
            if only is not None and idx != only:
                continue
            for half in range(2):
                arrive(far(1 - kind, layer, half, diag, me, (parts[half],)))
                start(pair(1 - kind, layer, diag, "pair_far", (parts[half],)))

    def far_partner(kind, layer):
        arrive(pair(1 - kind, layer, partner_of(diag), "pair_far", far_parts(layer, 0) + far_parts(layer, 1)))

    def near_partner(kind, layer, x_parts=None, y_parts=None):
        arrive(pair(kind, layer, partner_of(x_peer), "pair_x", x_parts or own_parts(layer)))
        arrive(pair(1 - kind, layer, partner_of(y_peer), "pair_y", y_parts or own_parts(layer)))

    def stage_own(kind):
        pack(kind, me, p0)
        forward(kind, 0)
        for layer in range(layers):
            arrive(pair(kind, layer, partner, "pair_own", own_parts(layer)))
        pack(kind, partner, p1)
        forward(kind, 1)
        start(own_x(kind, layers - 1, me, x_peer))
        start(own_y(kind, layers - 1, me, y_peer)[::-1])
        near_partner(kind, 0)
        far_arrive(kind, 0)
        near_partner(kind, 1)
        far_partner(kind, 0)

    def stage_one(kind):
        far_arrive(kind, 1)
        far_partner(kind, 1)

    def stage_two(kind):
        last = layers - 1
        early = far_parts(last, 0)[:-1] + far_parts(last, 1)[:-1]
        late = last_parts(0) + last_parts(1)
        forward(kind, last)
        near_partner(kind, last, ((0, 2),), ((1, 2),))

        @pl.when(core == 0)
        def _():
            start(extra(kind, 0, partner_of(x_peer), "extra", y_peer))
            start(extra(1 - kind, 1, partner_of(y_peer), "extra", x_peer))

        pack(kind, x_peer, p2)
        pack(1 - kind, y_peer, p4)
        near_partner(kind, last, ((1, 2),), ((0, 2),))
        far_arrive(kind, last, 0)
        pack(kind, partner_of(x_peer), p3)
        far_arrive(kind, last, 1)
        pack(1 - kind, partner_of(y_peer), p5)
        drain(kind)
        arrive(pair(1 - kind, last, partner_of(diag), "pair_far", early))

        @pl.when(core == 0)
        def _():
            far_arrive(kind, last, 2)
            for half in range(2):
                arrive(extra(1 - kind, half, partner_of(diag), "extra", me))
                start(extra(1 - kind, half, partner_of(diag), "pair_extra", partner))
            left(pair(1 - kind, last, diag, "pair_far", late))
            left(far(kind, last, 0, x_peer, y_peer, last_parts(0)))
            left(far(1 - kind, last, 1, y_peer, x_peer, last_parts(1)))
            left(extra(kind, 0, partner_of(x_peer), "extra", y_peer))
            left(extra(1 - kind, 1, partner_of(y_peer), "extra", x_peer))
            for half in range(2):
                left(extra(1 - kind, half, partner_of(diag), "pair_extra", partner))

        @pl.when(core == 1)
        def _():
            arrive(pair(1 - kind, last, partner_of(diag), "pair_far", late))
            for half in range(2):
                arrive(extra(1 - kind, half, diag, "pair_extra", me))

        left(pair(1 - kind, last, diag, "pair_far", early))
        left(far(kind, last, 0, x_peer, y_peer, far_parts(last, 0)[:-1]))
        left(far(1 - kind, last, 1, y_peer, x_peer, far_parts(last, 1)[:-1]))

    by_kind(stage_own)
    tok_load.wait()
    mlp_block(dims, 0, w_in, w_out, hidden_ref, hidden_ref, normed_ref, active_ref)
    by_kind(stage_one)
    mlp_block(dims, 1, w_in, w_out, hidden_ref, hidden_ref, normed_ref, active_ref)
    by_kind(stage_two)


def finish_kernel(dims, p0, p1, p2, p3, p4, p5, master_ref, one_ref, two_ref, w_in, w_out, last_ref, tgt_ref,
                  packed_hbm, master_hbm, one_hbm, two_hbm, loss_hbm,
                  loss_ref, far_ref, wide_ref, normed_ref, active_ref, hidden_ref, sem, far_sem):
    layers, model_dim, hidden_dim, rows, chunks = dims
    me, core, y_pos, x_peer, y_peer, diag = places()
    twin = 1 - 2 * core

    copies = []
    for which, (src, dst) in enumerate(((master_ref, master_hbm), (one_ref, one_hbm), (two_ref, two_hbm))):
        for layer in range(layers):
            copies.append(pltpu.make_async_copy(src.at[layer], dst.at[:, layer, :], sem.at[6 + which * layers + layer]))
    for idx, (ref, device) in enumerate(((p0, me), (p1, me + twin), (p2, x_peer), (p3, x_peer + twin), (p4, y_peer), (p5, y_peer + twin))):
        copies.append(pltpu.make_async_copy(ref, packed_hbm.at[pl.ds(device * chunks, chunks)], sem.at[idx]))
    for item in copies:
        item.start()

    far_copies = []
    for idx, device in enumerate((diag, diag + twin)):
        for y_value in range(2):
            @pl.when(y_pos == y_value)
            def _():
                spread_piece(dims, 1 - y_value, device, (w_in, w_out), wide_ref)

        def squeeze(at, _):
            block = wide_ref[pl.ds(pl.multiple_of(at * 128, 128), 128), :].astype(BF16).reshape(32, 4, LANES)
            far_ref[idx, pl.ds(at * 32, 32), :, :] = block[:, :layers, :]
            return 0

        lax.fori_loop(0, 4 * chunks // 128, squeeze, 0)
        far_copies.append(pltpu.make_async_copy(far_ref.at[idx], packed_hbm.at[pl.ds(device * chunks, chunks)], far_sem.at[idx]))
        far_copies[-1].start()

    mlp_block(dims, layers - 1, w_in, w_out, last_ref, hidden_ref, normed_ref, active_ref)

    for idx in range(rows // LANES):
        at = slice(idx * LANES, (idx + 1) * LANES)
        error = hidden_ref[at, :].astype(F32) - tgt_ref[at, :].astype(F32)
        error = error * error
        folded = error[:, 0:LANES]
        for col in range(LANES, model_dim, LANES):
            folded = folded + error[:, col:col + LANES]
        loss_ref[idx:idx + 1, :] = jnp.sum(folded.T, axis=0, keepdims=True) * (1.0 / model_dim)

    loss_copy = pltpu.make_async_copy(loss_ref, loss_hbm, far_sem.at[2])
    loss_copy.start()
    for item in copies + far_copies + [loss_copy]:
        item.wait()


def solution(mesh):
    group_size = mesh.shape["data"]
    state_spec = P(None, "data")
    row_spec = P("data", None)

    def local_step(grad_shard, master_shard, one_shard, two_shard, tok_rows, tgt_rows):
        rows, model_dim = tok_rows.shape
        layers, cols = master_shard.shape
        half_size = cols * group_size // 2
        hidden_dim = half_size // model_dim
        chunks = cols // LANES
        dims = (layers, model_dim, hidden_dim, rows, chunks)
        tiled = [a.reshape(layers, chunks, LANES).transpose(1, 0, 2) for a in (grad_shard, master_shard, one_shard, two_shard)]
        state_v = pltpu.VMEM((layers, chunks, LANES), F32)
        hbm = pl.BlockSpec(memory_space=pltpu.HBM)
        vmem = pl.BlockSpec(memory_space=pltpu.VMEM)
        state_out = state_v
        w_in_v = pltpu.VMEM((layers, model_dim, hidden_dim), BF16)
        w_out_v = pltpu.VMEM((layers, hidden_dim, model_dim), BF16)
        hidden_v = pltpu.VMEM((rows, model_dim), BF16)
        wide_v = pltpu.VMEM((4 * chunks, LANES), F32)
        normed_v = pltpu.VMEM((256, model_dim), BF16)
        active_v = pltpu.VMEM((256, hidden_dim), BF16)
        packed_v = pltpu.VMEM((4 * chunks, LANES), BF16)
        gathered = pl.pallas_call(
            functools.partial(gather_kernel, dims),
            name="gather_step",
            out_shape=(*(packed_v,) * 6, state_v, state_v, state_v, w_in_v, w_out_v, hidden_v),
            in_specs=[hbm] * 5,
            out_specs=(vmem,) * 12,
            scratch_shapes=[
                state_v, state_v, state_v, state_v,
                pltpu.VMEM((group_size, 1, LANES), F32),
                wide_v, normed_v, active_v,
                pltpu.SemaphoreType.DMA((5, layers)),
                pltpu.SemaphoreType.DMA((layers, 3)),
                pltpu.SemaphoreType.DMA((group_size,)),
                pltpu.SemaphoreType.DMA((group_size,)),
                pltpu.SemaphoreType.DMA((96,)),
                pltpu.SemaphoreType.DMA((96,)),
            ],
            compiler_params=pltpu.CompilerParams(collective_id=0, has_side_effects=True, vmem_limit_bytes=19 << 20),
        )(*[pltpu.with_memory_space_constraint(a, pltpu.HBM) for a in (*tiled, tok_rows)])
        gathered = [a.reshape(chunks, 4, LANES)[:, :layers, :] for a in gathered[:6]] + list(gathered[6:])
        state_tile = jax.ShapeDtypeStruct((chunks, layers, LANES), F32)
        weights, new_master, new_one, new_two, row_loss = pl.pallas_call(
            functools.partial(finish_kernel, dims),
            name="finish",
            out_shape=(jax.ShapeDtypeStruct((chunks * group_size, layers, LANES), BF16), state_tile, state_tile, state_tile,
                       jax.ShapeDtypeStruct((rows // LANES, LANES), F32)),
            in_specs=[vmem] * 13,
            out_specs=(hbm,) * 5,
            scratch_shapes=[
                pltpu.VMEM((rows // LANES, LANES), F32),
                pltpu.VMEM((2, chunks, layers, LANES), BF16),
                wide_v, normed_v, active_v, hidden_v,
                pltpu.SemaphoreType.DMA((6 + 3 * layers,)),
                pltpu.SemaphoreType.DMA((3,)),
            ],
            compiler_params=pltpu.CompilerParams(vmem_limit_bytes=14 << 20),
        )(*gathered, tgt_rows)

        def flat(a):
            return a.transpose(1, 0, 2).reshape(layers, a.shape[0] * LANES)

        return row_loss.reshape(rows), flat(weights), flat(new_master), flat(new_one), flat(new_two)

    return jax.shard_map(local_step, mesh=mesh, in_specs=(state_spec, state_spec, state_spec, state_spec, row_spec, row_spec), out_specs=(P("data"), P(), state_spec, state_spec, state_spec), check_vma=False)
```

```python
import functools

import jax
import jax.numpy as jnp
from jax import lax
from jax.experimental import pallas as pl
from jax.experimental.pallas import tpu as pltpu
from jax.sharding import PartitionSpec as P

LEARN_RATE = 0.01
BETA_ONE = 0.9
BETA_TWO = 0.95
ADAM_EPS = 1e-8
WEIGHT_DECAY = 0.1
ADAM_STEP = 10
CLIP_NORM = 1.0
NORM_EPS = 1e-6

MESH = pl.DeviceIdType.MESH
LANES = 128
GROUP = 8
F32 = jnp.float32
BF16 = jnp.bfloat16


def spread_piece(dims, kind, device, weights, wide_ref):
    layers, model_dim, hidden_dim, rows, chunks = dims
    per_row = (hidden_dim if kind == 0 else model_dim) // LANES
    count = chunks // per_row
    src = weights[kind]
    slot = lax.rem(device, 4)

    def spread(idx, _):
        row = pl.multiple_of(slot * count + idx * 16, 16)
        for layer in range(layers):
            for col in range(per_row):
                tile = src[layer, pl.ds(row, 16), col * LANES:(col + 1) * LANES].astype(F32)
                base = layer + 4 * (idx * (16 * per_row) + col)
                wide_ref[pl.ds(base, 8, stride=4 * per_row), :] = tile[0:8]
                wide_ref[pl.ds(base + 32 * per_row, 8, stride=4 * per_row), :] = tile[8:16]
        return 0

    lax.fori_loop(0, count // 16, spread, 0)


def mlp_block(dims, layer, w_in, w_out, source_ref, hidden_ref, normed_ref, active_ref):
    layers, model_dim, hidden_dim, rows, chunks = dims

    def block(idx, _):
        at = pl.ds(pl.multiple_of(idx * 256, 256), 256)
        hidden = source_ref[at, :].astype(F32)
        scale = lax.rsqrt(jnp.mean(hidden * hidden, axis=-1, keepdims=True) + NORM_EPS)
        normed_ref[...] = (hidden * scale).astype(BF16)
        for col in range(0, hidden_dim, 384):
            inner = jnp.dot(normed_ref[...], w_in[layer, :, col:col + 384], preferred_element_type=F32).astype(BF16)
            active_ref[:, col:col + 384] = jax.nn.gelu(inner.astype(F32), approximate=True).astype(BF16)
        for col in range(0, model_dim, 256):
            add = jnp.dot(active_ref[...], w_out[layer, :, col:col + 256], preferred_element_type=F32)
            hidden_ref[at, col:col + 256] = (source_ref[at, col:col + 256].astype(F32) + add).astype(BF16)
        return 0

    lax.fori_loop(0, rows // 256, block, 0)


def places():
    me = lax.axis_index("data")
    core = lax.rem(me, 2)
    x_pos = lax.rem(me // 2, 2)
    y_pos = me // 4
    x_peer = me + 2 - 4 * x_pos
    y_peer = me + 4 - 8 * y_pos
    return me, core, y_pos, x_peer, y_peer, x_peer + 4 - 8 * y_pos


def gather_kernel(dims, grad_hbm, master_hbm, one_hbm, two_hbm, tok_hbm,
                  p0, p1, p2, p3, p4, p5, master_out, one_out, two_out, w_in, w_out, hidden_ref,
                  grad_v, master_v, one_v, two_v,
                  part_ref, wide_ref, normed_ref, active_ref,
                  load_sem, grad_sem, part_send, part_recv, send_sem, recv_sem):
    layers, model_dim, hidden_dim, rows, chunks = dims
    in_rows = chunks * LANES // hidden_dim
    out_rows = chunks * LANES // model_dim

    me, core, y_pos, x_peer, y_peer, diag = places()
    partner = me + 1 - 2 * core

    state = ((grad_hbm, grad_v), (master_hbm, master_v), (one_hbm, one_v), (two_hbm, two_v))

    def load(which, layer):
        src, dst = state[which]
        return pltpu.make_async_copy(src.at[:, layer, :], dst.at[layer], load_sem.at[which, layer])

    span = chunks // 3

    def grad_load(layer, part):
        at = pl.ds(part * span, span)
        return pltpu.make_async_copy(grad_hbm.at[at, layer, :], grad_v.at[layer, at], grad_sem.at[layer, part])

    for layer in range(layers):
        for part in range(3):
            grad_load(layer, part).start()
    tok_load = pltpu.make_async_copy(tok_hbm, hidden_ref, load_sem.at[4, 0])

    barrier = pltpu.get_barrier_semaphore()
    for step in range(1, GROUP):
        pl.semaphore_signal(barrier, inc=1, device_id=(lax.rem(me + step, GROUP),), device_id_type=MESH)

    sums = tuple(jnp.zeros((8, LANES), F32) for _ in range(8))
    for layer in range(layers):
        for part in range(3):
            grad_load(layer, part).wait()
            if layer == layers - 1 and part == 2:
                for which in range(1, 4):
                    load(which, 0).start()

            def square(idx, carry):
                base = pl.multiple_of(part * span + idx * 64, 64)
                block = grad_v[layer, pl.ds(base, 64), :]
                return tuple(carry[k] + block[8 * k:8 * k + 8] * block[8 * k:8 * k + 8] for k in range(8))

            sums = lax.fori_loop(0, span // 64, square, sums)
    mine = ((sums[0] + sums[1]) + (sums[2] + sums[3])) + ((sums[4] + sums[5]) + (sums[6] + sums[7]))
    part_ref[me] = jnp.sum(mine, axis=0, keepdims=True)
    pl.semaphore_wait(barrier, GROUP - 1)

    def part_copy(step):
        return pltpu.make_async_remote_copy(
            src_ref=part_ref.at[me], dst_ref=part_ref.at[me],
            send_sem=part_send.at[step], recv_sem=part_recv.at[step],
            device_id=(lax.rem(me + step, GROUP),), device_id_type=MESH)

    def part_arrival(step):
        slot = lax.rem(me + GROUP - step, GROUP)
        return pltpu.make_async_remote_copy(
            src_ref=part_ref.at[slot], dst_ref=part_ref.at[slot],
            send_sem=part_send.at[step], recv_sem=part_recv.at[step],
            device_id=(me,), device_id_type=MESH)

    for step in range(1, GROUP):
        part_copy(step).start()
    for item in range(1, layers):
        for which in range(1, 4):
            load(which, item).start()
    tok_load.start()
    for which in range(1, 4):
        load(which, 0).wait()
    for step in range(1, GROUP):
        part_arrival(step).wait_recv()
    total = part_ref[0]
    for slot in range(1, GROUP):
        total = total + part_ref[slot]
    total = jnp.sum(total, axis=1, keepdims=True)
    clip = jnp.minimum(1.0, CLIP_NORM / jnp.sqrt(total))
    clip = jnp.broadcast_to(clip, (8, LANES))

    slots = {}

    def piece(kind, layer, device, part):
        ref, count = ((w_in, in_rows), (w_out, out_rows))[kind]
        span = count // part[1]
        at = lax.rem(device, 4) * count + part[0] * span
        return ref.at[layer, pl.ds(pl.multiple_of(at, 8), span), :]

    def copies(kind, layer, device, route, target, parts):
        out = []
        for part in parts:
            ref = piece(kind, layer, device, part)
            index = slots.setdefault((route, layer, part), len(slots))
            out.append(pltpu.make_async_remote_copy(
                src_ref=ref, dst_ref=ref, send_sem=send_sem.at[index],
                recv_sem=recv_sem.at[index], device_id=(target,), device_id_type=MESH))
        return out

    def start(items):
        for item in items:
            item.start()

    def arrive(items):
        for item in items:
            item.wait_recv()

    def left(items):
        for item in items:
            item.wait_send()

    def own_parts(layer):
        return ((0, 12), (1, 12), (1, 6), (2, 6), (1, 2)) if layer == 0 else ((0, 2), (1, 2))

    def far_parts(layer, half):
        return tuple((3 * half + at, 6) for at in range(3)) if layer == layers - 1 else ((half, 2),)

    def own_x(kind, layer, device, target, parts=None):
        return copies(kind, layer, device, "own_x", target, parts or own_parts(layer))

    def own_y(kind, layer, device, target, parts=None):
        return copies(kind, layer, device, "own_y", target, parts or own_parts(layer))

    def far(kind, layer, half, device, target, parts=None):
        return copies(kind, layer, device, "far", target, parts or far_parts(layer, half))

    def pair(kind, layer, device, route, parts):
        return copies(kind, layer, device, route, partner, parts)

    def by_kind(function):
        for y_value in range(2):
            @pl.when(y_pos == y_value)
            def _():
                function(y_value)

    one_scale = 1.0 / (1.0 - BETA_ONE ** ADAM_STEP)
    two_scale = 1.0 / (1.0 - BETA_TWO ** ADAM_STEP)

    def adam(layer, part):
        first = part[0] * (chunks // part[1])
        step = 144 if part[1] == 12 else 48

        def update(idx, _):
            base = pl.multiple_of(first + idx * step, 8)
            for k in range(step // 8):
                at = pl.ds(pl.multiple_of(base + 8 * k, 8), 8)
                clipped = grad_v[layer, at, :] * clip
                new_one = BETA_ONE * one_v[layer, at, :] + (1.0 - BETA_ONE) * clipped
                new_two = BETA_TWO * two_v[layer, at, :] + (1.0 - BETA_TWO) * clipped * clipped
                step_size = (new_one * one_scale) / (jnp.sqrt(new_two * two_scale) + ADAM_EPS)
                old = master_v[layer, at, :]
                master_out[layer, at, :] = old - LEARN_RATE * (step_size + WEIGHT_DECAY * old)
                one_out[layer, at, :] = new_one
                two_out[layer, at, :] = new_two
            return 0

        lax.fori_loop(0, chunks // part[1] // step, update, 0)

    def round_rows(kind, layer, part):
        width = hidden_dim if kind == 0 else model_dim
        count = in_rows if kind == 0 else out_rows
        per_row = width // LANES
        dst = w_in if kind == 0 else w_out
        slot = lax.rem(me, 4)

        step = 16 if count // part[1] % 16 == 0 else 8

        def body(idx, _):
            base = part[0] * (chunks // part[1]) + idx * (step * per_row)
            row = pl.multiple_of(slot * count + part[0] * (count // part[1]) + idx * step, 8)
            for col in range(per_row):
                block = master_out[layer, pl.ds(base + col, 8, stride=per_row), :]
                if step == 16:
                    low = master_out[layer, pl.ds(base + 8 * per_row + col, 8, stride=per_row), :]
                    block = jnp.concatenate([block, low], axis=0)
                dst[layer, pl.ds(row, step), col * LANES:(col + 1) * LANES] = block.astype(BF16)
            return 0

        lax.fori_loop(0, count // step // part[1], body, 0)

    for layer in range(layers):
        for which in range(1, 4) if layer else ():
            load(which, layer).wait()
        for part in own_parts(layer):
            adam(layer, part)

            def send_own(kind):
                round_rows(kind, layer, part)
                if layer < layers - 1:
                    start(own_x(kind, layer, me, x_peer, (part,)))
                    start(own_y(kind, layer, me, y_peer, (part,)))
                start(pair(kind, layer, me, "pair_own", (part,)))

            by_kind(send_own)

    def pack(kind, device, packed_ref):
        spread_piece(dims, kind, device, (w_in, w_out), wide_ref)

        def squeeze(idx, _):
            at = pl.ds(pl.multiple_of(idx * 256, 256), 256)
            packed_ref[at, :] = wide_ref[at, :].astype(BF16)
            return 0

        lax.fori_loop(0, 4 * chunks // 256, squeeze, 0)

    def partner_of(device):
        return device + 1 - 2 * core

    def drain(kind):
        for layer in range(layers):
            left(own_x(kind, layer, me, x_peer))
            left(own_y(kind, layer, me, y_peer))
            left(pair(kind, layer, me, "pair_own", own_parts(layer)))
            left(pair(kind, layer, x_peer, "pair_x", own_parts(layer)))
            left(pair(1 - kind, layer, y_peer, "pair_y", own_parts(layer)))
            if layer < layers - 1:
                left(pair(1 - kind, layer, diag, "pair_far", far_parts(layer, 0) + far_parts(layer, 1)))
                left(far(kind, layer, 0, x_peer, y_peer))
                left(far(1 - kind, layer, 1, y_peer, x_peer))
        for step in range(1, GROUP):
            part_copy(step).wait_send()

    def last_parts(half):
        return far_parts(layers - 1, half)[-1:]

    def start_far(kind, layer, half, device, target):
        if layer < layers - 1:
            start(far(kind, layer, half, device, target))
            return
        start(far(kind, layer, half, device, target, far_parts(layer, half)[:-1]))

        @pl.when(core == 0)
        def _():
            start(far(kind, layer, half, device, target, last_parts(half)))

    def extra(kind, half, device, route, target):
        return copies(kind, layers - 1, device, route, target, last_parts(half))

    def forward(kind, layer):
        x_order = own_parts(layer)
        y_order = x_order[::-1] if layer == layers - 1 else x_order
        for x_part, y_part in zip(x_order, y_order):
            arrive(own_x(kind, layer, x_peer, me, (x_part,)))
            if x_part in ((0, 2), (2, 6)):
                start_far(kind, layer, 0, x_peer, y_peer)
            start(pair(kind, layer, x_peer, "pair_x", (x_part,)))
            arrive(own_y(1 - kind, layer, y_peer, me, (y_part,)))
            if y_part == (1, 2):
                start_far(1 - kind, layer, 1, y_peer, x_peer)
            start(pair(1 - kind, layer, y_peer, "pair_y", (y_part,)))

    def far_arrive(kind, layer, only=None):
        for idx, parts in enumerate(zip(far_parts(layer, 0), far_parts(layer, 1))):
            if only is not None and idx != only:
                continue
            for half in range(2):
                arrive(far(1 - kind, layer, half, diag, me, (parts[half],)))
                start(pair(1 - kind, layer, diag, "pair_far", (parts[half],)))

    def far_partner(kind, layer):
        arrive(pair(1 - kind, layer, partner_of(diag), "pair_far", far_parts(layer, 0) + far_parts(layer, 1)))

    def near_partner(kind, layer, x_parts=None, y_parts=None):
        arrive(pair(kind, layer, partner_of(x_peer), "pair_x", x_parts or own_parts(layer)))
        arrive(pair(1 - kind, layer, partner_of(y_peer), "pair_y", y_parts or own_parts(layer)))

    def stage_own(kind):
        pack(kind, me, p0)
        forward(kind, 0)
        for layer in range(layers):
            arrive(pair(kind, layer, partner, "pair_own", own_parts(layer)))
        pack(kind, partner, p1)
        forward(kind, 1)
        start(own_x(kind, layers - 1, me, x_peer))
        start(own_y(kind, layers - 1, me, y_peer)[::-1])
        near_partner(kind, 0)
        far_arrive(kind, 0)
        near_partner(kind, 1)
        far_partner(kind, 0)

    def stage_one(kind):
        far_arrive(kind, 1)
        far_partner(kind, 1)

    def stage_two(kind):
        last = layers - 1
        early = far_parts(last, 0)[:-1] + far_parts(last, 1)[:-1]
        late = last_parts(0) + last_parts(1)
        forward(kind, last)
        near_partner(kind, last, ((0, 2),), ((1, 2),))

        @pl.when(core == 0)
        def _():
            start(extra(kind, 0, partner_of(x_peer), "extra", y_peer))
            start(extra(1 - kind, 1, partner_of(y_peer), "extra", x_peer))

        pack(kind, x_peer, p2)
        pack(1 - kind, y_peer, p4)
        near_partner(kind, last, ((1, 2),), ((0, 2),))
        far_arrive(kind, last, 0)
        pack(kind, partner_of(x_peer), p3)
        far_arrive(kind, last, 1)
        pack(1 - kind, partner_of(y_peer), p5)
        drain(kind)
        arrive(pair(1 - kind, last, partner_of(diag), "pair_far", early))

        @pl.when(core == 0)
        def _():
            far_arrive(kind, last, 2)
            for half in range(2):
                arrive(extra(1 - kind, half, partner_of(diag), "extra", me))
                start(extra(1 - kind, half, partner_of(diag), "pair_extra", partner))
            left(pair(1 - kind, last, diag, "pair_far", late))
            left(far(kind, last, 0, x_peer, y_peer, last_parts(0)))
            left(far(1 - kind, last, 1, y_peer, x_peer, last_parts(1)))
            left(extra(kind, 0, partner_of(x_peer), "extra", y_peer))
            left(extra(1 - kind, 1, partner_of(y_peer), "extra", x_peer))
            for half in range(2):
                left(extra(1 - kind, half, partner_of(diag), "pair_extra", partner))

        @pl.when(core == 1)
        def _():
            arrive(pair(1 - kind, last, partner_of(diag), "pair_far", late))
            for half in range(2):
                arrive(extra(1 - kind, half, diag, "pair_extra", me))

        left(pair(1 - kind, last, diag, "pair_far", early))
        left(far(kind, last, 0, x_peer, y_peer, far_parts(last, 0)[:-1]))
        left(far(1 - kind, last, 1, y_peer, x_peer, far_parts(last, 1)[:-1]))

    by_kind(stage_own)
    tok_load.wait()
    mlp_block(dims, 0, w_in, w_out, hidden_ref, hidden_ref, normed_ref, active_ref)
    by_kind(stage_one)
    mlp_block(dims, 1, w_in, w_out, hidden_ref, hidden_ref, normed_ref, active_ref)
    by_kind(stage_two)


def finish_kernel(dims, p0, p1, p2, p3, p4, p5, master_ref, one_ref, two_ref, w_in, w_out, last_ref, tgt_ref,
                  packed_hbm, master_hbm, one_hbm, two_hbm, loss_hbm,
                  loss_ref, far_ref, wide_ref, normed_ref, active_ref, hidden_ref, sem, far_sem):
    layers, model_dim, hidden_dim, rows, chunks = dims
    me, core, y_pos, x_peer, y_peer, diag = places()
    twin = 1 - 2 * core

    copies = []
    for which, (src, dst) in enumerate(((master_ref, master_hbm), (one_ref, one_hbm), (two_ref, two_hbm))):
        for layer in range(layers):
            copies.append(pltpu.make_async_copy(src.at[layer], dst.at[:, layer, :], sem.at[6 + which * layers + layer]))
    for idx, (ref, device) in enumerate(((p0, me), (p1, me + twin), (p2, x_peer), (p3, x_peer + twin), (p4, y_peer), (p5, y_peer + twin))):
        copies.append(pltpu.make_async_copy(ref, packed_hbm.at[pl.ds(device * chunks, chunks)], sem.at[idx]))
    for item in copies:
        item.start()

    far_copies = []
    for idx, device in enumerate((diag, diag + twin)):
        for y_value in range(2):
            @pl.when(y_pos == y_value)
            def _():
                spread_piece(dims, 1 - y_value, device, (w_in, w_out), wide_ref)

        def squeeze(at, _):
            block = wide_ref[pl.ds(pl.multiple_of(at * 128, 128), 128), :].astype(BF16).reshape(32, 4, LANES)
            far_ref[idx, pl.ds(at * 32, 32), :, :] = block[:, :layers, :]
            return 0

        lax.fori_loop(0, 4 * chunks // 128, squeeze, 0)
        far_copies.append(pltpu.make_async_copy(far_ref.at[idx], packed_hbm.at[pl.ds(device * chunks, chunks)], far_sem.at[idx]))
        far_copies[-1].start()

    mlp_block(dims, layers - 1, w_in, w_out, last_ref, hidden_ref, normed_ref, active_ref)

    for idx in range(rows // LANES):
        at = slice(idx * LANES, (idx + 1) * LANES)
        error = hidden_ref[at, :].astype(F32) - tgt_ref[at, :].astype(F32)
        error = error * error
        folded = error[:, 0:LANES]
        for col in range(LANES, model_dim, LANES):
            folded = folded + error[:, col:col + LANES]
        loss_ref[idx:idx + 1, :] = jnp.sum(folded.T, axis=0, keepdims=True) * (1.0 / model_dim)

    loss_copy = pltpu.make_async_copy(loss_ref, loss_hbm, far_sem.at[2])
    loss_copy.start()
    for item in copies + far_copies + [loss_copy]:
        item.wait()


def solution(mesh):
    group_size = mesh.shape["data"]
    state_spec = P(None, "data")
    row_spec = P("data", None)

    def local_step(grad_shard, master_shard, one_shard, two_shard, tok_rows, tgt_rows):
        rows, model_dim = tok_rows.shape
        layers, cols = master_shard.shape
        half_size = cols * group_size // 2
        hidden_dim = half_size // model_dim
        chunks = cols // LANES
        dims = (layers, model_dim, hidden_dim, rows, chunks)
        tiled = [a.reshape(layers, chunks, LANES).transpose(1, 0, 2) for a in (grad_shard, master_shard, one_shard, two_shard)]
        state_v = pltpu.VMEM((layers, chunks, LANES), F32)
        hbm = pl.BlockSpec(memory_space=pltpu.HBM)
        vmem = pl.BlockSpec(memory_space=pltpu.VMEM)
        state_out = state_v
        w_in_v = pltpu.VMEM((layers, model_dim, hidden_dim), BF16)
        w_out_v = pltpu.VMEM((layers, hidden_dim, model_dim), BF16)
        hidden_v = pltpu.VMEM((rows, model_dim), BF16)
        wide_v = pltpu.VMEM((4 * chunks, LANES), F32)
        normed_v = pltpu.VMEM((256, model_dim), BF16)
        active_v = pltpu.VMEM((256, hidden_dim), BF16)
        packed_v = pltpu.VMEM((4 * chunks, LANES), BF16)
        gathered = pl.pallas_call(
            functools.partial(gather_kernel, dims),
            name="gather_step",
            out_shape=(*(packed_v,) * 6, state_v, state_v, state_v, w_in_v, w_out_v, hidden_v),
            in_specs=[hbm] * 5,
            out_specs=(vmem,) * 12,
            scratch_shapes=[
                state_v, state_v, state_v, state_v,
                pltpu.VMEM((group_size, 1, LANES), F32),
                wide_v, normed_v, active_v,
                pltpu.SemaphoreType.DMA((5, layers)),
                pltpu.SemaphoreType.DMA((layers, 3)),
                pltpu.SemaphoreType.DMA((group_size,)),
                pltpu.SemaphoreType.DMA((group_size,)),
                pltpu.SemaphoreType.DMA((96,)),
                pltpu.SemaphoreType.DMA((96,)),
            ],
            compiler_params=pltpu.CompilerParams(collective_id=0, has_side_effects=True, vmem_limit_bytes=19 << 20),
        )(*[pltpu.with_memory_space_constraint(a, pltpu.HBM) for a in (*tiled, tok_rows)])
        gathered = [a.reshape(chunks, 4, LANES)[:, :layers, :] for a in gathered[:6]] + list(gathered[6:])
        state_tile = jax.ShapeDtypeStruct((chunks, layers, LANES), F32)
        weights, new_master, new_one, new_two, row_loss = pl.pallas_call(
            functools.partial(finish_kernel, dims),
            name="finish",
            out_shape=(jax.ShapeDtypeStruct((chunks * group_size, layers, LANES), BF16), state_tile, state_tile, state_tile,
                       jax.ShapeDtypeStruct((rows // LANES, LANES), F32)),
            in_specs=[vmem] * 13,
            out_specs=(hbm,) * 5,
            scratch_shapes=[
                pltpu.VMEM((rows // LANES, LANES), F32),
                pltpu.VMEM((2, chunks, layers, LANES), BF16),
                wide_v, normed_v, active_v, hidden_v,
                pltpu.SemaphoreType.DMA((6 + 3 * layers,)),
                pltpu.SemaphoreType.DMA((3,)),
            ],
            compiler_params=pltpu.CompilerParams(vmem_limit_bytes=14 << 20),
        )(*gathered, tgt_rows)

        def flat(a):
            return a.transpose(1, 0, 2).reshape(layers, a.shape[0] * LANES)

        return row_loss.reshape(rows), flat(weights), flat(new_master), flat(new_one), flat(new_two)

    return jax.shard_map(local_step, mesh=mesh, in_specs=(state_spec, state_spec, state_spec, state_spec, row_spec, row_spec), out_specs=(P("data"), P(), state_spec, state_spec, state_spec), check_vma=False)
```

```python
import functools

import jax
import jax.numpy as jnp
from jax import lax
from jax.experimental import pallas as pl
from jax.experimental.pallas import tpu as pltpu
from jax.sharding import PartitionSpec as P

LEARN_RATE = 0.01
BETA_ONE = 0.9
BETA_TWO = 0.95
ADAM_EPS = 1e-8
WEIGHT_DECAY = 0.1
ADAM_STEP = 10
CLIP_NORM = 1.0
NORM_EPS = 1e-6

MESH = pl.DeviceIdType.MESH
LANES = 128
GROUP = 8
F32 = jnp.float32
BF16 = jnp.bfloat16


def spread_piece(dims, kind, device, weights, wide_ref):
    layers, model_dim, hidden_dim, rows, chunks = dims
    per_row = (hidden_dim if kind == 0 else model_dim) // LANES
    count = chunks // per_row
    src = weights[kind]
    slot = lax.rem(device, 4)

    def spread(idx, _):
        row = pl.multiple_of(slot * count + idx * 16, 16)
        for layer in range(layers):
            for col in range(per_row):
                tile = src[layer, pl.ds(row, 16), col * LANES:(col + 1) * LANES].astype(F32)
                base = layer + 4 * (idx * (16 * per_row) + col)
                wide_ref[pl.ds(base, 8, stride=4 * per_row), :] = tile[0:8]
                wide_ref[pl.ds(base + 32 * per_row, 8, stride=4 * per_row), :] = tile[8:16]
        return 0

    lax.fori_loop(0, count // 16, spread, 0)


def mlp_block(dims, layer, w_in, w_out, source_ref, hidden_ref, normed_ref, active_ref):
    layers, model_dim, hidden_dim, rows, chunks = dims

    def block(idx, _):
        at = pl.ds(pl.multiple_of(idx * 256, 256), 256)
        hidden = source_ref[at, :].astype(F32)
        scale = lax.rsqrt(jnp.mean(hidden * hidden, axis=-1, keepdims=True) + NORM_EPS)
        normed_ref[...] = (hidden * scale).astype(BF16)
        for col in range(0, hidden_dim, 384):
            inner = jnp.dot(normed_ref[...], w_in[layer, :, col:col + 384], preferred_element_type=F32).astype(BF16)
            active_ref[:, col:col + 384] = jax.nn.gelu(inner.astype(F32), approximate=True).astype(BF16)
        for col in range(0, model_dim, 256):
            add = jnp.dot(active_ref[...], w_out[layer, :, col:col + 256], preferred_element_type=F32)
            hidden_ref[at, col:col + 256] = (source_ref[at, col:col + 256].astype(F32) + add).astype(BF16)
        return 0

    lax.fori_loop(0, rows // 256, block, 0)


def places():
    me = lax.axis_index("data")
    core = lax.rem(me, 2)
    x_pos = lax.rem(me // 2, 2)
    y_pos = me // 4
    x_peer = me + 2 - 4 * x_pos
    y_peer = me + 4 - 8 * y_pos
    return me, core, y_pos, x_peer, y_peer, x_peer + 4 - 8 * y_pos


def gather_kernel(dims, grad_hbm, master_hbm, one_hbm, two_hbm, tok_hbm,
                  p0, p1, p2, p3, p4, p5, master_out, one_out, two_out, w_in, w_out, hidden_ref,
                  grad_v, master_v, one_v, two_v,
                  part_ref, wide_ref, normed_ref, active_ref,
                  load_sem, grad_sem, part_send, part_recv, send_sem, recv_sem):
    layers, model_dim, hidden_dim, rows, chunks = dims
    in_rows = chunks * LANES // hidden_dim
    out_rows = chunks * LANES // model_dim

    me, core, y_pos, x_peer, y_peer, diag = places()
    partner = me + 1 - 2 * core

    state = ((grad_hbm, grad_v), (master_hbm, master_v), (one_hbm, one_v), (two_hbm, two_v))

    def load(which, layer):
        src, dst = state[which]
        return pltpu.make_async_copy(src.at[:, layer, :], dst.at[layer], load_sem.at[which, layer])

    span = chunks // 3

    def grad_load(layer, part):
        at = pl.ds(part * span, span)
        return pltpu.make_async_copy(grad_hbm.at[at, layer, :], grad_v.at[layer, at], grad_sem.at[layer, part])

    for layer in range(layers):
        for part in range(3):
            grad_load(layer, part).start()
    tok_load = pltpu.make_async_copy(tok_hbm, hidden_ref, load_sem.at[4, 0])

    barrier = pltpu.get_barrier_semaphore()
    for step in range(1, GROUP):
        pl.semaphore_signal(barrier, inc=1, device_id=(lax.rem(me + step, GROUP),), device_id_type=MESH)

    sums = tuple(jnp.zeros((8, LANES), F32) for _ in range(8))
    for layer in range(layers):
        for part in range(3):
            grad_load(layer, part).wait()
            if layer == layers - 1 and part == 2:
                for which in range(1, 4):
                    load(which, 0).start()

            def square(idx, carry):
                base = pl.multiple_of(part * span + idx * 64, 64)
                block = grad_v[layer, pl.ds(base, 64), :]
                return tuple(carry[k] + block[8 * k:8 * k + 8] * block[8 * k:8 * k + 8] for k in range(8))

            sums = lax.fori_loop(0, span // 64, square, sums)
    mine = ((sums[0] + sums[1]) + (sums[2] + sums[3])) + ((sums[4] + sums[5]) + (sums[6] + sums[7]))
    part_ref[me] = jnp.sum(mine, axis=0, keepdims=True)
    pl.semaphore_wait(barrier, GROUP - 1)

    def part_copy(step):
        return pltpu.make_async_remote_copy(
            src_ref=part_ref.at[me], dst_ref=part_ref.at[me],
            send_sem=part_send.at[step], recv_sem=part_recv.at[step],
            device_id=(lax.rem(me + step, GROUP),), device_id_type=MESH)

    def part_arrival(step):
        slot = lax.rem(me + GROUP - step, GROUP)
        return pltpu.make_async_remote_copy(
            src_ref=part_ref.at[slot], dst_ref=part_ref.at[slot],
            send_sem=part_send.at[step], recv_sem=part_recv.at[step],
            device_id=(me,), device_id_type=MESH)

    for step in range(1, GROUP):
        part_copy(step).start()
    for which in range(1, 4):
        load(which, 0).wait()
    for step in range(1, GROUP):
        part_arrival(step).wait_recv()
    total = part_ref[0]
    for slot in range(1, GROUP):
        total = total + part_ref[slot]
    total = jnp.sum(total, axis=1, keepdims=True)
    clip = jnp.minimum(1.0, CLIP_NORM / jnp.sqrt(total))
    clip = jnp.broadcast_to(clip, (8, LANES))

    slots = {}

    def piece(kind, layer, device, part):
        ref, count = ((w_in, in_rows), (w_out, out_rows))[kind]
        span = count // part[1]
        at = lax.rem(device, 4) * count + part[0] * span
        return ref.at[layer, pl.ds(pl.multiple_of(at, 8), span), :]

    def copies(kind, layer, device, route, target, parts):
        out = []
        for part in parts:
            ref = piece(kind, layer, device, part)
            index = slots.setdefault((route, layer, part), len(slots))
            out.append(pltpu.make_async_remote_copy(
                src_ref=ref, dst_ref=ref, send_sem=send_sem.at[index],
                recv_sem=recv_sem.at[index], device_id=(target,), device_id_type=MESH))
        return out

    def start(items):
        for item in items:
            item.start()

    def arrive(items):
        for item in items:
            item.wait_recv()

    def left(items):
        for item in items:
            item.wait_send()

    def own_parts(layer):
        return ((0, 12), (1, 12), (1, 6), (2, 6), (1, 2)) if layer == 0 else ((0, 2), (1, 2))

    def far_parts(layer, half):
        return tuple((3 * half + at, 6) for at in range(3)) if layer == layers - 1 else ((half, 2),)

    def own_x(kind, layer, device, target, parts=None):
        return copies(kind, layer, device, "own_x", target, parts or own_parts(layer))

    def own_y(kind, layer, device, target, parts=None):
        return copies(kind, layer, device, "own_y", target, parts or own_parts(layer))

    def far(kind, layer, half, device, target, parts=None):
        return copies(kind, layer, device, "far", target, parts or far_parts(layer, half))

    def pair(kind, layer, device, route, parts):
        return copies(kind, layer, device, route, partner, parts)

    def by_kind(function):
        for y_value in range(2):
            @pl.when(y_pos == y_value)
            def _():
                function(y_value)

    one_scale = 1.0 / (1.0 - BETA_ONE ** ADAM_STEP)
    two_scale = 1.0 / (1.0 - BETA_TWO ** ADAM_STEP)

    def adam(layer, part):
        first = part[0] * (chunks // part[1])
        step = 144 if part[1] == 12 else 48

        def update(idx, _):
            base = pl.multiple_of(first + idx * step, 8)
            for k in range(step // 8):
                at = pl.ds(pl.multiple_of(base + 8 * k, 8), 8)
                clipped = grad_v[layer, at, :] * clip
                new_one = BETA_ONE * one_v[layer, at, :] + (1.0 - BETA_ONE) * clipped
                new_two = BETA_TWO * two_v[layer, at, :] + (1.0 - BETA_TWO) * clipped * clipped
                step_size = (new_one * one_scale) / (jnp.sqrt(new_two * two_scale) + ADAM_EPS)
                old = master_v[layer, at, :]
                master_out[layer, at, :] = old - LEARN_RATE * (step_size + WEIGHT_DECAY * old)
                one_out[layer, at, :] = new_one
                two_out[layer, at, :] = new_two
            return 0

        lax.fori_loop(0, chunks // part[1] // step, update, 0)

    def round_rows(kind, layer, part):
        width = hidden_dim if kind == 0 else model_dim
        count = in_rows if kind == 0 else out_rows
        per_row = width // LANES
        dst = w_in if kind == 0 else w_out
        slot = lax.rem(me, 4)

        step = 16 if count // part[1] % 16 == 0 else 8

        def body(idx, _):
            base = part[0] * (chunks // part[1]) + idx * (step * per_row)
            row = pl.multiple_of(slot * count + part[0] * (count // part[1]) + idx * step, 8)
            for col in range(per_row):
                block = master_out[layer, pl.ds(base + col, 8, stride=per_row), :]
                if step == 16:
                    low = master_out[layer, pl.ds(base + 8 * per_row + col, 8, stride=per_row), :]
                    block = jnp.concatenate([block, low], axis=0)
                dst[layer, pl.ds(row, step), col * LANES:(col + 1) * LANES] = block.astype(BF16)
            return 0

        lax.fori_loop(0, count // step // part[1], body, 0)

    for layer in range(layers):
        for which in range(1, 4) if layer else ():
            load(which, layer).wait()
        for part in own_parts(layer):
            adam(layer, part)

            def send_own(kind):
                round_rows(kind, layer, part)
                if layer < layers - 1:
                    start(own_x(kind, layer, me, x_peer, (part,)))
                    start(own_y(kind, layer, me, y_peer, (part,)))
                start(pair(kind, layer, me, "pair_own", (part,)))

            by_kind(send_own)
            if layer == 0 and part == own_parts(0)[0]:
                for item in range(1, layers):
                    for which in range(1, 4):
                        load(which, item).start()
                tok_load.start()

    def pack(kind, device, packed_ref):
        spread_piece(dims, kind, device, (w_in, w_out), wide_ref)

        def squeeze(idx, _):
            at = pl.ds(pl.multiple_of(idx * 256, 256), 256)
            packed_ref[at, :] = wide_ref[at, :].astype(BF16)
            return 0

        lax.fori_loop(0, 4 * chunks // 256, squeeze, 0)

    def partner_of(device):
        return device + 1 - 2 * core

    def drain(kind):
        for layer in range(layers):
            left(own_x(kind, layer, me, x_peer))
            left(own_y(kind, layer, me, y_peer))
            left(pair(kind, layer, me, "pair_own", own_parts(layer)))
            left(pair(kind, layer, x_peer, "pair_x", own_parts(layer)))
            left(pair(1 - kind, layer, y_peer, "pair_y", own_parts(layer)))
            if layer < layers - 1:
                left(pair(1 - kind, layer, diag, "pair_far", far_parts(layer, 0) + far_parts(layer, 1)))
                left(far(kind, layer, 0, x_peer, y_peer))
                left(far(1 - kind, layer, 1, y_peer, x_peer))
        for step in range(1, GROUP):
            part_copy(step).wait_send()

    def last_parts(half):
        return far_parts(layers - 1, half)[-1:]

    def start_far(kind, layer, half, device, target):
        if layer < layers - 1:
            start(far(kind, layer, half, device, target))
            return
        start(far(kind, layer, half, device, target, far_parts(layer, half)[:-1]))

        @pl.when(core == 0)
        def _():
            start(far(kind, layer, half, device, target, last_parts(half)))

    def extra(kind, half, device, route, target):
        return copies(kind, layers - 1, device, route, target, last_parts(half))

    def forward(kind, layer):
        x_order = own_parts(layer)
        y_order = x_order[::-1] if layer == layers - 1 else x_order
        for x_part, y_part in zip(x_order, y_order):
            arrive(own_x(kind, layer, x_peer, me, (x_part,)))
            if x_part in ((0, 2), (2, 6)):
                start_far(kind, layer, 0, x_peer, y_peer)
            start(pair(kind, layer, x_peer, "pair_x", (x_part,)))
            arrive(own_y(1 - kind, layer, y_peer, me, (y_part,)))
            if y_part == (1, 2):
                start_far(1 - kind, layer, 1, y_peer, x_peer)
            start(pair(1 - kind, layer, y_peer, "pair_y", (y_part,)))

    def far_arrive(kind, layer, only=None):
        for idx, parts in enumerate(zip(far_parts(layer, 0), far_parts(layer, 1))):
            if only is not None and idx != only:
                continue
            for half in range(2):
                arrive(far(1 - kind, layer, half, diag, me, (parts[half],)))
                start(pair(1 - kind, layer, diag, "pair_far", (parts[half],)))

    def far_partner(kind, layer):
        arrive(pair(1 - kind, layer, partner_of(diag), "pair_far", far_parts(layer, 0) + far_parts(layer, 1)))

    def near_partner(kind, layer, x_parts=None, y_parts=None):
        arrive(pair(kind, layer, partner_of(x_peer), "pair_x", x_parts or own_parts(layer)))
        arrive(pair(1 - kind, layer, partner_of(y_peer), "pair_y", y_parts or own_parts(layer)))

    def stage_own(kind):
        pack(kind, me, p0)
        forward(kind, 0)
        for layer in range(layers):
            arrive(pair(kind, layer, partner, "pair_own", own_parts(layer)))
        pack(kind, partner, p1)
        forward(kind, 1)
        start(own_x(kind, layers - 1, me, x_peer))
        start(own_y(kind, layers - 1, me, y_peer)[::-1])
        near_partner(kind, 0)
        far_arrive(kind, 0)
        near_partner(kind, 1)
        far_partner(kind, 0)

    def stage_one(kind):
        far_arrive(kind, 1)
        far_partner(kind, 1)

    def stage_two(kind):
        last = layers - 1
        early = far_parts(last, 0)[:-1] + far_parts(last, 1)[:-1]
        late = last_parts(0) + last_parts(1)
        forward(kind, last)
        near_partner(kind, last, ((0, 2),), ((1, 2),))

        @pl.when(core == 0)
        def _():
            start(extra(kind, 0, partner_of(x_peer), "extra", y_peer))
            start(extra(1 - kind, 1, partner_of(y_peer), "extra", x_peer))

        pack(kind, x_peer, p2)
        pack(1 - kind, y_peer, p4)
        near_partner(kind, last, ((1, 2),), ((0, 2),))
        far_arrive(kind, last, 0)
        pack(kind, partner_of(x_peer), p3)
        far_arrive(kind, last, 1)
        pack(1 - kind, partner_of(y_peer), p5)
        drain(kind)
        arrive(pair(1 - kind, last, partner_of(diag), "pair_far", early))

        @pl.when(core == 0)
        def _():
            far_arrive(kind, last, 2)
            for half in range(2):
                arrive(extra(1 - kind, half, partner_of(diag), "extra", me))
                start(extra(1 - kind, half, partner_of(diag), "pair_extra", partner))
            left(pair(1 - kind, last, diag, "pair_far", late))
            left(far(kind, last, 0, x_peer, y_peer, last_parts(0)))
            left(far(1 - kind, last, 1, y_peer, x_peer, last_parts(1)))
            left(extra(kind, 0, partner_of(x_peer), "extra", y_peer))
            left(extra(1 - kind, 1, partner_of(y_peer), "extra", x_peer))
            for half in range(2):
                left(extra(1 - kind, half, partner_of(diag), "pair_extra", partner))

        @pl.when(core == 1)
        def _():
            arrive(pair(1 - kind, last, partner_of(diag), "pair_far", late))
            for half in range(2):
                arrive(extra(1 - kind, half, diag, "pair_extra", me))

        left(pair(1 - kind, last, diag, "pair_far", early))
        left(far(kind, last, 0, x_peer, y_peer, far_parts(last, 0)[:-1]))
        left(far(1 - kind, last, 1, y_peer, x_peer, far_parts(last, 1)[:-1]))

    by_kind(stage_own)
    tok_load.wait()
    mlp_block(dims, 0, w_in, w_out, hidden_ref, hidden_ref, normed_ref, active_ref)
    by_kind(stage_one)
    mlp_block(dims, 1, w_in, w_out, hidden_ref, hidden_ref, normed_ref, active_ref)
    by_kind(stage_two)


def finish_kernel(dims, p0, p1, p2, p3, p4, p5, master_ref, one_ref, two_ref, w_in, w_out, last_ref, tgt_ref,
                  packed_hbm, master_hbm, one_hbm, two_hbm, loss_hbm,
                  loss_ref, far_ref, wide_ref, normed_ref, active_ref, hidden_ref, sem, far_sem):
    layers, model_dim, hidden_dim, rows, chunks = dims
    me, core, y_pos, x_peer, y_peer, diag = places()
    twin = 1 - 2 * core

    copies = []
    for which, (src, dst) in enumerate(((master_ref, master_hbm), (one_ref, one_hbm), (two_ref, two_hbm))):
        for layer in range(layers):
            copies.append(pltpu.make_async_copy(src.at[layer], dst.at[:, layer, :], sem.at[6 + which * layers + layer]))
    for idx, (ref, device) in enumerate(((p0, me), (p1, me + twin), (p2, x_peer), (p3, x_peer + twin), (p4, y_peer), (p5, y_peer + twin))):
        copies.append(pltpu.make_async_copy(ref, packed_hbm.at[pl.ds(device * chunks, chunks)], sem.at[idx]))
    for item in copies:
        item.start()

    far_copies = []
    for idx, device in enumerate((diag, diag + twin)):
        for y_value in range(2):
            @pl.when(y_pos == y_value)
            def _():
                spread_piece(dims, 1 - y_value, device, (w_in, w_out), wide_ref)

        def squeeze(at, _):
            block = wide_ref[pl.ds(pl.multiple_of(at * 128, 128), 128), :].astype(BF16).reshape(32, 4, LANES)
            far_ref[idx, pl.ds(at * 32, 32), :, :] = block[:, :layers, :]
            return 0

        lax.fori_loop(0, 4 * chunks // 128, squeeze, 0)
        far_copies.append(pltpu.make_async_copy(far_ref.at[idx], packed_hbm.at[pl.ds(device * chunks, chunks)], far_sem.at[idx]))
        far_copies[-1].start()

    mlp_block(dims, layers - 1, w_in, w_out, last_ref, hidden_ref, normed_ref, active_ref)

    for idx in range(rows // LANES):
        at = slice(idx * LANES, (idx + 1) * LANES)
        error = hidden_ref[at, :].astype(F32) - tgt_ref[at, :].astype(F32)
        error = error * error
        folded = error[:, 0:LANES]
        for col in range(LANES, model_dim, LANES):
            folded = folded + error[:, col:col + LANES]
        loss_ref[idx:idx + 1, :] = jnp.sum(folded.T, axis=0, keepdims=True) * (1.0 / model_dim)

    loss_copy = pltpu.make_async_copy(loss_ref, loss_hbm, far_sem.at[2])
    loss_copy.start()
    for item in copies + far_copies + [loss_copy]:
        item.wait()


def solution(mesh):
    group_size = mesh.shape["data"]
    state_spec = P(None, "data")
    row_spec = P("data", None)

    def local_step(grad_shard, master_shard, one_shard, two_shard, tok_rows, tgt_rows):
        rows, model_dim = tok_rows.shape
        layers, cols = master_shard.shape
        half_size = cols * group_size // 2
        hidden_dim = half_size // model_dim
        chunks = cols // LANES
        dims = (layers, model_dim, hidden_dim, rows, chunks)
        tiled = [a.reshape(layers, chunks, LANES).transpose(1, 0, 2) for a in (grad_shard, master_shard, one_shard, two_shard)]
        state_v = pltpu.VMEM((layers, chunks, LANES), F32)
        hbm = pl.BlockSpec(memory_space=pltpu.HBM)
        vmem = pl.BlockSpec(memory_space=pltpu.VMEM)
        state_out = state_v
        w_in_v = pltpu.VMEM((layers, model_dim, hidden_dim), BF16)
        w_out_v = pltpu.VMEM((layers, hidden_dim, model_dim), BF16)
        hidden_v = pltpu.VMEM((rows, model_dim), BF16)
        wide_v = pltpu.VMEM((4 * chunks, LANES), F32)
        normed_v = pltpu.VMEM((256, model_dim), BF16)
        active_v = pltpu.VMEM((256, hidden_dim), BF16)
        packed_v = pltpu.VMEM((4 * chunks, LANES), BF16)
        gathered = pl.pallas_call(
            functools.partial(gather_kernel, dims),
            name="gather_step",
            out_shape=(*(packed_v,) * 6, state_v, state_v, state_v, w_in_v, w_out_v, hidden_v),
            in_specs=[hbm] * 5,
            out_specs=(vmem,) * 12,
            scratch_shapes=[
                state_v, state_v, state_v, state_v,
                pltpu.VMEM((group_size, 1, LANES), F32),
                wide_v, normed_v, active_v,
                pltpu.SemaphoreType.DMA((5, layers)),
                pltpu.SemaphoreType.DMA((layers, 3)),
                pltpu.SemaphoreType.DMA((group_size,)),
                pltpu.SemaphoreType.DMA((group_size,)),
                pltpu.SemaphoreType.DMA((96,)),
                pltpu.SemaphoreType.DMA((96,)),
            ],
            compiler_params=pltpu.CompilerParams(collective_id=0, has_side_effects=True, vmem_limit_bytes=19 << 20),
        )(*[pltpu.with_memory_space_constraint(a, pltpu.HBM) for a in (*tiled, tok_rows)])
        gathered = [a.reshape(chunks, 4, LANES)[:, :layers, :] for a in gathered[:6]] + list(gathered[6:])
        state_tile = jax.ShapeDtypeStruct((chunks, layers, LANES), F32)
        weights, new_master, new_one, new_two, row_loss = pl.pallas_call(
            functools.partial(finish_kernel, dims),
            name="finish",
            out_shape=(jax.ShapeDtypeStruct((chunks * group_size, layers, LANES), BF16), state_tile, state_tile, state_tile,
                       jax.ShapeDtypeStruct((rows // LANES, LANES), F32)),
            in_specs=[vmem] * 13,
            out_specs=(hbm,) * 5,
            scratch_shapes=[
                pltpu.VMEM((rows // LANES, LANES), F32),
                pltpu.VMEM((2, chunks, layers, LANES), BF16),
                wide_v, normed_v, active_v, hidden_v,
                pltpu.SemaphoreType.DMA((6 + 3 * layers,)),
                pltpu.SemaphoreType.DMA((3,)),
            ],
            compiler_params=pltpu.CompilerParams(vmem_limit_bytes=14 << 20),
        )(*gathered, tgt_rows)

        def flat(a):
            return a.transpose(1, 0, 2).reshape(layers, a.shape[0] * LANES)

        return row_loss.reshape(rows), flat(weights), flat(new_master), flat(new_one), flat(new_two)

    return jax.shard_map(local_step, mesh=mesh, in_specs=(state_spec, state_spec, state_spec, state_spec, row_spec, row_spec), out_specs=(P("data"), P(), state_spec, state_spec, state_spec), check_vma=False)
```

```python
import functools

import jax
import jax.numpy as jnp
from jax import lax
from jax.experimental import pallas as pl
from jax.experimental.pallas import tpu as pltpu
from jax.sharding import PartitionSpec as P

LEARN_RATE = 0.01
BETA_ONE = 0.9
BETA_TWO = 0.95
ADAM_EPS = 1e-8
WEIGHT_DECAY = 0.1
ADAM_STEP = 10
CLIP_NORM = 1.0
NORM_EPS = 1e-6

MESH = pl.DeviceIdType.MESH
LANES = 128
GROUP = 8
F32 = jnp.float32
BF16 = jnp.bfloat16


def spread_piece(dims, kind, device, weights, wide_ref):
    layers, model_dim, hidden_dim, rows, chunks = dims
    per_row = (hidden_dim if kind == 0 else model_dim) // LANES
    count = chunks // per_row
    src = weights[kind]
    slot = lax.rem(device, 4)

    def spread(idx, _):
        row = pl.multiple_of(slot * count + idx * 16, 16)
        for layer in range(layers):
            for col in range(per_row):
                tile = src[layer, pl.ds(row, 16), col * LANES:(col + 1) * LANES].astype(F32)
                base = layer + 4 * (idx * (16 * per_row) + col)
                wide_ref[pl.ds(base, 8, stride=4 * per_row), :] = tile[0:8]
                wide_ref[pl.ds(base + 32 * per_row, 8, stride=4 * per_row), :] = tile[8:16]
        return 0

    lax.fori_loop(0, count // 16, spread, 0)


def mlp_block(dims, layer, w_in, w_out, source_ref, hidden_ref, normed_ref, active_ref):
    layers, model_dim, hidden_dim, rows, chunks = dims

    def block(idx, _):
        at = pl.ds(pl.multiple_of(idx * 256, 256), 256)
        hidden = source_ref[at, :].astype(F32)
        scale = lax.rsqrt(jnp.mean(hidden * hidden, axis=-1, keepdims=True) + NORM_EPS)
        normed_ref[...] = (hidden * scale).astype(BF16)
        for col in range(0, hidden_dim, 384):
            inner = jnp.dot(normed_ref[...], w_in[layer, :, col:col + 384], preferred_element_type=F32).astype(BF16)
            active_ref[:, col:col + 384] = jax.nn.gelu(inner.astype(F32), approximate=True).astype(BF16)
        for col in range(0, model_dim, 256):
            add = jnp.dot(active_ref[...], w_out[layer, :, col:col + 256], preferred_element_type=F32)
            hidden_ref[at, col:col + 256] = (source_ref[at, col:col + 256].astype(F32) + add).astype(BF16)
        return 0

    lax.fori_loop(0, rows // 256, block, 0)


def places():
    me = lax.axis_index("data")
    core = lax.rem(me, 2)
    x_pos = lax.rem(me // 2, 2)
    y_pos = me // 4
    x_peer = me + 2 - 4 * x_pos
    y_peer = me + 4 - 8 * y_pos
    return me, core, y_pos, x_peer, y_peer, x_peer + 4 - 8 * y_pos


def gather_kernel(dims, grad_hbm, master_hbm, one_hbm, two_hbm, tok_hbm,
                  p0, p1, p2, p3, p4, p5, master_out, one_out, two_out, w_in, w_out, hidden_ref,
                  grad_v, master_v, one_v, two_v,
                  part_ref, wide_ref, normed_ref, active_ref,
                  load_sem, grad_sem, part_send, part_recv, send_sem, recv_sem):
    layers, model_dim, hidden_dim, rows, chunks = dims
    in_rows = chunks * LANES // hidden_dim
    out_rows = chunks * LANES // model_dim

    me, core, y_pos, x_peer, y_peer, diag = places()
    partner = me + 1 - 2 * core

    state = ((grad_hbm, grad_v), (master_hbm, master_v), (one_hbm, one_v), (two_hbm, two_v))

    def load(which, layer):
        src, dst = state[which]
        return pltpu.make_async_copy(src.at[:, layer, :], dst.at[layer], load_sem.at[which, layer])

    span = chunks // 3

    def grad_load(layer, part):
        at = pl.ds(part * span, span)
        return pltpu.make_async_copy(grad_hbm.at[at, layer, :], grad_v.at[layer, at], grad_sem.at[layer, part])

    for layer in range(layers):
        for part in range(3):
            grad_load(layer, part).start()
    tok_load = pltpu.make_async_copy(tok_hbm, hidden_ref, load_sem.at[4, 0])

    barrier = pltpu.get_barrier_semaphore()
    for step in range(1, GROUP):
        pl.semaphore_signal(barrier, inc=1, device_id=(lax.rem(me + step, GROUP),), device_id_type=MESH)

    sums = tuple(jnp.zeros((8, LANES), F32) for _ in range(8))
    for layer in range(layers):
        for part in range(3):
            grad_load(layer, part).wait()
            if layer == layers - 1 and part == 2:
                for which in range(1, 4):
                    load(which, 0).start()

            def square(idx, carry):
                base = pl.multiple_of(part * span + idx * 64, 64)
                block = grad_v[layer, pl.ds(base, 64), :]
                return tuple(carry[k] + block[8 * k:8 * k + 8] * block[8 * k:8 * k + 8] for k in range(8))

            sums = lax.fori_loop(0, span // 64, square, sums)
    mine = ((sums[0] + sums[1]) + (sums[2] + sums[3])) + ((sums[4] + sums[5]) + (sums[6] + sums[7]))
    part_ref[me] = jnp.sum(mine, axis=0, keepdims=True)
    pl.semaphore_wait(barrier, GROUP - 1)

    def part_copy(step):
        return pltpu.make_async_remote_copy(
            src_ref=part_ref.at[me], dst_ref=part_ref.at[me],
            send_sem=part_send.at[step], recv_sem=part_recv.at[step],
            device_id=(lax.rem(me + step, GROUP),), device_id_type=MESH)

    def part_arrival(step):
        slot = lax.rem(me + GROUP - step, GROUP)
        return pltpu.make_async_remote_copy(
            src_ref=part_ref.at[slot], dst_ref=part_ref.at[slot],
            send_sem=part_send.at[step], recv_sem=part_recv.at[step],
            device_id=(me,), device_id_type=MESH)

    for step in range(1, GROUP):
        part_copy(step).start()
    for item in range(1, layers):
        for which in range(1, 4):
            load(which, item).start()
    tok_load.start()
    for which in range(1, 4):
        load(which, 0).wait()
    for step in range(1, GROUP):
        part_arrival(step).wait_recv()
    total = part_ref[0]
    for slot in range(1, GROUP):
        total = total + part_ref[slot]
    total = jnp.sum(total, axis=1, keepdims=True)
    clip = jnp.minimum(1.0, CLIP_NORM / jnp.sqrt(total))
    clip = jnp.broadcast_to(clip, (8, LANES))

    slots = {}

    def piece(kind, layer, device, part):
        ref, count = ((w_in, in_rows), (w_out, out_rows))[kind]
        span = count // part[1]
        at = lax.rem(device, 4) * count + part[0] * span
        return ref.at[layer, pl.ds(pl.multiple_of(at, 8), span), :]

    def copies(kind, layer, device, route, target, parts):
        out = []
        for part in parts:
            ref = piece(kind, layer, device, part)
            index = slots.setdefault((route, layer, part), len(slots))
            out.append(pltpu.make_async_remote_copy(
                src_ref=ref, dst_ref=ref, send_sem=send_sem.at[index],
                recv_sem=recv_sem.at[index], device_id=(target,), device_id_type=MESH))
        return out

    def start(items):
        for item in items:
            item.start()

    def arrive(items):
        for item in items:
            item.wait_recv()

    def left(items):
        for item in items:
            item.wait_send()

    def own_parts(layer):
        return ((0, 12), (1, 12), (1, 6), (2, 6), (1, 2)) if layer == 0 else ((0, 2), (1, 2))

    def far_parts(layer, half):
        return tuple((3 * half + at, 6) for at in range(3)) if layer == layers - 1 else ((half, 2),)

    def own_x(kind, layer, device, target, parts=None):
        return copies(kind, layer, device, "own_x", target, parts or own_parts(layer))

    def own_y(kind, layer, device, target, parts=None):
        return copies(kind, layer, device, "own_y", target, parts or own_parts(layer))

    def far(kind, layer, half, device, target, parts=None):
        return copies(kind, layer, device, "far", target, parts or far_parts(layer, half))

    def pair(kind, layer, device, route, parts):
        return copies(kind, layer, device, route, partner, parts)

    def by_kind(function):
        for y_value in range(2):
            @pl.when(y_pos == y_value)
            def _():
                function(y_value)

    one_scale = 1.0 / (1.0 - BETA_ONE ** ADAM_STEP)
    two_scale = 1.0 / (1.0 - BETA_TWO ** ADAM_STEP)

    def adam(layer, part):
        first = part[0] * (chunks // part[1])
        step = 144 if part[1] == 12 else 48

        def update(idx, _):
            base = pl.multiple_of(first + idx * step, 8)
            for k in range(step // 8):
                at = pl.ds(pl.multiple_of(base + 8 * k, 8), 8)
                clipped = grad_v[layer, at, :] * clip
                new_one = BETA_ONE * one_v[layer, at, :] + (1.0 - BETA_ONE) * clipped
                new_two = BETA_TWO * two_v[layer, at, :] + (1.0 - BETA_TWO) * clipped * clipped
                step_size = (new_one * one_scale) / (jnp.sqrt(new_two * two_scale) + ADAM_EPS)
                old = master_v[layer, at, :]
                master_out[layer, at, :] = old - LEARN_RATE * (step_size + WEIGHT_DECAY * old)
                one_out[layer, at, :] = new_one
                two_out[layer, at, :] = new_two
            return 0

        lax.fori_loop(0, chunks // part[1] // step, update, 0)

    def round_rows(kind, layer, part):
        width = hidden_dim if kind == 0 else model_dim
        count = in_rows if kind == 0 else out_rows
        per_row = width // LANES
        dst = w_in if kind == 0 else w_out
        slot = lax.rem(me, 4)

        step = 16 if count // part[1] % 16 == 0 else 8

        def body(idx, _):
            base = part[0] * (chunks // part[1]) + idx * (step * per_row)
            row = pl.multiple_of(slot * count + part[0] * (count // part[1]) + idx * step, 8)
            for col in range(per_row):
                block = master_out[layer, pl.ds(base + col, 8, stride=per_row), :]
                if step == 16:
                    low = master_out[layer, pl.ds(base + 8 * per_row + col, 8, stride=per_row), :]
                    block = jnp.concatenate([block, low], axis=0)
                dst[layer, pl.ds(row, step), col * LANES:(col + 1) * LANES] = block.astype(BF16)
            return 0

        lax.fori_loop(0, count // step // part[1], body, 0)

    for layer in range(layers):
        for which in range(1, 4) if layer else ():
            load(which, layer).wait()
        for part in own_parts(layer):
            adam(layer, part)

            def send_own(kind):
                round_rows(kind, layer, part)
                if layer < layers - 1:
                    start(own_x(kind, layer, me, x_peer, (part,)))
                    start(own_y(kind, layer, me, y_peer, (part,)))
                start(pair(kind, layer, me, "pair_own", (part,)))

            by_kind(send_own)

    def pack(kind, device, packed_ref):
        spread_piece(dims, kind, device, (w_in, w_out), wide_ref)

        def squeeze(idx, _):
            at = pl.ds(pl.multiple_of(idx * 256, 256), 256)
            packed_ref[at, :] = wide_ref[at, :].astype(BF16)
            return 0

        lax.fori_loop(0, 4 * chunks // 256, squeeze, 0)

    def partner_of(device):
        return device + 1 - 2 * core

    def drain(kind):
        for layer in range(layers):
            left(own_x(kind, layer, me, x_peer))
            left(own_y(kind, layer, me, y_peer))
            left(pair(kind, layer, me, "pair_own", own_parts(layer)))
            left(pair(kind, layer, x_peer, "pair_x", own_parts(layer)))
            left(pair(1 - kind, layer, y_peer, "pair_y", own_parts(layer)))
            if layer < layers - 1:
                left(pair(1 - kind, layer, diag, "pair_far", far_parts(layer, 0) + far_parts(layer, 1)))
                left(far(kind, layer, 0, x_peer, y_peer))
                left(far(1 - kind, layer, 1, y_peer, x_peer))
        for step in range(1, GROUP):
            part_copy(step).wait_send()

    def last_parts(half):
        return far_parts(layers - 1, half)[-1:]

    def start_far(kind, layer, half, device, target):
        if layer < layers - 1:
            start(far(kind, layer, half, device, target))
            return
        start(far(kind, layer, half, device, target, far_parts(layer, half)[:-1]))

        @pl.when(core == 0)
        def _():
            start(far(kind, layer, half, device, target, last_parts(half)))

    def extra(kind, half, device, route, target):
        return copies(kind, layers - 1, device, route, target, last_parts(half))

    def forward(kind, layer):
        x_order = own_parts(layer)
        y_order = x_order[::-1] if layer == layers - 1 else x_order
        for x_part, y_part in zip(x_order, y_order):
            arrive(own_x(kind, layer, x_peer, me, (x_part,)))
            if x_part in ((0, 2), (2, 6)):
                start_far(kind, layer, 0, x_peer, y_peer)
            start(pair(kind, layer, x_peer, "pair_x", (x_part,)))
            arrive(own_y(1 - kind, layer, y_peer, me, (y_part,)))
            if y_part == (1, 2):
                start_far(1 - kind, layer, 1, y_peer, x_peer)
            start(pair(1 - kind, layer, y_peer, "pair_y", (y_part,)))

    def far_arrive(kind, layer, only=None):
        for idx, parts in enumerate(zip(far_parts(layer, 0), far_parts(layer, 1))):
            if only is not None and idx != only:
                continue
            for half in range(2):
                arrive(far(1 - kind, layer, half, diag, me, (parts[half],)))
                start(pair(1 - kind, layer, diag, "pair_far", (parts[half],)))

    def far_partner(kind, layer):
        arrive(pair(1 - kind, layer, partner_of(diag), "pair_far", far_parts(layer, 0) + far_parts(layer, 1)))

    def near_partner(kind, layer, x_parts=None, y_parts=None):
        arrive(pair(kind, layer, partner_of(x_peer), "pair_x", x_parts or own_parts(layer)))
        arrive(pair(1 - kind, layer, partner_of(y_peer), "pair_y", y_parts or own_parts(layer)))

    def stage_own(kind):
        pack(kind, me, p0)
        forward(kind, 0)
        for layer in range(layers):
            arrive(pair(kind, layer, partner, "pair_own", own_parts(layer)))
        pack(kind, partner, p1)
        forward(kind, 1)
        start(own_x(kind, layers - 1, me, x_peer))
        start(own_y(kind, layers - 1, me, y_peer)[::-1])
        near_partner(kind, 0)
        far_arrive(kind, 0)
        near_partner(kind, 1)
        far_partner(kind, 0)

    def stage_one(kind):
        far_arrive(kind, 1)
        far_partner(kind, 1)

    def stage_two(kind):
        last = layers - 1
        early = far_parts(last, 0)[:-1] + far_parts(last, 1)[:-1]
        late = last_parts(0) + last_parts(1)
        forward(kind, last)
        near_partner(kind, last, ((0, 2),), ((1, 2),))

        @pl.when(core == 0)
        def _():
            start(extra(kind, 0, partner_of(x_peer), "extra", y_peer))
            start(extra(1 - kind, 1, partner_of(y_peer), "extra", x_peer))

        pack(kind, x_peer, p2)
        pack(1 - kind, y_peer, p4)
        near_partner(kind, last, ((1, 2),), ((0, 2),))
        far_arrive(kind, last, 0)
        pack(kind, partner_of(x_peer), p3)
        far_arrive(kind, last, 1)
        pack(1 - kind, partner_of(y_peer), p5)
        drain(kind)
        arrive(pair(1 - kind, last, partner_of(diag), "pair_far", early))

        @pl.when(core == 0)
        def _():
            far_arrive(kind, last, 2)
            for half in range(2):
                arrive(extra(1 - kind, half, partner_of(diag), "extra", me))
                start(extra(1 - kind, half, partner_of(diag), "pair_extra", partner))
            left(pair(1 - kind, last, diag, "pair_far", late))
            left(far(kind, last, 0, x_peer, y_peer, last_parts(0)))
            left(far(1 - kind, last, 1, y_peer, x_peer, last_parts(1)))
            left(extra(kind, 0, partner_of(x_peer), "extra", y_peer))
            left(extra(1 - kind, 1, partner_of(y_peer), "extra", x_peer))
            for half in range(2):
                left(extra(1 - kind, half, partner_of(diag), "pair_extra", partner))

        @pl.when(core == 1)
        def _():
            arrive(pair(1 - kind, last, partner_of(diag), "pair_far", late))
            for half in range(2):
                arrive(extra(1 - kind, half, diag, "pair_extra", me))

        left(pair(1 - kind, last, diag, "pair_far", early))
        left(far(kind, last, 0, x_peer, y_peer, far_parts(last, 0)[:-1]))
        left(far(1 - kind, last, 1, y_peer, x_peer, far_parts(last, 1)[:-1]))

    by_kind(stage_own)
    tok_load.wait()
    mlp_block(dims, 0, w_in, w_out, hidden_ref, hidden_ref, normed_ref, active_ref)
    by_kind(stage_one)
    mlp_block(dims, 1, w_in, w_out, hidden_ref, hidden_ref, normed_ref, active_ref)
    by_kind(stage_two)


def finish_kernel(dims, p0, p1, p2, p3, p4, p5, master_ref, one_ref, two_ref, w_in, w_out, last_ref, tgt_ref,
                  packed_hbm, master_hbm, one_hbm, two_hbm, loss_hbm,
                  loss_ref, far_ref, wide_ref, normed_ref, active_ref, hidden_ref, sem, far_sem):
    layers, model_dim, hidden_dim, rows, chunks = dims
    me, core, y_pos, x_peer, y_peer, diag = places()
    twin = 1 - 2 * core

    copies = []
    for which, (src, dst) in enumerate(((master_ref, master_hbm), (one_ref, one_hbm), (two_ref, two_hbm))):
        for layer in range(layers):
            copies.append(pltpu.make_async_copy(src.at[layer], dst.at[:, layer, :], sem.at[6 + which * layers + layer]))
    for idx, (ref, device) in enumerate(((p0, me), (p1, me + twin), (p2, x_peer), (p3, x_peer + twin), (p4, y_peer), (p5, y_peer + twin))):
        copies.append(pltpu.make_async_copy(ref, packed_hbm.at[pl.ds(device * chunks, chunks)], sem.at[idx]))
    for idx, item in enumerate(copies):
        item.start(priority=idx % 2)

    far_copies = []
    for idx, device in enumerate((diag, diag + twin)):
        for y_value in range(2):
            @pl.when(y_pos == y_value)
            def _():
                spread_piece(dims, 1 - y_value, device, (w_in, w_out), wide_ref)

        def squeeze(at, _):
            block = wide_ref[pl.ds(pl.multiple_of(at * 128, 128), 128), :].astype(BF16).reshape(32, 4, LANES)
            far_ref[idx, pl.ds(at * 32, 32), :, :] = block[:, :layers, :]
            return 0

        lax.fori_loop(0, 4 * chunks // 128, squeeze, 0)
        far_copies.append(pltpu.make_async_copy(far_ref.at[idx], packed_hbm.at[pl.ds(device * chunks, chunks)], far_sem.at[idx]))
        far_copies[-1].start()

    mlp_block(dims, layers - 1, w_in, w_out, last_ref, hidden_ref, normed_ref, active_ref)

    for idx in range(rows // LANES):
        at = slice(idx * LANES, (idx + 1) * LANES)
        error = hidden_ref[at, :].astype(F32) - tgt_ref[at, :].astype(F32)
        error = error * error
        folded = error[:, 0:LANES]
        for col in range(LANES, model_dim, LANES):
            folded = folded + error[:, col:col + LANES]
        loss_ref[idx:idx + 1, :] = jnp.sum(folded.T, axis=0, keepdims=True) * (1.0 / model_dim)

    loss_copy = pltpu.make_async_copy(loss_ref, loss_hbm, far_sem.at[2])
    loss_copy.start()
    for item in copies + far_copies + [loss_copy]:
        item.wait()


def solution(mesh):
    group_size = mesh.shape["data"]
    state_spec = P(None, "data")
    row_spec = P("data", None)

    def local_step(grad_shard, master_shard, one_shard, two_shard, tok_rows, tgt_rows):
        rows, model_dim = tok_rows.shape
        layers, cols = master_shard.shape
        half_size = cols * group_size // 2
        hidden_dim = half_size // model_dim
        chunks = cols // LANES
        dims = (layers, model_dim, hidden_dim, rows, chunks)
        tiled = [a.reshape(layers, chunks, LANES).transpose(1, 0, 2) for a in (grad_shard, master_shard, one_shard, two_shard)]
        state_v = pltpu.VMEM((layers, chunks, LANES), F32)
        hbm = pl.BlockSpec(memory_space=pltpu.HBM)
        vmem = pl.BlockSpec(memory_space=pltpu.VMEM)
        state_out = state_v
        w_in_v = pltpu.VMEM((layers, model_dim, hidden_dim), BF16)
        w_out_v = pltpu.VMEM((layers, hidden_dim, model_dim), BF16)
        hidden_v = pltpu.VMEM((rows, model_dim), BF16)
        wide_v = pltpu.VMEM((4 * chunks, LANES), F32)
        normed_v = pltpu.VMEM((256, model_dim), BF16)
        active_v = pltpu.VMEM((256, hidden_dim), BF16)
        packed_v = pltpu.VMEM((4 * chunks, LANES), BF16)
        gathered = pl.pallas_call(
            functools.partial(gather_kernel, dims),
            name="gather_step",
            out_shape=(*(packed_v,) * 6, state_v, state_v, state_v, w_in_v, w_out_v, hidden_v),
            in_specs=[hbm] * 5,
            out_specs=(vmem,) * 12,
            scratch_shapes=[
                state_v, state_v, state_v, state_v,
                pltpu.VMEM((group_size, 1, LANES), F32),
                wide_v, normed_v, active_v,
                pltpu.SemaphoreType.DMA((5, layers)),
                pltpu.SemaphoreType.DMA((layers, 3)),
                pltpu.SemaphoreType.DMA((group_size,)),
                pltpu.SemaphoreType.DMA((group_size,)),
                pltpu.SemaphoreType.DMA((96,)),
                pltpu.SemaphoreType.DMA((96,)),
            ],
            compiler_params=pltpu.CompilerParams(collective_id=0, has_side_effects=True, vmem_limit_bytes=19 << 20),
        )(*[pltpu.with_memory_space_constraint(a, pltpu.HBM) for a in (*tiled, tok_rows)])
        gathered = [a.reshape(chunks, 4, LANES)[:, :layers, :] for a in gathered[:6]] + list(gathered[6:])
        state_tile = jax.ShapeDtypeStruct((chunks, layers, LANES), F32)
        weights, new_master, new_one, new_two, row_loss = pl.pallas_call(
            functools.partial(finish_kernel, dims),
            name="finish",
            out_shape=(jax.ShapeDtypeStruct((chunks * group_size, layers, LANES), BF16), state_tile, state_tile, state_tile,
                       jax.ShapeDtypeStruct((rows // LANES, LANES), F32)),
            in_specs=[vmem] * 13,
            out_specs=(hbm,) * 5,
            scratch_shapes=[
                pltpu.VMEM((rows // LANES, LANES), F32),
                pltpu.VMEM((2, chunks, layers, LANES), BF16),
                wide_v, normed_v, active_v, hidden_v,
                pltpu.SemaphoreType.DMA((6 + 3 * layers,)),
                pltpu.SemaphoreType.DMA((3,)),
            ],
            compiler_params=pltpu.CompilerParams(vmem_limit_bytes=14 << 20),
        )(*gathered, tgt_rows)

        def flat(a):
            return a.transpose(1, 0, 2).reshape(layers, a.shape[0] * LANES)

        return row_loss.reshape(rows), flat(weights), flat(new_master), flat(new_one), flat(new_two)

    return jax.shard_map(local_step, mesh=mesh, in_specs=(state_spec, state_spec, state_spec, state_spec, row_spec, row_spec), out_specs=(P("data"), P(), state_spec, state_spec, state_spec), check_vma=False)
```
